32 devices in a mesh: dp: 4 (over y, x), fsdp: 8 (over z, core).
Axes of the slice: x: 2, y: 2, z: 4, core: 2. Of those that a mesh axis runs over, the one named last changes fastest.
Arguments:
- token_ids: int32 [2, 4, 1024], P(None, 'dp'), may hold values from 0 to 50287
- target_ids: int32 [2, 4, 1024], P(None, 'dp'), may hold values from 0 to 50287
- seq_lengths: int32 [2, 4], replicated, may hold values from 512 to 1024, as said below
- embedding: float32 [50288, 1024], P('fsdp', 'dp'), may hold values from -0.5625 to 0.5625
- embedding_mom: float32 [50288, 1024], P('fsdp', 'dp'), may hold values from -0.00036621094 to 0.00036621094
- embedding_avg: float32 [50288, 1024], P('fsdp', 'dp'), may hold values from -1 to 1
- in_proj: float32 [2, 1024, 4384], P(None, ('dp', 'fsdp')), may hold values from -0.1875 to 0.1875
- in_proj_mom: float32 [2, 1024, 4384], P(None, ('dp', 'fsdp')), may hold values from -0.00036621094 to 0.00036621094
- in_proj_avg: float32 [2, 1024, 4384], P(None, ('dp', 'fsdp')), may hold values from -0.1875 to 0.1875
- out_proj: float32 [2, 2048, 1024], P(None, ('dp', 'fsdp')), may hold values from -0.125 to 0.125
- out_proj_mom: float32 [2, 2048, 1024], P(None, ('dp', 'fsdp')), may hold values from -0.00036621094 to 0.00036621094
- out_proj_avg: float32 [2, 2048, 1024], P(None, ('dp', 'fsdp')), may hold values from -0.125 to 0.125
- vector_params: float32 [30400], replicated, may hold values from -8 to 1.5, as said below
- vector_mom: float32 [30400], replicated, may hold values from -0.0014648438 to 0.0014648438
- vector_avg: float32 [30400], replicated, may hold values from -8 to 1.5, as said below
Outputs:
- loss_value: float32 [], replicated
- grad_norm: float32 [], replicated
- embedding_new: float32 [50288, 1024], P('fsdp', 'dp')
- embedding_mom_new: float32 [50288, 1024], P('fsdp', 'dp')
- embedding_avg_new: float32 [50288, 1024], P('fsdp', 'dp')
- embedding_bf16: bfloat16 [50288, 1024], P('fsdp', 'dp')
- in_proj_new: float32 [2, 1024, 4384], P(None, ('dp', 'fsdp'))
- in_proj_mom_new: float32 [2, 1024, 4384], P(None, ('dp', 'fsdp'))
- in_proj_avg_new: float32 [2, 1024, 4384], P(None, ('dp', 'fsdp'))
- in_proj_bf16: bfloat16 [2, 1024, 4384], P(None, ('dp', 'fsdp'))
- out_proj_new: float32 [2, 2048, 1024], P(None, ('dp', 'fsdp'))
- out_proj_mom_new: float32 [2, 2048, 1024], P(None, ('dp', 'fsdp'))
- out_proj_avg_new: float32 [2, 2048, 1024], P(None, ('dp', 'fsdp'))
- out_proj_bf16: bfloat16 [2, 2048, 1024], P(None, ('dp', 'fsdp'))
- vector_new: float32 [30400], replicated
- vector_mom_new: float32 [30400], replicated
- vector_avg_new: float32 [30400], replicated
- vector_bf16: bfloat16 [30400], replicated
The draws below stay inside these ranges and needn't reach their ends.
Inputs may be any that keep to these rules, and one draw needn't show every extreme that they name: `seq_lengths`: positions from a sequence's length on are padding. `vector_params`: laid out as the steps say. `vector_avg`: laid out as vector_params.
All inputs are finite; a program needn't handle non-finite values.
Results may differ from the reference program's by a relative error of at most 0.018.
Values may be sent and summed in bfloat16 or wider, within the bound.
A program may use at most 384 MiB of HBM per device.

```python
import math
import jax
import jax.numpy as jnp
import numpy as np
from jax import lax

D = 1024
HEADS = 32
HDIM = 64
NSTATE = 128
CONV = 4
VOCAB = 50288
SPAN = 256
LAYERS = 2
MB = 2
DI = 2048
XBC = 2304
ZW = 4384
PER = 14688
SMALL = 30400
SEQ = 1024
GROUPS = 4


def draw_seq_lengths(key, part):
    draw_key, pick_key = jax.random.split(jax.random.fold_in(key, 7))
    drawn = jax.random.randint(draw_key, (MB * GROUPS,), SEQ // 2, SEQ + 1)
    chosen = jax.random.randint(pick_key, (), 0, MB * GROUPS)
    filled = jnp.where(jnp.arange(MB * GROUPS) == chosen, SEQ, drawn)
    return filled.reshape(MB, GROUPS).astype(jnp.int32)


def draw_embedding(key, part):
    table_key = jax.random.fold_in(key, 21)
    rows = jnp.arange(VOCAB, dtype=jnp.float32)[:, None] / float(max(VOCAB - 1, 1))
    rise = 0.5 * jnp.exp(rows * math.log(3.0))
    base = jax.random.truncated_normal(table_key, -6.0, 6.0, (VOCAB, D), jnp.float32)
    return base * rise * (2.0 / math.sqrt(D))


def vector_draw(base_key):
    pieces = []
    for layer_index in range(LAYERS):
        subkeys = jax.random.split(jax.random.fold_in(base_key, layer_index), 7)
        pieces.append(jax.random.uniform(subkeys[0], (CONV * XBC,), jnp.float32, -0.5, 0.5))
        pieces.append(jax.random.uniform(subkeys[1], (XBC,), jnp.float32, -0.5, 0.5))
        step_log = jax.random.uniform(subkeys[2], (HEADS,), jnp.float32, math.log(0.001), math.log(0.5))
        pieces.append(jnp.log(jnp.expm1(jnp.exp(step_log))))
        pieces.append(jax.random.uniform(subkeys[3], (HEADS,), jnp.float32, math.log(0.01), math.log(2.0)))
        pieces.append(jax.random.uniform(subkeys[4], (HEADS,), jnp.float32, 0.5, 1.5))
        pieces.append(jax.random.uniform(subkeys[5], (D,), jnp.float32, 0.6, 1.4))
        pieces.append(jax.random.uniform(subkeys[6], (DI,), jnp.float32, 0.6, 1.4))
    pieces.append(jax.random.uniform(jax.random.fold_in(base_key, 1000), (D,), jnp.float32, 0.6, 1.4))
    return jnp.concatenate(pieces)


def draw_vector_params(key, part):
    return vector_draw(jax.random.fold_in(key, 11))


def draw_vector_avg(key, part):
    return vector_draw(jax.random.fold_in(key, 12))


def touch_ends(values, own_key, smallest, top_value):
    extent = values.shape
    place = [jax.random.randint(jax.random.fold_in(own_key, axis), (), 0, extent[axis]) for axis in range(len(extent))]
    values = values.at[tuple(place)].set(smallest)
    longest = extent.index(max(extent))
    place[longest] = (place[longest] + 1) % extent[longest]
    return values.at[tuple(place)].set(top_value)


def level_of(own_key, extent, shards, least, largest):
    level, own = 1.0, jax.random.fold_in(own_key, 6)
    for axis_at, shards_of in shards:
        draws = jnp.exp(jax.random.uniform(jax.random.fold_in(own, axis_at), (shards_of,), jnp.float32, least / len(shards), largest / len(shards)))
        level = level * jnp.repeat(draws, extent[axis_at] // shards_of).reshape([-1 if axis == axis_at else 1 for axis in range(len(extent))])
    return level


def rank_table(number_of, slope):
    loads = [(1 << 20) // math.isqrt(standing ** slope) + 1 for standing in range(1, number_of + 1)]
    deviation = 1 + sum(loads) // (1 << 30)
    return np.cumsum(np.array([max(1, weight // deviation) for weight in loads]))


def skewed_ids(key, extent, number_of, lean):
    listing = rank_table(number_of, lean)
    lot = jax.random.randint(jax.random.fold_in(key, 1), extent, 0, int(listing[number_of - 1]))
    rank = jnp.searchsorted(jnp.asarray(listing, jnp.int32), lot, side="right")
    return jax.random.permutation(jax.random.fold_in(key, 2), number_of)[rank].astype(jnp.int32)


def scatter_about(key, extent, scale, limit, shards=(), kind=jnp.bfloat16):
    level = level_of(key, extent, shards, -0.22, 0.18) if shards else 1.0
    values = jax.random.normal(key, extent, jnp.float32) * scale * level
    return jnp.minimum(jnp.maximum(values, -limit), limit).astype(kind)


def setup_inputs(seed: int = 0) -> dict:
    seeds = jax.random.split(jax.random.key(seed), 16)
    token_ids = touch_ends(skewed_ids(seeds[0], (MB, GROUPS, SEQ), VOCAB, 2), jax.random.fold_in(seeds[0], 3), 0, VOCAB - 1).astype(jnp.int32)
    target_ids = touch_ends(skewed_ids(seeds[1], (MB, GROUPS, SEQ), VOCAB, 2), jax.random.fold_in(seeds[1], 3), 0, VOCAB - 1).astype(jnp.int32)
    seq_lengths = draw_seq_lengths(jax.random.fold_in(seeds[15], 71), 0)
    embedding = draw_embedding(jax.random.fold_in(seeds[15], 71), 0)
    embedding_mom = scatter_about(seeds[4], (VOCAB, D), 0.000025, 0.00036621094, ((0, 8), (1, 4)), jnp.float32)
    embedding_avg = scatter_about(seeds[5], (VOCAB, D), 0.0625, 1.0, ((0, 8), (1, 4)), jnp.float32)
    in_proj = scatter_about(seeds[6], (LAYERS, D, ZW), D ** -0.5, 0.1875, ((1, 32),), jnp.float32)
    in_proj_mom = scatter_about(seeds[7], (LAYERS, D, ZW), 0.000025, 0.00036621094, ((1, 32),), jnp.float32)
    in_proj_avg = scatter_about(seeds[8], (LAYERS, D, ZW), D ** -0.5, 0.1875, ((1, 32),), jnp.float32)
    out_proj = scatter_about(seeds[9], (LAYERS, DI, D), DI ** -0.5, 0.125, ((1, 32),), jnp.float32)
    out_proj_mom = scatter_about(seeds[10], (LAYERS, DI, D), 0.000025, 0.00036621094, ((1, 32),), jnp.float32)
    out_proj_avg = scatter_about(seeds[11], (LAYERS, DI, D), DI ** -0.5, 0.125, ((1, 32),), jnp.float32)
    vector_params = draw_vector_params(jax.random.fold_in(seeds[15], 71), 0)
    vector_mom = scatter_about(seeds[13], (SMALL,), 0.0001, 0.0014648438, (), jnp.float32)
    vector_avg = draw_vector_avg(jax.random.fold_in(seeds[15], 71), 0)
    return {"token_ids": token_ids, "target_ids": target_ids, "seq_lengths": seq_lengths, "embedding": embedding, "embedding_mom": embedding_mom, "embedding_avg": embedding_avg, "in_proj": in_proj, "in_proj_mom": in_proj_mom, "in_proj_avg": in_proj_avg, "out_proj": out_proj, "out_proj_mom": out_proj_mom, "out_proj_avg": out_proj_avg, "vector_params": vector_params, "vector_mom": vector_mom, "vector_avg": vector_avg}


@jax.custom_vjp
def low(v):
    return lax.optimization_barrier(v.astype(jnp.bfloat16)).astype(jnp.float32)

@jax.custom_vjp
def low_back(v):
    return v

def low_keep(v):
    return (low(v), None)

def low_pass(kept, grad):
    return (grad,)

def back_keep(v):
    return (v, None)

def back_low(kept, grad):
    return (low(grad),)
low.defvjp(low_keep, low_pass)
low_back.defvjp(back_keep, back_low)
epsilon = 1e-05
z_weight = 0.001
clip_limit = 0.2
step_rate = 1000.0
highest = lax.Precision.HIGHEST

def matmul(left, right):
    return jnp.dot(left, right, precision=highest, preferred_element_type=jnp.float32)

def rms_scale(values, gain):
    return values * lax.rsqrt(lax.optimization_barrier(jnp.mean(values * values, axis=-1, keepdims=True)) + epsilon) * gain

def layer_vectors(vector_params, layer_index):
    offset = layer_index * PER
    conv_weight = vector_params[offset:offset + CONV * XBC].reshape(CONV, XBC)
    offset = offset + CONV * XBC
    conv_bias = vector_params[offset:offset + XBC]
    offset = offset + XBC
    dt_bias = vector_params[offset:offset + HEADS]
    offset = offset + HEADS
    decay_log = vector_params[offset:offset + HEADS]
    offset = offset + HEADS
    skip_gain = vector_params[offset:offset + HEADS]
    offset = offset + HEADS
    pre_gain = vector_params[offset:offset + D]
    offset = offset + D
    gate_gain = vector_params[offset:offset + DI]
    return (conv_weight, conv_bias, dt_bias, decay_log, skip_gain, pre_gain, gate_gain)

def span_step(state, packed, decay_rate, skip_gain):
    values, in_map, out_map, step_size = packed
    length_here = values.shape[0]
    log_decay = jnp.cumsum(step_size * decay_rate[None, :], axis=0)
    causal = jnp.arange(length_here)[:, None] >= jnp.arange(length_here)[None, :]
    spread = log_decay.T[:, :, None] - log_decay.T[:, None, :]
    weights = jnp.where(causal[None], jnp.exp(jnp.where(causal[None], spread, 0.0)), 0.0)
    inner = jnp.dot(out_map, in_map.T, precision=highest, preferred_element_type=jnp.float32)
    scaled = values * step_size[:, :, None]
    result = jnp.einsum('hts,shp->thp', weights * inner[None], scaled, precision=highest)
    result = result + jnp.exp(log_decay)[:, :, None] * jnp.einsum('tn,hpn->thp', out_map, state, precision=highest)
    result = result + skip_gain[None, :, None] * values
    tail = jnp.exp(log_decay[-1][None, :] - log_decay) * step_size
    new_state = jnp.exp(log_decay[-1])[:, None, None] * state + jnp.einsum('sh,shp,sn->hpn', tail, values, in_map, precision=highest)
    return (new_state, result)

def state_space(values, in_map, out_map, step_size, decay_rate, skip_gain):
    blocks = SEQ // SPAN
    packed = (values.reshape(blocks, SPAN, HEADS, HDIM), in_map.reshape(blocks, SPAN, NSTATE), out_map.reshape(blocks, SPAN, NSTATE), step_size.reshape(blocks, SPAN, HEADS))
    stepper = jax.checkpoint(lambda state, piece: span_step(state, piece, decay_rate, skip_gain))
    final_state, results = lax.scan(stepper, jnp.zeros((HEADS, HDIM, NSTATE), jnp.float32), packed)
    return results.reshape(SEQ, DI)

def logits_loss(final_low, table_low, labels_seq, valid):
    block_rows = math.gcd(SEQ, 512)
    blocks = SEQ // block_rows

    def block_step(accum, packed):
        rows_block, labels_block, valid_block = packed
        logits = low_back(jnp.dot(rows_block, table_low.T, precision=highest, preferred_element_type=jnp.float32))
        row_top = lax.optimization_barrier(jnp.max(logits, axis=1, keepdims=True))
        log_total = row_top[:, 0] + jnp.log(lax.optimization_barrier(jnp.sum(jnp.exp(logits - row_top), axis=1)))
        target = jnp.take_along_axis(logits, labels_block[:, None], axis=1)[:, 0]
        per_row = log_total - 0.9 * target - 0.1 * lax.optimization_barrier(jnp.mean(logits, axis=1)) + z_weight * log_total * log_total
        return (accum + jnp.sum(per_row * valid_block), None)
    packed = (final_low.reshape(blocks, block_rows, D), labels_seq.reshape(blocks, block_rows), valid.reshape(blocks, block_rows))
    total, unused = lax.scan(jax.checkpoint(block_step), jnp.float32(0.0), packed)
    return total

def sequence_total(table_low, in_low, out_low, vector_params, seq_ids, seq_labels, seq_length):
    hidden = low_back(table_low[seq_ids])
    for layer_index in range(LAYERS):
        conv_weight, conv_bias, dt_bias, decay_log, skip_gain, pre_gain, gate_gain = layer_vectors(vector_params, layer_index)
        normed = low(rms_scale(hidden, pre_gain))
        projected = low_back(matmul(normed, in_low[layer_index]))
        gate_part = projected[:, :DI]
        mixed_in = projected[:, DI:DI + XBC]
        padded = jnp.concatenate([jnp.zeros((CONV - 1, XBC), jnp.float32), mixed_in], axis=0)
        convolved = conv_bias + sum((conv_weight[tap] * padded[tap:tap + SEQ] for tap in range(CONV)))
        activated = jax.nn.silu(convolved)
        values = activated[:, :DI].reshape(SEQ, HEADS, HDIM)
        in_map = activated[:, DI:DI + NSTATE]
        out_map = activated[:, DI + NSTATE:]
        step_size = jax.nn.softplus(projected[:, DI + XBC:] + dt_bias)
        result = state_space(values, in_map, out_map, step_size, -jnp.exp(decay_log), skip_gain)
        gated = low(rms_scale(result * jax.nn.silu(gate_part), gate_gain))
        hidden = hidden + low_back(matmul(gated, out_low[layer_index]))
    final_low = low(rms_scale(hidden, vector_params[LAYERS * PER:]))
    valid = (jnp.arange(SEQ) < seq_length).astype(jnp.float32)
    return logits_loss(final_low, table_low, seq_labels, valid)

def advance(weight, moment, average, grad, factor):
    scaled = grad * factor
    moment_new = 0.5 * moment + scaled
    weight_new = weight - step_rate * (scaled + 0.5 * moment_new)
    average_new = 0.5 * average + 0.5 * weight_new
    return (weight_new, moment_new, average_new, weight_new.astype(jnp.bfloat16))

def reference(token_ids, target_ids, seq_lengths, embedding, embedding_mom, embedding_avg, in_proj, in_proj_mom, in_proj_avg, out_proj, out_proj_mom, out_proj_avg, vector_params, vector_mom, vector_avg):
    total_count = jnp.sum(seq_lengths).astype(jnp.float32)
    flat_ids = token_ids.reshape(MB * GROUPS, SEQ)
    flat_labels = target_ids.reshape(MB * GROUPS, SEQ)
    flat_lengths = seq_lengths.reshape(MB * GROUPS)

    def total_loss(table_in, in_weights, out_weights, vector_in):
        table_low = low(table_in)
        in_low = low(in_weights)
        out_low = low(out_weights)

        def one_sequence(accum, packed):
            seq_ids, seq_labels, seq_length = packed
            return (accum + sequence_total(table_low, in_low, out_low, vector_in, seq_ids, seq_labels, seq_length), None)
        total, unused = lax.scan(one_sequence, jnp.float32(0.0), (flat_ids, flat_labels, flat_lengths))
        return total / total_count
    loss_value, back_fn = jax.vjp(total_loss, embedding, in_proj, out_proj, vector_params)
    grad_table, grad_in, grad_out, grad_vector = back_fn(jnp.ones((), loss_value.dtype))
    squares = jnp.sum(grad_table * grad_table) + jnp.sum(grad_in * grad_in) + jnp.sum(grad_out * grad_out) + jnp.sum(grad_vector * grad_vector)
    grad_norm = jnp.sqrt(squares)
    factor = jnp.minimum(1.0, clip_limit / grad_norm)
    table_new, table_mom_new, table_avg_new, table_bf16 = advance(embedding, embedding_mom, embedding_avg, grad_table, factor)
    in_new, in_mom_new, in_avg_new, in_bf16 = advance(in_proj, in_proj_mom, in_proj_avg, grad_in, factor)
    out_new, out_mom_new, out_avg_new, out_bf16 = advance(out_proj, out_proj_mom, out_proj_avg, grad_out, factor)
    vec_new, vec_mom_new, vec_avg_new, vec_bf16 = advance(vector_params, vector_mom, vector_avg, grad_vector, factor)
    return (loss_value, grad_norm, table_new, table_mom_new, table_avg_new, table_bf16, in_new, in_mom_new, in_avg_new, in_bf16, out_new, out_mom_new, out_avg_new, out_bf16, vec_new, vec_mom_new, vec_avg_new, vec_bf16)
```

```python
import functools

import jax
import jax.numpy as jnp
from jax import lax
from jax.experimental import pallas as pl
from jax.experimental.pallas import tpu as pltpu
from jax.sharding import PartitionSpec as P


D = 1024
HEADS = 32
HDIM = 64
NSTATE = 128
CONV = 4
VOCAB = 50288
LAYERS = 2
MB = 2
DI = 2048
XBC = 2304
PER = 14688
LANES = 128
PAIRS = DI // LANES

epsilon = 1e-05
z_weight = 0.001
clip_limit = 0.2
step_rate = 1000.0
highest = lax.Precision.HIGHEST
bf16 = jnp.bfloat16
f32 = jnp.float32
VMEM_LIMIT = 62 * 1024 * 1024
OFF = -1e30


def dot_nn(a, b, precision=None):
    return lax.dot_general(
        a, b, (((1,), (0,)), ((), ())), precision=precision, preferred_element_type=f32
    )


def dot_nt(a, b, precision=None):
    return lax.dot_general(
        a, b, (((1,), (1,)), ((), ())), precision=precision, preferred_element_type=f32
    )


def dot_tn(a, b, precision=None):
    return lax.dot_general(
        a, b, (((0,), (0,)), ((), ())), precision=precision, preferred_element_type=f32
    )


def silu(v):
    return v * lax.logistic(v)


def silu_grad(v):
    s = lax.logistic(v)
    return s * (1.0 + v * (1.0 - s))


def local_call(kernel, ins, outs, scratch=(), in_smem=(), flops=0):
    total = sum(a.size * a.dtype.itemsize for a in ins)
    return pl.pallas_call(
        kernel,
        out_shape=[jax.ShapeDtypeStruct(shape, kind) for shape, kind in outs],
        in_specs=[
            pl.BlockSpec(memory_space=pltpu.SMEM if i in in_smem else pltpu.VMEM)
            for i in range(len(ins))
        ],
        out_specs=[pl.BlockSpec(memory_space=pltpu.VMEM) for _ in outs],
        scratch_shapes=list(scratch),
        compiler_params=pltpu.CompilerParams(vmem_limit_bytes=VMEM_LIMIT),
        cost_estimate=pl.CostEstimate(
            flops=flops or total, transcendentals=0, bytes_accessed=2 * total
        ),
    )(*ins)


def lookup_kernel(count_ref, row_ref, tok_ref, table_ref, out_ref, held):
    tokens = out_ref.shape[0]
    step = 512

    def clear(i, _):
        held[pl.ds(pl.multiple_of(i * step, step), step), :] = jnp.zeros(
            (step, held.shape[1]), f32
        )
        return 0

    lax.fori_loop(0, tokens // step, clear, 0)

    def move(i, _):
        for k in range(8):
            row = row_ref[i * 8 + k]
            tok = tok_ref[i * 8 + k]
            held[pl.ds(tok, 1), :] = table_ref[pl.ds(row, 1), :]
        return 0

    lax.fori_loop(0, (count_ref[0] + 7) // 8, move, 0)

    def put(i, _):
        rows = pl.ds(pl.multiple_of(i * step, step), step)
        out_ref[rows, :] = held[rows, :].astype(bf16)
        return 0

    lax.fori_loop(0, tokens // step, put, 0)


def spread_kernel(count_ref, row_ref, tok_ref, grad_ref, base_ref, out_ref, held):
    tokens = grad_ref.shape[0]
    step = 512
    rows_all = out_ref.shape[0]

    def take(i, _):
        rows = pl.ds(pl.multiple_of(i * step, step), step)
        held[rows, :] = grad_ref[rows, :].astype(f32)
        return 0

    lax.fori_loop(0, tokens // step, take, 0)
    held[pl.ds(tokens, 8), :] = jnp.zeros((8, held.shape[1]), f32)

    whole = rows_all // step

    def start(i, _):
        rows = pl.ds(pl.multiple_of(i * step, step), step)
        out_ref[rows, :] = base_ref[rows, :].astype(f32)
        return 0

    lax.fori_loop(0, whole, start, 0)
    if rows_all > whole * step:
        out_ref[whole * step :, :] = base_ref[whole * step :, :].astype(f32)

    def move(i, _):
        for k in range(8):
            row = row_ref[i * 8 + k]
            tok = tok_ref[i * 8 + k]
            out_ref[pl.ds(row, 1), :] = out_ref[pl.ds(row, 1), :] + held[pl.ds(tok, 1), :]
        return 0

    lax.fori_loop(0, (count_ref[0] + 7) // 8, move, 0)


MESH = pl.DeviceIdType.MESH


def remote(src, dst, send, recv, dp, fsdp):
    return pltpu.make_async_remote_copy(
        src_ref=src,
        dst_ref=dst,
        send_sem=send,
        recv_sem=recv,
        device_id=(dp, fsdp),
        device_id_type=MESH,
    )


def comm_call(kernel, number, ins, outs, scratch, in_spaces, out_spaces, sent):
    return pl.pallas_call(
        kernel,
        out_shape=[jax.ShapeDtypeStruct(shape, kind) for shape, kind in outs],
        in_specs=[pl.BlockSpec(memory_space=space) for space in in_spaces],
        out_specs=[pl.BlockSpec(memory_space=space) for space in out_spaces],
        scratch_shapes=list(scratch),
        compiler_params=pltpu.CompilerParams(
            collective_id=number, has_side_effects=True, vmem_limit_bytes=VMEM_LIMIT
        ),
        cost_estimate=pl.CostEstimate(flops=sent, transcendentals=0, bytes_accessed=2 * sent),
    )(*ins)


def chain_kernel(direction, steps, decay_ref, local_ref, out_ref, got, give, send, recv):
    dp = lax.axis_index("dp")
    me = lax.axis_index("fsdp")
    place = me // MB
    count = lax.axis_size("fsdp") // MB
    first = place == (0 if direction > 0 else count - 1)
    final = place == (count - 1 if direction > 0 else 0)
    part = DI // steps
    heads = part // HDIM
    barrier = pltpu.get_barrier_semaphore()

    @pl.when(jnp.logical_not(first))
    def _():
        pl.semaphore_signal(
            barrier, inc=1, device_id=(dp, me - MB * direction), device_id_type=MESH
        )

    @pl.when(jnp.logical_not(final))
    def _():
        pl.semaphore_wait(barrier, 1)

    @pl.when(first)
    def _():
        got[...] = jnp.zeros(got.shape, bf16)

    def copy(g):
        rows = pl.ds(g * part, part)
        return remote(
            give.at[rows], got.at[rows], send.at[g], recv.at[g], dp, me + MB * direction
        )

    for g in range(steps):
        rows = pl.ds(g * part, part)

        @pl.when(jnp.logical_not(first))
        def _():
            copy(g).wait_recv()

        @pl.when(jnp.logical_not(final))
        def _():
            for i in range(heads):
                h = pl.ds(g * part + i * HDIM, HDIM)
                give[h, :] = (
                    decay_ref[g * heads + i] * got[h, :].astype(f32) + local_ref[h, :]
                ).astype(bf16)
            copy(g).start()

        out_ref[rows, :] = got[rows, :]

    @pl.when(jnp.logical_not(final))
    def _():
        for g in range(steps):
            copy(g).wait_send()


CHAIN_STEPS = 8


def carry_chain(decay, local, direction):
    return comm_call(
        functools.partial(chain_kernel, direction, CHAIN_STEPS),
        1 if direction > 0 else 2,
        (decay, local),
        ((local.shape, bf16),),
        (
            pltpu.VMEM(local.shape, bf16),
            pltpu.VMEM(local.shape, bf16),
            pltpu.SemaphoreType.DMA((CHAIN_STEPS,)),
            pltpu.SemaphoreType.DMA((CHAIN_STEPS,)),
        ),
        (pltpu.SMEM, pltpu.VMEM),
        (pltpu.VMEM,),
        local.size * 2,
    )[0]


def bits_of(size):
    return [1 << b for b in range(size.bit_length() - 1)]


def total_kernel(in_ref, out_ref, work, got, send, recv):
    dp = lax.axis_index("dp")
    me = lax.axis_index("fsdp")
    half = in_ref.shape[0] // 2
    core = me % MB
    partners = [("f", b) for b in bits_of(lax.axis_size("fsdp")) if b > 1]
    partners += [("d", b) for b in bits_of(lax.axis_size("dp"))]

    def across(kind, bit):
        ids, other = (me, lambda v: (dp, v)) if kind == "f" else (dp, lambda v: (v, me))
        return other(jnp.where((ids // bit) % 2 == 1, ids - bit, ids + bit))

    mate = across("f", 1)
    barrier = pltpu.get_barrier_semaphore()
    for target in [mate] + [across(*p) for p in partners]:
        pl.semaphore_signal(barrier, inc=1, device_id=target, device_id_type=MESH)
    pl.semaphore_wait(barrier, 1 + len(partners))

    mine = pl.ds(pl.multiple_of(core * half, 8), half)
    theirs = pl.ds(pl.multiple_of((1 - core) * half, 8), half)
    copy = remote(in_ref.at[theirs], got.at[0], send.at[0], recv.at[0], *mate)
    copy.start()
    copy.wait()
    work[0] = in_ref[mine, :] + got[0]
    for i, p in enumerate(partners):
        copy = remote(work.at[i], got.at[i + 1], send.at[i + 1], recv.at[i + 1], *across(*p))
        copy.start()
        copy.wait()
        work[i + 1] = work[i] + got[i + 1]
    n = len(partners)
    copy = remote(work.at[n], got.at[n + 1], send.at[n + 1], recv.at[n + 1], *mate)
    copy.start()
    copy.wait()
    out_ref[mine, :] = work[n]
    out_ref[theirs, :] = got[n + 1]


def total_of(array):
    rows = array.shape[0]
    steps = len(bits_of(lax.axis_size("fsdp"))) - 1 + len(bits_of(lax.axis_size("dp")))
    return comm_call(
        total_kernel,
        3,
        (array,),
        ((array.shape, f32),),
        (
            pltpu.VMEM((steps + 1, rows // 2, LANES), f32),
            pltpu.VMEM((steps + 2, rows // 2, LANES), f32),
            pltpu.SemaphoreType.DMA((steps + 2,)),
            pltpu.SemaphoreType.DMA((steps + 2,)),
        ),
        (pltpu.VMEM,),
        (pltpu.VMEM,),
        array.size * 4 * 3,
    )[0]


def snake(place, size):
    return jnp.where(place < size // 2, place, size // 2 + size - 1 - place)


def wrap(value, size):
    return lax.rem(value + size, size)


def gather_kernel(*refs):
    arrays = 2 * LAYERS
    own = refs[:arrays]
    full = refs[arrays : 2 * arrays]
    local_sem, z_send, z_recv, ring_send, ring_recv, mate_send, mate_recv = refs[2 * arrays :]
    dp = lax.axis_index("dp")
    me = lax.axis_index("fsdp")
    size = lax.axis_size("dp")
    count = lax.axis_size("fsdp") // MB
    core = me % MB
    k = me // MB
    ring = snake(dp, size)
    reach = size // 2
    right = snake(wrap(ring + 1, size), size)
    left = snake(wrap(ring - 1, size), size)
    mate = k * MB + 1 - core
    up, down = me + MB, me - MB
    has_up, has_down = k < count - 1, k > 0
    barrier = pltpu.get_barrier_semaphore()
    for target in ((right, me), (left, me), (dp, mate)):
        pl.semaphore_signal(barrier, inc=1, device_id=target, device_id_type=MESH)

    @pl.when(has_up)
    def _():
        pl.semaphore_signal(barrier, inc=1, device_id=(dp, up), device_id_type=MESH)

    @pl.when(has_down)
    def _():
        pl.semaphore_signal(barrier, inc=1, device_id=(dp, down), device_id_type=MESH)

    pl.semaphore_wait(barrier, 3 + jnp.where(has_up, 1, 0) + jnp.where(has_down, 1, 0))

    def spot(a, d, z, c):
        return full[a].at[d, z, c]

    def chain(a, src, z, side):
        return remote(
            src, spot(a, dp, z, core), z_send.at[a, z], z_recv.at[a, z], dp, up if side == 0 else down
        )

    def chain_own(a, side):
        return remote(
            own[a],
            spot(a, dp, k, core),
            z_send.at[a, count + side],
            z_recv.at[a, k],
            dp,
            up if side == 0 else down,
        )

    def round_ring(a, src, d, z, side):
        return remote(
            src,
            spot(a, d, z, core),
            ring_send.at[a, side],
            ring_recv.at[a, d, z],
            right if side == 0 else left,
            me,
        )

    def to_mate(a, src, d, z):
        return remote(src, spot(a, d, z, core), mate_send.at[a], mate_recv.at[a], dp, mate)

    def carried(a, side):
        return (a < arrays // 2) == (side == 0)

    for a in range(arrays):

        @pl.when(has_up)
        def _(a=a):
            chain_own(a, 0).start()

        @pl.when(has_down)
        def _(a=a):
            chain_own(a, 1).start()

    for a in range(arrays):
        for side in (0, 1):
            round_ring(a, own[a], dp, k, side).start()
    for a in range(arrays):
        to_mate(a, own[a], dp, k).start()
        pltpu.make_async_copy(own[a], spot(a, dp, k, core), local_sem.at[a]).start()

    def ring_step(z, s):
        for side in (0, 1):
            origin = snake(wrap(ring - s if side == 0 else ring + s, size), size)
            for a in range(arrays):
                if s == reach and not carried(a, side):
                    continue
                piece = spot(a, origin, z, core)
                round_ring(a, piece, origin, z, side).wait_recv()
                if s + 1 < reach or (s + 1 == reach and carried(a, side)):
                    round_ring(a, piece, origin, z, side).start()
                to_mate(a, piece, origin, z).start()

    def arrive(z, side):
        for a in range(arrays):
            piece = spot(a, dp, z, core)
            chain(a, piece, z, side).wait_recv()

            @pl.when(has_up if side == 0 else has_down)
            def _(a=a, piece=piece):
                chain(a, piece, z, side).start()

            for way in (0, 1):
                round_ring(a, piece, dp, z, way).start()
            to_mate(a, piece, dp, z).start()

    def both_ways(far, act):
        if far == 0:
            act(k, 0)
            return

        @pl.when(k >= far)
        def _():
            act(k - far, 0)

        @pl.when(k + far < count)
        def _():
            act(k + far, 1)

    for turn in range(1, count + reach):
        if turn < count:
            both_ways(turn, arrive)
        for s in range(1, reach + 1):
            if 0 <= turn - s < count:
                both_ways(turn - s, lambda z, side, s=s: ring_step(z, s))

    for a in range(arrays):
        pltpu.make_async_copy(own[a], spot(a, dp, k, core), local_sem.at[a]).wait()
        for side in (0, 1):
            sent = full[a].at[pl.ds(0, reach if carried(a, side) else reach - 1), :, core]
            remote(sent, sent, ring_send.at[a, side], ring_recv.at[a, 0, 0], dp, mate).wait_send()
        whole = full[a].at[:, :, core]
        remote(whole, whole, mate_send.at[a], mate_recv.at[a], dp, mate).wait_send()
        whole = full[a].at[:, :, 1 - core]
        remote(whole, whole, mate_send.at[a], mate_recv.at[a], dp, mate).wait_recv()

        @pl.when(has_up)
        def _(a=a):
            chain_own(a, 0).wait_send()

        @pl.when(has_down)
        def _(a=a):
            chain_own(a, 1).wait_send()

        for far in range(1, count):

            @pl.when(jnp.logical_and(k >= far, has_up))
            def _(a=a, far=far):
                chain(a, spot(a, dp, k - far, core), k - far, 0).wait_send()

            @pl.when(jnp.logical_and(k + far < count, has_down))
            def _(a=a, far=far):
                chain(a, spot(a, dp, k + far, core), k + far, 1).wait_send()


def gather_layers(shards):
    size, count = lax.axis_size("dp"), lax.axis_size("fsdp") // MB
    arrays = len(shards)
    outs = comm_call(
        gather_kernel,
        4,
        shards,
        tuple(((size, count, MB) + s.shape, bf16) for s in shards),
        (
            pltpu.SemaphoreType.DMA((arrays,)),
            pltpu.SemaphoreType.DMA((arrays, count + 2)),
            pltpu.SemaphoreType.DMA((arrays, count)),
            pltpu.SemaphoreType.DMA((arrays, 2)),
            pltpu.SemaphoreType.DMA((arrays, size, count)),
            pltpu.SemaphoreType.DMA((arrays,)),
            pltpu.SemaphoreType.DMA((arrays,)),
        ),
        (pltpu.VMEM,) * arrays,
        (pl.ANY,) * arrays,
        sum(s.size * 2 for s in shards) * 24,
    )
    return [o.reshape(size * count * MB * s.shape[0], s.shape[1]) for o, s in zip(outs, shards)]


def add_rows(dst, first, *others):
    rows = dst.shape[0]
    step = min(rows, 16)

    def one(i, _):
        at = pl.ds(pl.multiple_of(i * step, step), step)
        total = first[at, :].astype(f32)
        for other in others:
            total = total + other[at, :].astype(f32)
        dst[at, :] = total.astype(dst.dtype)
        return 0

    lax.fori_loop(0, rows // step, one, 0)


def reduce_kernel(*refs):
    arrays = 2 * LAYERS
    grads = refs[:arrays]
    outs = refs[arrays : 2 * arrays]
    held, given, come, chained = (
        refs[(2 + i) * arrays : (3 + i) * arrays] for i in range(4)
    )
    load_sem, mate_send, mate_recv, ring_send, ring_recv, z_send, z_recv = refs[6 * arrays :]
    dp = lax.axis_index("dp")
    me = lax.axis_index("fsdp")
    size = lax.axis_size("dp")
    count = lax.axis_size("fsdp") // MB
    core = me % MB
    k = me // MB
    ring = snake(dp, size)
    reach = size // 2
    right = snake(wrap(ring + 1, size), size)
    left = snake(wrap(ring - 1, size), size)
    mate = k * MB + 1 - core
    up, down = me + MB, me - MB
    has_up, has_down = k < count - 1, k > 0

    def load(a):
        return pltpu.make_async_copy(grads[a].at[:, :, core], held[a], load_sem.at[a])

    for a in range(arrays):
        load(a).start()
    barrier = pltpu.get_barrier_semaphore()
    for target in ((right, me), (left, me), (dp, mate)):
        pl.semaphore_signal(barrier, inc=1, device_id=target, device_id_type=MESH)

    @pl.when(has_up)
    def _():
        pl.semaphore_signal(barrier, inc=1, device_id=(dp, up), device_id_type=MESH)

    @pl.when(has_down)
    def _():
        pl.semaphore_signal(barrier, inc=1, device_id=(dp, down), device_id_type=MESH)

    pl.semaphore_wait(barrier, 3 + jnp.where(has_up, 1, 0) + jnp.where(has_down, 1, 0))

    def away(j, side):
        return snake(wrap(ring + j if side == 0 else ring - j, size), size)

    def to_mate(a, d):
        return remote(
            grads[a].at[d, :, 1 - core], given[a].at[d], mate_send.at[a], mate_recv.at[a, d], dp, mate
        )

    def carried(a, side):
        return (a < arrays // 2) == (side == 0)

    def targets(j):
        if j == 0:
            return [dp]
        if j == reach:
            return [away(j, 0)]
        return [away(j, 0), away(j, 1)]

    for j in range(reach, -1, -1):
        for d in targets(j):
            for a in range(arrays):
                to_mate(a, d).start()

    for a in range(arrays):
        load(a).wait()

    def add_mate(d):
        for a in range(arrays):
            to_mate(a, d).wait_recv()

            def one(z, _, a=a):
                add_rows(held[a].at[d, z], held[a].at[d, z], given[a].at[d, z])
                return 0

            lax.fori_loop(0, count, one, 0)

    def first_step(a, side):
        d = away(reach, 0)
        return remote(
            held[a].at[d], come[a].at[side, 0], ring_send.at[a, side], ring_recv.at[a, side, 0, 0],
            right if side == 0 else left, me,
        )

    def next_step(a, side, s, z):
        d = away(reach - s, side)
        return remote(
            held[a].at[d, z], come[a].at[side, s, z], ring_send.at[a, side],
            ring_recv.at[a, side, s, z], right if side == 0 else left, me,
        )

    far_most = jnp.maximum(k, count - 1 - k)
    near_most = jnp.minimum(k, count - 1 - k)
    uneven = far_most - near_most
    long_side = jnp.where(count - 1 - k > k, 1, -1)

    def chunk_at(i):
        j = jnp.maximum(i - uneven, 0)
        paired = k + (1 - 2 * (j % 2)) * (near_most - j // 2)
        return jnp.where(i < uneven, k + long_side * (far_most - i), paired)

    add_mate(away(reach, 0))
    for a in range(arrays):
        first_step(a, 0 if carried(a, 0) else 1).start()
    for s in range(1, reach):
        for side in (0, 1):
            add_mate(away(reach - s, side))
        if s == 1:
            for a in range(arrays):
                first_step(a, 0 if carried(a, 0) else 1).wait_recv()

        def pass_on(i, _, s=s):
            z = chunk_at(i)
            for side in (0, 1):
                d = away(reach - s, side)
                for a in range(arrays):
                    if s > 1:
                        next_step(a, side, s - 1, z).wait_recv()
                    if s > 1 or carried(a, side):
                        add_rows(held[a].at[d, z], held[a].at[d, z], come[a].at[side, s - 1, z])
                    next_step(a, side, s, z).start()
            return 0

        lax.fori_loop(0, count, pass_on, 0)
    add_mate(dp)

    def along(a, side, z):
        return remote(
            held[a].at[dp, z], chained[a].at[side, z], z_send.at[a, z], z_recv.at[a, side, z],
            dp, up if side == 0 else down,
        )

    def finish(i, _):
        z = chunk_at(i)
        for a in range(arrays):
            for side in (0, 1):
                next_step(a, side, reach - 1, z).wait_recv()
            add_rows(
                held[a].at[dp, z],
                held[a].at[dp, z],
                come[a].at[0, reach - 1, z],
                come[a].at[1, reach - 1, z],
            )
            for side in (0, 1):
                beyond = z > k if side == 0 else z < k
                fed = has_down if side == 0 else has_up

                @pl.when(jnp.logical_and(fed, jnp.logical_or(beyond, z == k)))
                def _(a=a, side=side):
                    along(a, side, z).wait_recv()
                    add_rows(held[a].at[dp, z], held[a].at[dp, z], chained[a].at[side, z])

                @pl.when(beyond)
                def _(a=a, side=side):
                    along(a, side, z).start()

        return 0

    lax.fori_loop(0, count, finish, 0)
    for a in range(arrays):
        add_rows(outs[a], held[a].at[dp, k])
        for side in (0, 1):
            sent = held[a].at[pl.ds(0, reach if carried(a, side) else reach - 1)]
            remote(
                sent, sent, ring_send.at[a, side], ring_recv.at[a, side, 0, 0], dp, mate
            ).wait_send()
        remote(
            given[a], given[a], mate_send.at[a], mate_recv.at[a, 0], dp, mate
        ).wait_send()

    def sent_along(z, _):
        for a in range(arrays):

            @pl.when(z != k)
            def _(a=a):
                along(a, 0, z).wait_send()

        return 0

    lax.fori_loop(0, count, sent_along, 0)


def reduce_layers(grads):
    size, count = lax.axis_size("dp"), lax.axis_size("fsdp") // MB
    arrays = len(grads)
    reach = size // 2
    shards = [(g.shape[0] // (size * count * MB), g.shape[1]) for g in grads]
    blocks = [g.reshape((size, count, MB) + s) for g, s in zip(grads, shards)]
    return comm_call(
        reduce_kernel,
        5,
        blocks,
        tuple((s, f32) for s in shards),
        tuple(pltpu.VMEM((size, count) + s, bf16) for s in shards) * 2
        + tuple(pltpu.VMEM((2, reach, count) + s, bf16) for s in shards)
        + tuple(pltpu.VMEM((2, count) + s, bf16) for s in shards)
        + (
            pltpu.SemaphoreType.DMA((arrays,)),
            pltpu.SemaphoreType.DMA((arrays,)),
            pltpu.SemaphoreType.DMA((arrays, size)),
            pltpu.SemaphoreType.DMA((arrays, 2)),
            pltpu.SemaphoreType.DMA((arrays, 2, reach, count)),
            pltpu.SemaphoreType.DMA((arrays, count)),
            pltpu.SemaphoreType.DMA((arrays, 2, count)),
        ),
        (pl.ANY,) * arrays,
        (pltpu.VMEM,) * arrays,
        sum(g.size * 2 for g in grads),
    )


def pair_lanes(p):
    return pl.ds(pl.multiple_of(p * LANES, LANES), LANES)


def first_half(rows):
    return lax.broadcasted_iota(jnp.int32, (rows, LANES), 1) < HDIM


def spread_columns(values, column, per_pair, rows):
    half = first_half(rows)
    for p in range(PAIRS):
        left = jnp.broadcast_to(values[:, 2 * p : 2 * p + 1], (rows, LANES))
        right = jnp.broadcast_to(values[:, 2 * p + 1 : 2 * p + 2], (rows, LANES))
        if column is not None:
            column[2 * p] = left
            column[2 * p + 1] = right
        if per_pair is not None:
            per_pair[p] = jnp.where(half, left, right)


def front_kernel(
    proj_ref, halo_ref, cw_ref, cb_ref, dtb_ref, al_ref, sk_ref,
    pre_ref, y_ref, st_ref, dt_ref, cum_ref,
    pad, col, tcol, lcol, lrow,
):
    rows = proj_ref.shape[0]
    pad[0:8, :] = halo_ref[...]
    pad[8:, :] = proj_ref[:, DI : DI + XBC]

    def conv(i, _):
        xs = pair_lanes(i)
        out = jnp.broadcast_to(cb_ref[0:1, xs], (rows, LANES))
        for k in range(CONV):
            out = out + cw_ref[k : k + 1, xs] * pad[5 + k : 5 + k + rows, xs]
        pre_ref[:, xs] = out
        return 0

    lax.fori_loop(0, XBC // LANES, conv, 0)

    dt_ref[...] = jnp.zeros((rows, LANES), f32)
    dt_ref[:, 0:HEADS] = proj_ref[:, DI + XBC :]
    drive = dt_ref[...] + dtb_ref[...]
    dt = jnp.maximum(drive, 0.0) + jnp.log1p(jnp.exp(-jnp.abs(drive)))
    dt_ref[...] = dt
    rate = dt * (-jnp.exp(al_ref[...]))
    ri = lax.broadcasted_iota(jnp.int32, (rows, rows), 0)
    ci = lax.broadcasted_iota(jnp.int32, (rows, rows), 1)
    causal = ri >= ci
    cum = dot_nn(jnp.where(causal, 1.0, 0.0), rate, highest)
    cum_ref[...] = cum
    lrow[...] = cum.T
    spread_columns(cum, col, lcol, rows)
    spread_columns(dt, None, tcol, rows)
    bm = silu(pre_ref[:, DI : DI + NSTATE]).astype(bf16)
    cm = silu(pre_ref[:, DI + NSTATE :]).astype(bf16)
    cb = dot_nt(cm, bm)
    half = first_half(rows)

    def pair(p, _):
        xs = pair_lanes(p)
        x = silu(pre_ref[:, xs])
        xt = tcol[p] * x
        xtb = xt.astype(bf16)
        parts = []
        for j in range(2):
            h = 2 * p + j
            c = col[h]
            d = jnp.concatenate([c] * (rows // LANES), axis=1) - lrow[pl.ds(h, 1), :]
            m = (jnp.exp(jnp.where(causal, d, OFF)) * cb).astype(bf16)
            parts.append(dot_nn(m, xtb))
        y_ref[:, xs] = jnp.where(half, parts[0], parts[1]) + sk_ref[0:1, xs] * x
        lp = lcol[p]
        tail = jnp.exp(lp[rows - 1 : rows, :] - lp)
        st_ref[xs, :] = dot_tn((tail * xt).astype(bf16), bm)
        return 0

    lax.fori_loop(0, PAIRS, pair, 0)


def gate_kernel(
    y0_ref, proj_ref, pre_ref, cum_ref, sin_ref, gg_ref, y_ref, yn_ref, lcol
):
    rows = y0_ref.shape[0]
    spread_columns(cum_ref[...], None, lcol, rows)
    cm = silu(pre_ref[:, DI + NSTATE :]).astype(bf16)

    def pair(p, total):
        xs = pair_lanes(p)
        y = y0_ref[:, xs] + jnp.exp(lcol[p]) * dot_nt(cm, sin_ref[xs, :])
        y_ref[:, xs] = y
        g = y * silu(proj_ref[:, xs])
        return total + g * g

    total = lax.fori_loop(0, PAIRS, pair, jnp.zeros((rows, LANES), f32))
    scale = lax.rsqrt(jnp.sum(total, axis=1, keepdims=True) / DI + epsilon)

    def put(p, _):
        xs = pair_lanes(p)
        g = y_ref[:, xs] * silu(proj_ref[:, xs])
        yn_ref[:, xs] = (g * scale * gg_ref[0:1, xs]).astype(bf16)
        return 0

    lax.fori_loop(0, PAIRS, put, 0)


def ungate_kernel(
    dyn_ref, y_ref, proj_ref, pre_ref, cum_ref, gg_ref,
    dy_ref, dz_ref, dgg_ref, gst_ref, lcol,
):
    rows = y_ref.shape[0]
    spread_columns(cum_ref[...], None, lcol, rows)
    cm = silu(pre_ref[:, DI + NSTATE :]).astype(bf16)
    zero = jnp.zeros((rows, LANES), f32)

    def sums(p, carry):
        xs = pair_lanes(p)
        g = y_ref[:, xs] * silu(proj_ref[:, xs])
        return carry[0] + g * g, carry[1] + g * (dyn_ref[:, xs] * gg_ref[0:1, xs])

    square, cross = lax.fori_loop(0, PAIRS, sums, (zero, zero))
    scale = lax.rsqrt(jnp.sum(square, axis=1, keepdims=True) / DI + epsilon)
    mean = jnp.sum(cross, axis=1, keepdims=True) * scale / DI

    def pair(p, _):
        xs = pair_lanes(p)
        z = proj_ref[:, xs]
        y = y_ref[:, xs]
        sz = silu(z)
        ghat = y * sz * scale
        dyn = dyn_ref[:, xs]
        dgg_ref[0:1, xs] = jnp.sum(dyn * ghat, axis=0, keepdims=True)
        dg = scale * (dyn * gg_ref[0:1, xs] - ghat * mean)
        dy = dg * sz
        dy_ref[:, xs] = dy
        dz_ref[:, xs] = (dg * y * silu_grad(z)).astype(bf16)
        gst_ref[xs, :] = dot_tn((jnp.exp(lcol[p]) * dy).astype(bf16), cm)
        return 0

    lax.fori_loop(0, PAIRS, pair, 0)


def back_kernel(
    dy_ref, y_ref, proj_ref, halo_ref, pre_ref, dt_ref, cum_ref, sin_ref, gin_ref,
    cw_ref, dtb_ref, al_ref, sk_ref,
    dx_ref, dhalo_ref, ddr_ref, dcw_ref, dsm_ref,
    pad, grad, col, tcol, lcol, lrow, dcb, dbm, dcm, dlog, dtx, ends,
):
    rows = y_ref.shape[0]
    pad[0:8, :] = halo_ref[...]
    pad[8:, :] = proj_ref[:, DI : DI + XBC]
    grad[0:8, :] = jnp.zeros((8, XBC), f32)
    grad[rows + 8 :, :] = jnp.zeros((8, XBC), f32)
    cum = cum_ref[...]
    dt = dt_ref[...]
    lrow[...] = cum.T
    spread_columns(cum, col, lcol, rows)
    spread_columns(dt, None, tcol, rows)
    bm = silu(pre_ref[:, DI : DI + NSTATE]).astype(bf16)
    cm = silu(pre_ref[:, DI + NSTATE :]).astype(bf16)
    cbt = dot_nt(bm, cm)
    ri = lax.broadcasted_iota(jnp.int32, (rows, rows), 0)
    ci = lax.broadcasted_iota(jnp.int32, (rows, rows), 1)
    causal = ri <= ci
    half = first_half(rows)
    dcb[...] = jnp.zeros((rows, rows), f32)
    zero = jnp.zeros((rows, LANES), f32)
    dbm[...] = zero
    dcm[...] = zero
    dlog[...] = zero
    dtx[...] = zero
    ends[...] = jnp.zeros((16, LANES), f32)
    lane_row = lax.broadcasted_iota(jnp.int32, (LANES, LANES), 0)
    lane_col = lax.broadcasted_iota(jnp.int32, (LANES, LANES), 1)
    ones = jnp.ones((8, NSTATE), f32)

    def pair(p, _):
        xs = pair_lanes(p)
        pre = pre_ref[:, xs]
        x = silu(pre)
        tp = tcol[p]
        xt = tp * x
        dy = dy_ref[:, xs]
        dyb = dy.astype(bf16)
        parts = []
        for j in range(2):
            h = 2 * p + j
            c = col[h]
            d = lrow[pl.ds(h, 1), :] - jnp.concatenate([c] * (rows // LANES), axis=1)
            w = jnp.exp(jnp.where(causal, d, OFF))
            parts.append(dot_nn((w * cbt).astype(bf16), dyb))
            own = half if j == 0 else jnp.logical_not(half)
            q = dot_nt(jnp.where(own, xt, 0.0).astype(bf16), dyb)
            dcb[...] += w * q
        lp = lcol[p]
        last = lp[rows - 1 : rows, :]
        tail = jnp.exp(last - lp)
        gin = gin_ref[xs, :]
        sin = sin_ref[xs, :]
        dst = tail * dot_nt(bm, gin)
        dxt = jnp.where(half, parts[0], parts[1]) + dst
        dbm[...] += dot_nn((tail * xt).astype(bf16), gin)
        dcm[...] += dot_nn((jnp.exp(lp) * dy).astype(bf16), sin)
        sk = sk_ref[0:1, xs]
        pick = jnp.where(lane_col == 2 * p + jnp.where(lane_row >= HDIM, 1, 0), 1.0, 0.0)
        dlog[...] += dot_nn(dy * (y_ref[:, xs] - sk * x) - xt * dxt, pick, highest)
        dtx[...] += dot_nn(x * dxt, pick, highest)
        held = dot_nt(ones, gin.astype(f32) * sin.astype(f32), highest)
        end = jnp.sum(xt * dst, axis=0, keepdims=True) + jnp.exp(last) * held[0:1, :]
        skip = jnp.sum(dy * x, axis=0, keepdims=True)
        stacked = jnp.concatenate(
            [jnp.broadcast_to(end, (8, LANES)), jnp.broadcast_to(skip, (8, LANES))], axis=0
        )
        ends[...] += dot_nn(stacked, pick, highest)
        grad[pl.ds(8, rows), xs] = (tp * dxt + sk * dy) * silu_grad(pre)
        return 0

    lax.fori_loop(0, PAIRS, pair, 0)
    dcbb = dcb[...].astype(bf16)
    dc = dcm[...] + dot_tn(dcbb, bm)
    db = dbm[...] + dot_nn(dcbb, cm)
    grad[8 : 8 + rows, DI : DI + NSTATE] = db * silu_grad(pre_ref[:, DI : DI + NSTATE])
    grad[8 : 8 + rows, DI + NSTATE :] = dc * silu_grad(pre_ref[:, DI + NSTATE :])

    last_row = lax.broadcasted_iota(jnp.int32, (rows, LANES), 0) == rows - 1
    dl = dlog[...] + jnp.where(last_row, ends[0:1, :], 0.0)
    da = dot_nn(jnp.where(causal, 1.0, 0.0), dl, highest)
    decay = -jnp.exp(al_ref[...])
    ddt = dtx[...] + da * decay
    ddr_ref[...] = jnp.zeros((rows, LANES), f32)
    ddr_ref[:, 0:HEADS] = proj_ref[:, DI + XBC :]
    ddr = ddt * lax.logistic(ddr_ref[...] + dtb_ref[...])
    ddr_ref[...] = ddr
    dsm_ref[...] = jnp.zeros((8, LANES), f32)
    dsm_ref[0:1, :] = jnp.sum(ddr, axis=0, keepdims=True)
    dsm_ref[1:2, :] = jnp.sum(da * dt, axis=0, keepdims=True) * decay
    dsm_ref[2:3, :] = ends[8:9, :]

    def conv(i, _):
        xs = pair_lanes(i)
        own = grad[pl.ds(8, rows), xs]
        out = jnp.zeros((rows, LANES), f32)
        edge = jnp.zeros((8, LANES), f32)
        for k in range(CONV):
            wk = cw_ref[k : k + 1, xs]
            out = out + wk * grad[11 - k : 11 - k + rows, xs]
            edge = edge + wk * grad[3 - k : 11 - k, xs]
            dcw_ref[k : k + 1, xs] = jnp.sum(
                own * pad[5 + k : 5 + k + rows, xs], axis=0, keepdims=True
            )
        dcw_ref[4:5, xs] = jnp.sum(own, axis=0, keepdims=True)
        dx_ref[:, xs] = out
        dhalo_ref[:, xs] = edge
        return 0

    lax.fori_loop(0, XBC // LANES, conv, 0)


VTILE = 640
NTILE = 512


def head_specs(width, tokens):
    return dict(
        table=pl.BlockSpec((VTILE, width), lambda i: (i, 0)),
        kept=pl.BlockSpec((VTILE, tokens), lambda i: (i, 0)),
        row=pl.BlockSpec((1, tokens), lambda i: (0, 0)),
        tile_row=pl.BlockSpec((1, 1, tokens), lambda i: (i, 0, 0)),
    )


def head_params():
    return pltpu.CompilerParams(
        dimension_semantics=("arbitrary",), vmem_limit_bytes=VMEM_LIMIT
    )


def head_stats_kernel(vocab_rows, e_ref, ht_ref, lab_ref, q_ref, st_ref):
    first = pl.program_id(0) * VTILE
    tokens = ht_ref.shape[1]
    e = e_ref[...]

    def chunk(j, _):
        ns = pl.ds(pl.multiple_of(j * NTILE, NTILE), NTILE)
        logits = dot_nn(e, ht_ref[:, ns])
        rid = lax.broadcasted_iota(jnp.int32, (VTILE, NTILE), 0) + first
        real = rid < vocab_rows
        shown = jnp.where(real, logits, OFF)
        top = jnp.max(shown, axis=0, keepdims=True)
        p = jnp.exp(shown - top)
        q_ref[:, ns] = p.astype(bf16)
        st_ref[0, 0:1, ns] = top
        st_ref[0, 1:2, ns] = jnp.sum(p, axis=0, keepdims=True)
        hit = jnp.where(jnp.logical_and(real, rid == lab_ref[0:1, ns]), logits, 0.0)
        st_ref[0, 2:3, ns] = jnp.sum(hit, axis=0, keepdims=True)
        st_ref[0, 3:4, ns] = jnp.sum(jnp.where(real, logits, 0.0), axis=0, keepdims=True)
        return 0

    lax.fori_loop(0, tokens // NTILE, chunk, 0)


def head_stats(table, hidden_t, labels):
    vocab_rows, width = table.shape
    tokens = hidden_t.shape[1]
    tiles = pl.cdiv(vocab_rows, VTILE)
    sp = head_specs(width, tokens)
    return pl.pallas_call(
        functools.partial(head_stats_kernel, vocab_rows),
        name="head_stats",
        grid=(tiles,),
        in_specs=[
            sp["table"],
            pl.BlockSpec((width, tokens), lambda i: (0, 0)),
            sp["row"],
        ],
        out_specs=[sp["kept"], pl.BlockSpec((1, 8, tokens), lambda i: (i, 0, 0))],
        out_shape=[
            jax.ShapeDtypeStruct((tiles * VTILE, tokens), bf16),
            jax.ShapeDtypeStruct((tiles, 8, tokens), f32),
        ],
        compiler_params=head_params(),
        cost_estimate=pl.CostEstimate(
            flops=2 * vocab_rows * width * tokens,
            transcendentals=vocab_rows * tokens,
            bytes_accessed=2 * vocab_rows * (width + tokens),
        ),
    )(table, hidden_t, labels)


def logit_grads(q, fac, weight, rid, label):
    hit = jnp.where(rid == label, 0.9 + 0.1 / VOCAB, 0.1 / VOCAB)
    return (q.astype(f32) * fac - weight * hit).astype(bf16)


def head_rows_kernel(vocab_rows, e_ref, q_ref, fac_ref, w_ref, lab_ref, out_ref, et):
    first = pl.program_id(0) * VTILE
    tokens = q_ref.shape[1]

    @pl.when(pl.program_id(0) == 0)
    def _():
        out_ref[...] = jnp.zeros(out_ref.shape, f32)

    eid = lax.broadcasted_iota(jnp.int32, (VTILE, e_ref.shape[1]), 0) + first
    et[...] = jnp.where(eid < vocab_rows, e_ref[...].astype(f32), 0.0).T.astype(bf16)

    def chunk(j, _):
        ns = pl.ds(pl.multiple_of(j * NTILE, NTILE), NTILE)
        rid = lax.broadcasted_iota(jnp.int32, (VTILE, NTILE), 0) + first
        dl = logit_grads(
            q_ref[:, ns], fac_ref[0, 0:1, ns], w_ref[0:1, ns], rid, lab_ref[0:1, ns]
        )
        out_ref[:, ns] += dot_nn(et[...], dl)
        return 0

    lax.fori_loop(0, tokens // NTILE, chunk, 0)


def head_rows(table, kept, fac, weight, labels):
    vocab_rows, width = table.shape
    tokens = kept.shape[1]
    tiles = pl.cdiv(vocab_rows, VTILE)
    sp = head_specs(width, tokens)
    return pl.pallas_call(
        functools.partial(head_rows_kernel, vocab_rows),
        name="head_rows",
        grid=(tiles,),
        in_specs=[sp["table"], sp["kept"], sp["tile_row"], sp["row"], sp["row"]],
        out_specs=pl.BlockSpec((width, tokens), lambda i: (0, 0)),
        out_shape=jax.ShapeDtypeStruct((width, tokens), f32),
        scratch_shapes=[pltpu.VMEM((width, VTILE), bf16)],
        compiler_params=head_params(),
        cost_estimate=pl.CostEstimate(
            flops=2 * vocab_rows * width * tokens,
            transcendentals=0,
            bytes_accessed=2 * vocab_rows * (width + tokens),
        ),
    )(table, kept, fac, weight, labels)


def head_table_kernel(h_ref, q_ref, fac_ref, w_ref, lab_ref, out_ref, dl_ref):
    first = pl.program_id(0) * VTILE
    tokens = q_ref.shape[1]

    def chunk(j, _):
        ns = pl.ds(pl.multiple_of(j * NTILE, NTILE), NTILE)
        rid = lax.broadcasted_iota(jnp.int32, (VTILE, NTILE), 0) + first
        dl_ref[:, ns] = logit_grads(
            q_ref[:, ns], fac_ref[0, 0:1, ns], w_ref[0:1, ns], rid, lab_ref[0:1, ns]
        )
        return 0

    lax.fori_loop(0, tokens // NTILE, chunk, 0)

    def cols(j, _):
        ds = pl.ds(pl.multiple_of(j * 256, 256), 256)
        out_ref[:, ds] = dot_nn(dl_ref[...], h_ref[:, ds]).astype(bf16)
        return 0

    lax.fori_loop(0, h_ref.shape[1] // 256, cols, 0)


def head_table(hidden, kept, fac, weight, labels, vocab_rows):
    tokens, width = hidden.shape
    tiles = pl.cdiv(vocab_rows, VTILE)
    sp = head_specs(width, tokens)
    return pl.pallas_call(
        head_table_kernel,
        name="head_table",
        grid=(tiles,),
        in_specs=[
            pl.BlockSpec((tokens, width), lambda i: (0, 0)),
            sp["kept"],
            sp["tile_row"],
            sp["row"],
            sp["row"],
        ],
        out_specs=sp["table"],
        out_shape=jax.ShapeDtypeStruct((vocab_rows, width), bf16),
        scratch_shapes=[pltpu.VMEM((VTILE, tokens), bf16)],
        compiler_params=head_params(),
        cost_estimate=pl.CostEstimate(
            flops=2 * vocab_rows * width * tokens,
            transcendentals=0,
            bytes_accessed=2 * vocab_rows * (width + tokens),
        ),
    )(hidden, kept, fac, weight, labels)


def shift_chunks(block, distance):
    size = lax.axis_size("fsdp")
    route = [(i - 2 * distance, i) for i in range(size) if 0 <= i - 2 * distance < size]
    return lax.ppermute(block, "fsdp", route)


def after(value, earlier):
    return lax.optimization_barrier((value, earlier))[0]


def norm_scale(values):
    return lax.rsqrt(jnp.mean(values * values, axis=-1, keepdims=True) + epsilon)


def norm_back(grad, values, gain):
    scale = norm_scale(values)
    unit = values * scale
    inner = grad * gain
    back = scale * (inner - unit * jnp.mean(inner * unit, axis=-1, keepdims=True))
    return back, jnp.sum(grad * unit, axis=0)


def wide(row):
    return jnp.pad(row, (0, LANES - row.shape[0]))[None]


def layer_vectors(vector_params, layer_index):
    offset = layer_index * PER
    pieces = []
    for size in (CONV * XBC, XBC, HEADS, HEADS, HEADS, D, DI):
        pieces.append(vector_params[offset : offset + size])
        offset += size
    conv_w, conv_b, dt_bias, decay_log, skip, pre_gain, gate_gain = pieces
    return dict(
        conv_w=conv_w.reshape(CONV, XBC),
        conv_b=conv_b[None],
        dt_bias=wide(dt_bias),
        decay_log=wide(decay_log),
        skip=jnp.repeat(skip, HDIM)[None],
        pre_gain=pre_gain,
        gate_gain=gate_gain[None],
    )


def layer_forward(hidden, w_in, w_out, vec):
    rows = hidden.shape[0]
    normed = (hidden * norm_scale(hidden) * vec["pre_gain"]).astype(bf16)
    proj = jnp.dot(normed, w_in, preferred_element_type=f32)
    halo = shift_chunks(proj[rows - 8 :, DI : DI + XBC], 1)
    pre, y0, local, dt, cum = local_call(
        front_kernel,
        (proj, halo, vec["conv_w"], vec["conv_b"], vec["dt_bias"], vec["decay_log"], vec["skip"]),
        (
            ((rows, XBC), f32),
            ((rows, DI), f32),
            ((DI, NSTATE), f32),
            ((rows, LANES), f32),
            ((rows, LANES), f32),
        ),
        scratch=(
            pltpu.VMEM((rows + 8, XBC), f32),
            pltpu.VMEM((HEADS, rows, LANES), f32),
            pltpu.VMEM((PAIRS, rows, LANES), f32),
            pltpu.VMEM((PAIRS, rows, LANES), f32),
            pltpu.VMEM((LANES, rows), f32),
        ),
    )
    decay = jnp.exp(cum[rows - 1, :HEADS])
    entering = carry_chain(decay, local, 1)
    y, mixed = local_call(
        gate_kernel,
        (y0, proj, pre, cum, entering, vec["gate_gain"]),
        (((rows, DI), f32), ((rows, DI), bf16)),
        scratch=(pltpu.VMEM((PAIRS, rows, LANES), f32),),
    )
    branch = jnp.dot(mixed, w_out, preferred_element_type=f32)
    record = (hidden, normed, proj, halo, pre, dt, cum, decay, entering, y, mixed)
    return hidden + branch, record


def layer_backward(grad_hidden, w_in, w_out, vec, record):
    hidden, normed, proj, halo, pre, dt, cum, decay, entering, y, mixed = record
    rows = hidden.shape[0]
    grad_branch = grad_hidden.astype(bf16)
    grad_mixed = dot_nt(grad_branch, w_out)
    dy, dz, dgate, gstate = local_call(
        ungate_kernel,
        (grad_mixed, y, proj, pre, cum, vec["gate_gain"]),
        (
            ((rows, DI), f32),
            ((rows, DI), bf16),
            ((1, DI), f32),
            ((DI, NSTATE), f32),
        ),
        scratch=(pltpu.VMEM((PAIRS, rows, LANES), f32),),
    )
    later = carry_chain(decay, gstate, -1)
    grad_out = dot_tn(mixed, grad_branch).astype(bf16)
    dx, dhalo, ddr, dconv, dsmall = local_call(
        back_kernel,
        (
            dy, y, proj, halo, pre, dt, cum, entering, later,
            vec["conv_w"], vec["dt_bias"], vec["decay_log"], vec["skip"],
        ),
        (
            ((rows, XBC), f32),
            ((8, XBC), f32),
            ((rows, LANES), f32),
            ((8, XBC), f32),
            ((8, LANES), f32),
        ),
        scratch=(
            pltpu.VMEM((rows + 8, XBC), f32),
            pltpu.VMEM((rows + 16, XBC), f32),
            pltpu.VMEM((HEADS, rows, LANES), f32),
            pltpu.VMEM((PAIRS, rows, LANES), f32),
            pltpu.VMEM((PAIRS, rows, LANES), f32),
            pltpu.VMEM((LANES, rows), f32),
            pltpu.VMEM((rows, rows), f32),
            pltpu.VMEM((rows, LANES), f32),
            pltpu.VMEM((rows, LANES), f32),
            pltpu.VMEM((rows, LANES), f32),
            pltpu.VMEM((rows, LANES), f32),
            pltpu.VMEM((16, LANES), f32),
        ),
    )
    from_next = shift_chunks(dhalo, -1)
    dx = jnp.concatenate([dx[: rows - 8], dx[rows - 8 :] + from_next], axis=0)
    grad_proj = jnp.concatenate(
        [dz, dx.astype(bf16), ddr[:, :HEADS].astype(bf16)], axis=1
    )
    grad_normed = dot_nt(grad_proj, w_in)
    grad_in = dot_tn(normed, grad_proj).astype(bf16)
    grad_prev, dpre_gain = norm_back(grad_normed, hidden, vec["pre_gain"])
    grad_vec = jnp.concatenate(
        [
            dconv[:CONV].reshape(-1),
            dconv[CONV],
            dsmall[0, :HEADS],
            dsmall[1, :HEADS],
            jnp.sum(dsmall[2:3, :HEADS], axis=0),
            dpre_gain,
            dgate[0],
        ]
    )
    return grad_hidden + grad_prev, grad_in, grad_out, grad_vec


def advance(weight, moment, average, grad, factor):
    scaled = grad * factor
    moment_new = 0.5 * moment + scaled
    weight_new = weight - step_rate * (scaled + 0.5 * moment_new)
    average_new = 0.5 * average + 0.5 * weight_new
    return (weight_new, moment_new, average_new, weight_new.astype(bf16))


def whole_step(
    token_ids,
    target_ids,
    seq_lengths,
    embedding,
    embedding_mom,
    embedding_avg,
    in_proj,
    in_proj_mom,
    in_proj_avg,
    out_proj,
    out_proj_mom,
    out_proj_avg,
    vector_params,
    vector_mom,
    vector_avg,
):
    groups = lax.axis_size("dp")
    shards = lax.axis_size("fsdp")
    group_index = lax.axis_index("dp")
    shard_index = lax.axis_index("fsdp")
    chunks = shards // MB
    seq_rows = token_ids.shape[2]
    rows = seq_rows // chunks
    vocab_rows, own_cols = embedding.shape
    tokens = MB * seq_rows
    total_count = jnp.sum(seq_lengths).astype(f32)
    embed_low = embedding.astype(bf16)
    in_low = in_proj.astype(bf16)
    out_low = out_proj.astype(bf16)

    ids_all = lax.all_gather(token_ids[:, 0, :], "dp", axis=0)
    ids_all = ids_all.reshape(groups, MB, chunks, rows).transpose(2, 1, 0, 3).reshape(-1)
    every = ids_all.shape[0]
    local_ids = ids_all - shard_index * vocab_rows
    inside = (local_ids >= 0) & (local_ids < vocab_rows)
    sorted_ids, sorted_tok = lax.sort(
        (jnp.where(inside, local_ids, vocab_rows), jnp.arange(every, dtype=jnp.int32)),
        num_keys=1,
    )
    held_here = sorted_ids < vocab_rows
    count = jnp.sum(held_here.astype(jnp.int32)).reshape(1)
    row_list = jnp.where(held_here, sorted_ids, 0)
    tok_list = jnp.where(held_here, sorted_tok, every)
    (looked,) = local_call(
        lookup_kernel,
        (count, row_list, tok_list, embedding),
        (((every, own_cols), bf16),),
        scratch=(pltpu.VMEM((every + 8, own_cols), f32),),
        in_smem=(0, 1, 2),
    )
    mine = lax.psum_scatter(
        looked.reshape(shards * groups * rows, own_cols), "fsdp", scatter_dimension=0, tiled=True
    )
    mine = lax.all_to_all(mine.reshape(groups, rows, own_cols), "dp", 0, 0)
    hidden = mine.transpose(1, 0, 2).reshape(rows, D).astype(f32)

    shards = []
    for l in range(LAYERS):
        shards += [in_low[l], out_low[l]]
    shards = after(shards, looked)
    gathered = gather_layers(shards)
    w_in, w_out = gathered[0::2], gathered[1::2]
    embed_low = after(embed_low, gathered)
    table = lax.all_gather(embed_low, "dp", axis=1, tiled=True)

    vecs = [layer_vectors(vector_params, l) for l in range(LAYERS)]
    final_gain = vector_params[LAYERS * PER :]
    records = []
    for l in range(LAYERS):
        hidden, record = layer_forward(hidden, w_in[l], w_out[l], vecs[l])
        records.append(record)

    final_low = (hidden * norm_scale(hidden) * final_gain).astype(bf16)
    group_hidden = lax.all_gather(final_low, "fsdp", axis=0, tiled=True)

    def in_order(per_seq):
        return per_seq.reshape(MB, chunks, rows).transpose(1, 0, 2).reshape(1, tokens)

    labels = in_order(target_ids[:, 0, :])
    lengths = lax.dynamic_index_in_dim(seq_lengths, group_index, 1, keepdims=True)
    valid = in_order((jnp.arange(seq_rows)[None, :] < lengths).astype(f32))
    local_labels = labels - shard_index * vocab_rows
    kept, tile_stats = head_stats(table, group_hidden.T, local_labels)
    top = jnp.max(tile_stats[:, 0], axis=0)
    summed = jnp.sum(tile_stats[:, 1] * jnp.exp(tile_stats[:, 0] - top), axis=0)
    stats = jnp.stack(
        [top, summed, jnp.sum(tile_stats[:, 2], axis=0), jnp.sum(tile_stats[:, 3], axis=0)]
    )
    stats = lax.all_gather(stats, "fsdp", axis=0)
    row_top = jnp.max(stats[:, 0], axis=0)
    expsum = jnp.sum(stats[:, 1] * jnp.exp(stats[:, 0] - row_top), axis=0)
    target = jnp.sum(stats[:, 2], axis=0)
    logit_sum = jnp.sum(stats[:, 3], axis=0)
    log_total = row_top + jnp.log(expsum)
    per_row = log_total - 0.9 * target - 0.1 * logit_sum / VOCAB + z_weight * log_total * log_total
    own_mask = jnp.arange(tokens) // rows == shard_index
    loss_sum = jnp.sum(jnp.where(own_mask, per_row * valid[0], 0.0))
    weight = valid / total_count
    scale = weight[0] * (1.0 + 2.0 * z_weight * log_total)
    fac = (scale * jnp.exp(tile_stats[:, 0] - log_total))[:, None, :]

    rows_grad = head_rows(table, kept, fac, weight, local_labels)
    own_grad = lax.psum_scatter(
        rows_grad.T.astype(bf16), "fsdp", scatter_dimension=0, tiled=True
    ).astype(f32)
    table_grad = head_table(group_hidden, kept, fac, weight, local_labels, vocab_rows)
    table_part = lax.psum_scatter(table_grad, "dp", scatter_dimension=1, tiled=True)

    grad_hidden, dfinal = norm_back(after(own_grad, table_grad), hidden, final_gain)
    in_parts = [None] * LAYERS
    out_parts = [None] * LAYERS
    vec_parts = [None] * LAYERS
    for l in reversed(range(LAYERS)):
        grad_hidden, grad_in, grad_out, vec_parts[l] = layer_backward(
            grad_hidden, w_in[l], w_out[l], vecs[l], records[l]
        )
        if l == 0:
            sent = grad_hidden.astype(bf16).reshape(rows, groups, own_cols).transpose(1, 0, 2)
            sent = lax.all_to_all(sent, "dp", 0, 0)
            spread = lax.all_gather(sent, "fsdp", axis=0).reshape(every, own_cols)
        in_parts[l], out_parts[l] = grad_in, grad_out
    whole = []
    for l in range(LAYERS):
        whole += [in_parts[l], out_parts[l]]
    summed_parts = reduce_layers(whole)
    spread = after(spread, summed_parts)
    (table_total,) = local_call(
        spread_kernel,
        (count, row_list, tok_list, spread, table_part),
        (((vocab_rows, own_cols), f32),),
        scratch=(pltpu.VMEM((every + 8, own_cols), f32),),
        in_smem=(0, 1, 2),
    )
    grad_in_all = jnp.stack(summed_parts[0::2])
    grad_out_all = jnp.stack(summed_parts[1::2])
    owner_squares = (
        jnp.sum(grad_in_all * grad_in_all)
        + jnp.sum(grad_out_all * grad_out_all)
        + jnp.sum(table_total * table_total)
    )
    small = vector_params.shape[0]
    padded = pl.cdiv(small + 2, 16 * LANES) * 16 * LANES
    packed = jnp.concatenate(
        vec_parts
        + [
            dfinal,
            owner_squares.reshape(1),
            loss_sum.reshape(1),
            jnp.zeros((padded - small - 2,), f32),
        ]
    )
    packed = total_of(packed.reshape(-1, LANES)).reshape(-1)
    vector_total = packed[:small]
    squares_total, loss_total = packed[small], packed[small + 1]
    grad_norm = jnp.sqrt(squares_total + jnp.sum(vector_total * vector_total))
    factor = jnp.minimum(1.0, clip_limit / grad_norm)
    loss_value = loss_total / total_count
    return (
        loss_value,
        grad_norm,
        *advance(embedding, embedding_mom, embedding_avg, table_total, factor),
        *advance(in_proj, in_proj_mom, in_proj_avg, grad_in_all, factor),
        *advance(out_proj, out_proj_mom, out_proj_avg, grad_out_all, factor),
        *advance(vector_params, vector_mom, vector_avg, vector_total, factor),
    )


def solution(mesh):
    table_spec = P("fsdp", "dp")
    weight_spec = P(None, ("dp", "fsdp"), None)
    return jax.shard_map(
        whole_step,
        mesh=mesh,
        in_specs=(
            P(None, "dp", None),
            P(None, "dp", None),
            P(),
            *(table_spec,) * 3,
            *(weight_spec,) * 6,
            *(P(),) * 3,
        ),
        out_specs=(
            P(),
            P(),
            *(table_spec,) * 4,
            *(weight_spec,) * 8,
            *(P(),) * 4,
        ),
        check_vma=False,
    )
```

```python
import functools

import jax
import jax.numpy as jnp
from jax import lax
from jax.experimental import pallas as pl
from jax.experimental.pallas import tpu as pltpu
from jax.sharding import PartitionSpec as P


D = 1024
HEADS = 32
HDIM = 64
NSTATE = 128
CONV = 4
VOCAB = 50288
LAYERS = 2
MB = 2
DI = 2048
XBC = 2304
ZW = 4384
PER = 14688
LANES = 128
PAIRS = DI // LANES

epsilon = 1e-05
z_weight = 0.001
clip_limit = 0.2
step_rate = 1000.0
highest = lax.Precision.HIGHEST
bf16 = jnp.bfloat16
f32 = jnp.float32
VMEM_LIMIT = 62 * 1024 * 1024
OFF = -1e30


def dot_nn(a, b, precision=None):
    return lax.dot_general(
        a, b, (((1,), (0,)), ((), ())), precision=precision, preferred_element_type=f32
    )


def dot_nt(a, b, precision=None):
    return lax.dot_general(
        a, b, (((1,), (1,)), ((), ())), precision=precision, preferred_element_type=f32
    )


def dot_tn(a, b, precision=None):
    return lax.dot_general(
        a, b, (((0,), (0,)), ((), ())), precision=precision, preferred_element_type=f32
    )


def silu(v):
    return v * lax.logistic(v)


def silu_grad(v):
    s = lax.logistic(v)
    return s * (1.0 + v * (1.0 - s))


def local_call(kernel, ins, outs, scratch=(), in_smem=(), flops=0):
    total = sum(a.size * a.dtype.itemsize for a in ins)
    return pl.pallas_call(
        kernel,
        out_shape=[jax.ShapeDtypeStruct(shape, kind) for shape, kind in outs],
        in_specs=[
            pl.BlockSpec(memory_space=pltpu.SMEM if i in in_smem else pltpu.VMEM)
            for i in range(len(ins))
        ],
        out_specs=[pl.BlockSpec(memory_space=pltpu.VMEM) for _ in outs],
        scratch_shapes=list(scratch),
        compiler_params=pltpu.CompilerParams(vmem_limit_bytes=VMEM_LIMIT),
        cost_estimate=pl.CostEstimate(
            flops=flops or total, transcendentals=0, bytes_accessed=2 * total
        ),
    )(*ins)


def lookup_kernel(count_ref, row_ref, tok_ref, table_ref, out_ref, held):
    tokens = out_ref.shape[0]
    step = 512

    def clear(i, _):
        held[pl.ds(pl.multiple_of(i * step, step), step), :] = jnp.zeros(
            (step, held.shape[1]), f32
        )
        return 0

    lax.fori_loop(0, tokens // step, clear, 0)

    def move(i, _):
        for k in range(8):
            row = row_ref[i * 8 + k]
            tok = tok_ref[i * 8 + k]
            held[pl.ds(tok, 1), :] = table_ref[pl.ds(row, 1), :]
        return 0

    lax.fori_loop(0, (count_ref[0] + 7) // 8, move, 0)

    def put(i, _):
        rows = pl.ds(pl.multiple_of(i * step, step), step)
        out_ref[rows, :] = held[rows, :].astype(bf16)
        return 0

    lax.fori_loop(0, tokens // step, put, 0)


def spread_kernel(count_ref, row_ref, tok_ref, grad_ref, base_ref, out_ref, square_ref, held):
    tokens = grad_ref.shape[0]
    step = 512
    rows_all = out_ref.shape[0]

    def take(i, _):
        rows = pl.ds(pl.multiple_of(i * step, step), step)
        held[rows, :] = grad_ref[rows, :].astype(f32)
        return 0

    lax.fori_loop(0, tokens // step, take, 0)
    held[pl.ds(tokens, 8), :] = jnp.zeros((8, held.shape[1]), f32)

    whole = rows_all // step

    def start(i, _):
        rows = pl.ds(pl.multiple_of(i * step, step), step)
        out_ref[rows, :] = base_ref[rows, :].astype(f32)
        return 0

    lax.fori_loop(0, whole, start, 0)
    if rows_all > whole * step:
        out_ref[whole * step :, :] = base_ref[whole * step :, :].astype(f32)

    def move(i, _):
        for k in range(8):
            row = row_ref[i * 8 + k]
            tok = tok_ref[i * 8 + k]
            out_ref[pl.ds(row, 1), :] = out_ref[pl.ds(row, 1), :] + held[pl.ds(tok, 1), :]
        return 0

    lax.fori_loop(0, (count_ref[0] + 7) // 8, move, 0)

    def square(i, total):
        part = out_ref[pl.ds(pl.multiple_of(i * step, step), step), :]
        return total + jnp.sum((part * part).reshape(step // 8, 8, -1), axis=0)

    total = lax.fori_loop(0, whole, square, jnp.zeros(square_ref.shape, f32))
    square_ref[...] = total
    if rows_all > whole * step:
        part = out_ref[whole * step :, :]
        square_ref[0:1, :] += jnp.sum(part * part, axis=0, keepdims=True)


MESH = pl.DeviceIdType.MESH


def remote(src, dst, send, recv, dp, fsdp):
    return pltpu.make_async_remote_copy(
        src_ref=src,
        dst_ref=dst,
        send_sem=send,
        recv_sem=recv,
        device_id=(dp, fsdp),
        device_id_type=MESH,
    )


def comm_call(kernel, number, ins, outs, scratch, in_spaces, out_spaces, sent):
    return pl.pallas_call(
        kernel,
        out_shape=[jax.ShapeDtypeStruct(shape, kind) for shape, kind in outs],
        in_specs=[pl.BlockSpec(memory_space=space) for space in in_spaces],
        out_specs=[pl.BlockSpec(memory_space=space) for space in out_spaces],
        scratch_shapes=list(scratch),
        compiler_params=pltpu.CompilerParams(
            collective_id=number, has_side_effects=True, vmem_limit_bytes=VMEM_LIMIT
        ),
        cost_estimate=pl.CostEstimate(flops=sent, transcendentals=0, bytes_accessed=2 * sent),
    )(*ins)


def chain_kernel(direction, steps, decay_ref, local_ref, out_ref, got, give, send, recv):
    dp = lax.axis_index("dp")
    me = lax.axis_index("fsdp")
    place = me // MB
    count = lax.axis_size("fsdp") // MB
    first = place == (0 if direction > 0 else count - 1)
    final = place == (count - 1 if direction > 0 else 0)
    part = DI // steps
    heads = part // HDIM
    barrier = pltpu.get_barrier_semaphore()

    @pl.when(jnp.logical_not(first))
    def _():
        pl.semaphore_signal(
            barrier, inc=1, device_id=(dp, me - MB * direction), device_id_type=MESH
        )

    @pl.when(jnp.logical_not(final))
    def _():
        pl.semaphore_wait(barrier, 1)

    @pl.when(first)
    def _():
        got[...] = jnp.zeros(got.shape, bf16)

    def copy(g):
        rows = pl.ds(g * part, part)
        return remote(
            give.at[rows], got.at[rows], send.at[g], recv.at[g], dp, me + MB * direction
        )

    for g in range(steps):
        rows = pl.ds(g * part, part)

        @pl.when(jnp.logical_not(first))
        def _():
            copy(g).wait_recv()

        @pl.when(jnp.logical_not(final))
        def _():
            for i in range(heads):
                h = pl.ds(g * part + i * HDIM, HDIM)
                give[h, :] = (
                    decay_ref[g * heads + i] * got[h, :].astype(f32) + local_ref[h, :]
                ).astype(bf16)
            copy(g).start()

        out_ref[rows, :] = got[rows, :]

    @pl.when(jnp.logical_not(final))
    def _():
        for g in range(steps):
            copy(g).wait_send()


CHAIN_STEPS = 8


def carry_chain(decay, local, direction):
    return comm_call(
        functools.partial(chain_kernel, direction, CHAIN_STEPS),
        1 if direction > 0 else 2,
        (decay, local),
        ((local.shape, bf16),),
        (
            pltpu.VMEM(local.shape, bf16),
            pltpu.VMEM(local.shape, bf16),
            pltpu.SemaphoreType.DMA((CHAIN_STEPS,)),
            pltpu.SemaphoreType.DMA((CHAIN_STEPS,)),
        ),
        (pltpu.SMEM, pltpu.VMEM),
        (pltpu.VMEM,),
        local.size * 2,
    )[0]


def bits_of(size):
    return [1 << b for b in range(size.bit_length() - 1)]


def total_kernel(in_ref, out_ref, work, got, send, recv):
    dp = lax.axis_index("dp")
    me = lax.axis_index("fsdp")
    half = in_ref.shape[0] // 2
    core = me % MB
    partners = [("f", b) for b in bits_of(lax.axis_size("fsdp")) if b > 1]
    partners += [("d", b) for b in bits_of(lax.axis_size("dp"))]

    def across(kind, bit):
        ids, other = (me, lambda v: (dp, v)) if kind == "f" else (dp, lambda v: (v, me))
        return other(jnp.where((ids // bit) % 2 == 1, ids - bit, ids + bit))

    mate = across("f", 1)
    barrier = pltpu.get_barrier_semaphore()
    for target in [mate] + [across(*p) for p in partners]:
        pl.semaphore_signal(barrier, inc=1, device_id=target, device_id_type=MESH)
    pl.semaphore_wait(barrier, 1 + len(partners))

    mine = pl.ds(pl.multiple_of(core * half, 8), half)
    theirs = pl.ds(pl.multiple_of((1 - core) * half, 8), half)
    copy = remote(in_ref.at[theirs], got.at[0], send.at[0], recv.at[0], *mate)
    copy.start()
    copy.wait()
    work[0] = in_ref[mine, :] + got[0]
    for i, p in enumerate(partners):
        copy = remote(work.at[i], got.at[i + 1], send.at[i + 1], recv.at[i + 1], *across(*p))
        copy.start()
        copy.wait()
        work[i + 1] = work[i] + got[i + 1]
    n = len(partners)
    copy = remote(work.at[n], got.at[n + 1], send.at[n + 1], recv.at[n + 1], *mate)
    copy.start()
    copy.wait()
    out_ref[mine, :] = work[n]
    out_ref[theirs, :] = got[n + 1]


def total_of(array):
    rows = array.shape[0]
    steps = len(bits_of(lax.axis_size("fsdp"))) - 1 + len(bits_of(lax.axis_size("dp")))
    return comm_call(
        total_kernel,
        3,
        (array,),
        ((array.shape, f32),),
        (
            pltpu.VMEM((steps + 1, rows // 2, LANES), f32),
            pltpu.VMEM((steps + 2, rows // 2, LANES), f32),
            pltpu.SemaphoreType.DMA((steps + 2,)),
            pltpu.SemaphoreType.DMA((steps + 2,)),
        ),
        (pltpu.VMEM,),
        (pltpu.VMEM,),
        array.size * 4 * 3,
    )[0]


def snake(place, size):
    return jnp.where(place < size // 2, place, size // 2 + size - 1 - place)


def wrap(value, size):
    return lax.rem(value + size, size)


def gather_kernel(*refs):
    arrays = 2 * LAYERS
    own = refs[:arrays]
    full = refs[arrays : 2 * arrays]
    local_sem, z_send, z_recv, ring_send, ring_recv, mate_send, mate_recv = refs[2 * arrays :]
    dp = lax.axis_index("dp")
    me = lax.axis_index("fsdp")
    size = lax.axis_size("dp")
    count = lax.axis_size("fsdp") // MB
    core = me % MB
    k = me // MB
    ring = snake(dp, size)
    reach = size // 2
    right = snake(wrap(ring + 1, size), size)
    left = snake(wrap(ring - 1, size), size)
    mate = k * MB + 1 - core
    up, down = me + MB, me - MB
    has_up, has_down = k < count - 1, k > 0
    barrier = pltpu.get_barrier_semaphore()
    for target in ((right, me), (left, me), (dp, mate)):
        pl.semaphore_signal(barrier, inc=1, device_id=target, device_id_type=MESH)

    @pl.when(has_up)
    def _():
        pl.semaphore_signal(barrier, inc=1, device_id=(dp, up), device_id_type=MESH)

    @pl.when(has_down)
    def _():
        pl.semaphore_signal(barrier, inc=1, device_id=(dp, down), device_id_type=MESH)

    pl.semaphore_wait(barrier, 3 + jnp.where(has_up, 1, 0) + jnp.where(has_down, 1, 0))

    def spot(a, d, z, c):
        return full[a].at[d, z, c]

    def chain(a, src, z, side):
        return remote(
            src, spot(a, dp, z, core), z_send.at[a, z], z_recv.at[a, z], dp, up if side == 0 else down
        )

    def chain_own(a, side):
        return remote(
            own[a],
            spot(a, dp, k, core),
            z_send.at[a, count + side],
            z_recv.at[a, k],
            dp,
            up if side == 0 else down,
        )

    def round_ring(a, src, d, z, side):
        return remote(
            src,
            spot(a, d, z, core),
            ring_send.at[a, side],
            ring_recv.at[a, d, z],
            right if side == 0 else left,
            me,
        )

    def to_mate(a, src, d, z):
        return remote(src, spot(a, d, z, core), mate_send.at[a], mate_recv.at[a], dp, mate)

    def carried(a, side):
        return (a < arrays // 2) == (side == 0)

    for a in range(arrays):

        @pl.when(has_up)
        def _(a=a):
            chain_own(a, 0).start()

        @pl.when(has_down)
        def _(a=a):
            chain_own(a, 1).start()

    for a in range(arrays):
        for side in (0, 1):
            round_ring(a, own[a], dp, k, side).start()
    for a in range(arrays):
        to_mate(a, own[a], dp, k).start()
        pltpu.make_async_copy(own[a], spot(a, dp, k, core), local_sem.at[a]).start()

    def ring_step(z, s):
        for side in (0, 1):
            origin = snake(wrap(ring - s if side == 0 else ring + s, size), size)
            for a in range(arrays):
                if s == reach and not carried(a, side):
                    continue
                piece = spot(a, origin, z, core)
                round_ring(a, piece, origin, z, side).wait_recv()
                if s + 1 < reach or (s + 1 == reach and carried(a, side)):
                    round_ring(a, piece, origin, z, side).start()
                to_mate(a, piece, origin, z).start()

    def arrive(z, side):
        for a in range(arrays):
            piece = spot(a, dp, z, core)
            chain(a, piece, z, side).wait_recv()

            @pl.when(has_up if side == 0 else has_down)
            def _(a=a, piece=piece):
                chain(a, piece, z, side).start()

            for way in (0, 1):
                round_ring(a, piece, dp, z, way).start()
            to_mate(a, piece, dp, z).start()

    def both_ways(far, act):
        if far == 0:
            act(k, 0)
            return

        @pl.when(k >= far)
        def _():
            act(k - far, 0)

        @pl.when(k + far < count)
        def _():
            act(k + far, 1)

    for turn in range(1, count + reach):
        if turn < count:
            both_ways(turn, arrive)
        for s in range(1, reach + 1):
            if 0 <= turn - s < count:
                both_ways(turn - s, lambda z, side, s=s: ring_step(z, s))

    for a in range(arrays):
        pltpu.make_async_copy(own[a], spot(a, dp, k, core), local_sem.at[a]).wait()
        for side in (0, 1):
            sent = full[a].at[pl.ds(0, reach if carried(a, side) else reach - 1), :, core]
            remote(sent, sent, ring_send.at[a, side], ring_recv.at[a, 0, 0], dp, mate).wait_send()
        whole = full[a].at[:, :, core]
        remote(whole, whole, mate_send.at[a], mate_recv.at[a], dp, mate).wait_send()
        whole = full[a].at[:, :, 1 - core]
        remote(whole, whole, mate_send.at[a], mate_recv.at[a], dp, mate).wait_recv()

        @pl.when(has_up)
        def _(a=a):
            chain_own(a, 0).wait_send()

        @pl.when(has_down)
        def _(a=a):
            chain_own(a, 1).wait_send()

        for far in range(1, count):

            @pl.when(jnp.logical_and(k >= far, has_up))
            def _(a=a, far=far):
                chain(a, spot(a, dp, k - far, core), k - far, 0).wait_send()

            @pl.when(jnp.logical_and(k + far < count, has_down))
            def _(a=a, far=far):
                chain(a, spot(a, dp, k + far, core), k + far, 1).wait_send()


def gather_layers(shards):
    size, count = lax.axis_size("dp"), lax.axis_size("fsdp") // MB
    arrays = len(shards)
    outs = comm_call(
        gather_kernel,
        4,
        shards,
        tuple(((size, count, MB) + s.shape, bf16) for s in shards),
        (
            pltpu.SemaphoreType.DMA((arrays,)),
            pltpu.SemaphoreType.DMA((arrays, count + 2)),
            pltpu.SemaphoreType.DMA((arrays, count)),
            pltpu.SemaphoreType.DMA((arrays, 2)),
            pltpu.SemaphoreType.DMA((arrays, size, count)),
            pltpu.SemaphoreType.DMA((arrays,)),
            pltpu.SemaphoreType.DMA((arrays,)),
        ),
        (pltpu.VMEM,) * arrays,
        (pl.ANY,) * arrays,
        sum(s.size * 2 for s in shards) * 24,
    )
    return [o.reshape(size * count * MB * s.shape[0], s.shape[1]) for o, s in zip(outs, shards)]


def add_rows(dst, first, *others):
    rows = dst.shape[0]
    step = min(rows, 16)

    def one(i, _):
        at = pl.ds(pl.multiple_of(i * step, step), step)
        total = first[at, :].astype(f32)
        for other in others:
            total = total + other[at, :].astype(f32)
        dst[at, :] = total.astype(dst.dtype)
        return 0

    lax.fori_loop(0, rows // step, one, 0)


def reduce_kernel(*refs):
    arrays = 2 * LAYERS
    grads = refs[:arrays]
    outs = refs[arrays : 2 * arrays]
    held, given, come, chained = (
        refs[(2 + i) * arrays : (3 + i) * arrays] for i in range(4)
    )
    load_sem, mate_send, mate_recv, ring_send, ring_recv, z_send, z_recv = refs[6 * arrays :]
    dp = lax.axis_index("dp")
    me = lax.axis_index("fsdp")
    size = lax.axis_size("dp")
    count = lax.axis_size("fsdp") // MB
    core = me % MB
    k = me // MB
    ring = snake(dp, size)
    reach = size // 2
    right = snake(wrap(ring + 1, size), size)
    left = snake(wrap(ring - 1, size), size)
    mate = k * MB + 1 - core
    up, down = me + MB, me - MB
    has_up, has_down = k < count - 1, k > 0

    def load(a):
        return pltpu.make_async_copy(grads[a].at[:, :, core], held[a], load_sem.at[a])

    for a in range(arrays):
        load(a).start()
    barrier = pltpu.get_barrier_semaphore()
    for target in ((right, me), (left, me), (dp, mate)):
        pl.semaphore_signal(barrier, inc=1, device_id=target, device_id_type=MESH)

    @pl.when(has_up)
    def _():
        pl.semaphore_signal(barrier, inc=1, device_id=(dp, up), device_id_type=MESH)

    @pl.when(has_down)
    def _():
        pl.semaphore_signal(barrier, inc=1, device_id=(dp, down), device_id_type=MESH)

    pl.semaphore_wait(barrier, 3 + jnp.where(has_up, 1, 0) + jnp.where(has_down, 1, 0))

    def away(j, side):
        return snake(wrap(ring + j if side == 0 else ring - j, size), size)

    def to_mate(a, d):
        return remote(
            grads[a].at[d, :, 1 - core], given[a].at[d], mate_send.at[a], mate_recv.at[a, d], dp, mate
        )

    def carried(a, side):
        return (a < arrays // 2) == (side == 0)

    def targets(j):
        if j == 0:
            return [dp]
        if j == reach:
            return [away(j, 0)]
        return [away(j, 0), away(j, 1)]

    for j in range(reach, -1, -1):
        for d in targets(j):
            for a in range(arrays):
                to_mate(a, d).start()

    for a in range(arrays):
        load(a).wait()

    def add_mate(d):
        for a in range(arrays):
            to_mate(a, d).wait_recv()

            def one(z, _, a=a):
                add_rows(held[a].at[d, z], held[a].at[d, z], given[a].at[d, z])
                return 0

            lax.fori_loop(0, count, one, 0)

    def first_step(a, side):
        d = away(reach, 0)
        return remote(
            held[a].at[d], come[a].at[side, 0], ring_send.at[a, side], ring_recv.at[a, side, 0, 0],
            right if side == 0 else left, me,
        )

    def next_step(a, side, s, z):
        d = away(reach - s, side)
        return remote(
            held[a].at[d, z], come[a].at[side, s, z], ring_send.at[a, side],
            ring_recv.at[a, side, s, z], right if side == 0 else left, me,
        )

    far_most = jnp.maximum(k, count - 1 - k)
    near_most = jnp.minimum(k, count - 1 - k)
    uneven = far_most - near_most
    long_side = jnp.where(count - 1 - k > k, 1, -1)

    def chunk_at(i):
        j = jnp.maximum(i - uneven, 0)
        paired = k + (1 - 2 * (j % 2)) * (near_most - j // 2)
        return jnp.where(i < uneven, k + long_side * (far_most - i), paired)

    add_mate(away(reach, 0))
    for a in range(arrays):
        first_step(a, 0 if carried(a, 0) else 1).start()
    for s in range(1, reach):
        for side in (0, 1):
            add_mate(away(reach - s, side))
        if s == 1:
            for a in range(arrays):
                first_step(a, 0 if carried(a, 0) else 1).wait_recv()

        def pass_on(i, _, s=s):
            z = chunk_at(i)
            for side in (0, 1):
                d = away(reach - s, side)
                for a in range(arrays):
                    if s > 1:
                        next_step(a, side, s - 1, z).wait_recv()
                    if s > 1 or carried(a, side):
                        add_rows(held[a].at[d, z], held[a].at[d, z], come[a].at[side, s - 1, z])
                    next_step(a, side, s, z).start()
            return 0

        lax.fori_loop(0, count, pass_on, 0)
    add_mate(dp)

    def along(a, side, z):
        return remote(
            held[a].at[dp, z], chained[a].at[side, z], z_send.at[a, z], z_recv.at[a, side, z],
            dp, up if side == 0 else down,
        )

    def finish(i, _):
        z = chunk_at(i)
        for a in range(arrays):
            for side in (0, 1):
                next_step(a, side, reach - 1, z).wait_recv()
            add_rows(
                held[a].at[dp, z],
                held[a].at[dp, z],
                come[a].at[0, reach - 1, z],
                come[a].at[1, reach - 1, z],
            )
            for side in (0, 1):
                beyond = z > k if side == 0 else z < k
                fed = has_down if side == 0 else has_up

                @pl.when(jnp.logical_and(fed, jnp.logical_or(beyond, z == k)))
                def _(a=a, side=side):
                    along(a, side, z).wait_recv()
                    add_rows(held[a].at[dp, z], held[a].at[dp, z], chained[a].at[side, z])

                @pl.when(beyond)
                def _(a=a, side=side):
                    along(a, side, z).start()

        return 0

    lax.fori_loop(0, count, finish, 0)
    for a in range(arrays):
        add_rows(outs[a], held[a].at[dp, k])
        for side in (0, 1):
            sent = held[a].at[pl.ds(0, reach if carried(a, side) else reach - 1)]
            remote(
                sent, sent, ring_send.at[a, side], ring_recv.at[a, side, 0, 0], dp, mate
            ).wait_send()
        remote(
            given[a], given[a], mate_send.at[a], mate_recv.at[a, 0], dp, mate
        ).wait_send()

    def sent_along(z, _):
        for a in range(arrays):

            @pl.when(z != k)
            def _(a=a):
                along(a, 0, z).wait_send()

        return 0

    lax.fori_loop(0, count, sent_along, 0)


def reduce_layers(grads):
    size, count = lax.axis_size("dp"), lax.axis_size("fsdp") // MB
    arrays = len(grads)
    reach = size // 2
    shards = [(g.shape[0] // (size * count * MB), g.shape[1]) for g in grads]
    blocks = [g.reshape((size, count, MB) + s) for g, s in zip(grads, shards)]
    return comm_call(
        reduce_kernel,
        5,
        blocks,
        tuple((s, f32) for s in shards),
        tuple(pltpu.VMEM((size, count) + s, bf16) for s in shards) * 2
        + tuple(pltpu.VMEM((2, reach, count) + s, bf16) for s in shards)
        + tuple(pltpu.VMEM((2, count) + s, bf16) for s in shards)
        + (
            pltpu.SemaphoreType.DMA((arrays,)),
            pltpu.SemaphoreType.DMA((arrays,)),
            pltpu.SemaphoreType.DMA((arrays, size)),
            pltpu.SemaphoreType.DMA((arrays, 2)),
            pltpu.SemaphoreType.DMA((arrays, 2, reach, count)),
            pltpu.SemaphoreType.DMA((arrays, count)),
            pltpu.SemaphoreType.DMA((arrays, 2, count)),
        ),
        (pl.ANY,) * arrays,
        (pltpu.VMEM,) * arrays,
        sum(g.size * 2 for g in grads),
    )


def pair_lanes(p):
    return pl.ds(pl.multiple_of(p * LANES, LANES), LANES)


def first_half(rows):
    return lax.broadcasted_iota(jnp.int32, (rows, LANES), 1) < HDIM


def spread_columns(values, column, per_pair, rows):
    half = first_half(rows)
    for p in range(PAIRS):
        left = jnp.broadcast_to(values[:, 2 * p : 2 * p + 1], (rows, LANES))
        right = jnp.broadcast_to(values[:, 2 * p + 1 : 2 * p + 2], (rows, LANES))
        if column is not None:
            column[2 * p] = left
            column[2 * p + 1] = right
        if per_pair is not None:
            per_pair[p] = jnp.where(half, left, right)


def front_kernel(
    proj_ref, halo_ref, cw_ref, cb_ref, dtb_ref, al_ref, sk_ref,
    pre_ref, y_ref, st_ref, dt_ref, cum_ref,
    pad, col, tcol, lcol, lrow,
):
    rows = proj_ref.shape[0]
    pad[0:8, :] = halo_ref[...]
    pad[8:, :] = proj_ref[:, DI : DI + XBC]

    def conv(i, _):
        xs = pair_lanes(i)
        out = jnp.broadcast_to(cb_ref[0:1, xs], (rows, LANES))
        for k in range(CONV):
            out = out + cw_ref[k : k + 1, xs] * pad[5 + k : 5 + k + rows, xs]
        pre_ref[:, xs] = out
        return 0

    lax.fori_loop(0, XBC // LANES, conv, 0)

    dt_ref[...] = jnp.zeros((rows, LANES), f32)
    dt_ref[:, 0:HEADS] = proj_ref[:, DI + XBC :]
    drive = dt_ref[...] + dtb_ref[...]
    dt = jnp.maximum(drive, 0.0) + jnp.log1p(jnp.exp(-jnp.abs(drive)))
    dt_ref[...] = dt
    rate = dt * (-jnp.exp(al_ref[...]))
    ri = lax.broadcasted_iota(jnp.int32, (rows, rows), 0)
    ci = lax.broadcasted_iota(jnp.int32, (rows, rows), 1)
    causal = ri >= ci
    cum = dot_nn(jnp.where(causal, 1.0, 0.0), rate, highest)
    cum_ref[...] = cum
    lrow[...] = cum.T
    spread_columns(cum, col, lcol, rows)
    spread_columns(dt, None, tcol, rows)
    bm = silu(pre_ref[:, DI : DI + NSTATE]).astype(bf16)
    cm = silu(pre_ref[:, DI + NSTATE :]).astype(bf16)
    cb = dot_nt(cm, bm)
    half = first_half(rows)

    def pair(p, _):
        xs = pair_lanes(p)
        x = silu(pre_ref[:, xs])
        xt = tcol[p] * x
        xtb = xt.astype(bf16)
        parts = []
        for j in range(2):
            h = 2 * p + j
            c = col[h]
            d = jnp.concatenate([c] * (rows // LANES), axis=1) - lrow[pl.ds(h, 1), :]
            m = (jnp.exp(jnp.where(causal, d, OFF)) * cb).astype(bf16)
            parts.append(dot_nn(m, xtb))
        y_ref[:, xs] = jnp.where(half, parts[0], parts[1]) + sk_ref[0:1, xs] * x
        lp = lcol[p]
        tail = jnp.exp(lp[rows - 1 : rows, :] - lp)
        st_ref[xs, :] = dot_tn((tail * xt).astype(bf16), bm)
        return 0

    lax.fori_loop(0, PAIRS, pair, 0)


def gate_kernel(
    y0_ref, proj_ref, pre_ref, cum_ref, sin_ref, gg_ref, y_ref, yn_ref, lcol
):
    rows = y0_ref.shape[0]
    spread_columns(cum_ref[...], None, lcol, rows)
    cm = silu(pre_ref[:, DI + NSTATE :]).astype(bf16)

    def pair(p, total):
        xs = pair_lanes(p)
        y = y0_ref[:, xs] + jnp.exp(lcol[p]) * dot_nt(cm, sin_ref[xs, :])
        y_ref[:, xs] = y
        g = y * silu(proj_ref[:, xs])
        return total + g * g

    total = lax.fori_loop(0, PAIRS, pair, jnp.zeros((rows, LANES), f32))
    scale = lax.rsqrt(jnp.sum(total, axis=1, keepdims=True) / DI + epsilon)

    def put(p, _):
        xs = pair_lanes(p)
        g = y_ref[:, xs] * silu(proj_ref[:, xs])
        yn_ref[:, xs] = (g * scale * gg_ref[0:1, xs]).astype(bf16)
        return 0

    lax.fori_loop(0, PAIRS, put, 0)


def ungate_kernel(
    dyn_ref, y_ref, proj_ref, pre_ref, cum_ref, gg_ref,
    dy_ref, dz_ref, dgg_ref, gst_ref, lcol,
):
    rows = y_ref.shape[0]
    spread_columns(cum_ref[...], None, lcol, rows)
    cm = silu(pre_ref[:, DI + NSTATE :]).astype(bf16)
    zero = jnp.zeros((rows, LANES), f32)

    def sums(p, carry):
        xs = pair_lanes(p)
        g = y_ref[:, xs] * silu(proj_ref[:, xs])
        return carry[0] + g * g, carry[1] + g * (dyn_ref[:, xs] * gg_ref[0:1, xs])

    square, cross = lax.fori_loop(0, PAIRS, sums, (zero, zero))
    scale = lax.rsqrt(jnp.sum(square, axis=1, keepdims=True) / DI + epsilon)
    mean = jnp.sum(cross, axis=1, keepdims=True) * scale / DI

    def pair(p, _):
        xs = pair_lanes(p)
        z = proj_ref[:, xs]
        y = y_ref[:, xs]
        sz = silu(z)
        ghat = y * sz * scale
        dyn = dyn_ref[:, xs]
        dgg_ref[0:1, xs] = jnp.sum(dyn * ghat, axis=0, keepdims=True)
        dg = scale * (dyn * gg_ref[0:1, xs] - ghat * mean)
        dy = dg * sz
        dy_ref[:, xs] = dy
        dz_ref[:, xs] = (dg * y * silu_grad(z)).astype(bf16)
        gst_ref[xs, :] = dot_tn((jnp.exp(lcol[p]) * dy).astype(bf16), cm)
        return 0

    lax.fori_loop(0, PAIRS, pair, 0)


def back_kernel(
    dy_ref, y_ref, proj_ref, halo_ref, pre_ref, dt_ref, cum_ref, sin_ref, gin_ref,
    cw_ref, dtb_ref, al_ref, sk_ref,
    dx_ref, dhalo_ref, ddr_ref, dcw_ref, dsm_ref,
    pad, grad, col, tcol, lcol, lrow, dcb, dbm, dcm, dlog, dtx, ends,
):
    rows = y_ref.shape[0]
    pad[0:8, :] = halo_ref[...]
    pad[8:, :] = proj_ref[:, DI : DI + XBC]
    grad[0:8, :] = jnp.zeros((8, XBC), f32)
    grad[rows + 8 :, :] = jnp.zeros((8, XBC), f32)
    cum = cum_ref[...]
    dt = dt_ref[...]
    lrow[...] = cum.T
    spread_columns(cum, col, lcol, rows)
    spread_columns(dt, None, tcol, rows)
    bm = silu(pre_ref[:, DI : DI + NSTATE]).astype(bf16)
    cm = silu(pre_ref[:, DI + NSTATE :]).astype(bf16)
    cbt = dot_nt(bm, cm)
    ri = lax.broadcasted_iota(jnp.int32, (rows, rows), 0)
    ci = lax.broadcasted_iota(jnp.int32, (rows, rows), 1)
    causal = ri <= ci
    half = first_half(rows)
    dcb[...] = jnp.zeros((rows, rows), f32)
    zero = jnp.zeros((rows, LANES), f32)
    dbm[...] = zero
    dcm[...] = zero
    dlog[...] = zero
    dtx[...] = zero
    ends[...] = jnp.zeros((16, LANES), f32)
    lane_row = lax.broadcasted_iota(jnp.int32, (LANES, LANES), 0)
    lane_col = lax.broadcasted_iota(jnp.int32, (LANES, LANES), 1)
    ones = jnp.ones((8, NSTATE), f32)

    def pair(p, _):
        xs = pair_lanes(p)
        pre = pre_ref[:, xs]
        x = silu(pre)
        tp = tcol[p]
        xt = tp * x
        dy = dy_ref[:, xs]
        dyb = dy.astype(bf16)
        parts = []
        for j in range(2):
            h = 2 * p + j
            c = col[h]
            d = lrow[pl.ds(h, 1), :] - jnp.concatenate([c] * (rows // LANES), axis=1)
            w = jnp.exp(jnp.where(causal, d, OFF))
            parts.append(dot_nn((w * cbt).astype(bf16), dyb))
            own = half if j == 0 else jnp.logical_not(half)
            q = dot_nt(jnp.where(own, xt, 0.0).astype(bf16), dyb)
            dcb[...] += w * q
        lp = lcol[p]
        last = lp[rows - 1 : rows, :]
        tail = jnp.exp(last - lp)
        gin = gin_ref[xs, :]
        sin = sin_ref[xs, :]
        dst = tail * dot_nt(bm, gin)
        dxt = jnp.where(half, parts[0], parts[1]) + dst
        dbm[...] += dot_nn((tail * xt).astype(bf16), gin)
        dcm[...] += dot_nn((jnp.exp(lp) * dy).astype(bf16), sin)
        sk = sk_ref[0:1, xs]
        pick = jnp.where(lane_col == 2 * p + jnp.where(lane_row >= HDIM, 1, 0), 1.0, 0.0)
        dlog[...] += dot_nn(dy * (y_ref[:, xs] - sk * x) - xt * dxt, pick, highest)
        dtx[...] += dot_nn(x * dxt, pick, highest)
        held = dot_nt(ones, gin.astype(f32) * sin.astype(f32), highest)
        end = jnp.sum(xt * dst, axis=0, keepdims=True) + jnp.exp(last) * held[0:1, :]
        skip = jnp.sum(dy * x, axis=0, keepdims=True)
        stacked = jnp.concatenate(
            [jnp.broadcast_to(end, (8, LANES)), jnp.broadcast_to(skip, (8, LANES))], axis=0
        )
        ends[...] += dot_nn(stacked, pick, highest)
        grad[pl.ds(8, rows), xs] = (tp * dxt + sk * dy) * silu_grad(pre)
        return 0

    lax.fori_loop(0, PAIRS, pair, 0)
    dcbb = dcb[...].astype(bf16)
    dc = dcm[...] + dot_tn(dcbb, bm)
    db = dbm[...] + dot_nn(dcbb, cm)
    grad[8 : 8 + rows, DI : DI + NSTATE] = db * silu_grad(pre_ref[:, DI : DI + NSTATE])
    grad[8 : 8 + rows, DI + NSTATE :] = dc * silu_grad(pre_ref[:, DI + NSTATE :])

    last_row = lax.broadcasted_iota(jnp.int32, (rows, LANES), 0) == rows - 1
    dl = dlog[...] + jnp.where(last_row, ends[0:1, :], 0.0)
    da = dot_nn(jnp.where(causal, 1.0, 0.0), dl, highest)
    decay = -jnp.exp(al_ref[...])
    ddt = dtx[...] + da * decay
    ddr_ref[...] = jnp.zeros((rows, LANES), f32)
    ddr_ref[:, 0:HEADS] = proj_ref[:, DI + XBC :]
    ddr = ddt * lax.logistic(ddr_ref[...] + dtb_ref[...])
    ddr_ref[...] = ddr
    dsm_ref[...] = jnp.zeros((8, LANES), f32)
    dsm_ref[0:1, :] = jnp.sum(ddr, axis=0, keepdims=True)
    dsm_ref[1:2, :] = jnp.sum(da * dt, axis=0, keepdims=True) * decay
    dsm_ref[2:3, :] = ends[8:9, :]

    def conv(i, _):
        xs = pair_lanes(i)
        own = grad[pl.ds(8, rows), xs]
        out = jnp.zeros((rows, LANES), f32)
        edge = jnp.zeros((8, LANES), f32)
        for k in range(CONV):
            wk = cw_ref[k : k + 1, xs]
            out = out + wk * grad[11 - k : 11 - k + rows, xs]
            edge = edge + wk * grad[3 - k : 11 - k, xs]
            dcw_ref[k : k + 1, xs] = jnp.sum(
                own * pad[5 + k : 5 + k + rows, xs], axis=0, keepdims=True
            )
        dcw_ref[4:5, xs] = jnp.sum(own, axis=0, keepdims=True)
        dx_ref[:, xs] = out
        dhalo_ref[:, xs] = edge
        return 0

    lax.fori_loop(0, XBC // LANES, conv, 0)


VTILE = 1280
NTILE = 256


def head_specs(width, tokens):
    return dict(
        table=pl.BlockSpec((VTILE, width), lambda i: (i, 0)),
        hidden=pl.BlockSpec((tokens, width), lambda i: (0, 0)),
        kept=pl.BlockSpec((VTILE, tokens), lambda i: (i, 0)),
        row=pl.BlockSpec((1, tokens), lambda i: (0, 0)),
        tile_row=pl.BlockSpec((1, 1, tokens), lambda i: (i, 0, 0)),
    )


def head_call(kernel, grid, in_specs, out_specs, outs, scratch, ins, cells):
    return pl.pallas_call(
        kernel,
        grid=(grid,),
        in_specs=in_specs,
        out_specs=out_specs,
        out_shape=[jax.ShapeDtypeStruct(shape, kind) for shape, kind in outs],
        scratch_shapes=list(scratch),
        compiler_params=pltpu.CompilerParams(
            dimension_semantics=("arbitrary",), vmem_limit_bytes=VMEM_LIMIT
        ),
        cost_estimate=pl.CostEstimate(
            flops=2 * cells * D, transcendentals=cells, bytes_accessed=4 * cells
        ),
    )(*ins)


def head_stats_kernel(vocab_rows, e_ref, h_ref, lab_ref, q_ref, st_ref):
    first = pl.program_id(0) * VTILE
    tokens = h_ref.shape[0]

    def chunk(j, ragged):
        ns = pl.ds(pl.multiple_of(j * NTILE, NTILE), NTILE)
        logits = dot_nt(e_ref[...], h_ref[ns, :])
        rid = lax.broadcasted_iota(jnp.int32, (VTILE, NTILE), 0)
        if ragged:
            logits = jnp.where(rid < vocab_rows - first, logits, OFF)
        top = jnp.max(logits, axis=0, keepdims=True)
        p = jnp.exp(logits - top)
        q_ref[:, ns] = p.astype(bf16)
        st_ref[0, 0:1, ns] = top
        st_ref[0, 1:2, ns] = jnp.sum(p, axis=0, keepdims=True)
        label = lab_ref[0:1, ns]
        hit = jnp.where(rid == label - first, logits, 0.0)
        inside = jnp.logical_and(label >= 0, label < vocab_rows)
        st_ref[0, 2:3, ns] = jnp.where(inside, jnp.sum(hit, axis=0, keepdims=True), 0.0)

    def run(ragged):
        lax.fori_loop(
            0, tokens // NTILE, lambda j, _: (chunk(j, ragged), 0)[1], 0, unroll=UNROLL
        )

    end = pl.program_id(0) == pl.num_programs(0) - 1

    @pl.when(end)
    def _():
        run(True)

    @pl.when(jnp.logical_not(end))
    def _():
        run(False)


UNROLL = 8


def head_stats(table, hidden, labels):
    vocab_rows, width = table.shape
    tokens = hidden.shape[0]
    tiles = pl.cdiv(vocab_rows, VTILE)
    sp = head_specs(width, tokens)
    return head_call(
        functools.partial(head_stats_kernel, vocab_rows),
        tiles,
        [sp["table"], sp["hidden"], sp["row"]],
        [sp["kept"], pl.BlockSpec((1, 8, tokens), lambda i: (i, 0, 0))],
        [((tiles * VTILE, tokens), bf16), ((tiles, 8, tokens), f32)],
        (),
        (table, hidden, labels),
        vocab_rows * tokens,
    )


def logit_grads(q, fac, weight, rid, label):
    other = weight * (0.1 / VOCAB)
    return (q.astype(f32) * fac - jnp.where(rid == label, other + 0.9 * weight, other)).astype(bf16)


def head_rows_kernel(vocab_rows, e_ref, q_ref, fac_ref, w_ref, lab_ref, out_ref, acc, et):
    step = pl.program_id(0)
    first = step * VTILE
    tokens = q_ref.shape[1]

    @pl.when(step == 0)
    def _():
        acc[...] = jnp.zeros(acc.shape, f32)

    eid = lax.broadcasted_iota(jnp.int32, (VTILE, e_ref.shape[1]), 0)
    et[...] = jnp.where(eid < vocab_rows - first, e_ref[...].astype(f32), 0.0).T.astype(bf16)

    def chunk(j, _):
        ns = pl.ds(pl.multiple_of(j * NTILE, NTILE), NTILE)
        rid = lax.broadcasted_iota(jnp.int32, (VTILE, NTILE), 0)
        dl = logit_grads(
            q_ref[:, ns], fac_ref[0, 0:1, ns], w_ref[0:1, ns], rid, lab_ref[0:1, ns] - first
        )
        acc[:, ns] += dot_nn(et[...], dl)
        return 0

    lax.fori_loop(0, tokens // NTILE, chunk, 0, unroll=UNROLL)

    @pl.when(step == pl.num_programs(0) - 1)
    def _():
        def put(j, _):
            ns = pl.ds(pl.multiple_of(j * NTILE, NTILE), NTILE)
            out_ref[ns, :] = acc[:, ns].T.astype(bf16)
            return 0

        lax.fori_loop(0, tokens // NTILE, put, 0)


def head_rows(table, kept, fac, weight, labels):
    vocab_rows, width = table.shape
    tokens = kept.shape[1]
    sp = head_specs(width, tokens)
    return head_call(
        functools.partial(head_rows_kernel, vocab_rows),
        pl.cdiv(vocab_rows, VTILE),
        [sp["table"], sp["kept"], sp["tile_row"], sp["row"], sp["row"]],
        [sp["hidden"]],
        [((tokens, width), bf16)],
        (pltpu.VMEM((width, tokens), f32), pltpu.VMEM((width, VTILE), bf16)),
        (table, kept, fac, weight, labels),
        vocab_rows * tokens,
    )[0]


def head_table_kernel(h_ref, q_ref, fac_ref, w_ref, lab_ref, out_ref, dl_ref):
    first = pl.program_id(0) * VTILE
    tokens = q_ref.shape[1]

    def chunk(j, _):
        ns = pl.ds(pl.multiple_of(j * NTILE, NTILE), NTILE)
        rid = lax.broadcasted_iota(jnp.int32, (VTILE, NTILE), 0)
        dl_ref[:, ns] = logit_grads(
            q_ref[:, ns], fac_ref[0, 0:1, ns], w_ref[0:1, ns], rid, lab_ref[0:1, ns] - first
        )
        return 0

    lax.fori_loop(0, tokens // NTILE, chunk, 0, unroll=UNROLL)

    def cols(j, _):
        ds = pl.ds(pl.multiple_of(j * 256, 256), 256)
        out_ref[:, ds] = dot_nn(dl_ref[...], h_ref[:, ds]).astype(bf16)
        return 0

    lax.fori_loop(0, h_ref.shape[1] // 256, cols, 0, unroll=True)


def head_table(hidden, kept, fac, weight, labels, vocab_rows):
    tokens, width = hidden.shape
    sp = head_specs(width, tokens)
    return head_call(
        head_table_kernel,
        pl.cdiv(vocab_rows, VTILE),
        [sp["hidden"], sp["kept"], sp["tile_row"], sp["row"], sp["row"]],
        [sp["table"]],
        [((vocab_rows, width), bf16)],
        (pltpu.VMEM((VTILE, tokens), bf16),),
        (hidden, kept, fac, weight, labels),
        vocab_rows * tokens,
    )[0]


def weight_grads_kernel(u_ref, dp_ref, yn_ref, db_ref, in_ref, out_ref):
    wide_cols = dp_ref.shape[1]
    for c in range(0, wide_cols, 1024):
        cs = pl.ds(c, min(1024, wide_cols - c))
        in_ref[:, cs] = dot_tn(u_ref[...], dp_ref[:, cs]).astype(bf16)
    out_ref[...] = dot_tn(yn_ref[...], db_ref[...]).astype(bf16)


def weight_grads(normed, grad_proj, mixed, grad_branch):
    rows = normed.shape[0]
    steps = D // LANES
    part = DI // steps
    return head_call(
        weight_grads_kernel,
        steps,
        [
            pl.BlockSpec((rows, LANES), lambda i: (0, i)),
            pl.BlockSpec((rows, ZW), lambda i: (0, 0)),
            pl.BlockSpec((rows, part), lambda i: (0, i)),
            pl.BlockSpec((rows, D), lambda i: (0, 0)),
        ],
        [pl.BlockSpec((LANES, ZW), lambda i: (i, 0)), pl.BlockSpec((part, D), lambda i: (i, 0))],
        [((D, ZW), bf16), ((DI, D), bf16)],
        (),
        (normed, grad_proj, mixed, grad_branch),
        rows * (ZW + DI),
    )


def shift_chunks(block, distance):
    size = lax.axis_size("fsdp")
    route = [(i - 2 * distance, i) for i in range(size) if 0 <= i - 2 * distance < size]
    return lax.ppermute(block, "fsdp", route)


def after(value, earlier):
    return lax.optimization_barrier((value, earlier))[0]


def norm_scale(values):
    return lax.rsqrt(jnp.mean(values * values, axis=-1, keepdims=True) + epsilon)


def norm_back(grad, values, gain):
    scale = norm_scale(values)
    unit = values * scale
    inner = grad * gain
    back = scale * (inner - unit * jnp.mean(inner * unit, axis=-1, keepdims=True))
    return back, jnp.sum(grad * unit, axis=0)


def wide(row):
    return jnp.pad(row, (0, LANES - row.shape[0]))[None]


def layer_vectors(vector_params, layer_index):
    offset = layer_index * PER
    pieces = []
    for size in (CONV * XBC, XBC, HEADS, HEADS, HEADS, D, DI):
        pieces.append(vector_params[offset : offset + size])
        offset += size
    conv_w, conv_b, dt_bias, decay_log, skip, pre_gain, gate_gain = pieces
    return dict(
        conv_w=conv_w.reshape(CONV, XBC),
        conv_b=conv_b[None],
        dt_bias=wide(dt_bias),
        decay_log=wide(decay_log),
        skip=jnp.repeat(skip, HDIM)[None],
        pre_gain=pre_gain,
        gate_gain=gate_gain[None],
    )


def layer_forward(hidden, w_in, w_out, vec):
    rows = hidden.shape[0]
    normed = (hidden * norm_scale(hidden) * vec["pre_gain"]).astype(bf16)
    proj = jnp.dot(normed, w_in, preferred_element_type=f32)
    halo = shift_chunks(proj[rows - 8 :, DI : DI + XBC], 1)
    pre, y0, local, dt, cum = local_call(
        front_kernel,
        (proj, halo, vec["conv_w"], vec["conv_b"], vec["dt_bias"], vec["decay_log"], vec["skip"]),
        (
            ((rows, XBC), f32),
            ((rows, DI), f32),
            ((DI, NSTATE), f32),
            ((rows, LANES), f32),
            ((rows, LANES), f32),
        ),
        scratch=(
            pltpu.VMEM((rows + 8, XBC), f32),
            pltpu.VMEM((HEADS, rows, LANES), f32),
            pltpu.VMEM((PAIRS, rows, LANES), f32),
            pltpu.VMEM((PAIRS, rows, LANES), f32),
            pltpu.VMEM((LANES, rows), f32),
        ),
    )
    decay = jnp.exp(cum[rows - 1, :HEADS])
    entering = carry_chain(decay, local, 1)
    y, mixed = local_call(
        gate_kernel,
        (y0, proj, pre, cum, entering, vec["gate_gain"]),
        (((rows, DI), f32), ((rows, DI), bf16)),
        scratch=(pltpu.VMEM((PAIRS, rows, LANES), f32),),
    )
    branch = jnp.dot(mixed, w_out, preferred_element_type=f32)
    record = (hidden, normed, proj, halo, pre, dt, cum, decay, entering, y, mixed)
    return hidden + branch, record


def layer_backward(grad_hidden, w_in, w_out, vec, record):
    hidden, normed, proj, halo, pre, dt, cum, decay, entering, y, mixed = record
    rows = hidden.shape[0]
    grad_branch = grad_hidden.astype(bf16)
    grad_mixed = dot_nt(grad_branch, w_out)
    dy, dz, dgate, gstate = local_call(
        ungate_kernel,
        (grad_mixed, y, proj, pre, cum, vec["gate_gain"]),
        (
            ((rows, DI), f32),
            ((rows, DI), bf16),
            ((1, DI), f32),
            ((DI, NSTATE), f32),
        ),
        scratch=(pltpu.VMEM((PAIRS, rows, LANES), f32),),
    )
    later = carry_chain(decay, gstate, -1)
    dx, dhalo, ddr, dconv, dsmall = local_call(
        back_kernel,
        (
            dy, y, proj, halo, pre, dt, cum, entering, later,
            vec["conv_w"], vec["dt_bias"], vec["decay_log"], vec["skip"],
        ),
        (
            ((rows, XBC), f32),
            ((8, XBC), f32),
            ((rows, LANES), f32),
            ((8, XBC), f32),
            ((8, LANES), f32),
        ),
        scratch=(
            pltpu.VMEM((rows + 8, XBC), f32),
            pltpu.VMEM((rows + 16, XBC), f32),
            pltpu.VMEM((HEADS, rows, LANES), f32),
            pltpu.VMEM((PAIRS, rows, LANES), f32),
            pltpu.VMEM((PAIRS, rows, LANES), f32),
            pltpu.VMEM((LANES, rows), f32),
            pltpu.VMEM((rows, rows), f32),
            pltpu.VMEM((rows, LANES), f32),
            pltpu.VMEM((rows, LANES), f32),
            pltpu.VMEM((rows, LANES), f32),
            pltpu.VMEM((rows, LANES), f32),
            pltpu.VMEM((16, LANES), f32),
        ),
    )
    from_next = shift_chunks(dhalo, -1)
    dx = jnp.concatenate([dx[: rows - 8], dx[rows - 8 :] + from_next], axis=0)
    grad_proj = jnp.concatenate(
        [dz, dx.astype(bf16), ddr[:, :HEADS].astype(bf16)], axis=1
    )
    grad_normed = dot_nt(grad_proj, w_in)
    grad_in, grad_out = weight_grads(normed, grad_proj, mixed, grad_branch)
    grad_prev, dpre_gain = norm_back(grad_normed, hidden, vec["pre_gain"])
    grad_vec = jnp.concatenate(
        [
            dconv[:CONV].reshape(-1),
            dconv[CONV],
            dsmall[0, :HEADS],
            dsmall[1, :HEADS],
            jnp.sum(dsmall[2:3, :HEADS], axis=0),
            dpre_gain,
            dgate[0],
        ]
    )
    return grad_hidden + grad_prev, grad_in, grad_out, grad_vec


def advance(weight, moment, average, grad, factor):
    scaled = grad * factor
    moment_new = 0.5 * moment + scaled
    weight_new = weight - step_rate * (scaled + 0.5 * moment_new)
    average_new = 0.5 * average + 0.5 * weight_new
    return (weight_new, moment_new, average_new, weight_new.astype(bf16))


def whole_step(
    token_ids,
    target_ids,
    seq_lengths,
    embedding,
    embedding_mom,
    embedding_avg,
    in_proj,
    in_proj_mom,
    in_proj_avg,
    out_proj,
    out_proj_mom,
    out_proj_avg,
    vector_params,
    vector_mom,
    vector_avg,
):
    groups = lax.axis_size("dp")
    shards = lax.axis_size("fsdp")
    group_index = lax.axis_index("dp")
    shard_index = lax.axis_index("fsdp")
    chunks = shards // MB
    seq_rows = token_ids.shape[2]
    rows = seq_rows // chunks
    vocab_rows, own_cols = embedding.shape
    tokens = MB * seq_rows
    total_count = jnp.sum(seq_lengths).astype(f32)
    embed_low = embedding.astype(bf16)
    in_low = in_proj.astype(bf16)
    out_low = out_proj.astype(bf16)

    ids_all = lax.all_gather(token_ids[:, 0, :], "dp", axis=0)
    ids_all = ids_all.reshape(groups, MB, chunks, rows).transpose(2, 1, 0, 3).reshape(-1)
    every = ids_all.shape[0]
    local_ids = ids_all - shard_index * vocab_rows
    inside = (local_ids >= 0) & (local_ids < vocab_rows)
    sorted_ids, sorted_tok = lax.sort(
        (jnp.where(inside, local_ids, vocab_rows), jnp.arange(every, dtype=jnp.int32)),
        num_keys=1,
    )
    held_here = sorted_ids < vocab_rows
    count = jnp.sum(held_here.astype(jnp.int32)).reshape(1)
    row_list = jnp.where(held_here, sorted_ids, 0)
    tok_list = jnp.where(held_here, sorted_tok, every)
    (looked,) = local_call(
        lookup_kernel,
        (count, row_list, tok_list, embedding),
        (((every, own_cols), bf16),),
        scratch=(pltpu.VMEM((every + 8, own_cols), f32),),
        in_smem=(0, 1, 2),
    )
    mine = lax.psum_scatter(
        looked.reshape(shards * groups * rows, own_cols), "fsdp", scatter_dimension=0, tiled=True
    )
    mine = lax.all_to_all(mine.reshape(groups, rows, own_cols), "dp", 0, 0)
    hidden = mine.transpose(1, 0, 2).reshape(rows, D).astype(f32)

    shards = []
    for l in range(LAYERS):
        shards += [in_low[l], out_low[l]]
    shards = after(shards, looked)
    gathered = gather_layers(shards)
    w_in, w_out = gathered[0::2], gathered[1::2]
    embed_low = after(embed_low, gathered)
    table = lax.all_gather(embed_low, "dp", axis=1, tiled=True)

    vecs = [layer_vectors(vector_params, l) for l in range(LAYERS)]
    final_gain = vector_params[LAYERS * PER :]
    records = []
    for l in range(LAYERS):
        hidden, record = layer_forward(hidden, w_in[l], w_out[l], vecs[l])
        records.append(record)

    final_low = (hidden * norm_scale(hidden) * final_gain).astype(bf16)
    group_hidden = lax.all_gather(final_low, "fsdp", axis=0, tiled=True)

    def in_order(per_seq):
        return per_seq.reshape(MB, chunks, rows).transpose(1, 0, 2).reshape(1, tokens)

    labels = in_order(target_ids[:, 0, :])
    lengths = lax.dynamic_index_in_dim(seq_lengths, group_index, 1, keepdims=True)
    valid = in_order((jnp.arange(seq_rows)[None, :] < lengths).astype(f32))
    local_labels = labels - shard_index * vocab_rows
    kept, tile_stats = head_stats(table, group_hidden, local_labels)
    top = jnp.max(tile_stats[:, 0], axis=0)
    summed = jnp.sum(tile_stats[:, 1] * jnp.exp(tile_stats[:, 0] - top), axis=0)
    stats = lax.all_gather(jnp.stack([top, summed]), "fsdp", axis=0)
    row_top = jnp.max(stats[:, 0], axis=0)
    expsum = jnp.sum(stats[:, 1] * jnp.exp(stats[:, 0] - row_top), axis=0)
    log_total = row_top + jnp.log(expsum)
    own_mask = jnp.arange(tokens) // rows == shard_index
    per_row = jnp.where(own_mask, log_total + z_weight * log_total * log_total, 0.0)
    loss_sum = jnp.sum((per_row - 0.9 * jnp.sum(tile_stats[:, 2], axis=0)) * valid[0])
    weight = valid / total_count
    scale = weight[0] * (1.0 + 2.0 * z_weight * log_total)
    fac = (scale * jnp.exp(tile_stats[:, 0] - log_total))[:, None, :]
    own_valid = lax.dynamic_slice_in_dim(valid[0], shard_index * rows, rows)
    hidden_sum = jnp.sum(final_low.astype(f32) * own_valid[:, None], axis=0)
    column_sum = jnp.zeros((groups, own_cols), f32)
    column_sum = jnp.where(
        jnp.arange(groups)[:, None] == group_index, jnp.sum(embed_low.astype(f32), axis=0), column_sum
    ).reshape(D)

    rows_grad = head_rows(table, kept, fac, weight, local_labels)
    own_grad = lax.psum_scatter(
        rows_grad, "fsdp", scatter_dimension=0, tiled=True
    ).astype(f32)
    table_grad = head_table(group_hidden, kept, fac, weight, local_labels, vocab_rows)
    table_part = lax.psum_scatter(table_grad, "dp", scatter_dimension=1, tiled=True)

    grad_hidden, dfinal = norm_back(after(own_grad, table_grad), hidden, final_gain)
    in_parts = [None] * LAYERS
    out_parts = [None] * LAYERS
    vec_parts = [None] * LAYERS
    for l in reversed(range(LAYERS)):
        grad_hidden, grad_in, grad_out, vec_parts[l] = layer_backward(
            grad_hidden, w_in[l], w_out[l], vecs[l], records[l]
        )
        if l == 0:
            sent = grad_hidden.astype(bf16).reshape(rows, groups, own_cols).transpose(1, 0, 2)
            sent = lax.all_to_all(sent, "dp", 0, 0)
            spread = lax.all_gather(sent, "fsdp", axis=0).reshape(every, own_cols)
        in_parts[l], out_parts[l] = grad_in, grad_out
    whole = []
    for l in range(LAYERS):
        whole += [in_parts[l], out_parts[l]]
    summed_parts = reduce_layers(whole)
    spread = after(spread, summed_parts)
    table_total, table_squares = local_call(
        spread_kernel,
        (count, row_list, tok_list, spread, table_part),
        (((vocab_rows, own_cols), f32), ((8, own_cols), f32)),
        scratch=(pltpu.VMEM((every + 8, own_cols), f32),),
        in_smem=(0, 1, 2),
    )
    grad_in_all = jnp.stack(summed_parts[0::2])
    grad_out_all = jnp.stack(summed_parts[1::2])
    owner_squares = (
        jnp.sum(grad_in_all * grad_in_all)
        + jnp.sum(grad_out_all * grad_out_all)
        + jnp.sum(table_squares)
    )
    small = vector_params.shape[0]
    used = small + 2 * D + 2
    padded = pl.cdiv(used, 16 * LANES) * 16 * LANES
    packed = jnp.concatenate(
        vec_parts
        + [
            dfinal,
            hidden_sum,
            column_sum,
            owner_squares.reshape(1),
            loss_sum.reshape(1),
            jnp.zeros((padded - used,), f32),
        ]
    )
    packed = total_of(packed.reshape(-1, LANES)).reshape(-1)
    vector_total = packed[:small]
    hidden_total = packed[small : small + D]
    column_total = packed[small + D : small + 2 * D]
    squares_total = packed[used - 2]
    mean_part = jnp.sum(hidden_total * column_total) * (0.1 / VOCAB)
    loss_total = packed[used - 1] - mean_part
    grad_norm = jnp.sqrt(squares_total + jnp.sum(vector_total * vector_total))
    factor = jnp.minimum(1.0, clip_limit / grad_norm)
    loss_value = loss_total / total_count
    return (
        loss_value,
        grad_norm,
        *advance(embedding, embedding_mom, embedding_avg, table_total, factor),
        *advance(in_proj, in_proj_mom, in_proj_avg, grad_in_all, factor),
        *advance(out_proj, out_proj_mom, out_proj_avg, grad_out_all, factor),
        *advance(vector_params, vector_mom, vector_avg, vector_total, factor),
    )


def solution(mesh):
    table_spec = P("fsdp", "dp")
    weight_spec = P(None, ("dp", "fsdp"), None)
    return jax.shard_map(
        whole_step,
        mesh=mesh,
        in_specs=(
            P(None, "dp", None),
            P(None, "dp", None),
            P(),
            *(table_spec,) * 3,
            *(weight_spec,) * 6,
            *(P(),) * 3,
        ),
        out_specs=(
            P(),
            P(),
            *(table_spec,) * 4,
            *(weight_spec,) * 8,
            *(P(),) * 4,
        ),
        check_vma=False,
    )
```

```python
import functools

import jax
import jax.numpy as jnp
from jax import lax
from jax.experimental import pallas as pl
from jax.experimental.pallas import tpu as pltpu
from jax.sharding import PartitionSpec as P


D = 1024
HEADS = 32
HDIM = 64
NSTATE = 128
CONV = 4
VOCAB = 50288
LAYERS = 2
MB = 2
DI = 2048
XBC = 2304
ZW = 4384
PER = 14688
LANES = 128
PAIRS = DI // LANES

epsilon = 1e-05
z_weight = 0.001
clip_limit = 0.2
step_rate = 1000.0
highest = lax.Precision.HIGHEST
bf16 = jnp.bfloat16
f32 = jnp.float32
VMEM_LIMIT = 62 * 1024 * 1024
OFF = -1e30


def dot_nn(a, b, precision=None):
    return lax.dot_general(
        a, b, (((1,), (0,)), ((), ())), precision=precision, preferred_element_type=f32
    )


def dot_nt(a, b, precision=None):
    return lax.dot_general(
        a, b, (((1,), (1,)), ((), ())), precision=precision, preferred_element_type=f32
    )


def dot_tn(a, b, precision=None):
    return lax.dot_general(
        a, b, (((0,), (0,)), ((), ())), precision=precision, preferred_element_type=f32
    )


def silu(v):
    return v * lax.logistic(v)


def silu_grad(v):
    s = lax.logistic(v)
    return s * (1.0 + v * (1.0 - s))


def local_call(kernel, ins, outs, scratch=(), in_smem=(), flops=0):
    total = sum(a.size * a.dtype.itemsize for a in ins)
    return pl.pallas_call(
        kernel,
        out_shape=[jax.ShapeDtypeStruct(shape, kind) for shape, kind in outs],
        in_specs=[
            pl.BlockSpec(memory_space=pltpu.SMEM if i in in_smem else pltpu.VMEM)
            for i in range(len(ins))
        ],
        out_specs=[pl.BlockSpec(memory_space=pltpu.VMEM) for _ in outs],
        scratch_shapes=list(scratch),
        compiler_params=pltpu.CompilerParams(vmem_limit_bytes=VMEM_LIMIT),
        cost_estimate=pl.CostEstimate(
            flops=flops or total, transcendentals=0, bytes_accessed=2 * total
        ),
    )(*ins)


def lookup_kernel(count_ref, row_ref, tok_ref, table_ref, out_ref, held):
    tokens = out_ref.shape[0]
    step = 512

    def clear(i, _):
        held[pl.ds(pl.multiple_of(i * step, step), step), :] = jnp.zeros(
            (step, held.shape[1]), f32
        )
        return 0

    lax.fori_loop(0, tokens // step, clear, 0)

    def move(i, _):
        for k in range(8):
            row = row_ref[i * 8 + k]
            tok = tok_ref[i * 8 + k]
            held[pl.ds(tok, 1), :] = table_ref[pl.ds(row, 1), :]
        return 0

    lax.fori_loop(0, (count_ref[0] + 7) // 8, move, 0)

    def put(i, _):
        rows = pl.ds(pl.multiple_of(i * step, step), step)
        out_ref[rows, :] = held[rows, :].astype(bf16)
        return 0

    lax.fori_loop(0, tokens // step, put, 0)


def spread_kernel(count_ref, row_ref, tok_ref, grad_ref, base_ref, out_ref, square_ref, held):
    tokens = grad_ref.shape[0]
    step = 512
    rows_all = out_ref.shape[0]

    def take(i, _):
        rows = pl.ds(pl.multiple_of(i * step, step), step)
        held[rows, :] = grad_ref[rows, :].astype(f32)
        return 0

    lax.fori_loop(0, tokens // step, take, 0)
    held[pl.ds(tokens, 8), :] = jnp.zeros((8, held.shape[1]), f32)

    whole = rows_all // step

    def start(i, _):
        rows = pl.ds(pl.multiple_of(i * step, step), step)
        out_ref[rows, :] = base_ref[rows, :].astype(f32)
        return 0

    lax.fori_loop(0, whole, start, 0)
    if rows_all > whole * step:
        out_ref[whole * step :, :] = base_ref[whole * step :, :].astype(f32)

    def move(i, _):
        for k in range(8):
            row = row_ref[i * 8 + k]
            tok = tok_ref[i * 8 + k]
            out_ref[pl.ds(row, 1), :] = out_ref[pl.ds(row, 1), :] + held[pl.ds(tok, 1), :]
        return 0

    lax.fori_loop(0, (count_ref[0] + 7) // 8, move, 0)

    def square(i, total):
        part = out_ref[pl.ds(pl.multiple_of(i * step, step), step), :]
        return total + jnp.sum((part * part).reshape(step // 8, 8, -1), axis=0)

    total = lax.fori_loop(0, whole, square, jnp.zeros(square_ref.shape, f32))
    square_ref[...] = total
    if rows_all > whole * step:
        part = out_ref[whole * step :, :]
        square_ref[0:1, :] += jnp.sum(part * part, axis=0, keepdims=True)


MESH = pl.DeviceIdType.MESH


def remote(src, dst, send, recv, dp, fsdp):
    return pltpu.make_async_remote_copy(
        src_ref=src,
        dst_ref=dst,
        send_sem=send,
        recv_sem=recv,
        device_id=(dp, fsdp),
        device_id_type=MESH,
    )


def comm_call(kernel, number, ins, outs, scratch, in_spaces, out_spaces, sent):
    return pl.pallas_call(
        kernel,
        out_shape=[jax.ShapeDtypeStruct(shape, kind) for shape, kind in outs],
        in_specs=[pl.BlockSpec(memory_space=space) for space in in_spaces],
        out_specs=[pl.BlockSpec(memory_space=space) for space in out_spaces],
        scratch_shapes=list(scratch),
        compiler_params=pltpu.CompilerParams(
            collective_id=number, has_side_effects=True, vmem_limit_bytes=VMEM_LIMIT
        ),
        cost_estimate=pl.CostEstimate(flops=sent, transcendentals=0, bytes_accessed=2 * sent),
    )(*ins)


def chain_kernel(direction, steps, decay_ref, local_ref, out_ref, got, give, send, recv):
    dp = lax.axis_index("dp")
    me = lax.axis_index("fsdp")
    place = me // MB
    count = lax.axis_size("fsdp") // MB
    first = place == (0 if direction > 0 else count - 1)
    final = place == (count - 1 if direction > 0 else 0)
    part = DI // steps
    heads = part // HDIM
    barrier = pltpu.get_barrier_semaphore()

    @pl.when(jnp.logical_not(first))
    def _():
        pl.semaphore_signal(
            barrier, inc=1, device_id=(dp, me - MB * direction), device_id_type=MESH
        )

    @pl.when(jnp.logical_not(final))
    def _():
        pl.semaphore_wait(barrier, 1)

    @pl.when(first)
    def _():
        got[...] = jnp.zeros(got.shape, bf16)

    def copy(g):
        rows = pl.ds(g * part, part)
        return remote(
            give.at[rows], got.at[rows], send.at[g], recv.at[g], dp, me + MB * direction
        )

    for g in range(steps):
        rows = pl.ds(g * part, part)

        @pl.when(jnp.logical_not(first))
        def _():
            copy(g).wait_recv()

        @pl.when(jnp.logical_not(final))
        def _():
            for i in range(heads):
                h = pl.ds(g * part + i * HDIM, HDIM)
                give[h, :] = (
                    decay_ref[g * heads + i] * got[h, :].astype(f32) + local_ref[h, :]
                ).astype(bf16)
            copy(g).start()

        out_ref[rows, :] = got[rows, :]

    @pl.when(jnp.logical_not(final))
    def _():
        for g in range(steps):
            copy(g).wait_send()


CHAIN_STEPS = 8


def carry_chain(decay, local, direction):
    return comm_call(
        functools.partial(chain_kernel, direction, CHAIN_STEPS),
        1 if direction > 0 else 2,
        (decay, local),
        ((local.shape, bf16),),
        (
            pltpu.VMEM(local.shape, bf16),
            pltpu.VMEM(local.shape, bf16),
            pltpu.SemaphoreType.DMA((CHAIN_STEPS,)),
            pltpu.SemaphoreType.DMA((CHAIN_STEPS,)),
        ),
        (pltpu.SMEM, pltpu.VMEM),
        (pltpu.VMEM,),
        local.size * 2,
    )[0]


def bits_of(size):
    return [1 << b for b in range(size.bit_length() - 1)]


def total_kernel(in_ref, out_ref, work, got, send, recv):
    dp = lax.axis_index("dp")
    me = lax.axis_index("fsdp")
    half = in_ref.shape[0] // 2
    core = me % MB
    partners = [("f", b) for b in bits_of(lax.axis_size("fsdp")) if b > 1]
    partners += [("d", b) for b in bits_of(lax.axis_size("dp"))]

    def across(kind, bit):
        ids, other = (me, lambda v: (dp, v)) if kind == "f" else (dp, lambda v: (v, me))
        return other(jnp.where((ids // bit) % 2 == 1, ids - bit, ids + bit))

    mate = across("f", 1)
    barrier = pltpu.get_barrier_semaphore()
    for target in [mate] + [across(*p) for p in partners]:
        pl.semaphore_signal(barrier, inc=1, device_id=target, device_id_type=MESH)
    pl.semaphore_wait(barrier, 1 + len(partners))

    mine = pl.ds(pl.multiple_of(core * half, 8), half)
    theirs = pl.ds(pl.multiple_of((1 - core) * half, 8), half)
    copy = remote(in_ref.at[theirs], got.at[0], send.at[0], recv.at[0], *mate)
    copy.start()
    copy.wait()
    work[0] = in_ref[mine, :] + got[0]
    for i, p in enumerate(partners):
        copy = remote(work.at[i], got.at[i + 1], send.at[i + 1], recv.at[i + 1], *across(*p))
        copy.start()
        copy.wait()
        work[i + 1] = work[i] + got[i + 1]
    n = len(partners)
    copy = remote(work.at[n], got.at[n + 1], send.at[n + 1], recv.at[n + 1], *mate)
    copy.start()
    copy.wait()
    out_ref[mine, :] = work[n]
    out_ref[theirs, :] = got[n + 1]


def total_of(array):
    rows = array.shape[0]
    steps = len(bits_of(lax.axis_size("fsdp"))) - 1 + len(bits_of(lax.axis_size("dp")))
    return comm_call(
        total_kernel,
        3,
        (array,),
        ((array.shape, f32),),
        (
            pltpu.VMEM((steps + 1, rows // 2, LANES), f32),
            pltpu.VMEM((steps + 2, rows // 2, LANES), f32),
            pltpu.SemaphoreType.DMA((steps + 2,)),
            pltpu.SemaphoreType.DMA((steps + 2,)),
        ),
        (pltpu.VMEM,),
        (pltpu.VMEM,),
        array.size * 4 * 3,
    )[0]


def snake(place, size):
    return jnp.where(place < size // 2, place, size // 2 + size - 1 - place)


def wrap(value, size):
    return lax.rem(value + size, size)


def gather_kernel(*refs):
    arrays = 2 * LAYERS
    own = refs[:arrays]
    full = refs[arrays : 2 * arrays]
    local_sem, z_send, z_recv, ring_send, ring_recv, mate_send, mate_recv = refs[2 * arrays :]
    dp = lax.axis_index("dp")
    me = lax.axis_index("fsdp")
    size = lax.axis_size("dp")
    count = lax.axis_size("fsdp") // MB
    core = me % MB
    k = me // MB
    ring = snake(dp, size)
    reach = size // 2
    right = snake(wrap(ring + 1, size), size)
    left = snake(wrap(ring - 1, size), size)
    mate = k * MB + 1 - core
    up, down = me + MB, me - MB
    has_up, has_down = k < count - 1, k > 0
    barrier = pltpu.get_barrier_semaphore()
    for target in ((right, me), (left, me), (dp, mate)):
        pl.semaphore_signal(barrier, inc=1, device_id=target, device_id_type=MESH)

    @pl.when(has_up)
    def _():
        pl.semaphore_signal(barrier, inc=1, device_id=(dp, up), device_id_type=MESH)

    @pl.when(has_down)
    def _():
        pl.semaphore_signal(barrier, inc=1, device_id=(dp, down), device_id_type=MESH)

    pl.semaphore_wait(barrier, 3 + jnp.where(has_up, 1, 0) + jnp.where(has_down, 1, 0))

    def spot(a, d, z, c):
        return full[a].at[d, z, c]

    def chain(a, src, z, side):
        return remote(
            src, spot(a, dp, z, core), z_send.at[a, z], z_recv.at[a, z], dp, up if side == 0 else down
        )

    def chain_own(a, side):
        return remote(
            own[a],
            spot(a, dp, k, core),
            z_send.at[a, count + side],
            z_recv.at[a, k],
            dp,
            up if side == 0 else down,
        )

    def round_ring(a, src, d, z, side):
        return remote(
            src,
            spot(a, d, z, core),
            ring_send.at[a, side],
            ring_recv.at[a, d, z],
            right if side == 0 else left,
            me,
        )

    def to_mate(a, src, d, z):
        return remote(src, spot(a, d, z, core), mate_send.at[a], mate_recv.at[a], dp, mate)

    def carried(a, side):
        return (a < arrays // 2) == (side == 0)

    for a in range(arrays):

        @pl.when(has_up)
        def _(a=a):
            chain_own(a, 0).start()

        @pl.when(has_down)
        def _(a=a):
            chain_own(a, 1).start()

    for a in range(arrays):
        for side in (0, 1):
            round_ring(a, own[a], dp, k, side).start()
    for a in range(arrays):
        to_mate(a, own[a], dp, k).start()
        pltpu.make_async_copy(own[a], spot(a, dp, k, core), local_sem.at[a]).start()

    def ring_step(z, s):
        for side in (0, 1):
            origin = snake(wrap(ring - s if side == 0 else ring + s, size), size)
            for a in range(arrays):
                if s == reach and not carried(a, side):
                    continue
                piece = spot(a, origin, z, core)
                round_ring(a, piece, origin, z, side).wait_recv()
                if s + 1 < reach or (s + 1 == reach and carried(a, side)):
                    round_ring(a, piece, origin, z, side).start()
                to_mate(a, piece, origin, z).start()

    def arrive(z, side):
        for a in range(arrays):
            piece = spot(a, dp, z, core)
            chain(a, piece, z, side).wait_recv()

            @pl.when(has_up if side == 0 else has_down)
            def _(a=a, piece=piece):
                chain(a, piece, z, side).start()

            for way in (0, 1):
                round_ring(a, piece, dp, z, way).start()
            to_mate(a, piece, dp, z).start()

    def both_ways(far, act):
        if far == 0:
            act(k, 0)
            return

        @pl.when(k >= far)
        def _():
            act(k - far, 0)

        @pl.when(k + far < count)
        def _():
            act(k + far, 1)

    for turn in range(1, count + reach):
        if turn < count:
            both_ways(turn, arrive)
        for s in range(1, reach + 1):
            if 0 <= turn - s < count:
                both_ways(turn - s, lambda z, side, s=s: ring_step(z, s))

    for a in range(arrays):
        pltpu.make_async_copy(own[a], spot(a, dp, k, core), local_sem.at[a]).wait()
        for side in (0, 1):
            sent = full[a].at[pl.ds(0, reach if carried(a, side) else reach - 1), :, core]
            remote(sent, sent, ring_send.at[a, side], ring_recv.at[a, 0, 0], dp, mate).wait_send()
        whole = full[a].at[:, :, core]
        remote(whole, whole, mate_send.at[a], mate_recv.at[a], dp, mate).wait_send()
        whole = full[a].at[:, :, 1 - core]
        remote(whole, whole, mate_send.at[a], mate_recv.at[a], dp, mate).wait_recv()

        @pl.when(has_up)
        def _(a=a):
            chain_own(a, 0).wait_send()

        @pl.when(has_down)
        def _(a=a):
            chain_own(a, 1).wait_send()

        for far in range(1, count):

            @pl.when(jnp.logical_and(k >= far, has_up))
            def _(a=a, far=far):
                chain(a, spot(a, dp, k - far, core), k - far, 0).wait_send()

            @pl.when(jnp.logical_and(k + far < count, has_down))
            def _(a=a, far=far):
                chain(a, spot(a, dp, k + far, core), k + far, 1).wait_send()


def gather_layers(shards):
    size, count = lax.axis_size("dp"), lax.axis_size("fsdp") // MB
    arrays = len(shards)
    outs = comm_call(
        gather_kernel,
        4,
        shards,
        tuple(((size, count, MB) + s.shape, bf16) for s in shards),
        (
            pltpu.SemaphoreType.DMA((arrays,)),
            pltpu.SemaphoreType.DMA((arrays, count + 2)),
            pltpu.SemaphoreType.DMA((arrays, count)),
            pltpu.SemaphoreType.DMA((arrays, 2)),
            pltpu.SemaphoreType.DMA((arrays, size, count)),
            pltpu.SemaphoreType.DMA((arrays,)),
            pltpu.SemaphoreType.DMA((arrays,)),
        ),
        (pltpu.VMEM,) * arrays,
        (pl.ANY,) * arrays,
        sum(s.size * 2 for s in shards) * 24,
    )
    return [o.reshape(size * count * MB * s.shape[0], s.shape[1]) for o, s in zip(outs, shards)]


def add_rows(dst, first, *others):
    rows = dst.shape[0]
    step = min(rows, 16)

    def one(i, _):
        at = pl.ds(pl.multiple_of(i * step, step), step)
        total = first[at, :].astype(f32)
        for other in others:
            total = total + other[at, :].astype(f32)
        dst[at, :] = total.astype(dst.dtype)
        return 0

    lax.fori_loop(0, rows // step, one, 0)


def reduce_kernel(*refs):
    arrays = 2 * LAYERS
    grads = refs[:arrays]
    outs = refs[arrays : 2 * arrays]
    held, given, come, chained = (
        refs[(2 + i) * arrays : (3 + i) * arrays] for i in range(4)
    )
    load_sem, mate_send, mate_recv, ring_send, ring_recv, z_send, z_recv = refs[6 * arrays :]
    dp = lax.axis_index("dp")
    me = lax.axis_index("fsdp")
    size = lax.axis_size("dp")
    count = lax.axis_size("fsdp") // MB
    core = me % MB
    k = me // MB
    ring = snake(dp, size)
    reach = size // 2
    right = snake(wrap(ring + 1, size), size)
    left = snake(wrap(ring - 1, size), size)
    mate = k * MB + 1 - core
    up, down = me + MB, me - MB
    has_up, has_down = k < count - 1, k > 0

    def load(a):
        return pltpu.make_async_copy(grads[a].at[:, :, core], held[a], load_sem.at[a])

    for a in range(arrays):
        load(a).start()
    barrier = pltpu.get_barrier_semaphore()
    for target in ((right, me), (left, me), (dp, mate)):
        pl.semaphore_signal(barrier, inc=1, device_id=target, device_id_type=MESH)

    @pl.when(has_up)
    def _():
        pl.semaphore_signal(barrier, inc=1, device_id=(dp, up), device_id_type=MESH)

    @pl.when(has_down)
    def _():
        pl.semaphore_signal(barrier, inc=1, device_id=(dp, down), device_id_type=MESH)

    pl.semaphore_wait(barrier, 3 + jnp.where(has_up, 1, 0) + jnp.where(has_down, 1, 0))

    def away(j, side):
        return snake(wrap(ring + j if side == 0 else ring - j, size), size)

    def to_mate(a, d):
        return remote(
            grads[a].at[d, :, 1 - core], given[a].at[d], mate_send.at[a], mate_recv.at[a, d], dp, mate
        )

    def carried(a, side):
        return (a < arrays // 2) == (side == 0)

    def targets(j):
        if j == 0:
            return [dp]
        if j == reach:
            return [away(j, 0)]
        return [away(j, 0), away(j, 1)]

    for j in range(reach, -1, -1):
        for d in targets(j):
            for a in range(arrays):
                to_mate(a, d).start()

    for a in range(arrays):
        load(a).wait()

    def add_mate(d):
        for a in range(arrays):
            to_mate(a, d).wait_recv()

            def one(z, _, a=a):
                add_rows(held[a].at[d, z], held[a].at[d, z], given[a].at[d, z])
                return 0

            lax.fori_loop(0, count, one, 0)

    def first_step(a, side):
        d = away(reach, 0)
        return remote(
            held[a].at[d], come[a].at[side, 0], ring_send.at[a, side], ring_recv.at[a, side, 0, 0],
            right if side == 0 else left, me,
        )

    def next_step(a, side, s, z):
        d = away(reach - s, side)
        return remote(
            held[a].at[d, z], come[a].at[side, s, z], ring_send.at[a, side],
            ring_recv.at[a, side, s, z], right if side == 0 else left, me,
        )

    far_most = jnp.maximum(k, count - 1 - k)
    near_most = jnp.minimum(k, count - 1 - k)
    uneven = far_most - near_most
    long_side = jnp.where(count - 1 - k > k, 1, -1)

    def chunk_at(i):
        j = jnp.maximum(i - uneven, 0)
        paired = k + (1 - 2 * (j % 2)) * (near_most - j // 2)
        return jnp.where(i < uneven, k + long_side * (far_most - i), paired)

    add_mate(away(reach, 0))
    for a in range(arrays):
        first_step(a, 0 if carried(a, 0) else 1).start()
    for s in range(1, reach):
        for side in (0, 1):
            add_mate(away(reach - s, side))
        if s == 1:
            for a in range(arrays):
                first_step(a, 0 if carried(a, 0) else 1).wait_recv()

        def pass_on(i, _, s=s):
            z = chunk_at(i)
            for side in (0, 1):
                d = away(reach - s, side)
                for a in range(arrays):
                    if s > 1:
                        next_step(a, side, s - 1, z).wait_recv()
                    if s > 1 or carried(a, side):
                        add_rows(held[a].at[d, z], held[a].at[d, z], come[a].at[side, s - 1, z])
                    next_step(a, side, s, z).start()
            return 0

        lax.fori_loop(0, count, pass_on, 0)
    add_mate(dp)

    def along(a, side, z):
        return remote(
            held[a].at[dp, z], chained[a].at[side, z], z_send.at[a, z], z_recv.at[a, side, z],
            dp, up if side == 0 else down,
        )

    def finish(i, _):
        z = chunk_at(i)
        for a in range(arrays):
            for side in (0, 1):
                next_step(a, side, reach - 1, z).wait_recv()
            add_rows(
                held[a].at[dp, z],
                held[a].at[dp, z],
                come[a].at[0, reach - 1, z],
                come[a].at[1, reach - 1, z],
            )
            for side in (0, 1):
                beyond = z > k if side == 0 else z < k
                fed = has_down if side == 0 else has_up

                @pl.when(jnp.logical_and(fed, jnp.logical_or(beyond, z == k)))
                def _(a=a, side=side):
                    along(a, side, z).wait_recv()
                    add_rows(held[a].at[dp, z], held[a].at[dp, z], chained[a].at[side, z])

                @pl.when(beyond)
                def _(a=a, side=side):
                    along(a, side, z).start()

        return 0

    lax.fori_loop(0, count, finish, 0)
    for a in range(arrays):
        add_rows(outs[a], held[a].at[dp, k])
        for side in (0, 1):
            sent = held[a].at[pl.ds(0, reach if carried(a, side) else reach - 1)]
            remote(
                sent, sent, ring_send.at[a, side], ring_recv.at[a, side, 0, 0], dp, mate
            ).wait_send()
        remote(
            given[a], given[a], mate_send.at[a], mate_recv.at[a, 0], dp, mate
        ).wait_send()

    def sent_along(z, _):
        for a in range(arrays):

            @pl.when(z != k)
            def _(a=a):
                along(a, 0, z).wait_send()

        return 0

    lax.fori_loop(0, count, sent_along, 0)


def reduce_layers(grads):
    size, count = lax.axis_size("dp"), lax.axis_size("fsdp") // MB
    arrays = len(grads)
    reach = size // 2
    shards = [(g.shape[0] // (size * count * MB), g.shape[1]) for g in grads]
    blocks = [g.reshape((size, count, MB) + s) for g, s in zip(grads, shards)]
    return comm_call(
        reduce_kernel,
        5,
        blocks,
        tuple((s, f32) for s in shards),
        tuple(pltpu.VMEM((size, count) + s, bf16) for s in shards) * 2
        + tuple(pltpu.VMEM((2, reach, count) + s, bf16) for s in shards)
        + tuple(pltpu.VMEM((2, count) + s, bf16) for s in shards)
        + (
            pltpu.SemaphoreType.DMA((arrays,)),
            pltpu.SemaphoreType.DMA((arrays,)),
            pltpu.SemaphoreType.DMA((arrays, size)),
            pltpu.SemaphoreType.DMA((arrays, 2)),
            pltpu.SemaphoreType.DMA((arrays, 2, reach, count)),
            pltpu.SemaphoreType.DMA((arrays, count)),
            pltpu.SemaphoreType.DMA((arrays, 2, count)),
        ),
        (pl.ANY,) * arrays,
        (pltpu.VMEM,) * arrays,
        sum(g.size * 2 for g in grads),
    )


def pair_lanes(p):
    return pl.ds(pl.multiple_of(p * LANES, LANES), LANES)


def first_half(rows):
    return lax.broadcasted_iota(jnp.int32, (rows, LANES), 1) < HDIM


def spread_columns(values, column, per_pair, rows):
    half = first_half(rows)
    for p in range(PAIRS):
        left = jnp.broadcast_to(values[:, 2 * p : 2 * p + 1], (rows, LANES))
        right = jnp.broadcast_to(values[:, 2 * p + 1 : 2 * p + 2], (rows, LANES))
        if column is not None:
            column[2 * p] = left
            column[2 * p + 1] = right
        if per_pair is not None:
            per_pair[p] = jnp.where(half, left, right)


def front_kernel(
    proj_ref, halo_ref, cw_ref, cb_ref, dtb_ref, al_ref, sk_ref,
    pre_ref, y_ref, st_ref, dt_ref, cum_ref,
    pad, col, tcol, lcol, lrow,
):
    rows = proj_ref.shape[0]
    pad[0:8, :] = halo_ref[...]
    pad[8:, :] = proj_ref[:, DI : DI + XBC]

    def conv(i, _):
        xs = pair_lanes(i)
        out = jnp.broadcast_to(cb_ref[0:1, xs], (rows, LANES))
        for k in range(CONV):
            out = out + cw_ref[k : k + 1, xs] * pad[5 + k : 5 + k + rows, xs]
        pre_ref[:, xs] = out
        return 0

    lax.fori_loop(0, XBC // LANES, conv, 0)

    dt_ref[...] = jnp.zeros((rows, LANES), f32)
    dt_ref[:, 0:HEADS] = proj_ref[:, DI + XBC :]
    drive = dt_ref[...] + dtb_ref[...]
    dt = jnp.maximum(drive, 0.0) + jnp.log1p(jnp.exp(-jnp.abs(drive)))
    dt_ref[...] = dt
    rate = dt * (-jnp.exp(al_ref[...]))
    ri = lax.broadcasted_iota(jnp.int32, (rows, rows), 0)
    ci = lax.broadcasted_iota(jnp.int32, (rows, rows), 1)
    causal = ri >= ci
    cum = dot_nn(jnp.where(causal, 1.0, 0.0), rate, highest)
    cum_ref[...] = cum
    lrow[...] = cum.T
    spread_columns(cum, col, lcol, rows)
    spread_columns(dt, None, tcol, rows)
    bm = silu(pre_ref[:, DI : DI + NSTATE]).astype(bf16)
    cm = silu(pre_ref[:, DI + NSTATE :]).astype(bf16)
    cb = dot_nt(cm, bm)
    half = first_half(rows)

    def pair(p, _):
        xs = pair_lanes(p)
        x = silu(pre_ref[:, xs])
        xt = tcol[p] * x
        xtb = xt.astype(bf16)
        parts = []
        for j in range(2):
            h = 2 * p + j
            c = col[h]
            d = jnp.concatenate([c] * (rows // LANES), axis=1) - lrow[pl.ds(h, 1), :]
            m = (jnp.exp(jnp.where(causal, d, OFF)) * cb).astype(bf16)
            parts.append(dot_nn(m, xtb))
        y_ref[:, xs] = jnp.where(half, parts[0], parts[1]) + sk_ref[0:1, xs] * x
        lp = lcol[p]
        tail = jnp.exp(lp[rows - 1 : rows, :] - lp)
        st_ref[xs, :] = dot_tn((tail * xt).astype(bf16), bm)
        return 0

    lax.fori_loop(0, PAIRS, pair, 0)


def gate_kernel(
    y0_ref, proj_ref, pre_ref, cum_ref, sin_ref, gg_ref, y_ref, yn_ref, lcol
):
    rows = y0_ref.shape[0]
    spread_columns(cum_ref[...], None, lcol, rows)
    cm = silu(pre_ref[:, DI + NSTATE :]).astype(bf16)

    def pair(p, total):
        xs = pair_lanes(p)
        y = y0_ref[:, xs] + jnp.exp(lcol[p]) * dot_nt(cm, sin_ref[xs, :])
        y_ref[:, xs] = y
        g = y * silu(proj_ref[:, xs])
        return total + g * g

    total = lax.fori_loop(0, PAIRS, pair, jnp.zeros((rows, LANES), f32))
    scale = lax.rsqrt(jnp.sum(total, axis=1, keepdims=True) / DI + epsilon)

    def put(p, _):
        xs = pair_lanes(p)
        g = y_ref[:, xs] * silu(proj_ref[:, xs])
        yn_ref[:, xs] = (g * scale * gg_ref[0:1, xs]).astype(bf16)
        return 0

    lax.fori_loop(0, PAIRS, put, 0)


def ungate_kernel(
    dyn_ref, y_ref, proj_ref, pre_ref, cum_ref, gg_ref,
    dy_ref, dz_ref, dgg_ref, gst_ref, lcol,
):
    rows = y_ref.shape[0]
    spread_columns(cum_ref[...], None, lcol, rows)
    cm = silu(pre_ref[:, DI + NSTATE :]).astype(bf16)
    zero = jnp.zeros((rows, LANES), f32)

    def sums(p, carry):
        xs = pair_lanes(p)
        g = y_ref[:, xs] * silu(proj_ref[:, xs])
        return carry[0] + g * g, carry[1] + g * (dyn_ref[:, xs] * gg_ref[0:1, xs])

    square, cross = lax.fori_loop(0, PAIRS, sums, (zero, zero))
    scale = lax.rsqrt(jnp.sum(square, axis=1, keepdims=True) / DI + epsilon)
    mean = jnp.sum(cross, axis=1, keepdims=True) * scale / DI

    def pair(p, _):
        xs = pair_lanes(p)
        z = proj_ref[:, xs]
        y = y_ref[:, xs]
        sz = silu(z)
        ghat = y * sz * scale
        dyn = dyn_ref[:, xs]
        dgg_ref[0:1, xs] = jnp.sum(dyn * ghat, axis=0, keepdims=True)
        dg = scale * (dyn * gg_ref[0:1, xs] - ghat * mean)
        dy = dg * sz
        dy_ref[:, xs] = dy
        dz_ref[:, xs] = (dg * y * silu_grad(z)).astype(bf16)
        gst_ref[xs, :] = dot_tn((jnp.exp(lcol[p]) * dy).astype(bf16), cm)
        return 0

    lax.fori_loop(0, PAIRS, pair, 0)


def back_kernel(
    dy_ref, y_ref, proj_ref, halo_ref, pre_ref, dt_ref, cum_ref, sin_ref, gin_ref,
    cw_ref, dtb_ref, al_ref, sk_ref,
    dx_ref, dhalo_ref, ddr_ref, dcw_ref, dsm_ref,
    pad, grad, col, tcol, lcol, lrow, dcb, dbm, dcm, dlog, dtx, ends,
):
    rows = y_ref.shape[0]
    pad[0:8, :] = halo_ref[...]
    pad[8:, :] = proj_ref[:, DI : DI + XBC]
    grad[0:8, :] = jnp.zeros((8, XBC), f32)
    grad[rows + 8 :, :] = jnp.zeros((8, XBC), f32)
    cum = cum_ref[...]
    dt = dt_ref[...]
    lrow[...] = cum.T
    spread_columns(cum, col, lcol, rows)
    spread_columns(dt, None, tcol, rows)
    bm = silu(pre_ref[:, DI : DI + NSTATE]).astype(bf16)
    cm = silu(pre_ref[:, DI + NSTATE :]).astype(bf16)
    cbt = dot_nt(bm, cm)
    ri = lax.broadcasted_iota(jnp.int32, (rows, rows), 0)
    ci = lax.broadcasted_iota(jnp.int32, (rows, rows), 1)
    causal = ri <= ci
    half = first_half(rows)
    dcb[...] = jnp.zeros((rows, rows), f32)
    zero = jnp.zeros((rows, LANES), f32)
    dbm[...] = zero
    dcm[...] = zero
    dlog[...] = zero
    dtx[...] = zero
    ends[...] = jnp.zeros((16, LANES), f32)
    lane_row = lax.broadcasted_iota(jnp.int32, (LANES, LANES), 0)
    lane_col = lax.broadcasted_iota(jnp.int32, (LANES, LANES), 1)
    ones = jnp.ones((8, NSTATE), f32)

    def pair(p, _):
        xs = pair_lanes(p)
        pre = pre_ref[:, xs]
        x = silu(pre)
        tp = tcol[p]
        xt = tp * x
        dy = dy_ref[:, xs]
        dyb = dy.astype(bf16)
        parts = []
        for j in range(2):
            h = 2 * p + j
            c = col[h]
            d = lrow[pl.ds(h, 1), :] - jnp.concatenate([c] * (rows // LANES), axis=1)
            w = jnp.exp(jnp.where(causal, d, OFF))
            parts.append(dot_nn((w * cbt).astype(bf16), dyb))
            own = half if j == 0 else jnp.logical_not(half)
            q = dot_nt(jnp.where(own, xt, 0.0).astype(bf16), dyb)
            dcb[...] += w * q
        lp = lcol[p]
        last = lp[rows - 1 : rows, :]
        tail = jnp.exp(last - lp)
        gin = gin_ref[xs, :]
        sin = sin_ref[xs, :]
        dst = tail * dot_nt(bm, gin)
        dxt = jnp.where(half, parts[0], parts[1]) + dst
        dbm[...] += dot_nn((tail * xt).astype(bf16), gin)
        dcm[...] += dot_nn((jnp.exp(lp) * dy).astype(bf16), sin)
        sk = sk_ref[0:1, xs]
        pick = jnp.where(lane_col == 2 * p + jnp.where(lane_row >= HDIM, 1, 0), 1.0, 0.0)
        dlog[...] += dot_nn(dy * (y_ref[:, xs] - sk * x) - xt * dxt, pick, highest)
        dtx[...] += dot_nn(x * dxt, pick, highest)
        held = dot_nt(ones, gin.astype(f32) * sin.astype(f32), highest)
        end = jnp.sum(xt * dst, axis=0, keepdims=True) + jnp.exp(last) * held[0:1, :]
        skip = jnp.sum(dy * x, axis=0, keepdims=True)
        stacked = jnp.concatenate(
            [jnp.broadcast_to(end, (8, LANES)), jnp.broadcast_to(skip, (8, LANES))], axis=0
        )
        ends[...] += dot_nn(stacked, pick, highest)
        grad[pl.ds(8, rows), xs] = (tp * dxt + sk * dy) * silu_grad(pre)
        return 0

    lax.fori_loop(0, PAIRS, pair, 0)
    dcbb = dcb[...].astype(bf16)
    dc = dcm[...] + dot_tn(dcbb, bm)
    db = dbm[...] + dot_nn(dcbb, cm)
    grad[8 : 8 + rows, DI : DI + NSTATE] = db * silu_grad(pre_ref[:, DI : DI + NSTATE])
    grad[8 : 8 + rows, DI + NSTATE :] = dc * silu_grad(pre_ref[:, DI + NSTATE :])

    last_row = lax.broadcasted_iota(jnp.int32, (rows, LANES), 0) == rows - 1
    dl = dlog[...] + jnp.where(last_row, ends[0:1, :], 0.0)
    da = dot_nn(jnp.where(causal, 1.0, 0.0), dl, highest)
    decay = -jnp.exp(al_ref[...])
    ddt = dtx[...] + da * decay
    ddr_ref[...] = jnp.zeros((rows, LANES), f32)
    ddr_ref[:, 0:HEADS] = proj_ref[:, DI + XBC :]
    ddr = ddt * lax.logistic(ddr_ref[...] + dtb_ref[...])
    ddr_ref[...] = ddr
    dsm_ref[...] = jnp.zeros((8, LANES), f32)
    dsm_ref[0:1, :] = jnp.sum(ddr, axis=0, keepdims=True)
    dsm_ref[1:2, :] = jnp.sum(da * dt, axis=0, keepdims=True) * decay
    dsm_ref[2:3, :] = ends[8:9, :]

    def conv(i, _):
        xs = pair_lanes(i)
        own = grad[pl.ds(8, rows), xs]
        out = jnp.zeros((rows, LANES), f32)
        edge = jnp.zeros((8, LANES), f32)
        for k in range(CONV):
            wk = cw_ref[k : k + 1, xs]
            out = out + wk * grad[11 - k : 11 - k + rows, xs]
            edge = edge + wk * grad[3 - k : 11 - k, xs]
            dcw_ref[k : k + 1, xs] = jnp.sum(
                own * pad[5 + k : 5 + k + rows, xs], axis=0, keepdims=True
            )
        dcw_ref[4:5, xs] = jnp.sum(own, axis=0, keepdims=True)
        dx_ref[:, xs] = out
        dhalo_ref[:, xs] = edge
        return 0

    lax.fori_loop(0, XBC // LANES, conv, 0)


VTILE = 1280
NTILE = 256


def head_specs(width, tokens):
    return dict(
        table=pl.BlockSpec((VTILE, width), lambda i: (i, 0)),
        hidden=pl.BlockSpec((tokens, width), lambda i: (0, 0)),
        kept=pl.BlockSpec((VTILE, tokens), lambda i: (i, 0)),
        row=pl.BlockSpec((1, tokens), lambda i: (0, 0)),
        tile_row=pl.BlockSpec((1, 1, tokens), lambda i: (i, 0, 0)),
    )


def head_call(kernel, grid, in_specs, out_specs, outs, scratch, ins, cells):
    return pl.pallas_call(
        kernel,
        grid=(grid,),
        in_specs=in_specs,
        out_specs=out_specs,
        out_shape=[jax.ShapeDtypeStruct(shape, kind) for shape, kind in outs],
        scratch_shapes=list(scratch),
        compiler_params=pltpu.CompilerParams(
            dimension_semantics=("arbitrary",), vmem_limit_bytes=VMEM_LIMIT
        ),
        cost_estimate=pl.CostEstimate(
            flops=2 * cells * D, transcendentals=cells, bytes_accessed=4 * cells
        ),
    )(*ins)


UNROLL = 8


def head_stats_kernel(
    table_ref, own_ref, lab_ref, w_ref,
    q_ref, all_ref, lse_ref, fac_ref, hit_ref,
    kept, tops, sums, hits, shown, own_sem, put_sem, z_send, z_recv, m_send, m_recv, s_send, s_recv,
):
    dp = lax.axis_index("dp")
    me = lax.axis_index("fsdp")
    shards = lax.axis_size("fsdp")
    count = shards // MB
    core = me % MB
    k = me // MB
    mate = k * MB + 1 - core
    vocab_rows = table_ref.shape[0]
    rows = own_ref.shape[0]
    tiles = tops.shape[0]
    barrier = pltpu.get_barrier_semaphore()
    for other in range(1, shards):
        pl.semaphore_signal(
            barrier, inc=1, device_id=(dp, lax.rem(me + other, shards)), device_id_type=MESH
        )
    pl.semaphore_wait(barrier, shards - 1)

    near = jnp.minimum(k, count - 1 - k)
    long_side = jnp.where(count - 1 - k > k, 1, -1)

    def chunk_at(i):
        paired = k + (2 * (i % 2) - 1) * ((i + 1) // 2)
        return jnp.where(i <= 2 * near, paired, k + long_side * (i - near))

    def along(z):
        return remote(
            own_ref, all_ref.at[me], z_send.at[z], z_recv.at[k], dp, z * MB + core
        )

    def landed(z):
        return remote(
            own_ref, all_ref.at[z * MB + core], z_send.at[z], z_recv.at[z], dp, me
        )

    def to_mate(z):
        at = all_ref.at[z * MB + core]
        return remote(at, at, m_send.at[z], m_recv.at[z], dp, mate)

    def from_mate(z):
        at = all_ref.at[z * MB + 1 - core]
        return remote(at, at, m_send.at[z], m_recv.at[z], dp, mate)

    keep = pltpu.make_async_copy(own_ref, all_ref.at[me], own_sem)
    keep.start()
    for i in range(1, count):
        along(chunk_at(i)).start()
    keep.wait()
    to_mate(k).start()
    whole = vocab_rows - vocab_rows % 16
    for slot in range(2):
        kept[slot, whole:, :] = jnp.zeros((kept.shape[1] - whole, rows), bf16)

    def put(step, b):
        return pltpu.make_async_copy(
            kept.at[step % 2],
            q_ref.at[:, pl.ds(pl.multiple_of(b * rows, rows), rows)],
            put_sem.at[step % 2],
        )

    def block(step, b):
        @pl.when(step >= 2)
        def _():
            put(step, b).wait()

        slot = step % 2
        ns = pl.ds(pl.multiple_of(b * rows, rows), rows)
        h = all_ref[b]
        label = lab_ref[0:1, ns]
        for t in range(tiles):
            first = t * VTILE
            size = min(VTILE, vocab_rows - first)
            logits = dot_nt(table_ref[first : first + size, :], h)
            top = jnp.max(logits, axis=0, keepdims=True)
            p = jnp.exp(logits - top)
            kept[slot, first : first + size, :] = p.astype(bf16)
            tops[t, 0:1, ns] = top
            sums[t, 0:1, ns] = jnp.sum(p, axis=0, keepdims=True)
            rid = lax.broadcasted_iota(jnp.int32, (size, rows), 0)
            hits[t, 0:1, ns] = jnp.sum(
                jnp.where(rid == label - first, logits, 0.0), axis=0, keepdims=True
            )
        put(step, b).start()

    def chunk(i, _):
        z = chunk_at(i)

        @pl.when(i > 0)
        def _():
            landed(z).wait_recv()
            to_mate(z).start()

        block(2 * i, z * MB + core)
        from_mate(z).wait_recv()
        block(2 * i + 1, z * MB + 1 - core)
        return 0

    lax.fori_loop(0, count, chunk, 0)
    top = tops[0, 0:1, :]
    for t in range(1, tiles):
        top = jnp.maximum(top, tops[t, 0:1, :])
    total = jnp.zeros_like(top)
    hit = jnp.zeros_like(top)
    for t in range(tiles):
        total = total + sums[t, 0:1, :] * jnp.exp(tops[t, 0:1, :] - top)
        hit = hit + hits[t, 0:1, :]
    hit_ref[...] = hit
    shown[me, 0:1, :] = top
    shown[me, 1:2, :] = total

    def tell(other):
        at = shown.at[me]
        return remote(
            at, at, s_send.at[other], s_recv.at[me], dp, lax.rem(me + other, shards)
        )

    def told(other):
        at = shown.at[lax.rem(me + other, shards)]
        return remote(
            at, at, s_send.at[other], s_recv.at[lax.rem(me + other, shards)], dp, mate
        )

    for other in range(1, shards):
        tell(other).start()
    for other in range(1, shards):
        told(other).wait_recv()
    top = shown[0, 0:1, :]
    for f in range(1, shards):
        top = jnp.maximum(top, shown[f, 0:1, :])
    total = jnp.zeros_like(top)
    for f in range(shards):
        total = total + shown[f, 1:2, :] * jnp.exp(shown[f, 0:1, :] - top)
    lse = top + jnp.log(total)
    lse_ref[...] = lse
    scale = w_ref[...] * (1.0 + 2.0 * z_weight * lse)
    for t in range(tiles):
        fac_ref[t, 0:1, :] = scale * jnp.exp(tops[t, 0:1, :] - lse)
    for other in range(1, shards):
        tell(other).wait_send()
    for i in range(1, count):
        along(chunk_at(i)).wait_send()
    for z in range(count):
        to_mate(z).wait_send()
    put(0, 0).wait()
    put(1, 0).wait()


def head_stats(table, own, labels, weight):
    vocab_rows, width = table.shape
    rows = own.shape[0]
    shards = lax.axis_size("fsdp")
    count = shards // MB
    tokens = shards * rows
    tiles = pl.cdiv(vocab_rows, VTILE)
    kept, everyone, lse, fac, hit = comm_call(
        head_stats_kernel,
        6,
        (table, own, labels, weight),
        (
            ((tiles * VTILE, tokens), bf16),
            ((shards, rows, width), bf16),
            ((1, tokens), f32),
            ((tiles, 1, tokens), f32),
            ((1, tokens), f32),
        ),
        (
            pltpu.VMEM((2, tiles * VTILE, rows), bf16),
            pltpu.VMEM((tiles, 1, tokens), f32),
            pltpu.VMEM((tiles, 1, tokens), f32),
            pltpu.VMEM((tiles, 1, tokens), f32),
            pltpu.VMEM((shards, 2, tokens), f32),
            pltpu.SemaphoreType.DMA,
            pltpu.SemaphoreType.DMA((2,)),
            pltpu.SemaphoreType.DMA((count,)),
            pltpu.SemaphoreType.DMA((count,)),
            pltpu.SemaphoreType.DMA((count,)),
            pltpu.SemaphoreType.DMA((count,)),
            pltpu.SemaphoreType.DMA((shards,)),
            pltpu.SemaphoreType.DMA((shards,)),
        ),
        (pltpu.VMEM,) * 4,
        (pl.ANY, pltpu.VMEM, pltpu.VMEM, pltpu.VMEM, pltpu.VMEM),
        own.size * 2 * 7,
    )
    return kept, everyone.reshape(tokens, width), lse, fac, hit


def logit_grads(q, fac, weight, rid, label):
    other = weight * (0.1 / VOCAB)
    return (q.astype(f32) * fac - jnp.where(rid == label, other + 0.9 * weight, other)).astype(bf16)


def head_rows_kernel(vocab_rows, e_ref, q_ref, fac_ref, w_ref, lab_ref, out_ref, acc, et):
    step = pl.program_id(0)
    first = step * VTILE
    tokens = q_ref.shape[1]

    @pl.when(step == 0)
    def _():
        acc[...] = jnp.zeros(acc.shape, f32)

    eid = lax.broadcasted_iota(jnp.int32, (VTILE, e_ref.shape[1]), 0)
    et[...] = jnp.where(eid < vocab_rows - first, e_ref[...].astype(f32), 0.0).T.astype(bf16)

    def chunk(j, _):
        ns = pl.ds(pl.multiple_of(j * NTILE, NTILE), NTILE)
        rid = lax.broadcasted_iota(jnp.int32, (VTILE, NTILE), 0)
        dl = logit_grads(
            q_ref[:, ns], fac_ref[0, 0:1, ns], w_ref[0:1, ns], rid, lab_ref[0:1, ns] - first
        )
        acc[:, ns] += dot_nn(et[...], dl)
        return 0

    lax.fori_loop(0, tokens // NTILE, chunk, 0, unroll=UNROLL)

    @pl.when(step == pl.num_programs(0) - 1)
    def _():
        def put(j, _):
            ns = pl.ds(pl.multiple_of(j * NTILE, NTILE), NTILE)
            out_ref[ns, :] = acc[:, ns].T.astype(bf16)
            return 0

        lax.fori_loop(0, tokens // NTILE, put, 0)


def head_rows(table, kept, fac, weight, labels):
    vocab_rows, width = table.shape
    tokens = kept.shape[1]
    sp = head_specs(width, tokens)
    return head_call(
        functools.partial(head_rows_kernel, vocab_rows),
        pl.cdiv(vocab_rows, VTILE),
        [sp["table"], sp["kept"], sp["tile_row"], sp["row"], sp["row"]],
        [sp["hidden"]],
        [((tokens, width), bf16)],
        (pltpu.VMEM((width, tokens), f32), pltpu.VMEM((width, VTILE), bf16)),
        (table, kept, fac, weight, labels),
        vocab_rows * tokens,
    )[0]


def head_table_kernel(h_ref, q_ref, fac_ref, w_ref, lab_ref, out_ref, dl_ref):
    first = pl.program_id(0) * VTILE
    tokens = q_ref.shape[1]

    def chunk(j, _):
        ns = pl.ds(pl.multiple_of(j * NTILE, NTILE), NTILE)
        rid = lax.broadcasted_iota(jnp.int32, (VTILE, NTILE), 0)
        dl_ref[:, ns] = logit_grads(
            q_ref[:, ns], fac_ref[0, 0:1, ns], w_ref[0:1, ns], rid, lab_ref[0:1, ns] - first
        )
        return 0

    lax.fori_loop(0, tokens // NTILE, chunk, 0, unroll=UNROLL)

    def cols(j, _):
        ds = pl.ds(pl.multiple_of(j * 256, 256), 256)
        out_ref[:, ds] = dot_nn(dl_ref[...], h_ref[:, ds]).astype(bf16)
        return 0

    lax.fori_loop(0, h_ref.shape[1] // 256, cols, 0, unroll=True)


def head_table(hidden, kept, fac, weight, labels, vocab_rows):
    tokens, width = hidden.shape
    sp = head_specs(width, tokens)
    return head_call(
        head_table_kernel,
        pl.cdiv(vocab_rows, VTILE),
        [sp["hidden"], sp["kept"], sp["tile_row"], sp["row"], sp["row"]],
        [sp["table"]],
        [((vocab_rows, width), bf16)],
        (pltpu.VMEM((VTILE, tokens), bf16),),
        (hidden, kept, fac, weight, labels),
        vocab_rows * tokens,
    )[0]


def weight_grads_kernel(u_ref, dp_ref, yn_ref, db_ref, in_ref, out_ref):
    wide_cols = dp_ref.shape[1]
    for c in range(0, wide_cols, 1024):
        cs = pl.ds(c, min(1024, wide_cols - c))
        in_ref[:, cs] = dot_tn(u_ref[...], dp_ref[:, cs]).astype(bf16)
    out_ref[...] = dot_tn(yn_ref[...], db_ref[...]).astype(bf16)


def weight_grads(normed, grad_proj, mixed, grad_branch):
    rows = normed.shape[0]
    steps = D // LANES
    part = DI // steps
    return head_call(
        weight_grads_kernel,
        steps,
        [
            pl.BlockSpec((rows, LANES), lambda i: (0, i)),
            pl.BlockSpec((rows, ZW), lambda i: (0, 0)),
            pl.BlockSpec((rows, part), lambda i: (0, i)),
            pl.BlockSpec((rows, D), lambda i: (0, 0)),
        ],
        [pl.BlockSpec((LANES, ZW), lambda i: (i, 0)), pl.BlockSpec((part, D), lambda i: (i, 0))],
        [((D, ZW), bf16), ((DI, D), bf16)],
        (),
        (normed, grad_proj, mixed, grad_branch),
        rows * (ZW + DI),
    )


def shift_chunks(block, distance):
    size = lax.axis_size("fsdp")
    route = [(i - 2 * distance, i) for i in range(size) if 0 <= i - 2 * distance < size]
    return lax.ppermute(block, "fsdp", route)


def after(value, earlier):
    return lax.optimization_barrier((value, earlier))[0]


def norm_scale(values):
    return lax.rsqrt(jnp.mean(values * values, axis=-1, keepdims=True) + epsilon)


def norm_back(grad, values, gain):
    scale = norm_scale(values)
    unit = values * scale
    inner = grad * gain
    back = scale * (inner - unit * jnp.mean(inner * unit, axis=-1, keepdims=True))
    return back, jnp.sum(grad * unit, axis=0)


def wide(row):
    return jnp.pad(row, (0, LANES - row.shape[0]))[None]


def layer_vectors(vector_params, layer_index):
    offset = layer_index * PER
    pieces = []
    for size in (CONV * XBC, XBC, HEADS, HEADS, HEADS, D, DI):
        pieces.append(vector_params[offset : offset + size])
        offset += size
    conv_w, conv_b, dt_bias, decay_log, skip, pre_gain, gate_gain = pieces
    return dict(
        conv_w=conv_w.reshape(CONV, XBC),
        conv_b=conv_b[None],
        dt_bias=wide(dt_bias),
        decay_log=wide(decay_log),
        skip=jnp.repeat(skip, HDIM)[None],
        pre_gain=pre_gain,
        gate_gain=gate_gain[None],
    )


def layer_forward(hidden, w_in, w_out, vec):
    rows = hidden.shape[0]
    normed = (hidden * norm_scale(hidden) * vec["pre_gain"]).astype(bf16)
    proj = jnp.dot(normed, w_in, preferred_element_type=f32)
    halo = shift_chunks(proj[rows - 8 :, DI : DI + XBC], 1)
    pre, y0, local, dt, cum = local_call(
        front_kernel,
        (proj, halo, vec["conv_w"], vec["conv_b"], vec["dt_bias"], vec["decay_log"], vec["skip"]),
        (
            ((rows, XBC), f32),
            ((rows, DI), f32),
            ((DI, NSTATE), f32),
            ((rows, LANES), f32),
            ((rows, LANES), f32),
        ),
        scratch=(
            pltpu.VMEM((rows + 8, XBC), f32),
            pltpu.VMEM((HEADS, rows, LANES), f32),
            pltpu.VMEM((PAIRS, rows, LANES), f32),
            pltpu.VMEM((PAIRS, rows, LANES), f32),
            pltpu.VMEM((LANES, rows), f32),
        ),
    )
    decay = jnp.exp(cum[rows - 1, :HEADS])
    entering = carry_chain(decay, local, 1)
    y, mixed = local_call(
        gate_kernel,
        (y0, proj, pre, cum, entering, vec["gate_gain"]),
        (((rows, DI), f32), ((rows, DI), bf16)),
        scratch=(pltpu.VMEM((PAIRS, rows, LANES), f32),),
    )
    branch = jnp.dot(mixed, w_out, preferred_element_type=f32)
    record = (hidden, normed, proj, halo, pre, dt, cum, decay, entering, y, mixed)
    return hidden + branch, record


def layer_backward(grad_hidden, w_in, w_out, vec, record):
    hidden, normed, proj, halo, pre, dt, cum, decay, entering, y, mixed = record
    rows = hidden.shape[0]
    grad_branch = grad_hidden.astype(bf16)
    grad_mixed = dot_nt(grad_branch, w_out)
    dy, dz, dgate, gstate = local_call(
        ungate_kernel,
        (grad_mixed, y, proj, pre, cum, vec["gate_gain"]),
        (
            ((rows, DI), f32),
            ((rows, DI), bf16),
            ((1, DI), f32),
            ((DI, NSTATE), f32),
        ),
        scratch=(pltpu.VMEM((PAIRS, rows, LANES), f32),),
    )
    later = carry_chain(decay, gstate, -1)
    dx, dhalo, ddr, dconv, dsmall = local_call(
        back_kernel,
        (
            dy, y, proj, halo, pre, dt, cum, entering, later,
            vec["conv_w"], vec["dt_bias"], vec["decay_log"], vec["skip"],
        ),
        (
            ((rows, XBC), f32),
            ((8, XBC), f32),
            ((rows, LANES), f32),
            ((8, XBC), f32),
            ((8, LANES), f32),
        ),
        scratch=(
            pltpu.VMEM((rows + 8, XBC), f32),
            pltpu.VMEM((rows + 16, XBC), f32),
            pltpu.VMEM((HEADS, rows, LANES), f32),
            pltpu.VMEM((PAIRS, rows, LANES), f32),
            pltpu.VMEM((PAIRS, rows, LANES), f32),
            pltpu.VMEM((LANES, rows), f32),
            pltpu.VMEM((rows, rows), f32),
            pltpu.VMEM((rows, LANES), f32),
            pltpu.VMEM((rows, LANES), f32),
            pltpu.VMEM((rows, LANES), f32),
            pltpu.VMEM((rows, LANES), f32),
            pltpu.VMEM((16, LANES), f32),
        ),
    )
    from_next = shift_chunks(dhalo, -1)
    dx = jnp.concatenate([dx[: rows - 8], dx[rows - 8 :] + from_next], axis=0)
    grad_proj = jnp.concatenate(
        [dz, dx.astype(bf16), ddr[:, :HEADS].astype(bf16)], axis=1
    )
    grad_normed = dot_nt(grad_proj, w_in)
    grad_in, grad_out = weight_grads(normed, grad_proj, mixed, grad_branch)
    grad_prev, dpre_gain = norm_back(grad_normed, hidden, vec["pre_gain"])
    grad_vec = jnp.concatenate(
        [
            dconv[:CONV].reshape(-1),
            dconv[CONV],
            dsmall[0, :HEADS],
            dsmall[1, :HEADS],
            jnp.sum(dsmall[2:3, :HEADS], axis=0),
            dpre_gain,
            dgate[0],
        ]
    )
    return grad_hidden + grad_prev, grad_in, grad_out, grad_vec


def advance(weight, moment, average, grad, factor):
    scaled = grad * factor
    moment_new = 0.5 * moment + scaled
    weight_new = weight - step_rate * (scaled + 0.5 * moment_new)
    average_new = 0.5 * average + 0.5 * weight_new
    return (weight_new, moment_new, average_new, weight_new.astype(bf16))


def whole_step(
    token_ids,
    target_ids,
    seq_lengths,
    embedding,
    embedding_mom,
    embedding_avg,
    in_proj,
    in_proj_mom,
    in_proj_avg,
    out_proj,
    out_proj_mom,
    out_proj_avg,
    vector_params,
    vector_mom,
    vector_avg,
):
    groups = lax.axis_size("dp")
    shards = lax.axis_size("fsdp")
    group_index = lax.axis_index("dp")
    shard_index = lax.axis_index("fsdp")
    chunks = shards // MB
    seq_rows = token_ids.shape[2]
    rows = seq_rows // chunks
    vocab_rows, own_cols = embedding.shape
    tokens = MB * seq_rows
    total_count = jnp.sum(seq_lengths).astype(f32)
    embed_low = embedding.astype(bf16)
    in_low = in_proj.astype(bf16)
    out_low = out_proj.astype(bf16)

    ids_all = lax.all_gather(token_ids[:, 0, :], "dp", axis=0)
    ids_all = ids_all.reshape(groups, MB, chunks, rows).transpose(2, 1, 0, 3).reshape(-1)
    every = ids_all.shape[0]
    local_ids = ids_all - shard_index * vocab_rows
    inside = (local_ids >= 0) & (local_ids < vocab_rows)
    sorted_ids, sorted_tok = lax.sort(
        (jnp.where(inside, local_ids, vocab_rows), jnp.arange(every, dtype=jnp.int32)),
        num_keys=1,
    )
    held_here = sorted_ids < vocab_rows
    count = jnp.sum(held_here.astype(jnp.int32)).reshape(1)
    row_list = jnp.where(held_here, sorted_ids, 0)
    tok_list = jnp.where(held_here, sorted_tok, every)
    (looked,) = local_call(
        lookup_kernel,
        (count, row_list, tok_list, embedding),
        (((every, own_cols), bf16),),
        scratch=(pltpu.VMEM((every + 8, own_cols), f32),),
        in_smem=(0, 1, 2),
    )
    mine = lax.psum_scatter(
        looked.reshape(shards * groups * rows, own_cols), "fsdp", scatter_dimension=0, tiled=True
    )
    mine = lax.all_to_all(mine.reshape(groups, rows, own_cols), "dp", 0, 0)
    hidden = mine.transpose(1, 0, 2).reshape(rows, D).astype(f32)

    shards = []
    for l in range(LAYERS):
        shards += [in_low[l], out_low[l]]
    shards = after(shards, looked)
    gathered = gather_layers(shards)
    w_in, w_out = gathered[0::2], gathered[1::2]
    embed_low = after(embed_low, gathered)
    table = lax.all_gather(embed_low, "dp", axis=1, tiled=True)

    vecs = [layer_vectors(vector_params, l) for l in range(LAYERS)]
    final_gain = vector_params[LAYERS * PER :]
    records = []
    for l in range(LAYERS):
        hidden, record = layer_forward(hidden, w_in[l], w_out[l], vecs[l])
        records.append(record)

    final_low = (hidden * norm_scale(hidden) * final_gain).astype(bf16)

    def in_order(per_seq):
        return per_seq.reshape(MB, chunks, rows).transpose(1, 0, 2).reshape(1, tokens)

    labels = in_order(target_ids[:, 0, :])
    lengths = lax.dynamic_index_in_dim(seq_lengths, group_index, 1, keepdims=True)
    valid = in_order((jnp.arange(seq_rows)[None, :] < lengths).astype(f32))
    local_labels = labels - shard_index * vocab_rows
    weight = valid / total_count
    kept, group_hidden, lse, fac, target = head_stats(table, final_low, local_labels, weight)
    own_mask = jnp.arange(tokens) // rows == shard_index
    per_row = jnp.where(own_mask, lse[0] + z_weight * lse[0] * lse[0], 0.0)
    loss_sum = jnp.sum((per_row - 0.9 * target[0]) * valid[0])
    own_valid = lax.dynamic_slice_in_dim(valid[0], shard_index * rows, rows)
    hidden_sum = jnp.sum(final_low.astype(f32) * own_valid[:, None], axis=0)
    column_sum = jnp.zeros((groups, own_cols), f32)
    column_sum = jnp.where(
        jnp.arange(groups)[:, None] == group_index, jnp.sum(embed_low.astype(f32), axis=0), column_sum
    ).reshape(D)

    rows_grad = head_rows(table, kept, fac, weight, local_labels)
    own_grad = lax.psum_scatter(
        rows_grad, "fsdp", scatter_dimension=0, tiled=True
    ).astype(f32)
    table_grad = head_table(group_hidden, kept, fac, weight, local_labels, vocab_rows)
    table_part = lax.psum_scatter(table_grad, "dp", scatter_dimension=1, tiled=True)

    grad_hidden, dfinal = norm_back(after(own_grad, table_grad), hidden, final_gain)
    in_parts = [None] * LAYERS
    out_parts = [None] * LAYERS
    vec_parts = [None] * LAYERS
    for l in reversed(range(LAYERS)):
        grad_hidden, grad_in, grad_out, vec_parts[l] = layer_backward(
            grad_hidden, w_in[l], w_out[l], vecs[l], records[l]
        )
        if l == 0:
            sent = grad_hidden.astype(bf16).reshape(rows, groups, own_cols).transpose(1, 0, 2)
            sent = lax.all_to_all(sent, "dp", 0, 0)
            spread = lax.all_gather(sent, "fsdp", axis=0).reshape(every, own_cols)
        in_parts[l], out_parts[l] = grad_in, grad_out
    whole = []
    for l in range(LAYERS):
        whole += [in_parts[l], out_parts[l]]
    summed_parts = reduce_layers(whole)
    spread = after(spread, summed_parts)
    table_total, table_squares = local_call(
        spread_kernel,
        (count, row_list, tok_list, spread, table_part),
        (((vocab_rows, own_cols), f32), ((8, own_cols), f32)),
        scratch=(pltpu.VMEM((every + 8, own_cols), f32),),
        in_smem=(0, 1, 2),
    )
    grad_in_all = jnp.stack(summed_parts[0::2])
    grad_out_all = jnp.stack(summed_parts[1::2])
    owner_squares = (
        jnp.sum(grad_in_all * grad_in_all)
        + jnp.sum(grad_out_all * grad_out_all)
        + jnp.sum(table_squares)
    )
    small = vector_params.shape[0]
    used = small + 2 * D + 2
    padded = pl.cdiv(used, 16 * LANES) * 16 * LANES
    packed = jnp.concatenate(
        vec_parts
        + [
            dfinal,
            hidden_sum,
            column_sum,
            owner_squares.reshape(1),
            loss_sum.reshape(1),
            jnp.zeros((padded - used,), f32),
        ]
    )
    packed = total_of(packed.reshape(-1, LANES)).reshape(-1)
    vector_total = packed[:small]
    hidden_total = packed[small : small + D]
    column_total = packed[small + D : small + 2 * D]
    squares_total = packed[used - 2]
    mean_part = jnp.sum(hidden_total * column_total) * (0.1 / VOCAB)
    loss_total = packed[used - 1] - mean_part
    grad_norm = jnp.sqrt(squares_total + jnp.sum(vector_total * vector_total))
    factor = jnp.minimum(1.0, clip_limit / grad_norm)
    loss_value = loss_total / total_count
    return (
        loss_value,
        grad_norm,
        *advance(embedding, embedding_mom, embedding_avg, table_total, factor),
        *advance(in_proj, in_proj_mom, in_proj_avg, grad_in_all, factor),
        *advance(out_proj, out_proj_mom, out_proj_avg, grad_out_all, factor),
        *advance(vector_params, vector_mom, vector_avg, vector_total, factor),
    )


def solution(mesh):
    table_spec = P("fsdp", "dp")
    weight_spec = P(None, ("dp", "fsdp"), None)
    return jax.shard_map(
        whole_step,
        mesh=mesh,
        in_specs=(
            P(None, "dp", None),
            P(None, "dp", None),
            P(),
            *(table_spec,) * 3,
            *(weight_spec,) * 6,
            *(P(),) * 3,
        ),
        out_specs=(
            P(),
            P(),
            *(table_spec,) * 4,
            *(weight_spec,) * 8,
            *(P(),) * 4,
        ),
        check_vma=False,
    )
```

```python
import functools

import jax
import jax.numpy as jnp
from jax import lax
from jax.experimental import pallas as pl
from jax.experimental.pallas import tpu as pltpu
from jax.sharding import PartitionSpec as P


D = 1024
HEADS = 32
HDIM = 64
NSTATE = 128
CONV = 4
VOCAB = 50288
LAYERS = 2
MB = 2
DI = 2048
XBC = 2304
ZW = 4384
PER = 14688
LANES = 128
PAIRS = DI // LANES

epsilon = 1e-05
z_weight = 0.001
clip_limit = 0.2
step_rate = 1000.0
highest = lax.Precision.HIGHEST
bf16 = jnp.bfloat16
f32 = jnp.float32
VMEM_LIMIT = 62 * 1024 * 1024
OFF = -1e30


def dot_nn(a, b, precision=None):
    return lax.dot_general(
        a, b, (((1,), (0,)), ((), ())), precision=precision, preferred_element_type=f32
    )


def dot_nt(a, b, precision=None):
    return lax.dot_general(
        a, b, (((1,), (1,)), ((), ())), precision=precision, preferred_element_type=f32
    )


def dot_tn(a, b, precision=None):
    return lax.dot_general(
        a, b, (((0,), (0,)), ((), ())), precision=precision, preferred_element_type=f32
    )


def silu(v):
    return v * lax.logistic(v)


def silu_grad(v):
    s = lax.logistic(v)
    return s * (1.0 + v * (1.0 - s))


def local_call(kernel, ins, outs, scratch=(), in_smem=(), flops=0):
    total = sum(a.size * a.dtype.itemsize for a in ins)
    return pl.pallas_call(
        kernel,
        out_shape=[jax.ShapeDtypeStruct(shape, kind) for shape, kind in outs],
        in_specs=[
            pl.BlockSpec(memory_space=pltpu.SMEM if i in in_smem else pltpu.VMEM)
            for i in range(len(ins))
        ],
        out_specs=[pl.BlockSpec(memory_space=pltpu.VMEM) for _ in outs],
        scratch_shapes=list(scratch),
        compiler_params=pltpu.CompilerParams(vmem_limit_bytes=VMEM_LIMIT),
        cost_estimate=pl.CostEstimate(
            flops=flops or total, transcendentals=0, bytes_accessed=2 * total
        ),
    )(*ins)


def lookup_kernel(count_ref, row_ref, tok_ref, table_ref, out_ref, held):
    tokens = out_ref.shape[0]
    step = 512

    def clear(i, _):
        held[pl.ds(pl.multiple_of(i * step, step), step), :] = jnp.zeros(
            (step, held.shape[1]), f32
        )
        return 0

    lax.fori_loop(0, tokens // step, clear, 0)

    def move(i, _):
        for k in range(8):
            row = row_ref[i * 8 + k]
            tok = tok_ref[i * 8 + k]
            held[pl.ds(tok, 1), :] = table_ref[pl.ds(row, 1), :]
        return 0

    lax.fori_loop(0, (count_ref[0] + 7) // 8, move, 0)

    def put(i, _):
        rows = pl.ds(pl.multiple_of(i * step, step), step)
        out_ref[rows, :] = held[rows, :].astype(bf16)
        return 0

    lax.fori_loop(0, tokens // step, put, 0)


def spread_kernel(count_ref, row_ref, tok_ref, grad_ref, base_ref, out_ref, square_ref, held):
    tokens = grad_ref.shape[0]
    step = 512
    rows_all = out_ref.shape[0]

    def take(i, _):
        rows = pl.ds(pl.multiple_of(i * step, step), step)
        held[rows, :] = grad_ref[rows, :].astype(f32)
        return 0

    lax.fori_loop(0, tokens // step, take, 0)
    held[pl.ds(tokens, 8), :] = jnp.zeros((8, held.shape[1]), f32)

    whole = rows_all // step

    def start(i, _):
        rows = pl.ds(pl.multiple_of(i * step, step), step)
        out_ref[rows, :] = base_ref[rows, :].astype(f32)
        return 0

    lax.fori_loop(0, whole, start, 0)
    if rows_all > whole * step:
        out_ref[whole * step :, :] = base_ref[whole * step :, :].astype(f32)

    def move(i, _):
        for k in range(8):
            row = row_ref[i * 8 + k]
            tok = tok_ref[i * 8 + k]
            out_ref[pl.ds(row, 1), :] = out_ref[pl.ds(row, 1), :] + held[pl.ds(tok, 1), :]
        return 0

    lax.fori_loop(0, (count_ref[0] + 7) // 8, move, 0)

    def square(i, total):
        part = out_ref[pl.ds(pl.multiple_of(i * step, step), step), :]
        return total + jnp.sum((part * part).reshape(step // 8, 8, -1), axis=0)

    total = lax.fori_loop(0, whole, square, jnp.zeros(square_ref.shape, f32))
    square_ref[...] = total
    if rows_all > whole * step:
        part = out_ref[whole * step :, :]
        square_ref[0:1, :] += jnp.sum(part * part, axis=0, keepdims=True)


MESH = pl.DeviceIdType.MESH


def remote(src, dst, send, recv, dp, fsdp):
    return pltpu.make_async_remote_copy(
        src_ref=src,
        dst_ref=dst,
        send_sem=send,
        recv_sem=recv,
        device_id=(dp, fsdp),
        device_id_type=MESH,
    )


def comm_call(kernel, number, ins, outs, scratch, in_spaces, out_spaces, sent):
    return pl.pallas_call(
        kernel,
        out_shape=[jax.ShapeDtypeStruct(shape, kind) for shape, kind in outs],
        in_specs=[pl.BlockSpec(memory_space=space) for space in in_spaces],
        out_specs=[pl.BlockSpec(memory_space=space) for space in out_spaces],
        scratch_shapes=list(scratch),
        compiler_params=pltpu.CompilerParams(
            collective_id=number, has_side_effects=True, vmem_limit_bytes=VMEM_LIMIT
        ),
        cost_estimate=pl.CostEstimate(flops=sent, transcendentals=0, bytes_accessed=2 * sent),
    )(*ins)


CHAIN_STEPS = 8
PART = DI // CHAIN_STEPS


def chunk_place(direction):
    place = lax.axis_index("fsdp") // MB
    count = lax.axis_size("fsdp") // MB
    first = place == (0 if direction > 0 else count - 1)
    final = place == (count - 1 if direction > 0 else 0)
    return first, final


def chain_barrier(direction, first, final):
    dp = lax.axis_index("dp")
    me = lax.axis_index("fsdp")
    barrier = pltpu.get_barrier_semaphore()

    @pl.when(jnp.logical_not(first))
    def _():
        pl.semaphore_signal(
            barrier, inc=1, device_id=(dp, me - MB * direction), device_id_type=MESH
        )

    @pl.when(jnp.logical_not(final))
    def _():
        pl.semaphore_wait(barrier, 1)


def to_next(src, dst, send, recv, direction):
    dp = lax.axis_index("dp")
    return remote(src, dst, send, recv, dp, lax.axis_index("fsdp") + MB * direction)


def chain_step(g, direction, first, final, got, give, local, col, rows, send, recv):
    def copy():
        at = pl.ds(pl.multiple_of(g * PART, PART), PART)
        return to_next(give.at[at], got.at[at], send.at[g], recv.at[g], direction)

    @pl.when(jnp.logical_not(first))
    def _():
        copy().wait_recv()

    @pl.when(jnp.logical_not(final))
    def _():
        for i in range(PART // HDIM):
            h = pl.ds(pl.multiple_of(g * PART + i * HDIM, HDIM), HDIM)
            decay = jnp.exp(col[g * (PART // HDIM) + i, rows - 1 : rows, :])
            give[h, :] = (decay * got[h, :].astype(f32) + local[h, :]).astype(bf16)
        copy().start()


def chain_end(direction, final, got, give, send, recv):
    @pl.when(jnp.logical_not(final))
    def _():
        for g in range(CHAIN_STEPS):
            at = pl.ds(g * PART, PART)
            to_next(give.at[at], got.at[at], send.at[g], recv.at[g], direction).wait_send()


def bits_of(size):
    return [1 << b for b in range(size.bit_length() - 1)]


def total_kernel(in_ref, out_ref, work, got, send, recv):
    dp = lax.axis_index("dp")
    me = lax.axis_index("fsdp")
    half = in_ref.shape[0] // 2
    core = me % MB
    partners = [("f", b) for b in bits_of(lax.axis_size("fsdp")) if b > 1]
    partners += [("d", b) for b in bits_of(lax.axis_size("dp"))]

    def across(kind, bit):
        ids, other = (me, lambda v: (dp, v)) if kind == "f" else (dp, lambda v: (v, me))
        return other(jnp.where((ids // bit) % 2 == 1, ids - bit, ids + bit))

    mate = across("f", 1)
    barrier = pltpu.get_barrier_semaphore()
    for target in [mate] + [across(*p) for p in partners]:
        pl.semaphore_signal(barrier, inc=1, device_id=target, device_id_type=MESH)
    pl.semaphore_wait(barrier, 1 + len(partners))

    mine = pl.ds(pl.multiple_of(core * half, 8), half)
    theirs = pl.ds(pl.multiple_of((1 - core) * half, 8), half)
    copy = remote(in_ref.at[theirs], got.at[0], send.at[0], recv.at[0], *mate)
    copy.start()
    copy.wait()
    work[0] = in_ref[mine, :] + got[0]
    for i, p in enumerate(partners):
        copy = remote(work.at[i], got.at[i + 1], send.at[i + 1], recv.at[i + 1], *across(*p))
        copy.start()
        copy.wait()
        work[i + 1] = work[i] + got[i + 1]
    n = len(partners)
    copy = remote(work.at[n], got.at[n + 1], send.at[n + 1], recv.at[n + 1], *mate)
    copy.start()
    copy.wait()
    out_ref[mine, :] = work[n]
    out_ref[theirs, :] = got[n + 1]


def total_of(array):
    rows = array.shape[0]
    steps = len(bits_of(lax.axis_size("fsdp"))) - 1 + len(bits_of(lax.axis_size("dp")))
    return comm_call(
        total_kernel,
        3,
        (array,),
        ((array.shape, f32),),
        (
            pltpu.VMEM((steps + 1, rows // 2, LANES), f32),
            pltpu.VMEM((steps + 2, rows // 2, LANES), f32),
            pltpu.SemaphoreType.DMA((steps + 2,)),
            pltpu.SemaphoreType.DMA((steps + 2,)),
        ),
        (pltpu.VMEM,),
        (pltpu.VMEM,),
        array.size * 4 * 3,
    )[0]


def snake(place, size):
    return jnp.where(place < size // 2, place, size // 2 + size - 1 - place)


def wrap(value, size):
    return lax.rem(value + size, size)


def gather_kernel(*refs):
    arrays = 2 * LAYERS
    own = refs[:arrays]
    full = refs[arrays : 2 * arrays]
    local_sem, z_send, z_recv, ring_send, ring_recv, mate_send, mate_recv = refs[2 * arrays :]
    dp = lax.axis_index("dp")
    me = lax.axis_index("fsdp")
    size = lax.axis_size("dp")
    count = lax.axis_size("fsdp") // MB
    core = me % MB
    k = me // MB
    ring = snake(dp, size)
    reach = size // 2
    right = snake(wrap(ring + 1, size), size)
    left = snake(wrap(ring - 1, size), size)
    mate = k * MB + 1 - core
    up, down = me + MB, me - MB
    has_up, has_down = k < count - 1, k > 0
    barrier = pltpu.get_barrier_semaphore()
    for target in ((right, me), (left, me), (dp, mate)):
        pl.semaphore_signal(barrier, inc=1, device_id=target, device_id_type=MESH)

    @pl.when(has_up)
    def _():
        pl.semaphore_signal(barrier, inc=1, device_id=(dp, up), device_id_type=MESH)

    @pl.when(has_down)
    def _():
        pl.semaphore_signal(barrier, inc=1, device_id=(dp, down), device_id_type=MESH)

    pl.semaphore_wait(barrier, 3 + jnp.where(has_up, 1, 0) + jnp.where(has_down, 1, 0))

    def spot(a, d, z, c):
        return full[a].at[d, z, c]

    def chain(a, src, z, side):
        return remote(
            src, spot(a, dp, z, core), z_send.at[a, z], z_recv.at[a, z], dp, up if side == 0 else down
        )

    def chain_own(a, side):
        return remote(
            own[a],
            spot(a, dp, k, core),
            z_send.at[a, count + side],
            z_recv.at[a, k],
            dp,
            up if side == 0 else down,
        )

    def round_ring(a, src, d, z, side):
        return remote(
            src,
            spot(a, d, z, core),
            ring_send.at[a, side],
            ring_recv.at[a, d, z],
            right if side == 0 else left,
            me,
        )

    def to_mate(a, src, d, z):
        return remote(src, spot(a, d, z, core), mate_send.at[a], mate_recv.at[a], dp, mate)

    def carried(a, side):
        return (a < arrays // 2) == (side == 0)

    for a in range(arrays):

        @pl.when(has_up)
        def _(a=a):
            chain_own(a, 0).start()

        @pl.when(has_down)
        def _(a=a):
            chain_own(a, 1).start()

    for a in range(arrays):
        for side in (0, 1):
            round_ring(a, own[a], dp, k, side).start()
    for a in range(arrays):
        to_mate(a, own[a], dp, k).start()
        pltpu.make_async_copy(own[a], spot(a, dp, k, core), local_sem.at[a]).start()

    def ring_step(z, s):
        for side in (0, 1):
            origin = snake(wrap(ring - s if side == 0 else ring + s, size), size)
            for a in range(arrays):
                if s == reach and not carried(a, side):
                    continue
                piece = spot(a, origin, z, core)
                round_ring(a, piece, origin, z, side).wait_recv()
                if s + 1 < reach or (s + 1 == reach and carried(a, side)):
                    round_ring(a, piece, origin, z, side).start()
                to_mate(a, piece, origin, z).start()

    def arrive(z, side):
        for a in range(arrays):
            piece = spot(a, dp, z, core)
            chain(a, piece, z, side).wait_recv()

            @pl.when(has_up if side == 0 else has_down)
            def _(a=a, piece=piece):
                chain(a, piece, z, side).start()

            for way in (0, 1):
                round_ring(a, piece, dp, z, way).start()
            to_mate(a, piece, dp, z).start()

    def both_ways(far, act):
        if far == 0:
            act(k, 0)
            return

        @pl.when(k >= far)
        def _():
            act(k - far, 0)

        @pl.when(k + far < count)
        def _():
            act(k + far, 1)

    for turn in range(1, count + reach):
        if turn < count:
            both_ways(turn, arrive)
        for s in range(1, reach + 1):
            if 0 <= turn - s < count:
                both_ways(turn - s, lambda z, side, s=s: ring_step(z, s))

    for a in range(arrays):
        pltpu.make_async_copy(own[a], spot(a, dp, k, core), local_sem.at[a]).wait()
        for side in (0, 1):
            sent = full[a].at[pl.ds(0, reach if carried(a, side) else reach - 1), :, core]
            remote(sent, sent, ring_send.at[a, side], ring_recv.at[a, 0, 0], dp, mate).wait_send()
        whole = full[a].at[:, :, core]
        remote(whole, whole, mate_send.at[a], mate_recv.at[a], dp, mate).wait_send()
        whole = full[a].at[:, :, 1 - core]
        remote(whole, whole, mate_send.at[a], mate_recv.at[a], dp, mate).wait_recv()

        @pl.when(has_up)
        def _(a=a):
            chain_own(a, 0).wait_send()

        @pl.when(has_down)
        def _(a=a):
            chain_own(a, 1).wait_send()

        for far in range(1, count):

            @pl.when(jnp.logical_and(k >= far, has_up))
            def _(a=a, far=far):
                chain(a, spot(a, dp, k - far, core), k - far, 0).wait_send()

            @pl.when(jnp.logical_and(k + far < count, has_down))
            def _(a=a, far=far):
                chain(a, spot(a, dp, k + far, core), k + far, 1).wait_send()


def gather_layers(shards):
    size, count = lax.axis_size("dp"), lax.axis_size("fsdp") // MB
    arrays = len(shards)
    outs = comm_call(
        gather_kernel,
        4,
        shards,
        tuple(((size, count, MB) + s.shape, bf16) for s in shards),
        (
            pltpu.SemaphoreType.DMA((arrays,)),
            pltpu.SemaphoreType.DMA((arrays, count + 2)),
            pltpu.SemaphoreType.DMA((arrays, count)),
            pltpu.SemaphoreType.DMA((arrays, 2)),
            pltpu.SemaphoreType.DMA((arrays, size, count)),
            pltpu.SemaphoreType.DMA((arrays,)),
            pltpu.SemaphoreType.DMA((arrays,)),
        ),
        (pltpu.VMEM,) * arrays,
        (pl.ANY,) * arrays,
        sum(s.size * 2 for s in shards) * 24,
    )
    return [o.reshape(size * count * MB * s.shape[0], s.shape[1]) for o, s in zip(outs, shards)]


def add_rows(dst, first, *others):
    rows = dst.shape[0]
    step = min(rows, 16)

    def one(i, _):
        at = pl.ds(pl.multiple_of(i * step, step), step)
        total = first[at, :].astype(f32)
        for other in others:
            total = total + other[at, :].astype(f32)
        dst[at, :] = total.astype(dst.dtype)
        return 0

    lax.fori_loop(0, rows // step, one, 0)


def reduce_kernel(*refs):
    arrays = 2 * LAYERS
    grads = refs[:arrays]
    outs = refs[arrays : 2 * arrays]
    held, given, come, chained = (
        refs[(2 + i) * arrays : (3 + i) * arrays] for i in range(4)
    )
    load_sem, mate_send, mate_recv, ring_send, ring_recv, z_send, z_recv = refs[6 * arrays :]
    dp = lax.axis_index("dp")
    me = lax.axis_index("fsdp")
    size = lax.axis_size("dp")
    count = lax.axis_size("fsdp") // MB
    core = me % MB
    k = me // MB
    ring = snake(dp, size)
    reach = size // 2
    right = snake(wrap(ring + 1, size), size)
    left = snake(wrap(ring - 1, size), size)
    mate = k * MB + 1 - core
    up, down = me + MB, me - MB
    has_up, has_down = k < count - 1, k > 0

    def load(a):
        return pltpu.make_async_copy(grads[a].at[:, :, core], held[a], load_sem.at[a])

    for a in range(arrays):
        load(a).start()
    barrier = pltpu.get_barrier_semaphore()
    for target in ((right, me), (left, me), (dp, mate)):
        pl.semaphore_signal(barrier, inc=1, device_id=target, device_id_type=MESH)

    @pl.when(has_up)
    def _():
        pl.semaphore_signal(barrier, inc=1, device_id=(dp, up), device_id_type=MESH)

    @pl.when(has_down)
    def _():
        pl.semaphore_signal(barrier, inc=1, device_id=(dp, down), device_id_type=MESH)

    pl.semaphore_wait(barrier, 3 + jnp.where(has_up, 1, 0) + jnp.where(has_down, 1, 0))

    def away(j, side):
        return snake(wrap(ring + j if side == 0 else ring - j, size), size)

    def to_mate(a, d):
        return remote(
            grads[a].at[d, :, 1 - core], given[a].at[d], mate_send.at[a], mate_recv.at[a, d], dp, mate
        )

    def carried(a, side):
        return (a < arrays // 2) == (side == 0)

    def targets(j):
        if j == 0:
            return [dp]
        if j == reach:
            return [away(j, 0)]
        return [away(j, 0), away(j, 1)]

    for j in range(reach, -1, -1):
        for d in targets(j):
            for a in range(arrays):
                to_mate(a, d).start()

    for a in range(arrays):
        load(a).wait()

    def add_mate(d):
        for a in range(arrays):
            to_mate(a, d).wait_recv()

            def one(z, _, a=a):
                add_rows(held[a].at[d, z], held[a].at[d, z], given[a].at[d, z])
                return 0

            lax.fori_loop(0, count, one, 0)

    def first_step(a, side):
        d = away(reach, 0)
        return remote(
            held[a].at[d], come[a].at[side, 0], ring_send.at[a, side], ring_recv.at[a, side, 0, 0],
            right if side == 0 else left, me,
        )

    def next_step(a, side, s, z):
        d = away(reach - s, side)
        return remote(
            held[a].at[d, z], come[a].at[side, s, z], ring_send.at[a, side],
            ring_recv.at[a, side, s, z], right if side == 0 else left, me,
        )

    far_most = jnp.maximum(k, count - 1 - k)
    near_most = jnp.minimum(k, count - 1 - k)
    uneven = far_most - near_most
    long_side = jnp.where(count - 1 - k > k, 1, -1)

    def chunk_at(i):
        j = jnp.maximum(i - uneven, 0)
        paired = k + (1 - 2 * (j % 2)) * (near_most - j // 2)
        return jnp.where(i < uneven, k + long_side * (far_most - i), paired)

    add_mate(away(reach, 0))
    for a in range(arrays):
        first_step(a, 0 if carried(a, 0) else 1).start()
    for s in range(1, reach):
        for side in (0, 1):
            add_mate(away(reach - s, side))
        if s == 1:
            for a in range(arrays):
                first_step(a, 0 if carried(a, 0) else 1).wait_recv()

        def pass_on(i, _, s=s):
            z = chunk_at(i)
            for side in (0, 1):
                d = away(reach - s, side)
                for a in range(arrays):
                    if s > 1:
                        next_step(a, side, s - 1, z).wait_recv()
                    if s > 1 or carried(a, side):
                        add_rows(held[a].at[d, z], held[a].at[d, z], come[a].at[side, s - 1, z])
                    next_step(a, side, s, z).start()
            return 0

        lax.fori_loop(0, count, pass_on, 0)
    add_mate(dp)

    def along(a, side, z):
        return remote(
            held[a].at[dp, z], chained[a].at[side, z], z_send.at[a, z], z_recv.at[a, side, z],
            dp, up if side == 0 else down,
        )

    def finish(i, _):
        z = chunk_at(i)
        for a in range(arrays):
            for side in (0, 1):
                next_step(a, side, reach - 1, z).wait_recv()
            add_rows(
                held[a].at[dp, z],
                held[a].at[dp, z],
                come[a].at[0, reach - 1, z],
                come[a].at[1, reach - 1, z],
            )
            for side in (0, 1):
                beyond = z > k if side == 0 else z < k
                fed = has_down if side == 0 else has_up

                @pl.when(jnp.logical_and(fed, jnp.logical_or(beyond, z == k)))
                def _(a=a, side=side):
                    along(a, side, z).wait_recv()
                    add_rows(held[a].at[dp, z], held[a].at[dp, z], chained[a].at[side, z])

                @pl.when(beyond)
                def _(a=a, side=side):
                    along(a, side, z).start()

        return 0

    lax.fori_loop(0, count, finish, 0)
    for a in range(arrays):
        add_rows(outs[a], held[a].at[dp, k])
        for side in (0, 1):
            sent = held[a].at[pl.ds(0, reach if carried(a, side) else reach - 1)]
            remote(
                sent, sent, ring_send.at[a, side], ring_recv.at[a, side, 0, 0], dp, mate
            ).wait_send()
        remote(
            given[a], given[a], mate_send.at[a], mate_recv.at[a, 0], dp, mate
        ).wait_send()

    def sent_along(z, _):
        for a in range(arrays):

            @pl.when(z != k)
            def _(a=a):
                along(a, 0, z).wait_send()

        return 0

    lax.fori_loop(0, count, sent_along, 0)


def reduce_layers(grads):
    size, count = lax.axis_size("dp"), lax.axis_size("fsdp") // MB
    arrays = len(grads)
    reach = size // 2
    shards = [(g.shape[0] // (size * count * MB), g.shape[1]) for g in grads]
    blocks = [g.reshape((size, count, MB) + s) for g, s in zip(grads, shards)]
    return comm_call(
        reduce_kernel,
        5,
        blocks,
        tuple((s, f32) for s in shards),
        tuple(pltpu.VMEM((size, count) + s, bf16) for s in shards) * 2
        + tuple(pltpu.VMEM((2, reach, count) + s, bf16) for s in shards)
        + tuple(pltpu.VMEM((2, count) + s, bf16) for s in shards)
        + (
            pltpu.SemaphoreType.DMA((arrays,)),
            pltpu.SemaphoreType.DMA((arrays,)),
            pltpu.SemaphoreType.DMA((arrays, size)),
            pltpu.SemaphoreType.DMA((arrays, 2)),
            pltpu.SemaphoreType.DMA((arrays, 2, reach, count)),
            pltpu.SemaphoreType.DMA((arrays, count)),
            pltpu.SemaphoreType.DMA((arrays, 2, count)),
        ),
        (pl.ANY,) * arrays,
        (pltpu.VMEM,) * arrays,
        sum(g.size * 2 for g in grads),
    )


def pair_lanes(p):
    return pl.ds(pl.multiple_of(p * LANES, LANES), LANES)


def first_half(rows):
    return lax.broadcasted_iota(jnp.int32, (rows, LANES), 1) < HDIM


def spread_columns(values, column, per_pair, rows):
    half = first_half(rows)
    for p in range(PAIRS):
        left = jnp.broadcast_to(values[:, 2 * p : 2 * p + 1], (rows, LANES))
        right = jnp.broadcast_to(values[:, 2 * p + 1 : 2 * p + 2], (rows, LANES))
        if column is not None:
            column[2 * p] = left
            column[2 * p + 1] = right
        if per_pair is not None:
            per_pair[p] = jnp.where(half, left, right)


def scan_kernel(
    proj_ref, cw_ref, cb_ref, dtb_ref, al_ref, sk_ref, gg_ref,
    pre_ref, y_ref, yn_ref, dt_ref, cum_ref, got, halo_ref,
    pad, col, tcol, lcol, lrow, st, give, square, edge_send, edge_recv, send, recv,
):
    rows = proj_ref.shape[0]
    first, final = chunk_place(1)
    chain_barrier(1, first, final)
    edge = to_next(
        proj_ref.at[pl.ds(rows - 8, 8), pl.ds(DI, XBC)], halo_ref, edge_send, edge_recv, 1
    )

    @pl.when(jnp.logical_not(final))
    def _():
        edge.start()

    @pl.when(first)
    def _():
        halo_ref[...] = jnp.zeros(halo_ref.shape, f32)
        got[...] = jnp.zeros(got.shape, bf16)

    pad[8:, :] = proj_ref[:, DI : DI + XBC]
    dt_ref[...] = jnp.zeros((rows, LANES), f32)
    dt_ref[:, 0:HEADS] = proj_ref[:, DI + XBC :]
    drive = dt_ref[...] + dtb_ref[...]
    dt = jnp.maximum(drive, 0.0) + jnp.log1p(jnp.exp(-jnp.abs(drive)))
    dt_ref[...] = dt
    rate = dt * (-jnp.exp(al_ref[...]))
    ri = lax.broadcasted_iota(jnp.int32, (rows, rows), 0)
    ci = lax.broadcasted_iota(jnp.int32, (rows, rows), 1)
    causal = ri >= ci
    cum = dot_nn(jnp.where(causal, 1.0, 0.0), rate, highest)
    cum_ref[...] = cum
    lrow[...] = cum.T
    spread_columns(cum, col, lcol, rows)
    spread_columns(dt, None, tcol, rows)

    @pl.when(jnp.logical_not(first))
    def _():
        edge.wait_recv()

    pad[0:8, :] = halo_ref[...]

    def conv(i, _):
        xs = pair_lanes(i)
        out = jnp.broadcast_to(cb_ref[0:1, xs], (rows, LANES))
        for k in range(CONV):
            out = out + cw_ref[k : k + 1, xs] * pad[5 + k : 5 + k + rows, xs]
        pre_ref[:, xs] = out
        return 0

    lax.fori_loop(0, XBC // LANES, conv, 0)
    bm = silu(pre_ref[:, DI : DI + NSTATE]).astype(bf16)
    cm = silu(pre_ref[:, DI + NSTATE :]).astype(bf16)
    cb = dot_nt(cm, bm)
    half = first_half(rows)

    def states(p, _):
        xs = pair_lanes(p)
        lp = lcol[p]
        tail = jnp.exp(lp[rows - 1 : rows, :] - lp) * tcol[p]
        st[xs, :] = dot_tn((tail * silu(pre_ref[:, xs])).astype(bf16), bm)
        return 0

    lax.fori_loop(0, PAIRS, states, 0, unroll=2)
    square[...] = jnp.zeros(square.shape, f32)

    def pair(p):
        xs = pair_lanes(p)
        x = silu(pre_ref[:, xs])
        xtb = (tcol[p] * x).astype(bf16)
        parts = []
        for j in range(2):
            h = 2 * p + j
            c = col[h]
            d = jnp.concatenate([c] * (rows // LANES), axis=1) - lrow[pl.ds(h, 1), :]
            m = (jnp.exp(jnp.where(causal, d, OFF)) * cb).astype(bf16)
            parts.append(dot_nn(m, xtb))
        y = jnp.where(half, parts[0], parts[1]) + sk_ref[0:1, xs] * x
        y = y + jnp.exp(lcol[p]) * dot_nt(cm, got[xs, :])
        y_ref[:, xs] = y
        g = y * silu(proj_ref[:, xs])
        return g * g

    def step(g, _):
        chain_step(g, 1, first, final, got, give, st, col, rows, send, recv)
        total = square[...]
        for i in range(PART // LANES):
            total = total + pair(g * (PART // LANES) + i)
        square[...] = total
        return 0

    lax.fori_loop(0, CHAIN_STEPS, step, 0)
    scale = lax.rsqrt(jnp.sum(square[...], axis=1, keepdims=True) / DI + epsilon)

    def put(p, _):
        xs = pair_lanes(p)
        g = y_ref[:, xs] * silu(proj_ref[:, xs])
        yn_ref[:, xs] = (g * scale * gg_ref[0:1, xs]).astype(bf16)
        return 0

    lax.fori_loop(0, PAIRS, put, 0, unroll=2)

    @pl.when(jnp.logical_not(final))
    def _():
        edge.wait_send()

    chain_end(1, final, got, give, send, recv)


def back_kernel(
    dyn_ref, y_ref, proj_ref, halo_ref, pre_ref, dt_ref, cum_ref, sin_ref,
    cw_ref, dtb_ref, al_ref, sk_ref, gg_ref,
    dp_ref, dcw_ref, dsm_ref, dgg_ref,
    pad, grad, col, tcol, lcol, lrow, dcb, dbm, dcm, dlog, dtx, ends, dy_ref, drive_ref,
    got, give, gst, dx_ref, edge_ref, from_ref, edge_send, edge_recv, send, recv,
):
    rows = y_ref.shape[0]
    first, final = chunk_place(-1)
    chain_barrier(-1, first, final)

    @pl.when(first)
    def _():
        from_ref[...] = jnp.zeros(from_ref.shape, f32)
        got[...] = jnp.zeros(got.shape, bf16)

    cum = cum_ref[...]
    dt = dt_ref[...]
    lrow[...] = cum.T
    spread_columns(cum, col, lcol, rows)
    spread_columns(dt, None, tcol, rows)
    bm = silu(pre_ref[:, DI : DI + NSTATE]).astype(bf16)
    cm = silu(pre_ref[:, DI + NSTATE :]).astype(bf16)
    zero = jnp.zeros((rows, LANES), f32)

    def sums(p, carry):
        xs = pair_lanes(p)
        g = y_ref[:, xs] * silu(proj_ref[:, xs])
        return carry[0] + g * g, carry[1] + g * (dyn_ref[:, xs] * gg_ref[0:1, xs])

    square, cross = lax.fori_loop(0, PAIRS, sums, (zero, zero))
    scale = lax.rsqrt(jnp.sum(square, axis=1, keepdims=True) / DI + epsilon)
    mean = jnp.sum(cross, axis=1, keepdims=True) * scale / DI

    def ungate(p, _):
        xs = pair_lanes(p)
        z = proj_ref[:, xs]
        y = y_ref[:, xs]
        sg = lax.logistic(z)
        sz = z * sg
        ghat = y * sz * scale
        dyn = dyn_ref[:, xs]
        dgg_ref[0:1, xs] = jnp.sum(dyn * ghat, axis=0, keepdims=True)
        dg = scale * (dyn * gg_ref[0:1, xs] - ghat * mean)
        dy = dg * sz
        dy_ref[:, xs] = dy
        dp_ref[:, xs] = (dg * y * (sg * (1.0 + z * (1.0 - sg)))).astype(bf16)
        gst[xs, :] = dot_tn((jnp.exp(lcol[p]) * dy).astype(bf16), cm)
        return 0

    lax.fori_loop(0, PAIRS, ungate, 0, unroll=2)
    pad[0:8, :] = halo_ref[...]
    pad[8:, :] = proj_ref[:, DI : DI + XBC]
    grad[0:8, :] = jnp.zeros((8, XBC), f32)
    grad[rows + 8 :, :] = jnp.zeros((8, XBC), f32)
    cbt = dot_nt(bm, cm)
    ri = lax.broadcasted_iota(jnp.int32, (rows, rows), 0)
    ci = lax.broadcasted_iota(jnp.int32, (rows, rows), 1)
    causal = ri <= ci
    half = first_half(rows)
    dcb[...] = jnp.zeros((rows, rows), f32)
    dbm[...] = zero
    dcm[...] = zero
    dlog[...] = zero
    dtx[...] = zero
    ends[...] = jnp.zeros((16, LANES), f32)
    lane_row = lax.broadcasted_iota(jnp.int32, (LANES, LANES), 0)
    lane_col = lax.broadcasted_iota(jnp.int32, (LANES, LANES), 1)
    ones = jnp.ones((8, NSTATE), f32)

    def pair(p):
        xs = pair_lanes(p)
        pre = pre_ref[:, xs]
        sg = lax.logistic(pre)
        x = pre * sg
        tp = tcol[p]
        xt = tp * x
        dy = dy_ref[:, xs]
        dyb = dy.astype(bf16)
        parts = []
        for j in range(2):
            h = 2 * p + j
            c = col[h]
            d = lrow[pl.ds(h, 1), :] - jnp.concatenate([c] * (rows // LANES), axis=1)
            w = jnp.exp(jnp.where(causal, d, OFF))
            parts.append(dot_nn((w * cbt).astype(bf16), dyb))
            own = half if j == 0 else jnp.logical_not(half)
            q = dot_nt(jnp.where(own, xt, 0.0).astype(bf16), dyb)
            dcb[...] += w * q
        lp = lcol[p]
        last = lp[rows - 1 : rows, :]
        tail = jnp.exp(last - lp)
        gin = got[xs, :]
        sin = sin_ref[xs, :]
        dst = tail * dot_nt(bm, gin)
        dxt = jnp.where(half, parts[0], parts[1]) + dst
        dbm[...] += dot_nn((tail * xt).astype(bf16), gin)
        dcm[...] += dot_nn((jnp.exp(lp) * dy).astype(bf16), sin)
        sk = sk_ref[0:1, xs]
        pick = jnp.where(lane_col == 2 * p + jnp.where(lane_row >= HDIM, 1, 0), 1.0, 0.0)
        dlog[...] += dot_nn(dy * (y_ref[:, xs] - sk * x) - xt * dxt, pick, highest)
        dtx[...] += dot_nn(x * dxt, pick, highest)
        held = dot_nt(ones, gin.astype(f32) * sin.astype(f32), highest)
        end = jnp.sum(xt * dst, axis=0, keepdims=True) + jnp.exp(last) * held[0:1, :]
        skip = jnp.sum(dy * x, axis=0, keepdims=True)
        stacked = jnp.concatenate(
            [jnp.broadcast_to(end, (8, LANES)), jnp.broadcast_to(skip, (8, LANES))], axis=0
        )
        ends[...] += dot_nn(stacked, pick, highest)
        grad[pl.ds(8, rows), xs] = (tp * dxt + sk * dy) * (sg * (1.0 + pre * (1.0 - sg)))

    def step(g, _):
        chain_step(g, -1, first, final, got, give, gst, col, rows, send, recv)
        for i in range(PART // LANES):
            pair(g * (PART // LANES) + i)
        return 0

    lax.fori_loop(0, CHAIN_STEPS, step, 0)
    dcbb = dcb[...].astype(bf16)
    dc = dcm[...] + dot_tn(dcbb, bm)
    db = dbm[...] + dot_nn(dcbb, cm)
    grad[8 : 8 + rows, DI : DI + NSTATE] = db * silu_grad(pre_ref[:, DI : DI + NSTATE])
    grad[8 : 8 + rows, DI + NSTATE :] = dc * silu_grad(pre_ref[:, DI + NSTATE :])

    def edges(i, _):
        xs = pair_lanes(i)
        edge = jnp.zeros((8, LANES), f32)
        for k in range(CONV):
            edge = edge + cw_ref[k : k + 1, xs] * grad[3 - k : 11 - k, xs]
        edge_ref[:, xs] = edge
        return 0

    lax.fori_loop(0, XBC // LANES, edges, 0)
    edge = to_next(edge_ref, from_ref, edge_send, edge_recv, -1)

    @pl.when(jnp.logical_not(final))
    def _():
        edge.start()

    last_row = lax.broadcasted_iota(jnp.int32, (rows, LANES), 0) == rows - 1
    dl = dlog[...] + jnp.where(last_row, ends[0:1, :], 0.0)
    da = dot_nn(jnp.where(causal, 1.0, 0.0), dl, highest)
    decay = -jnp.exp(al_ref[...])
    ddt = dtx[...] + da * decay
    drive_ref[...] = jnp.zeros((rows, LANES), f32)
    drive_ref[:, 0:HEADS] = proj_ref[:, DI + XBC :]
    ddr = ddt * lax.logistic(drive_ref[...] + dtb_ref[...])
    dp_ref[:, DI + XBC :] = ddr[:, 0:HEADS].astype(bf16)
    dsm_ref[...] = jnp.zeros((8, LANES), f32)
    dsm_ref[0:1, :] = jnp.sum(ddr, axis=0, keepdims=True)
    dsm_ref[1:2, :] = jnp.sum(da * dt, axis=0, keepdims=True) * decay
    dsm_ref[2:3, :] = ends[8:9, :]

    def conv(i, _):
        xs = pair_lanes(i)
        own = grad[pl.ds(8, rows), xs]
        out = jnp.zeros((rows, LANES), f32)
        for k in range(CONV):
            out = out + cw_ref[k : k + 1, xs] * grad[11 - k : 11 - k + rows, xs]
            dcw_ref[k : k + 1, xs] = jnp.sum(
                own * pad[5 + k : 5 + k + rows, xs], axis=0, keepdims=True
            )
        dcw_ref[4:5, xs] = jnp.sum(own, axis=0, keepdims=True)
        dx_ref[:, xs] = out
        return 0

    lax.fori_loop(0, XBC // LANES, conv, 0)

    @pl.when(jnp.logical_not(first))
    def _():
        edge.wait_recv()

    dx_ref[rows - 8 :, :] += from_ref[...]
    dp_ref[:, DI : DI + XBC] = dx_ref[...].astype(bf16)

    @pl.when(jnp.logical_not(final))
    def _():
        edge.wait_send()

    chain_end(-1, final, got, give, send, recv)


VTILE = 1280
NTILE = 256


def head_specs(width, tokens):
    return dict(
        table=pl.BlockSpec((VTILE, width), lambda i: (i, 0)),
        hidden=pl.BlockSpec((tokens, width), lambda i: (0, 0)),
        kept=pl.BlockSpec((VTILE, tokens), lambda i: (i, 0)),
        row=pl.BlockSpec((1, tokens), lambda i: (0, 0)),
        tile_row=pl.BlockSpec((1, 1, tokens), lambda i: (i, 0, 0)),
    )


def head_call(kernel, grid, in_specs, out_specs, outs, scratch, ins, cells):
    return pl.pallas_call(
        kernel,
        grid=(grid,),
        in_specs=in_specs,
        out_specs=out_specs,
        out_shape=[jax.ShapeDtypeStruct(shape, kind) for shape, kind in outs],
        scratch_shapes=list(scratch),
        compiler_params=pltpu.CompilerParams(
            dimension_semantics=("arbitrary",), vmem_limit_bytes=VMEM_LIMIT
        ),
        cost_estimate=pl.CostEstimate(
            flops=2 * cells * D, transcendentals=cells, bytes_accessed=4 * cells
        ),
    )(*ins)


UNROLL = 8


def head_stats_kernel(
    table_ref, own_ref, lab_ref, w_ref,
    q_ref, all_ref, lse_ref, fac_ref, hit_ref,
    kept, tops, sums, hits, shown, own_sem, put_sem, z_send, z_recv, m_send, m_recv, s_send, s_recv,
):
    dp = lax.axis_index("dp")
    me = lax.axis_index("fsdp")
    shards = lax.axis_size("fsdp")
    count = shards // MB
    core = me % MB
    k = me // MB
    mate = k * MB + 1 - core
    vocab_rows = table_ref.shape[0]
    rows = own_ref.shape[0]
    tiles = tops.shape[0]
    barrier = pltpu.get_barrier_semaphore()
    for other in range(1, shards):
        pl.semaphore_signal(
            barrier, inc=1, device_id=(dp, lax.rem(me + other, shards)), device_id_type=MESH
        )
    pl.semaphore_wait(barrier, shards - 1)

    near = jnp.minimum(k, count - 1 - k)
    long_side = jnp.where(count - 1 - k > k, 1, -1)

    def chunk_at(i):
        paired = k + (2 * (i % 2) - 1) * ((i + 1) // 2)
        return jnp.where(i <= 2 * near, paired, k + long_side * (i - near))

    def along(z, side):
        at = all_ref.at[z * MB + core]
        return remote(
            at, at, z_send.at[side, z], z_recv.at[z], dp, me + MB if side == 0 else me - MB
        )

    def to_mate(z):
        at = all_ref.at[z * MB + core]
        return remote(at, at, m_send.at[z], m_recv.at[z], dp, mate)

    def from_mate(z):
        at = all_ref.at[z * MB + 1 - core]
        return remote(at, at, m_send.at[z], m_recv.at[z], dp, mate)

    keep = pltpu.make_async_copy(own_ref, all_ref.at[me], own_sem)
    keep.start()
    keep.wait()

    @pl.when(k < count - 1)
    def _():
        along(k, 0).start()

    @pl.when(k > 0)
    def _():
        along(k, 1).start()

    to_mate(k).start()
    whole = vocab_rows - vocab_rows % 16
    for slot in range(2):
        kept[slot, whole:, :] = jnp.zeros((kept.shape[1] - whole, rows), bf16)

    def put(step, b):
        return pltpu.make_async_copy(
            kept.at[step % 2],
            q_ref.at[:, pl.ds(pl.multiple_of(b * rows, rows), rows)],
            put_sem.at[step % 2],
        )

    def block(step, b):
        @pl.when(step >= 2)
        def _():
            put(step, b).wait()

        slot = step % 2
        ns = pl.ds(pl.multiple_of(b * rows, rows), rows)
        h = all_ref[b]
        label = lab_ref[0:1, ns]
        for t in range(tiles):
            first = t * VTILE
            size = min(VTILE, vocab_rows - first)
            logits = dot_nt(table_ref[first : first + size, :], h)
            top = jnp.max(logits, axis=0, keepdims=True)
            p = jnp.exp(logits - top)
            kept[slot, first : first + size, :] = p.astype(bf16)
            tops[t, 0:1, ns] = top
            sums[t, 0:1, ns] = jnp.sum(p, axis=0, keepdims=True)
            rid = lax.broadcasted_iota(jnp.int32, (size, rows), 0)
            hits[t, 0:1, ns] = jnp.sum(
                jnp.where(rid == label - first, logits, 0.0), axis=0, keepdims=True
            )
        put(step, b).start()

    def chunk(i, _):
        z = chunk_at(i)

        @pl.when(jnp.logical_and(i > 0, k >= i))
        def _():
            along(k - i, 0).wait_recv()

            @pl.when(k < count - 1)
            def _():
                along(k - i, 0).start()

            to_mate(k - i).start()

        @pl.when(jnp.logical_and(i > 0, k + i < count))
        def _():
            along(k + i, 1).wait_recv()

            @pl.when(k > 0)
            def _():
                along(k + i, 1).start()

            to_mate(k + i).start()

        block(2 * i, z * MB + core)
        from_mate(z).wait_recv()
        block(2 * i + 1, z * MB + 1 - core)
        return 0

    lax.fori_loop(0, count, chunk, 0)
    top = tops[0, 0:1, :]
    for t in range(1, tiles):
        top = jnp.maximum(top, tops[t, 0:1, :])
    total = jnp.zeros_like(top)
    hit = jnp.zeros_like(top)
    for t in range(tiles):
        total = total + sums[t, 0:1, :] * jnp.exp(tops[t, 0:1, :] - top)
        hit = hit + hits[t, 0:1, :]
    hit_ref[...] = hit
    shown[me, 0:1, :] = top
    shown[me, 1:2, :] = total

    def tell(other):
        at = shown.at[me]
        return remote(
            at, at, s_send.at[other], s_recv.at[me], dp, lax.rem(me + other, shards)
        )

    def told(other):
        at = shown.at[lax.rem(me + other, shards)]
        return remote(
            at, at, s_send.at[other], s_recv.at[lax.rem(me + other, shards)], dp, mate
        )

    for other in range(1, shards):
        tell(other).start()
    for other in range(1, shards):
        told(other).wait_recv()
    top = shown[0, 0:1, :]
    for f in range(1, shards):
        top = jnp.maximum(top, shown[f, 0:1, :])
    total = jnp.zeros_like(top)
    for f in range(shards):
        total = total + shown[f, 1:2, :] * jnp.exp(shown[f, 0:1, :] - top)
    lse = top + jnp.log(total)
    lse_ref[...] = lse
    scale = w_ref[...] * (1.0 + 2.0 * z_weight * lse)
    for t in range(tiles):
        fac_ref[t, 0:1, :] = scale * jnp.exp(tops[t, 0:1, :] - lse)
    for other in range(1, shards):
        tell(other).wait_send()
    for z in range(count):

        @pl.when(jnp.logical_and(k >= z, k < count - 1))
        def _(z=z):
            along(z, 0).wait_send()

        @pl.when(jnp.logical_and(k <= z, k > 0))
        def _(z=z):
            along(z, 1).wait_send()

        to_mate(z).wait_send()
    put(0, 0).wait()
    put(1, 0).wait()


def head_stats(table, own, labels, weight):
    vocab_rows, width = table.shape
    rows = own.shape[0]
    shards = lax.axis_size("fsdp")
    count = shards // MB
    tokens = shards * rows
    tiles = pl.cdiv(vocab_rows, VTILE)
    kept, everyone, lse, fac, hit = comm_call(
        head_stats_kernel,
        6,
        (table, own, labels, weight),
        (
            ((tiles * VTILE, tokens), bf16),
            ((shards, rows, width), bf16),
            ((1, tokens), f32),
            ((tiles, 1, tokens), f32),
            ((1, tokens), f32),
        ),
        (
            pltpu.VMEM((2, tiles * VTILE, rows), bf16),
            pltpu.VMEM((tiles, 1, tokens), f32),
            pltpu.VMEM((tiles, 1, tokens), f32),
            pltpu.VMEM((tiles, 1, tokens), f32),
            pltpu.VMEM((shards, 2, tokens), f32),
            pltpu.SemaphoreType.DMA,
            pltpu.SemaphoreType.DMA((2,)),
            pltpu.SemaphoreType.DMA((2, count)),
            pltpu.SemaphoreType.DMA((count,)),
            pltpu.SemaphoreType.DMA((count,)),
            pltpu.SemaphoreType.DMA((count,)),
            pltpu.SemaphoreType.DMA((shards,)),
            pltpu.SemaphoreType.DMA((shards,)),
        ),
        (pltpu.VMEM,) * 4,
        (pl.ANY, pltpu.VMEM, pltpu.VMEM, pltpu.VMEM, pltpu.VMEM),
        own.size * 2 * 7,
    )
    return kept, everyone.reshape(tokens, width), lse, fac, hit


def logit_grads(q, fac, weight, rid, label):
    other = weight * (0.1 / VOCAB)
    return (q.astype(f32) * fac - jnp.where(rid == label, other + 0.9 * weight, other)).astype(bf16)


def head_rows_kernel(vocab_rows, e_ref, q_ref, fac_ref, w_ref, lab_ref, out_ref, acc, et):
    step = pl.program_id(0)
    first = step * VTILE
    tokens = q_ref.shape[1]

    @pl.when(step == 0)
    def _():
        acc[...] = jnp.zeros(acc.shape, f32)

    eid = lax.broadcasted_iota(jnp.int32, (VTILE, e_ref.shape[1]), 0)
    et[...] = jnp.where(eid < vocab_rows - first, e_ref[...].astype(f32), 0.0).T.astype(bf16)

    def chunk(j, _):
        ns = pl.ds(pl.multiple_of(j * NTILE, NTILE), NTILE)
        rid = lax.broadcasted_iota(jnp.int32, (VTILE, NTILE), 0)
        dl = logit_grads(
            q_ref[:, ns], fac_ref[0, 0:1, ns], w_ref[0:1, ns], rid, lab_ref[0:1, ns] - first
        )
        acc[:, ns] += dot_nn(et[...], dl)
        return 0

    lax.fori_loop(0, tokens // NTILE, chunk, 0, unroll=UNROLL)

    @pl.when(step == pl.num_programs(0) - 1)
    def _():
        def put(j, _):
            ns = pl.ds(pl.multiple_of(j * NTILE, NTILE), NTILE)
            out_ref[ns, :] = acc[:, ns].T.astype(bf16)
            return 0

        lax.fori_loop(0, tokens // NTILE, put, 0)


def head_rows(table, kept, fac, weight, labels):
    vocab_rows, width = table.shape
    tokens = kept.shape[1]
    sp = head_specs(width, tokens)
    return head_call(
        functools.partial(head_rows_kernel, vocab_rows),
        pl.cdiv(vocab_rows, VTILE),
        [sp["table"], sp["kept"], sp["tile_row"], sp["row"], sp["row"]],
        [sp["hidden"]],
        [((tokens, width), bf16)],
        (pltpu.VMEM((width, tokens), f32), pltpu.VMEM((width, VTILE), bf16)),
        (table, kept, fac, weight, labels),
        vocab_rows * tokens,
    )[0]


def head_table_kernel(h_ref, q_ref, fac_ref, w_ref, lab_ref, out_ref, dl_ref):
    first = pl.program_id(0) * VTILE
    tokens = q_ref.shape[1]

    def chunk(j, _):
        ns = pl.ds(pl.multiple_of(j * NTILE, NTILE), NTILE)
        rid = lax.broadcasted_iota(jnp.int32, (VTILE, NTILE), 0)
        dl_ref[:, ns] = logit_grads(
            q_ref[:, ns], fac_ref[0, 0:1, ns], w_ref[0:1, ns], rid, lab_ref[0:1, ns] - first
        )
        return 0

    lax.fori_loop(0, tokens // NTILE, chunk, 0, unroll=UNROLL)

    def cols(j, _):
        ds = pl.ds(pl.multiple_of(j * 256, 256), 256)
        out_ref[:, ds] = dot_nn(dl_ref[...], h_ref[:, ds]).astype(bf16)
        return 0

    lax.fori_loop(0, h_ref.shape[1] // 256, cols, 0, unroll=True)


def head_table(hidden, kept, fac, weight, labels, vocab_rows):
    tokens, width = hidden.shape
    sp = head_specs(width, tokens)
    return head_call(
        head_table_kernel,
        pl.cdiv(vocab_rows, VTILE),
        [sp["hidden"], sp["kept"], sp["tile_row"], sp["row"], sp["row"]],
        [sp["table"]],
        [((vocab_rows, width), bf16)],
        (pltpu.VMEM((VTILE, tokens), bf16),),
        (hidden, kept, fac, weight, labels),
        vocab_rows * tokens,
    )[0]


def weight_grads_kernel(u_ref, dp_ref, yn_ref, db_ref, in_ref, out_ref):
    wide_cols = dp_ref.shape[1]
    for c in range(0, wide_cols, 1024):
        cs = pl.ds(c, min(1024, wide_cols - c))
        in_ref[:, cs] = dot_tn(u_ref[...], dp_ref[:, cs]).astype(bf16)
    out_ref[...] = dot_tn(yn_ref[...], db_ref[...]).astype(bf16)


def weight_grads(normed, grad_proj, mixed, grad_branch):
    rows = normed.shape[0]
    steps = D // LANES
    part = DI // steps
    return head_call(
        weight_grads_kernel,
        steps,
        [
            pl.BlockSpec((rows, LANES), lambda i: (0, i)),
            pl.BlockSpec((rows, ZW), lambda i: (0, 0)),
            pl.BlockSpec((rows, part), lambda i: (0, i)),
            pl.BlockSpec((rows, D), lambda i: (0, 0)),
        ],
        [pl.BlockSpec((LANES, ZW), lambda i: (i, 0)), pl.BlockSpec((part, D), lambda i: (i, 0))],
        [((D, ZW), bf16), ((DI, D), bf16)],
        (),
        (normed, grad_proj, mixed, grad_branch),
        rows * (ZW + DI),
    )


def after(value, earlier):
    return lax.optimization_barrier((value, earlier))[0]


def norm_scale(values):
    return lax.rsqrt(jnp.mean(values * values, axis=-1, keepdims=True) + epsilon)


def norm_back(grad, values, gain):
    scale = norm_scale(values)
    unit = values * scale
    inner = grad * gain
    back = scale * (inner - unit * jnp.mean(inner * unit, axis=-1, keepdims=True))
    return back, jnp.sum(grad * unit, axis=0)


def wide(row):
    return jnp.pad(row, (0, LANES - row.shape[0]))[None]


def layer_vectors(vector_params, layer_index):
    offset = layer_index * PER
    pieces = []
    for size in (CONV * XBC, XBC, HEADS, HEADS, HEADS, D, DI):
        pieces.append(vector_params[offset : offset + size])
        offset += size
    conv_w, conv_b, dt_bias, decay_log, skip, pre_gain, gate_gain = pieces
    return dict(
        conv_w=conv_w.reshape(CONV, XBC),
        conv_b=conv_b[None],
        dt_bias=wide(dt_bias),
        decay_log=wide(decay_log),
        skip=jnp.repeat(skip, HDIM)[None],
        pre_gain=pre_gain,
        gate_gain=gate_gain[None],
    )


def layer_forward(hidden, w_in, w_out, vec):
    rows = hidden.shape[0]
    normed = (hidden * norm_scale(hidden) * vec["pre_gain"]).astype(bf16)
    proj = jnp.dot(normed, w_in, preferred_element_type=f32)
    pre, y, mixed, dt, cum, entering, halo = comm_call(
        scan_kernel,
        1,
        (
            proj, vec["conv_w"], vec["conv_b"], vec["dt_bias"], vec["decay_log"], vec["skip"],
            vec["gate_gain"],
        ),
        (
            ((rows, XBC), f32),
            ((rows, DI), f32),
            ((rows, DI), bf16),
            ((rows, LANES), f32),
            ((rows, LANES), f32),
            ((DI, NSTATE), bf16),
            ((8, XBC), f32),
        ),
        (
            pltpu.VMEM((rows + 8, XBC), f32),
            pltpu.VMEM((HEADS, rows, LANES), f32),
            pltpu.VMEM((PAIRS, rows, LANES), f32),
            pltpu.VMEM((PAIRS, rows, LANES), f32),
            pltpu.VMEM((LANES, rows), f32),
            pltpu.VMEM((DI, NSTATE), f32),
            pltpu.VMEM((DI, NSTATE), bf16),
            pltpu.VMEM((rows, LANES), f32),
            pltpu.SemaphoreType.DMA,
            pltpu.SemaphoreType.DMA,
            pltpu.SemaphoreType.DMA((CHAIN_STEPS,)),
            pltpu.SemaphoreType.DMA((CHAIN_STEPS,)),
        ),
        (pltpu.VMEM,) * 7,
        (pltpu.VMEM,) * 7,
        DI * NSTATE * 2,
    )
    branch = jnp.dot(mixed, w_out, preferred_element_type=f32)
    record = (hidden, normed, proj, halo, pre, dt, cum, entering, y, mixed)
    return hidden + branch, record


def layer_backward(grad_hidden, w_in, w_out, vec, record):
    hidden, normed, proj, halo, pre, dt, cum, entering, y, mixed = record
    rows = hidden.shape[0]
    grad_branch = grad_hidden.astype(bf16)
    grad_mixed = dot_nt(grad_branch, w_out)
    grad_proj, dconv, dsmall, dgate = comm_call(
        back_kernel,
        2,
        (
            grad_mixed, y, proj, halo, pre, dt, cum, entering,
            vec["conv_w"], vec["dt_bias"], vec["decay_log"], vec["skip"], vec["gate_gain"],
        ),
        (
            ((rows, ZW), bf16),
            ((8, XBC), f32),
            ((8, LANES), f32),
            ((1, DI), f32),
        ),
        (
            pltpu.VMEM((rows + 8, XBC), f32),
            pltpu.VMEM((rows + 16, XBC), f32),
            pltpu.VMEM((HEADS, rows, LANES), f32),
            pltpu.VMEM((PAIRS, rows, LANES), f32),
            pltpu.VMEM((PAIRS, rows, LANES), f32),
            pltpu.VMEM((LANES, rows), f32),
            pltpu.VMEM((rows, rows), f32),
            pltpu.VMEM((rows, LANES), f32),
            pltpu.VMEM((rows, LANES), f32),
            pltpu.VMEM((rows, LANES), f32),
            pltpu.VMEM((rows, LANES), f32),
            pltpu.VMEM((16, LANES), f32),
            pltpu.VMEM((rows, DI), f32),
            pltpu.VMEM((rows, LANES), f32),
            pltpu.VMEM((DI, NSTATE), bf16),
            pltpu.VMEM((DI, NSTATE), bf16),
            pltpu.VMEM((DI, NSTATE), f32),
            pltpu.VMEM((rows, XBC), f32),
            pltpu.VMEM((8, XBC), f32),
            pltpu.VMEM((8, XBC), f32),
            pltpu.SemaphoreType.DMA,
            pltpu.SemaphoreType.DMA,
            pltpu.SemaphoreType.DMA((CHAIN_STEPS,)),
            pltpu.SemaphoreType.DMA((CHAIN_STEPS,)),
        ),
        (pltpu.VMEM,) * 13,
        (pltpu.VMEM,) * 4,
        DI * NSTATE * 2,
    )
    grad_normed = dot_nt(grad_proj, w_in)
    grad_in, grad_out = weight_grads(normed, grad_proj, mixed, grad_branch)
    grad_prev, dpre_gain = norm_back(grad_normed, hidden, vec["pre_gain"])
    grad_vec = jnp.concatenate(
        [
            dconv[:CONV].reshape(-1),
            dconv[CONV],
            dsmall[0, :HEADS],
            dsmall[1, :HEADS],
            dsmall[2, :HEADS],
            dpre_gain,
            dgate[0],
        ]
    )
    return grad_hidden + grad_prev, grad_in, grad_out, grad_vec


def advance(weight, moment, average, grad, factor):
    scaled = grad * factor
    moment_new = 0.5 * moment + scaled
    weight_new = weight - step_rate * (scaled + 0.5 * moment_new)
    average_new = 0.5 * average + 0.5 * weight_new
    return (weight_new, moment_new, average_new, weight_new.astype(bf16))


def whole_step(
    token_ids,
    target_ids,
    seq_lengths,
    embedding,
    embedding_mom,
    embedding_avg,
    in_proj,
    in_proj_mom,
    in_proj_avg,
    out_proj,
    out_proj_mom,
    out_proj_avg,
    vector_params,
    vector_mom,
    vector_avg,
):
    groups = lax.axis_size("dp")
    shards = lax.axis_size("fsdp")
    group_index = lax.axis_index("dp")
    shard_index = lax.axis_index("fsdp")
    chunks = shards // MB
    seq_rows = token_ids.shape[2]
    rows = seq_rows // chunks
    vocab_rows, own_cols = embedding.shape
    tokens = MB * seq_rows
    total_count = jnp.sum(seq_lengths).astype(f32)
    embed_low = embedding.astype(bf16)
    in_low = in_proj.astype(bf16)
    out_low = out_proj.astype(bf16)

    ids_all = lax.all_gather(token_ids[:, 0, :], "dp", axis=0)
    ids_all = ids_all.reshape(groups, MB, chunks, rows).transpose(2, 1, 0, 3).reshape(-1)
    every = ids_all.shape[0]
    local_ids = ids_all - shard_index * vocab_rows
    inside = (local_ids >= 0) & (local_ids < vocab_rows)
    sorted_ids, sorted_tok = lax.sort(
        (jnp.where(inside, local_ids, vocab_rows), jnp.arange(every, dtype=jnp.int32)),
        num_keys=1,
    )
    held_here = sorted_ids < vocab_rows
    count = jnp.sum(held_here.astype(jnp.int32)).reshape(1)
    row_list = jnp.where(held_here, sorted_ids, 0)
    tok_list = jnp.where(held_here, sorted_tok, every)
    (looked,) = local_call(
        lookup_kernel,
        (count, row_list, tok_list, embedding),
        (((every, own_cols), bf16),),
        scratch=(pltpu.VMEM((every + 8, own_cols), f32),),
        in_smem=(0, 1, 2),
    )
    mine = lax.psum_scatter(
        looked.reshape(shards * groups * rows, own_cols), "fsdp", scatter_dimension=0, tiled=True
    )
    mine = lax.all_to_all(mine.reshape(groups, rows, own_cols), "dp", 0, 0)
    hidden = mine.transpose(1, 0, 2).reshape(rows, D).astype(f32)

    shards = []
    for l in range(LAYERS):
        shards += [in_low[l], out_low[l]]
    shards = after(shards, looked)
    gathered = gather_layers(shards)
    w_in, w_out = gathered[0::2], gathered[1::2]
    embed_low = after(embed_low, gathered)
    table = lax.all_gather(embed_low, "dp", axis=1, tiled=True)

    vecs = [layer_vectors(vector_params, l) for l in range(LAYERS)]
    final_gain = vector_params[LAYERS * PER :]
    records = []
    for l in range(LAYERS):
        hidden, record = layer_forward(hidden, w_in[l], w_out[l], vecs[l])
        records.append(record)

    final_low = (hidden * norm_scale(hidden) * final_gain).astype(bf16)

    def in_order(per_seq):
        return per_seq.reshape(MB, chunks, rows).transpose(1, 0, 2).reshape(1, tokens)

    labels = in_order(target_ids[:, 0, :])
    lengths = lax.dynamic_index_in_dim(seq_lengths, group_index, 1, keepdims=True)
    valid = in_order((jnp.arange(seq_rows)[None, :] < lengths).astype(f32))
    local_labels = labels - shard_index * vocab_rows
    weight = valid / total_count
    kept, group_hidden, lse, fac, target = head_stats(table, final_low, local_labels, weight)
    own_mask = jnp.arange(tokens) // rows == shard_index
    per_row = jnp.where(own_mask, lse[0] + z_weight * lse[0] * lse[0], 0.0)
    loss_sum = jnp.sum((per_row - 0.9 * target[0]) * valid[0])
    own_valid = lax.dynamic_slice_in_dim(valid[0], shard_index * rows, rows)
    hidden_sum = jnp.sum(final_low.astype(f32) * own_valid[:, None], axis=0)
    column_sum = jnp.zeros((groups, own_cols), f32)
    column_sum = jnp.where(
        jnp.arange(groups)[:, None] == group_index, jnp.sum(embed_low.astype(f32), axis=0), column_sum
    ).reshape(D)

    rows_grad = head_rows(table, kept, fac, weight, local_labels)
    own_grad = lax.psum_scatter(
        rows_grad, "fsdp", scatter_dimension=0, tiled=True
    ).astype(f32)
    table_grad = head_table(group_hidden, kept, fac, weight, local_labels, vocab_rows)
    table_part = lax.psum_scatter(table_grad, "dp", scatter_dimension=1, tiled=True)

    grad_hidden, dfinal = norm_back(after(own_grad, table_grad), hidden, final_gain)
    in_parts = [None] * LAYERS
    out_parts = [None] * LAYERS
    vec_parts = [None] * LAYERS
    for l in reversed(range(LAYERS)):
        grad_hidden, grad_in, grad_out, vec_parts[l] = layer_backward(
            grad_hidden, w_in[l], w_out[l], vecs[l], records[l]
        )
        if l == 0:
            sent = grad_hidden.astype(bf16).reshape(rows, groups, own_cols).transpose(1, 0, 2)
            sent = lax.all_to_all(sent, "dp", 0, 0)
            spread = lax.all_gather(sent, "fsdp", axis=0).reshape(every, own_cols)
        in_parts[l], out_parts[l] = grad_in, grad_out
    whole = []
    for l in range(LAYERS):
        whole += [in_parts[l], out_parts[l]]
    summed_parts = reduce_layers(whole)
    spread = after(spread, summed_parts)
    table_total, table_squares = local_call(
        spread_kernel,
        (count, row_list, tok_list, spread, table_part),
        (((vocab_rows, own_cols), f32), ((8, own_cols), f32)),
        scratch=(pltpu.VMEM((every + 8, own_cols), f32),),
        in_smem=(0, 1, 2),
    )
    grad_in_all = jnp.stack(summed_parts[0::2])
    grad_out_all = jnp.stack(summed_parts[1::2])
    owner_squares = (
        jnp.sum(grad_in_all * grad_in_all)
        + jnp.sum(grad_out_all * grad_out_all)
        + jnp.sum(table_squares)
    )
    small = vector_params.shape[0]
    used = small + 2 * D + 2
    padded = pl.cdiv(used, 16 * LANES) * 16 * LANES
    packed = jnp.concatenate(
        vec_parts
        + [
            dfinal,
            hidden_sum,
            column_sum,
            owner_squares.reshape(1),
            loss_sum.reshape(1),
            jnp.zeros((padded - used,), f32),
        ]
    )
    packed = total_of(packed.reshape(-1, LANES)).reshape(-1)
    vector_total = packed[:small]
    hidden_total = packed[small : small + D]
    column_total = packed[small + D : small + 2 * D]
    squares_total = packed[used - 2]
    mean_part = jnp.sum(hidden_total * column_total) * (0.1 / VOCAB)
    loss_total = packed[used - 1] - mean_part
    grad_norm = jnp.sqrt(squares_total + jnp.sum(vector_total * vector_total))
    factor = jnp.minimum(1.0, clip_limit / grad_norm)
    loss_value = loss_total / total_count
    return (
        loss_value,
        grad_norm,
        *advance(embedding, embedding_mom, embedding_avg, table_total, factor),
        *advance(in_proj, in_proj_mom, in_proj_avg, grad_in_all, factor),
        *advance(out_proj, out_proj_mom, out_proj_avg, grad_out_all, factor),
        *advance(vector_params, vector_mom, vector_avg, vector_total, factor),
    )


def solution(mesh):
    table_spec = P("fsdp", "dp")
    weight_spec = P(None, ("dp", "fsdp"), None)
    return jax.shard_map(
        whole_step,
        mesh=mesh,
        in_specs=(
            P(None, "dp", None),
            P(None, "dp", None),
            P(),
            *(table_spec,) * 3,
            *(weight_spec,) * 6,
            *(P(),) * 3,
        ),
        out_specs=(
            P(),
            P(),
            *(table_spec,) * 4,
            *(weight_spec,) * 8,
            *(P(),) * 4,
        ),
        check_vma=False,
    )
```

```python
import functools

import jax
import jax.numpy as jnp
from jax import lax
from jax.experimental import pallas as pl
from jax.experimental.pallas import tpu as pltpu
from jax.sharding import PartitionSpec as P


D = 1024
HEADS = 32
HDIM = 64
NSTATE = 128
CONV = 4
VOCAB = 50288
LAYERS = 2
MB = 2
DI = 2048
XBC = 2304
ZW = 4384
PER = 14688
LANES = 128
PAIRS = DI // LANES

epsilon = 1e-05
z_weight = 0.001
clip_limit = 0.2
step_rate = 1000.0
highest = lax.Precision.HIGHEST
bf16 = jnp.bfloat16
f32 = jnp.float32
VMEM_LIMIT = 62 * 1024 * 1024
OFF = -1e30


def dot_nn(a, b, precision=None):
    return lax.dot_general(
        a, b, (((1,), (0,)), ((), ())), precision=precision, preferred_element_type=f32
    )


def dot_nt(a, b, precision=None):
    return lax.dot_general(
        a, b, (((1,), (1,)), ((), ())), precision=precision, preferred_element_type=f32
    )


def dot_tn(a, b, precision=None):
    return lax.dot_general(
        a, b, (((0,), (0,)), ((), ())), precision=precision, preferred_element_type=f32
    )


def silu(v):
    return v * lax.logistic(v)


def silu_grad(v):
    s = lax.logistic(v)
    return s * (1.0 + v * (1.0 - s))


def local_call(kernel, ins, outs, scratch=(), in_smem=(), flops=0):
    total = sum(a.size * a.dtype.itemsize for a in ins)
    return pl.pallas_call(
        kernel,
        out_shape=[jax.ShapeDtypeStruct(shape, kind) for shape, kind in outs],
        in_specs=[
            pl.BlockSpec(memory_space=pltpu.SMEM if i in in_smem else pltpu.VMEM)
            for i in range(len(ins))
        ],
        out_specs=[pl.BlockSpec(memory_space=pltpu.VMEM) for _ in outs],
        scratch_shapes=list(scratch),
        compiler_params=pltpu.CompilerParams(vmem_limit_bytes=VMEM_LIMIT),
        cost_estimate=pl.CostEstimate(
            flops=flops or total, transcendentals=0, bytes_accessed=2 * total
        ),
    )(*ins)


def lookup_kernel(count_ref, row_ref, tok_ref, table_ref, out_ref, low_ref, sum_ref, held):
    tokens = out_ref.shape[0]
    step = 512

    def clear(i, _):
        held[pl.ds(pl.multiple_of(i * step, step), step), :] = jnp.zeros(
            (step, held.shape[1]), f32
        )
        return 0

    lax.fori_loop(0, tokens // step, clear, 0)

    def move(i, _):
        for k in range(8):
            row = row_ref[i * 8 + k]
            tok = tok_ref[i * 8 + k]
            held[pl.ds(tok, 1), :] = table_ref[pl.ds(row, 1), :]
        return 0

    lax.fori_loop(0, (count_ref[0] + 7) // 8, move, 0)

    def put(i, _):
        rows = pl.ds(pl.multiple_of(i * step, step), step)
        out_ref[rows, :] = held[rows, :].astype(bf16)
        return 0

    lax.fori_loop(0, tokens // step, put, 0)
    rows_all = table_ref.shape[0]
    whole = rows_all // step

    def cast(i, total):
        rows = pl.ds(pl.multiple_of(i * step, step), step)
        low = table_ref[rows, :].astype(bf16)
        low_ref[rows, :] = low
        return total + jnp.sum(low.astype(f32).reshape(step // 8, 8, -1), axis=0)

    sum_ref[...] = lax.fori_loop(0, whole, cast, jnp.zeros(sum_ref.shape, f32))
    if rows_all > whole * step:
        low = table_ref[whole * step :, :].astype(bf16)
        low_ref[whole * step :, :] = low
        sum_ref[0:1, :] += jnp.sum(low.astype(f32), axis=0, keepdims=True)


def spread_kernel(count_ref, row_ref, tok_ref, grad_ref, base_ref, out_ref, square_ref, held):
    tokens = grad_ref.shape[0]
    step = 512
    rows_all = out_ref.shape[0]

    def take(i, _):
        rows = pl.ds(pl.multiple_of(i * step, step), step)
        held[rows, :] = grad_ref[rows, :].astype(f32)
        return 0

    lax.fori_loop(0, tokens // step, take, 0)
    held[pl.ds(tokens, 8), :] = jnp.zeros((8, held.shape[1]), f32)

    whole = rows_all // step

    def start(i, _):
        rows = pl.ds(pl.multiple_of(i * step, step), step)
        out_ref[rows, :] = base_ref[rows, :].astype(f32)
        return 0

    lax.fori_loop(0, whole, start, 0)
    if rows_all > whole * step:
        out_ref[whole * step :, :] = base_ref[whole * step :, :].astype(f32)

    def move(i, _):
        for k in range(8):
            row = row_ref[i * 8 + k]
            tok = tok_ref[i * 8 + k]
            out_ref[pl.ds(row, 1), :] = out_ref[pl.ds(row, 1), :] + held[pl.ds(tok, 1), :]
        return 0

    lax.fori_loop(0, (count_ref[0] + 7) // 8, move, 0)

    def square(i, total):
        part = out_ref[pl.ds(pl.multiple_of(i * step, step), step), :]
        return total + jnp.sum((part * part).reshape(step // 8, 8, -1), axis=0)

    total = lax.fori_loop(0, whole, square, jnp.zeros(square_ref.shape, f32))
    square_ref[...] = total
    if rows_all > whole * step:
        part = out_ref[whole * step :, :]
        square_ref[0:1, :] += jnp.sum(part * part, axis=0, keepdims=True)


MESH = pl.DeviceIdType.MESH


def remote(src, dst, send, recv, dp, fsdp):
    return pltpu.make_async_remote_copy(
        src_ref=src,
        dst_ref=dst,
        send_sem=send,
        recv_sem=recv,
        device_id=(dp, fsdp),
        device_id_type=MESH,
    )


def comm_call(kernel, number, ins, outs, scratch, in_spaces, out_spaces, sent):
    return pl.pallas_call(
        kernel,
        out_shape=[jax.ShapeDtypeStruct(shape, kind) for shape, kind in outs],
        in_specs=[pl.BlockSpec(memory_space=space) for space in in_spaces],
        out_specs=[pl.BlockSpec(memory_space=space) for space in out_spaces],
        scratch_shapes=list(scratch),
        compiler_params=pltpu.CompilerParams(
            collective_id=number, has_side_effects=True, vmem_limit_bytes=VMEM_LIMIT
        ),
        cost_estimate=pl.CostEstimate(flops=sent, transcendentals=0, bytes_accessed=2 * sent),
    )(*ins)


def greet_groups():
    dp = lax.axis_index("dp")
    me = lax.axis_index("fsdp")
    groups = lax.axis_size("dp")
    barrier = pltpu.get_barrier_semaphore()
    others = [lax.rem(dp + other, groups) for other in range(1, groups)]
    for other in others:
        pl.semaphore_signal(barrier, inc=1, device_id=(other, me), device_id_type=MESH)
    pl.semaphore_wait(barrier, groups - 1)
    return dp, me, others


def share_kernel(in_ref, out_ref, send, recv):
    dp, me, others = greet_groups()
    for other in others:
        remote(in_ref, out_ref.at[dp], send.at[other], recv.at[dp], other, me).start()
    out_ref[dp] = in_ref[...]
    for other in others:
        copy = remote(in_ref, out_ref.at[other], send.at[other], recv.at[other], other, me)
        copy.wait_recv()
        copy.wait_send()


def to_rows_kernel(in_ref, out_ref, landed, send, recv):
    dp, me, others = greet_groups()
    for other in others:
        remote(in_ref.at[other], landed.at[dp], send.at[other], recv.at[dp], other, me).start()
    landed[dp] = in_ref[dp]
    for other in others:
        remote(in_ref.at[other], landed.at[other], send.at[other], recv.at[other], other, me).wait_recv()
    cols = in_ref.shape[2]
    for g in range(in_ref.shape[0]):
        out_ref[:, g * cols : (g + 1) * cols] = landed[g].astype(f32)
    for other in others:
        remote(in_ref.at[other], landed.at[other], send.at[other], recv.at[other], other, me).wait_send()


def to_columns_kernel(in_ref, out_ref, parts, send, recv):
    dp, me, others = greet_groups()
    cols = out_ref.shape[2]
    for g in range(out_ref.shape[0]):
        parts[g] = in_ref[:, g * cols : (g + 1) * cols].astype(bf16)
    for other in others:
        remote(parts.at[other], out_ref.at[dp], send.at[other], recv.at[dp], other, me).start()
    out_ref[dp] = parts[dp]
    for other in others:
        copy = remote(parts.at[other], out_ref.at[other], send.at[other], recv.at[other], other, me)
        copy.wait_recv()
        copy.wait_send()


def group_call(kernel, number, array, out, scratch=()):
    groups = lax.axis_size("dp")
    return comm_call(
        kernel,
        number,
        (array,),
        (out,),
        tuple(scratch)
        + (pltpu.SemaphoreType.DMA((groups,)), pltpu.SemaphoreType.DMA((groups,))),
        (pltpu.VMEM,),
        (pltpu.VMEM,),
        array.size * 2,
    )[0]


CHAIN_STEPS = 8
PART = DI // CHAIN_STEPS


def chunk_place(direction):
    place = lax.axis_index("fsdp") // MB
    count = lax.axis_size("fsdp") // MB
    first = place == (0 if direction > 0 else count - 1)
    final = place == (count - 1 if direction > 0 else 0)
    return first, final


def chain_barrier(direction, first, final):
    dp = lax.axis_index("dp")
    me = lax.axis_index("fsdp")
    barrier = pltpu.get_barrier_semaphore()

    @pl.when(jnp.logical_not(first))
    def _():
        pl.semaphore_signal(
            barrier, inc=1, device_id=(dp, me - MB * direction), device_id_type=MESH
        )

    @pl.when(jnp.logical_not(final))
    def _():
        pl.semaphore_wait(barrier, 1)


def to_next(src, dst, send, recv, direction):
    dp = lax.axis_index("dp")
    return remote(src, dst, send, recv, dp, lax.axis_index("fsdp") + MB * direction)


def chain_step(g, direction, first, final, got, give, local, col, rows, send, recv):
    def copy():
        at = pl.ds(pl.multiple_of(g * PART, PART), PART)
        return to_next(give.at[at], got.at[at], send.at[g], recv.at[g], direction)

    @pl.when(jnp.logical_not(first))
    def _():
        copy().wait_recv()

    @pl.when(jnp.logical_not(final))
    def _():
        for i in range(PART // HDIM):
            h = pl.ds(pl.multiple_of(g * PART + i * HDIM, HDIM), HDIM)
            decay = jnp.exp(col[g * (PART // HDIM) + i, rows - 1 : rows, :])
            give[h, :] = (decay * got[h, :].astype(f32) + local[h, :]).astype(bf16)
        copy().start()


def chain_end(direction, final, got, give, send, recv):
    @pl.when(jnp.logical_not(final))
    def _():
        for g in range(CHAIN_STEPS):
            at = pl.ds(g * PART, PART)
            to_next(give.at[at], got.at[at], send.at[g], recv.at[g], direction).wait_send()


def bits_of(size):
    return [1 << b for b in range(size.bit_length() - 1)]


def total_kernel(in_ref, out_ref, work, got, send, recv):
    dp = lax.axis_index("dp")
    me = lax.axis_index("fsdp")
    half = in_ref.shape[0] // 2
    core = me % MB
    partners = [("f", b) for b in bits_of(lax.axis_size("fsdp")) if b > 1]
    partners += [("d", b) for b in bits_of(lax.axis_size("dp"))]

    def across(kind, bit):
        ids, other = (me, lambda v: (dp, v)) if kind == "f" else (dp, lambda v: (v, me))
        return other(jnp.where((ids // bit) % 2 == 1, ids - bit, ids + bit))

    mate = across("f", 1)
    barrier = pltpu.get_barrier_semaphore()
    for target in [mate] + [across(*p) for p in partners]:
        pl.semaphore_signal(barrier, inc=1, device_id=target, device_id_type=MESH)
    pl.semaphore_wait(barrier, 1 + len(partners))

    mine = pl.ds(pl.multiple_of(core * half, 8), half)
    theirs = pl.ds(pl.multiple_of((1 - core) * half, 8), half)
    copy = remote(in_ref.at[theirs], got.at[0], send.at[0], recv.at[0], *mate)
    copy.start()
    copy.wait()
    work[0] = in_ref[mine, :] + got[0]
    for i, p in enumerate(partners):
        copy = remote(work.at[i], got.at[i + 1], send.at[i + 1], recv.at[i + 1], *across(*p))
        copy.start()
        copy.wait()
        work[i + 1] = work[i] + got[i + 1]
    n = len(partners)
    copy = remote(work.at[n], got.at[n + 1], send.at[n + 1], recv.at[n + 1], *mate)
    copy.start()
    copy.wait()
    out_ref[mine, :] = work[n]
    out_ref[theirs, :] = got[n + 1]


def total_of(array):
    rows = array.shape[0]
    steps = len(bits_of(lax.axis_size("fsdp"))) - 1 + len(bits_of(lax.axis_size("dp")))
    return comm_call(
        total_kernel,
        3,
        (array,),
        ((array.shape, f32),),
        (
            pltpu.VMEM((steps + 1, rows // 2, LANES), f32),
            pltpu.VMEM((steps + 2, rows // 2, LANES), f32),
            pltpu.SemaphoreType.DMA((steps + 2,)),
            pltpu.SemaphoreType.DMA((steps + 2,)),
        ),
        (pltpu.VMEM,),
        (pltpu.VMEM,),
        array.size * 4 * 3,
    )[0]


def snake(place, size):
    return jnp.where(place < size // 2, place, size // 2 + size - 1 - place)


def wrap(value, size):
    return lax.rem(value + size, size)


def gather_kernel(*refs):
    arrays = 2 * LAYERS
    own = refs[:arrays]
    full = refs[arrays : 2 * arrays]
    local_sem, z_send, z_recv, ring_send, ring_recv, mate_send, mate_recv = refs[2 * arrays :]
    dp = lax.axis_index("dp")
    me = lax.axis_index("fsdp")
    size = lax.axis_size("dp")
    count = lax.axis_size("fsdp") // MB
    core = me % MB
    k = me // MB
    ring = snake(dp, size)
    reach = size // 2
    right = snake(wrap(ring + 1, size), size)
    left = snake(wrap(ring - 1, size), size)
    mate = k * MB + 1 - core
    up, down = me + MB, me - MB
    has_up, has_down = k < count - 1, k > 0
    barrier = pltpu.get_barrier_semaphore()
    for target in ((right, me), (left, me), (dp, mate)):
        pl.semaphore_signal(barrier, inc=1, device_id=target, device_id_type=MESH)

    @pl.when(has_up)
    def _():
        pl.semaphore_signal(barrier, inc=1, device_id=(dp, up), device_id_type=MESH)

    @pl.when(has_down)
    def _():
        pl.semaphore_signal(barrier, inc=1, device_id=(dp, down), device_id_type=MESH)

    pl.semaphore_wait(barrier, 3 + jnp.where(has_up, 1, 0) + jnp.where(has_down, 1, 0))

    def spot(a, d, z, c):
        return full[a].at[d, z, c]

    def chain(a, src, z, side):
        return remote(
            src, spot(a, dp, z, core), z_send.at[a, z], z_recv.at[a, z], dp, up if side == 0 else down
        )

    def chain_own(a, side):
        return remote(
            own[a],
            spot(a, dp, k, core),
            z_send.at[a, count + side],
            z_recv.at[a, k],
            dp,
            up if side == 0 else down,
        )

    def round_ring(a, src, d, z, side):
        return remote(
            src,
            spot(a, d, z, core),
            ring_send.at[a, side],
            ring_recv.at[a, d, z],
            right if side == 0 else left,
            me,
        )

    def to_mate(a, src, d, z):
        return remote(src, spot(a, d, z, core), mate_send.at[a], mate_recv.at[a], dp, mate)

    def carried(a, side):
        return (a < arrays // 2) == (side == 0)

    for a in range(arrays):

        @pl.when(has_up)
        def _(a=a):
            chain_own(a, 0).start()

        @pl.when(has_down)
        def _(a=a):
            chain_own(a, 1).start()

    for a in range(arrays):
        for side in (0, 1):
            round_ring(a, own[a], dp, k, side).start()
    for a in range(arrays):
        to_mate(a, own[a], dp, k).start()
        pltpu.make_async_copy(own[a], spot(a, dp, k, core), local_sem.at[a]).start()

    def ring_step(z, s):
        for side in (0, 1):
            origin = snake(wrap(ring - s if side == 0 else ring + s, size), size)
            for a in range(arrays):
                if s == reach and not carried(a, side):
                    continue
                piece = spot(a, origin, z, core)
                round_ring(a, piece, origin, z, side).wait_recv()
                if s + 1 < reach or (s + 1 == reach and carried(a, side)):
                    round_ring(a, piece, origin, z, side).start()
                to_mate(a, piece, origin, z).start()

    def arrive(z, side):
        for a in range(arrays):
            piece = spot(a, dp, z, core)
            chain(a, piece, z, side).wait_recv()

            @pl.when(has_up if side == 0 else has_down)
            def _(a=a, piece=piece):
                chain(a, piece, z, side).start()

            for way in (0, 1):
                round_ring(a, piece, dp, z, way).start()
            to_mate(a, piece, dp, z).start()

    def both_ways(far, act):
        if far == 0:
            act(k, 0)
            return

        @pl.when(k >= far)
        def _():
            act(k - far, 0)

        @pl.when(k + far < count)
        def _():
            act(k + far, 1)

    for turn in range(1, count + reach):
        if turn < count:
            both_ways(turn, arrive)
        for s in range(1, reach + 1):
            if 0 <= turn - s < count:
                both_ways(turn - s, lambda z, side, s=s: ring_step(z, s))

    for a in range(arrays):
        pltpu.make_async_copy(own[a], spot(a, dp, k, core), local_sem.at[a]).wait()
        for side in (0, 1):
            sent = full[a].at[pl.ds(0, reach if carried(a, side) else reach - 1), :, core]
            remote(sent, sent, ring_send.at[a, side], ring_recv.at[a, 0, 0], dp, mate).wait_send()
        whole = full[a].at[:, :, core]
        remote(whole, whole, mate_send.at[a], mate_recv.at[a], dp, mate).wait_send()
        whole = full[a].at[:, :, 1 - core]
        remote(whole, whole, mate_send.at[a], mate_recv.at[a], dp, mate).wait_recv()

        @pl.when(has_up)
        def _(a=a):
            chain_own(a, 0).wait_send()

        @pl.when(has_down)
        def _(a=a):
            chain_own(a, 1).wait_send()

        for far in range(1, count):

            @pl.when(jnp.logical_and(k >= far, has_up))
            def _(a=a, far=far):
                chain(a, spot(a, dp, k - far, core), k - far, 0).wait_send()

            @pl.when(jnp.logical_and(k + far < count, has_down))
            def _(a=a, far=far):
                chain(a, spot(a, dp, k + far, core), k + far, 1).wait_send()


def gather_layers(shards):
    size, count = lax.axis_size("dp"), lax.axis_size("fsdp") // MB
    arrays = len(shards)
    outs = comm_call(
        gather_kernel,
        4,
        shards,
        tuple(((size, count, MB) + s.shape, bf16) for s in shards),
        (
            pltpu.SemaphoreType.DMA((arrays,)),
            pltpu.SemaphoreType.DMA((arrays, count + 2)),
            pltpu.SemaphoreType.DMA((arrays, count)),
            pltpu.SemaphoreType.DMA((arrays, 2)),
            pltpu.SemaphoreType.DMA((arrays, size, count)),
            pltpu.SemaphoreType.DMA((arrays,)),
            pltpu.SemaphoreType.DMA((arrays,)),
        ),
        (pltpu.VMEM,) * arrays,
        (pl.ANY,) * arrays,
        sum(s.size * 2 for s in shards) * 24,
    )
    return [o.reshape(size * count * MB * s.shape[0], s.shape[1]) for o, s in zip(outs, shards)]


def add_rows(dst, first, *others):
    rows = dst.shape[0]
    step = min(rows, 16)

    def one(i, _):
        at = pl.ds(pl.multiple_of(i * step, step), step)
        total = first[at, :].astype(f32)
        for other in others:
            total = total + other[at, :].astype(f32)
        dst[at, :] = total.astype(dst.dtype)
        return 0

    lax.fori_loop(0, rows // step, one, 0)


def reduce_kernel(*refs):
    arrays = 2 * LAYERS
    grads = refs[:arrays]
    outs = refs[arrays : 2 * arrays]
    held, given, come, chained = (
        refs[(2 + i) * arrays : (3 + i) * arrays] for i in range(4)
    )
    load_sem, mate_send, mate_recv, ring_send, ring_recv, z_send, z_recv = refs[6 * arrays :]
    dp = lax.axis_index("dp")
    me = lax.axis_index("fsdp")
    size = lax.axis_size("dp")
    count = lax.axis_size("fsdp") // MB
    core = me % MB
    k = me // MB
    ring = snake(dp, size)
    reach = size // 2
    right = snake(wrap(ring + 1, size), size)
    left = snake(wrap(ring - 1, size), size)
    mate = k * MB + 1 - core
    up, down = me + MB, me - MB
    has_up, has_down = k < count - 1, k > 0

    def load(a):
        return pltpu.make_async_copy(grads[a].at[:, :, core], held[a], load_sem.at[a])

    for a in range(arrays):
        load(a).start()
    barrier = pltpu.get_barrier_semaphore()
    for target in ((right, me), (left, me), (dp, mate)):
        pl.semaphore_signal(barrier, inc=1, device_id=target, device_id_type=MESH)

    @pl.when(has_up)
    def _():
        pl.semaphore_signal(barrier, inc=1, device_id=(dp, up), device_id_type=MESH)

    @pl.when(has_down)
    def _():
        pl.semaphore_signal(barrier, inc=1, device_id=(dp, down), device_id_type=MESH)

    pl.semaphore_wait(barrier, 3 + jnp.where(has_up, 1, 0) + jnp.where(has_down, 1, 0))

    def away(j, side):
        return snake(wrap(ring + j if side == 0 else ring - j, size), size)

    def to_mate(a, d):
        return remote(
            grads[a].at[d, :, 1 - core], given[a].at[d], mate_send.at[a], mate_recv.at[a, d], dp, mate
        )

    def carried(a, side):
        return (a < arrays // 2) == (side == 0)

    def targets(j):
        if j == 0:
            return [dp]
        if j == reach:
            return [away(j, 0)]
        return [away(j, 0), away(j, 1)]

    for j in range(reach, -1, -1):
        for d in targets(j):
            for a in range(arrays):
                to_mate(a, d).start()

    for a in range(arrays):
        load(a).wait()

    def add_mate(d):
        for a in range(arrays):
            to_mate(a, d).wait_recv()

            def one(z, _, a=a):
                add_rows(held[a].at[d, z], held[a].at[d, z], given[a].at[d, z])
                return 0

            lax.fori_loop(0, count, one, 0)

    def first_step(a, side):
        d = away(reach, 0)
        return remote(
            held[a].at[d], come[a].at[side, 0], ring_send.at[a, side], ring_recv.at[a, side, 0, 0],
            right if side == 0 else left, me,
        )

    def next_step(a, side, s, z):
        d = away(reach - s, side)
        return remote(
            held[a].at[d, z], come[a].at[side, s, z], ring_send.at[a, side],
            ring_recv.at[a, side, s, z], right if side == 0 else left, me,
        )

    far_most = jnp.maximum(k, count - 1 - k)
    near_most = jnp.minimum(k, count - 1 - k)
    uneven = far_most - near_most
    long_side = jnp.where(count - 1 - k > k, 1, -1)

    def chunk_at(i):
        j = jnp.maximum(i - uneven, 0)
        paired = k + (1 - 2 * (j % 2)) * (near_most - j // 2)
        return jnp.where(i < uneven, k + long_side * (far_most - i), paired)

    add_mate(away(reach, 0))
    for a in range(arrays):
        first_step(a, 0 if carried(a, 0) else 1).start()
    for s in range(1, reach):
        for side in (0, 1):
            add_mate(away(reach - s, side))
        if s == 1:
            for a in range(arrays):
                first_step(a, 0 if carried(a, 0) else 1).wait_recv()

        def pass_on(i, _, s=s):
            z = chunk_at(i)
            for side in (0, 1):
                d = away(reach - s, side)
                for a in range(arrays):
                    if s > 1:
                        next_step(a, side, s - 1, z).wait_recv()
                    if s > 1 or carried(a, side):
                        add_rows(held[a].at[d, z], held[a].at[d, z], come[a].at[side, s - 1, z])
                    next_step(a, side, s, z).start()
            return 0

        lax.fori_loop(0, count, pass_on, 0)
    add_mate(dp)

    def along(a, side, z):
        return remote(
            held[a].at[dp, z], chained[a].at[side, z], z_send.at[a, z], z_recv.at[a, side, z],
            dp, up if side == 0 else down,
        )

    def finish(i, _):
        z = chunk_at(i)
        for a in range(arrays):
            for side in (0, 1):
                next_step(a, side, reach - 1, z).wait_recv()
            add_rows(
                held[a].at[dp, z],
                held[a].at[dp, z],
                come[a].at[0, reach - 1, z],
                come[a].at[1, reach - 1, z],
            )
            for side in (0, 1):
                beyond = z > k if side == 0 else z < k
                fed = has_down if side == 0 else has_up

                @pl.when(jnp.logical_and(fed, jnp.logical_or(beyond, z == k)))
                def _(a=a, side=side):
                    along(a, side, z).wait_recv()
                    add_rows(held[a].at[dp, z], held[a].at[dp, z], chained[a].at[side, z])

                @pl.when(beyond)
                def _(a=a, side=side):
                    along(a, side, z).start()

        return 0

    lax.fori_loop(0, count, finish, 0)
    for a in range(arrays):
        add_rows(outs[a], held[a].at[dp, k])
        for side in (0, 1):
            sent = held[a].at[pl.ds(0, reach if carried(a, side) else reach - 1)]
            remote(
                sent, sent, ring_send.at[a, side], ring_recv.at[a, side, 0, 0], dp, mate
            ).wait_send()
        remote(
            given[a], given[a], mate_send.at[a], mate_recv.at[a, 0], dp, mate
        ).wait_send()

    def sent_along(z, _):
        for a in range(arrays):

            @pl.when(z != k)
            def _(a=a):
                along(a, 0, z).wait_send()

        return 0

    lax.fori_loop(0, count, sent_along, 0)


def reduce_layers(grads):
    size, count = lax.axis_size("dp"), lax.axis_size("fsdp") // MB
    arrays = len(grads)
    reach = size // 2
    shards = [(g.shape[0] // (size * count * MB), g.shape[1]) for g in grads]
    blocks = [g.reshape((size, count, MB) + s) for g, s in zip(grads, shards)]
    return comm_call(
        reduce_kernel,
        5,
        blocks,
        tuple((s, f32) for s in shards),
        tuple(pltpu.VMEM((size, count) + s, bf16) for s in shards) * 2
        + tuple(pltpu.VMEM((2, reach, count) + s, bf16) for s in shards)
        + tuple(pltpu.VMEM((2, count) + s, bf16) for s in shards)
        + (
            pltpu.SemaphoreType.DMA((arrays,)),
            pltpu.SemaphoreType.DMA((arrays,)),
            pltpu.SemaphoreType.DMA((arrays, size)),
            pltpu.SemaphoreType.DMA((arrays, 2)),
            pltpu.SemaphoreType.DMA((arrays, 2, reach, count)),
            pltpu.SemaphoreType.DMA((arrays, count)),
            pltpu.SemaphoreType.DMA((arrays, 2, count)),
        ),
        (pl.ANY,) * arrays,
        (pltpu.VMEM,) * arrays,
        sum(g.size * 2 for g in grads),
    )


def pair_lanes(p):
    return pl.ds(pl.multiple_of(p * LANES, LANES), LANES)


def first_half(rows):
    return lax.broadcasted_iota(jnp.int32, (rows, LANES), 1) < HDIM


def spread_columns(values, column, per_pair, rows):
    half = first_half(rows)
    for p in range(PAIRS):
        left = jnp.broadcast_to(values[:, 2 * p : 2 * p + 1], (rows, LANES))
        right = jnp.broadcast_to(values[:, 2 * p + 1 : 2 * p + 2], (rows, LANES))
        if column is not None:
            column[2 * p] = left
            column[2 * p + 1] = right
        if per_pair is not None:
            per_pair[p] = jnp.where(half, left, right)


def scan_kernel(
    proj_ref, cw_ref, cb_ref, dtb_ref, al_ref, sk_ref, gg_ref,
    pre_ref, y_ref, yn_ref, dt_ref, cum_ref, got, halo_ref,
    pad, col, tcol, lcol, lrow, st, give, square, edge_send, edge_recv, send, recv,
):
    rows = proj_ref.shape[0]
    first, final = chunk_place(1)
    chain_barrier(1, first, final)
    edge = to_next(
        proj_ref.at[pl.ds(rows - 8, 8), pl.ds(DI, XBC)], halo_ref, edge_send, edge_recv, 1
    )

    @pl.when(jnp.logical_not(final))
    def _():
        edge.start()

    @pl.when(first)
    def _():
        halo_ref[...] = jnp.zeros(halo_ref.shape, f32)
        got[...] = jnp.zeros(got.shape, bf16)

    pad[8:, :] = proj_ref[:, DI : DI + XBC]
    dt_ref[...] = jnp.zeros((rows, LANES), f32)
    dt_ref[:, 0:HEADS] = proj_ref[:, DI + XBC :]
    drive = dt_ref[...] + dtb_ref[...]
    dt = jnp.maximum(drive, 0.0) + jnp.log1p(jnp.exp(-jnp.abs(drive)))
    dt_ref[...] = dt
    rate = dt * (-jnp.exp(al_ref[...]))
    ri = lax.broadcasted_iota(jnp.int32, (rows, rows), 0)
    ci = lax.broadcasted_iota(jnp.int32, (rows, rows), 1)
    causal = ri >= ci
    cum = dot_nn(jnp.where(causal, 1.0, 0.0), rate, highest)
    cum_ref[...] = cum
    lrow[...] = cum.T
    spread_columns(cum, col, lcol, rows)
    spread_columns(dt, None, tcol, rows)

    @pl.when(jnp.logical_not(first))
    def _():
        edge.wait_recv()

    pad[0:8, :] = halo_ref[...]

    def conv(i, _):
        xs = pair_lanes(i)
        out = jnp.broadcast_to(cb_ref[0:1, xs], (rows, LANES))
        for k in range(CONV):
            out = out + cw_ref[k : k + 1, xs] * pad[5 + k : 5 + k + rows, xs]
        pre_ref[:, xs] = out
        return 0

    lax.fori_loop(0, XBC // LANES, conv, 0)
    bm = silu(pre_ref[:, DI : DI + NSTATE]).astype(bf16)
    cm = silu(pre_ref[:, DI + NSTATE :]).astype(bf16)
    cb = dot_nt(cm, bm)
    half = first_half(rows)

    def states(p, _):
        xs = pair_lanes(p)
        lp = lcol[p]
        tail = jnp.exp(lp[rows - 1 : rows, :] - lp) * tcol[p]
        st[xs, :] = dot_tn((tail * silu(pre_ref[:, xs])).astype(bf16), bm)
        return 0

    lax.fori_loop(0, PAIRS, states, 0, unroll=2)
    square[...] = jnp.zeros(square.shape, f32)

    def pair(p):
        xs = pair_lanes(p)
        x = silu(pre_ref[:, xs])
        xtb = (tcol[p] * x).astype(bf16)
        parts = []
        for j in range(2):
            h = 2 * p + j
            c = col[h]
            d = jnp.concatenate([c] * (rows // LANES), axis=1) - lrow[pl.ds(h, 1), :]
            m = (jnp.exp(jnp.where(causal, d, OFF)) * cb).astype(bf16)
            parts.append(dot_nn(m, xtb))
        y = jnp.where(half, parts[0], parts[1]) + sk_ref[0:1, xs] * x
        y = y + jnp.exp(lcol[p]) * dot_nt(cm, got[xs, :])
        y_ref[:, xs] = y
        g = y * silu(proj_ref[:, xs])
        return g * g

    def step(g, _):
        chain_step(g, 1, first, final, got, give, st, col, rows, send, recv)
        total = square[...]
        for i in range(PART // LANES):
            total = total + pair(g * (PART // LANES) + i)
        square[...] = total
        return 0

    lax.fori_loop(0, CHAIN_STEPS, step, 0)
    scale = lax.rsqrt(jnp.sum(square[...], axis=1, keepdims=True) / DI + epsilon)

    def put(p, _):
        xs = pair_lanes(p)
        g = y_ref[:, xs] * silu(proj_ref[:, xs])
        yn_ref[:, xs] = (g * scale * gg_ref[0:1, xs]).astype(bf16)
        return 0

    lax.fori_loop(0, PAIRS, put, 0, unroll=2)

    @pl.when(jnp.logical_not(final))
    def _():
        edge.wait_send()

    chain_end(1, final, got, give, send, recv)


def back_kernel(
    dyn_ref, y_ref, proj_ref, halo_ref, pre_ref, dt_ref, cum_ref, sin_ref,
    cw_ref, dtb_ref, al_ref, sk_ref, gg_ref,
    dp_ref, dcw_ref, dsm_ref, dgg_ref,
    pad, grad, col, tcol, lcol, lrow, dcb, dbm, dcm, dlog, dtx, ends, dy_ref, drive_ref,
    got, give, gst, dx_ref, edge_ref, from_ref, edge_send, edge_recv, send, recv,
):
    rows = y_ref.shape[0]
    first, final = chunk_place(-1)
    chain_barrier(-1, first, final)

    @pl.when(first)
    def _():
        from_ref[...] = jnp.zeros(from_ref.shape, f32)
        got[...] = jnp.zeros(got.shape, bf16)

    cum = cum_ref[...]
    dt = dt_ref[...]
    lrow[...] = cum.T
    spread_columns(cum, col, lcol, rows)
    spread_columns(dt, None, tcol, rows)
    bm = silu(pre_ref[:, DI : DI + NSTATE]).astype(bf16)
    cm = silu(pre_ref[:, DI + NSTATE :]).astype(bf16)
    zero = jnp.zeros((rows, LANES), f32)

    def sums(p, carry):
        xs = pair_lanes(p)
        g = y_ref[:, xs] * silu(proj_ref[:, xs])
        return carry[0] + g * g, carry[1] + g * (dyn_ref[:, xs] * gg_ref[0:1, xs])

    square, cross = lax.fori_loop(0, PAIRS, sums, (zero, zero))
    scale = lax.rsqrt(jnp.sum(square, axis=1, keepdims=True) / DI + epsilon)
    mean = jnp.sum(cross, axis=1, keepdims=True) * scale / DI

    def ungate(p, _):
        xs = pair_lanes(p)
        z = proj_ref[:, xs]
        y = y_ref[:, xs]
        sg = lax.logistic(z)
        sz = z * sg
        ghat = y * sz * scale
        dyn = dyn_ref[:, xs]
        dgg_ref[0:1, xs] = jnp.sum(dyn * ghat, axis=0, keepdims=True)
        dg = scale * (dyn * gg_ref[0:1, xs] - ghat * mean)
        dy = dg * sz
        dy_ref[:, xs] = dy
        dp_ref[:, xs] = (dg * y * (sg * (1.0 + z * (1.0 - sg)))).astype(bf16)
        gst[xs, :] = dot_tn((jnp.exp(lcol[p]) * dy).astype(bf16), cm)
        return 0

    lax.fori_loop(0, PAIRS, ungate, 0, unroll=2)
    pad[0:8, :] = halo_ref[...]
    pad[8:, :] = proj_ref[:, DI : DI + XBC]
    grad[0:8, :] = jnp.zeros((8, XBC), f32)
    grad[rows + 8 :, :] = jnp.zeros((8, XBC), f32)
    cbt = dot_nt(bm, cm)
    ri = lax.broadcasted_iota(jnp.int32, (rows, rows), 0)
    ci = lax.broadcasted_iota(jnp.int32, (rows, rows), 1)
    causal = ri <= ci
    half = first_half(rows)
    dcb[...] = jnp.zeros((rows, rows), f32)
    dbm[...] = zero
    dcm[...] = zero
    dlog[...] = zero
    dtx[...] = zero
    ends[...] = jnp.zeros((16, LANES), f32)
    lane_row = lax.broadcasted_iota(jnp.int32, (LANES, LANES), 0)
    lane_col = lax.broadcasted_iota(jnp.int32, (LANES, LANES), 1)
    ones = jnp.ones((8, NSTATE), f32)

    def pair(p):
        xs = pair_lanes(p)
        pre = pre_ref[:, xs]
        sg = lax.logistic(pre)
        x = pre * sg
        tp = tcol[p]
        xt = tp * x
        dy = dy_ref[:, xs]
        dyb = dy.astype(bf16)
        parts = []
        for j in range(2):
            h = 2 * p + j
            c = col[h]
            d = lrow[pl.ds(h, 1), :] - jnp.concatenate([c] * (rows // LANES), axis=1)
            w = jnp.exp(jnp.where(causal, d, OFF))
            parts.append(dot_nn((w * cbt).astype(bf16), dyb))
            own = half if j == 0 else jnp.logical_not(half)
            q = dot_nt(jnp.where(own, xt, 0.0).astype(bf16), dyb)
            dcb[...] += w * q
        lp = lcol[p]
        last = lp[rows - 1 : rows, :]
        tail = jnp.exp(last - lp)
        gin = got[xs, :]
        sin = sin_ref[xs, :]
        dst = tail * dot_nt(bm, gin)
        dxt = jnp.where(half, parts[0], parts[1]) + dst
        dbm[...] += dot_nn((tail * xt).astype(bf16), gin)
        dcm[...] += dot_nn((jnp.exp(lp) * dy).astype(bf16), sin)
        sk = sk_ref[0:1, xs]
        pick = jnp.where(lane_col == 2 * p + jnp.where(lane_row >= HDIM, 1, 0), 1.0, 0.0)
        dlog[...] += dot_nn(dy * (y_ref[:, xs] - sk * x) - xt * dxt, pick, highest)
        dtx[...] += dot_nn(x * dxt, pick, highest)
        held = dot_nt(ones, gin.astype(f32) * sin.astype(f32), highest)
        end = jnp.sum(xt * dst, axis=0, keepdims=True) + jnp.exp(last) * held[0:1, :]
        skip = jnp.sum(dy * x, axis=0, keepdims=True)
        stacked = jnp.concatenate(
            [jnp.broadcast_to(end, (8, LANES)), jnp.broadcast_to(skip, (8, LANES))], axis=0
        )
        ends[...] += dot_nn(stacked, pick, highest)
        grad[pl.ds(8, rows), xs] = (tp * dxt + sk * dy) * (sg * (1.0 + pre * (1.0 - sg)))

    def step(g, _):
        chain_step(g, -1, first, final, got, give, gst, col, rows, send, recv)
        for i in range(PART // LANES):
            pair(g * (PART // LANES) + i)
        return 0

    lax.fori_loop(0, CHAIN_STEPS, step, 0)
    dcbb = dcb[...].astype(bf16)
    dc = dcm[...] + dot_tn(dcbb, bm)
    db = dbm[...] + dot_nn(dcbb, cm)
    grad[8 : 8 + rows, DI : DI + NSTATE] = db * silu_grad(pre_ref[:, DI : DI + NSTATE])
    grad[8 : 8 + rows, DI + NSTATE :] = dc * silu_grad(pre_ref[:, DI + NSTATE :])

    def edges(i, _):
        xs = pair_lanes(i)
        edge = jnp.zeros((8, LANES), f32)
        for k in range(CONV):
            edge = edge + cw_ref[k : k + 1, xs] * grad[3 - k : 11 - k, xs]
        edge_ref[:, xs] = edge
        return 0

    lax.fori_loop(0, XBC // LANES, edges, 0)
    edge = to_next(edge_ref, from_ref, edge_send, edge_recv, -1)

    @pl.when(jnp.logical_not(final))
    def _():
        edge.start()

    last_row = lax.broadcasted_iota(jnp.int32, (rows, LANES), 0) == rows - 1
    dl = dlog[...] + jnp.where(last_row, ends[0:1, :], 0.0)
    da = dot_nn(jnp.where(causal, 1.0, 0.0), dl, highest)
    decay = -jnp.exp(al_ref[...])
    ddt = dtx[...] + da * decay
    drive_ref[...] = jnp.zeros((rows, LANES), f32)
    drive_ref[:, 0:HEADS] = proj_ref[:, DI + XBC :]
    ddr = ddt * lax.logistic(drive_ref[...] + dtb_ref[...])
    dp_ref[:, DI + XBC :] = ddr[:, 0:HEADS].astype(bf16)
    dsm_ref[...] = jnp.zeros((8, LANES), f32)
    dsm_ref[0:1, :] = jnp.sum(ddr, axis=0, keepdims=True)
    dsm_ref[1:2, :] = jnp.sum(da * dt, axis=0, keepdims=True) * decay
    dsm_ref[2:3, :] = ends[8:9, :]

    def conv(i, _):
        xs = pair_lanes(i)
        own = grad[pl.ds(8, rows), xs]
        out = jnp.zeros((rows, LANES), f32)
        for k in range(CONV):
            out = out + cw_ref[k : k + 1, xs] * grad[11 - k : 11 - k + rows, xs]
            dcw_ref[k : k + 1, xs] = jnp.sum(
                own * pad[5 + k : 5 + k + rows, xs], axis=0, keepdims=True
            )
        dcw_ref[4:5, xs] = jnp.sum(own, axis=0, keepdims=True)
        dx_ref[:, xs] = out
        return 0

    lax.fori_loop(0, XBC // LANES, conv, 0)

    @pl.when(jnp.logical_not(first))
    def _():
        edge.wait_recv()

    dx_ref[rows - 8 :, :] += from_ref[...]
    dp_ref[:, DI : DI + XBC] = dx_ref[...].astype(bf16)

    @pl.when(jnp.logical_not(final))
    def _():
        edge.wait_send()

    chain_end(-1, final, got, give, send, recv)


VTILE = 1280
NTILE = 256


def head_specs(width, tokens):
    return dict(
        table=pl.BlockSpec((VTILE, width), lambda i: (i, 0)),
        hidden=pl.BlockSpec((tokens, width), lambda i: (0, 0)),
        kept=pl.BlockSpec((VTILE, tokens), lambda i: (i, 0)),
        row=pl.BlockSpec((1, tokens), lambda i: (0, 0)),
        tile_row=pl.BlockSpec((1, 1, tokens), lambda i: (i, 0, 0)),
    )


def head_call(kernel, grid, in_specs, out_specs, outs, scratch, ins, cells):
    return pl.pallas_call(
        kernel,
        grid=(grid,),
        in_specs=in_specs,
        out_specs=out_specs,
        out_shape=[jax.ShapeDtypeStruct(shape, kind) for shape, kind in outs],
        scratch_shapes=list(scratch),
        compiler_params=pltpu.CompilerParams(
            dimension_semantics=("arbitrary",), vmem_limit_bytes=VMEM_LIMIT
        ),
        cost_estimate=pl.CostEstimate(
            flops=2 * cells * D, transcendentals=cells, bytes_accessed=4 * cells
        ),
    )(*ins)


UNROLL = 8


def head_stats_kernel(
    lead_ref, table_ref, own_ref, lab_ref, w_ref,
    q_ref, all_ref, lse_ref, fac_ref, hit_ref,
    kept, tops, sums, hits, shown, own_sem, put_sem, z_send, z_recv, m_send, m_recv, s_send, s_recv,
):
    dp = lax.axis_index("dp")
    me = lax.axis_index("fsdp")
    shards = lax.axis_size("fsdp")
    count = shards // MB
    core = me % MB
    k = me // MB
    mate = k * MB + 1 - core
    vocab_rows = lead_ref.shape[0] + table_ref.shape[0]
    rows = own_ref.shape[0]
    tiles = tops.shape[0]
    barrier = pltpu.get_barrier_semaphore()
    for other in range(1, shards):
        pl.semaphore_signal(
            barrier, inc=1, device_id=(dp, lax.rem(me + other, shards)), device_id_type=MESH
        )
    pl.semaphore_wait(barrier, shards - 1)

    near = jnp.minimum(k, count - 1 - k)
    long_side = jnp.where(count - 1 - k > k, 1, -1)

    def chunk_at(i):
        paired = k + (2 * (i % 2) - 1) * ((i + 1) // 2)
        return jnp.where(i <= 2 * near, paired, k + long_side * (i - near))

    def along(z, side):
        at = all_ref.at[z * MB + core]
        return remote(
            at, at, z_send.at[side, z], z_recv.at[z], dp, me + MB if side == 0 else me - MB
        )

    def to_mate(z):
        at = all_ref.at[z * MB + core]
        return remote(at, at, m_send.at[z], m_recv.at[z], dp, mate)

    def from_mate(z):
        at = all_ref.at[z * MB + 1 - core]
        return remote(at, at, m_send.at[z], m_recv.at[z], dp, mate)

    keep = pltpu.make_async_copy(own_ref, all_ref.at[me], own_sem)
    keep.start()
    keep.wait()

    @pl.when(k < count - 1)
    def _():
        along(k, 0).start()

    @pl.when(k > 0)
    def _():
        along(k, 1).start()

    to_mate(k).start()
    whole = vocab_rows - vocab_rows % 16
    for slot in range(2):
        kept[slot, whole:, :] = jnp.zeros((kept.shape[1] - whole, rows), bf16)

    def put(step, b):
        return pltpu.make_async_copy(
            kept.at[step % 2],
            q_ref.at[:, pl.ds(pl.multiple_of(b * rows, rows), rows)],
            put_sem.at[step % 2],
        )

    def block(step, b):
        @pl.when(step >= 2)
        def _():
            put(step, b).wait()

        slot = step % 2
        ns = pl.ds(pl.multiple_of(b * rows, rows), rows)
        h = all_ref[b]
        label = lab_ref[0:1, ns]
        for t in range(tiles):
            first = t * VTILE
            size = min(VTILE, vocab_rows - first)
            part = lead_ref[...] if t == 0 else table_ref[first - VTILE : first - VTILE + size, :]
            logits = dot_nt(part, h)
            top = jnp.max(logits, axis=0, keepdims=True)
            p = jnp.exp(logits - top)
            kept[slot, first : first + size, :] = p.astype(bf16)
            tops[t, 0:1, ns] = top
            sums[t, 0:1, ns] = jnp.sum(p, axis=0, keepdims=True)
            rid = lax.broadcasted_iota(jnp.int32, (size, rows), 0)
            hits[t, 0:1, ns] = jnp.sum(
                jnp.where(rid == label - first, logits, 0.0), axis=0, keepdims=True
            )
        put(step, b).start()

    def chunk(i, _):
        z = chunk_at(i)

        @pl.when(jnp.logical_and(i > 0, k >= i))
        def _():
            along(k - i, 0).wait_recv()

            @pl.when(k < count - 1)
            def _():
                along(k - i, 0).start()

            to_mate(k - i).start()

        @pl.when(jnp.logical_and(i > 0, k + i < count))
        def _():
            along(k + i, 1).wait_recv()

            @pl.when(k > 0)
            def _():
                along(k + i, 1).start()

            to_mate(k + i).start()

        block(2 * i, z * MB + core)
        from_mate(z).wait_recv()
        block(2 * i + 1, z * MB + 1 - core)
        return 0

    lax.fori_loop(0, count, chunk, 0)
    top = tops[0, 0:1, :]
    for t in range(1, tiles):
        top = jnp.maximum(top, tops[t, 0:1, :])
    total = jnp.zeros_like(top)
    hit = jnp.zeros_like(top)
    for t in range(tiles):
        total = total + sums[t, 0:1, :] * jnp.exp(tops[t, 0:1, :] - top)
        hit = hit + hits[t, 0:1, :]
    hit_ref[...] = hit
    shown[me, 0:1, :] = top
    shown[me, 1:2, :] = total

    def tell(other):
        at = shown.at[me]
        return remote(
            at, at, s_send.at[other], s_recv.at[me], dp, lax.rem(me + other, shards)
        )

    def told(other):
        at = shown.at[lax.rem(me + other, shards)]
        return remote(
            at, at, s_send.at[other], s_recv.at[lax.rem(me + other, shards)], dp, mate
        )

    for other in range(1, shards):
        tell(other).start()
    for other in range(1, shards):
        told(other).wait_recv()
    top = shown[0, 0:1, :]
    for f in range(1, shards):
        top = jnp.maximum(top, shown[f, 0:1, :])
    total = jnp.zeros_like(top)
    for f in range(shards):
        total = total + shown[f, 1:2, :] * jnp.exp(shown[f, 0:1, :] - top)
    lse = top + jnp.log(total)
    lse_ref[...] = lse
    scale = w_ref[...] * (1.0 + 2.0 * z_weight * lse)
    for t in range(tiles):
        fac_ref[t, 0:1, :] = scale * jnp.exp(tops[t, 0:1, :] - lse)
    for other in range(1, shards):
        tell(other).wait_send()
    for z in range(count):

        @pl.when(jnp.logical_and(k >= z, k < count - 1))
        def _(z=z):
            along(z, 0).wait_send()

        @pl.when(jnp.logical_and(k <= z, k > 0))
        def _(z=z):
            along(z, 1).wait_send()

        to_mate(z).wait_send()
    put(0, 0).wait()
    put(1, 0).wait()


def head_stats(lead, table, own, labels, weight):
    vocab_rows, width = lead.shape[0] + table.shape[0], table.shape[1]
    rows = own.shape[0]
    shards = lax.axis_size("fsdp")
    count = shards // MB
    tokens = shards * rows
    tiles = pl.cdiv(vocab_rows, VTILE)
    kept, everyone, lse, fac, hit = comm_call(
        head_stats_kernel,
        6,
        (lead, table, own, labels, weight),
        (
            ((tiles * VTILE, tokens), bf16),
            ((shards, rows, width), bf16),
            ((1, tokens), f32),
            ((tiles, 1, tokens), f32),
            ((1, tokens), f32),
        ),
        (
            pltpu.VMEM((2, tiles * VTILE, rows), bf16),
            pltpu.VMEM((tiles, 1, tokens), f32),
            pltpu.VMEM((tiles, 1, tokens), f32),
            pltpu.VMEM((tiles, 1, tokens), f32),
            pltpu.VMEM((shards, 2, tokens), f32),
            pltpu.SemaphoreType.DMA,
            pltpu.SemaphoreType.DMA((2,)),
            pltpu.SemaphoreType.DMA((2, count)),
            pltpu.SemaphoreType.DMA((count,)),
            pltpu.SemaphoreType.DMA((count,)),
            pltpu.SemaphoreType.DMA((count,)),
            pltpu.SemaphoreType.DMA((shards,)),
            pltpu.SemaphoreType.DMA((shards,)),
        ),
        (pltpu.VMEM,) * 5,
        (pl.ANY, pltpu.VMEM, pltpu.VMEM, pltpu.VMEM, pltpu.VMEM),
        own.size * 2 * 7,
    )
    return kept, everyone.reshape(tokens, width), lse, fac, hit


def logit_grads(q, fac, weight, rid, label):
    other = weight * (0.1 / VOCAB)
    return (q.astype(f32) * fac - jnp.where(rid == label, other + 0.9 * weight, other)).astype(bf16)


def head_rows_kernel(vocab_rows, lead_ref, e_ref, q_ref, fac_ref, w_ref, lab_ref, out_ref, acc, et):
    step = pl.program_id(0)
    first = step * VTILE
    tokens = q_ref.shape[1]

    @pl.when(step == 0)
    def _():
        acc[...] = jnp.zeros(acc.shape, f32)

    @pl.when(step == 0)
    def _():
        et[...] = lead_ref[...].astype(f32).T.astype(bf16)

    @pl.when(step > 0)
    def _():
        eid = lax.broadcasted_iota(jnp.int32, (VTILE, e_ref.shape[1]), 0)
        et[...] = jnp.where(eid < vocab_rows - first, e_ref[...].astype(f32), 0.0).T.astype(bf16)


    def chunk(j, _):
        ns = pl.ds(pl.multiple_of(j * NTILE, NTILE), NTILE)
        rid = lax.broadcasted_iota(jnp.int32, (VTILE, NTILE), 0)
        dl = logit_grads(
            q_ref[:, ns], fac_ref[0, 0:1, ns], w_ref[0:1, ns], rid, lab_ref[0:1, ns] - first
        )
        acc[:, ns] += dot_nn(et[...], dl)
        return 0

    lax.fori_loop(0, tokens // NTILE, chunk, 0, unroll=UNROLL)

    @pl.when(step == pl.num_programs(0) - 1)
    def _():
        def put(j, _):
            ns = pl.ds(pl.multiple_of(j * NTILE, NTILE), NTILE)
            out_ref[ns, :] = acc[:, ns].T.astype(bf16)
            return 0

        lax.fori_loop(0, tokens // NTILE, put, 0)


def head_rows(lead, table, kept, fac, weight, labels):
    vocab_rows, width = lead.shape[0] + table.shape[0], table.shape[1]
    tokens = kept.shape[1]
    sp = head_specs(width, tokens)
    return head_call(
        functools.partial(head_rows_kernel, vocab_rows),
        pl.cdiv(vocab_rows, VTILE),
        [
            pl.BlockSpec((VTILE, width), lambda i: (0, 0)),
            pl.BlockSpec((VTILE, width), lambda i: (jnp.maximum(i - 1, 0), 0)),
            sp["kept"],
            sp["tile_row"],
            sp["row"],
            sp["row"],
        ],
        [sp["hidden"]],
        [((tokens, width), bf16)],
        (pltpu.VMEM((width, tokens), f32), pltpu.VMEM((width, VTILE), bf16)),
        (lead, table, kept, fac, weight, labels),
        vocab_rows * tokens,
    )[0]


def head_table_kernel(h_ref, q_ref, fac_ref, w_ref, lab_ref, out_ref, dl_ref):
    first = pl.program_id(0) * VTILE
    tokens = q_ref.shape[1]

    def chunk(j, _):
        ns = pl.ds(pl.multiple_of(j * NTILE, NTILE), NTILE)
        rid = lax.broadcasted_iota(jnp.int32, (VTILE, NTILE), 0)
        dl_ref[:, ns] = logit_grads(
            q_ref[:, ns], fac_ref[0, 0:1, ns], w_ref[0:1, ns], rid, lab_ref[0:1, ns] - first
        )
        return 0

    lax.fori_loop(0, tokens // NTILE, chunk, 0, unroll=UNROLL)

    def cols(j, _):
        ds = pl.ds(pl.multiple_of(j * 256, 256), 256)
        out_ref[:, ds] = dot_nn(dl_ref[...], h_ref[:, ds]).astype(bf16)
        return 0

    lax.fori_loop(0, h_ref.shape[1] // 256, cols, 0, unroll=True)


def head_table(hidden, kept, fac, weight, labels, vocab_rows):
    tokens, width = hidden.shape
    sp = head_specs(width, tokens)
    return head_call(
        head_table_kernel,
        pl.cdiv(vocab_rows, VTILE),
        [sp["hidden"], sp["kept"], sp["tile_row"], sp["row"], sp["row"]],
        [sp["table"]],
        [((vocab_rows, width), bf16)],
        (pltpu.VMEM((VTILE, tokens), bf16),),
        (hidden, kept, fac, weight, labels),
        vocab_rows * tokens,
    )[0]


def weight_grads_kernel(u_ref, dp_ref, yn_ref, db_ref, in_ref, out_ref):
    wide_cols = dp_ref.shape[1]
    for c in range(0, wide_cols, 1024):
        cs = pl.ds(c, min(1024, wide_cols - c))
        in_ref[:, cs] = dot_tn(u_ref[...], dp_ref[:, cs]).astype(bf16)
    out_ref[...] = dot_tn(yn_ref[...], db_ref[...]).astype(bf16)


def weight_grads(normed, grad_proj, mixed, grad_branch):
    rows = normed.shape[0]
    steps = D // LANES
    part = DI // steps
    return head_call(
        weight_grads_kernel,
        steps,
        [
            pl.BlockSpec((rows, LANES), lambda i: (0, i)),
            pl.BlockSpec((rows, ZW), lambda i: (0, 0)),
            pl.BlockSpec((rows, part), lambda i: (0, i)),
            pl.BlockSpec((rows, D), lambda i: (0, 0)),
        ],
        [pl.BlockSpec((LANES, ZW), lambda i: (i, 0)), pl.BlockSpec((part, D), lambda i: (i, 0))],
        [((D, ZW), bf16), ((DI, D), bf16)],
        (),
        (normed, grad_proj, mixed, grad_branch),
        rows * (ZW + DI),
    )


def after(value, earlier):
    return lax.optimization_barrier((value, earlier))[0]


def norm_scale(values):
    return lax.rsqrt(jnp.mean(values * values, axis=-1, keepdims=True) + epsilon)


def norm_back(grad, values, gain):
    scale = norm_scale(values)
    unit = values * scale
    inner = grad * gain
    back = scale * (inner - unit * jnp.mean(inner * unit, axis=-1, keepdims=True))
    return back, jnp.sum(grad * unit, axis=0)


def wide(row):
    return jnp.pad(row, (0, LANES - row.shape[0]))[None]


def layer_vectors(vector_params, layer_index):
    offset = layer_index * PER
    pieces = []
    for size in (CONV * XBC, XBC, HEADS, HEADS, HEADS, D, DI):
        pieces.append(vector_params[offset : offset + size])
        offset += size
    conv_w, conv_b, dt_bias, decay_log, skip, pre_gain, gate_gain = pieces
    return dict(
        conv_w=conv_w.reshape(CONV, XBC),
        conv_b=conv_b[None],
        dt_bias=wide(dt_bias),
        decay_log=wide(decay_log),
        skip=jnp.repeat(skip, HDIM)[None],
        pre_gain=pre_gain,
        gate_gain=gate_gain[None],
    )


def layer_forward(hidden, w_in, w_out, vec):
    rows = hidden.shape[0]
    normed = (hidden * norm_scale(hidden) * vec["pre_gain"]).astype(bf16)
    proj = jnp.dot(normed, w_in, preferred_element_type=f32)
    pre, y, mixed, dt, cum, entering, halo = comm_call(
        scan_kernel,
        1,
        (
            proj, vec["conv_w"], vec["conv_b"], vec["dt_bias"], vec["decay_log"], vec["skip"],
            vec["gate_gain"],
        ),
        (
            ((rows, XBC), f32),
            ((rows, DI), f32),
            ((rows, DI), bf16),
            ((rows, LANES), f32),
            ((rows, LANES), f32),
            ((DI, NSTATE), bf16),
            ((8, XBC), f32),
        ),
        (
            pltpu.VMEM((rows + 8, XBC), f32),
            pltpu.VMEM((HEADS, rows, LANES), f32),
            pltpu.VMEM((PAIRS, rows, LANES), f32),
            pltpu.VMEM((PAIRS, rows, LANES), f32),
            pltpu.VMEM((LANES, rows), f32),
            pltpu.VMEM((DI, NSTATE), f32),
            pltpu.VMEM((DI, NSTATE), bf16),
            pltpu.VMEM((rows, LANES), f32),
            pltpu.SemaphoreType.DMA,
            pltpu.SemaphoreType.DMA,
            pltpu.SemaphoreType.DMA((CHAIN_STEPS,)),
            pltpu.SemaphoreType.DMA((CHAIN_STEPS,)),
        ),
        (pltpu.VMEM,) * 7,
        (pltpu.VMEM,) * 7,
        DI * NSTATE * 2,
    )
    branch = jnp.dot(mixed, w_out, preferred_element_type=f32)
    record = (hidden, normed, proj, halo, pre, dt, cum, entering, y, mixed)
    return hidden + branch, record


def layer_backward(grad_hidden, w_in, w_out, vec, record):
    hidden, normed, proj, halo, pre, dt, cum, entering, y, mixed = record
    rows = hidden.shape[0]
    grad_branch = grad_hidden.astype(bf16)
    grad_mixed = dot_nt(grad_branch, w_out)
    grad_proj, dconv, dsmall, dgate = comm_call(
        back_kernel,
        2,
        (
            grad_mixed, y, proj, halo, pre, dt, cum, entering,
            vec["conv_w"], vec["dt_bias"], vec["decay_log"], vec["skip"], vec["gate_gain"],
        ),
        (
            ((rows, ZW), bf16),
            ((8, XBC), f32),
            ((8, LANES), f32),
            ((1, DI), f32),
        ),
        (
            pltpu.VMEM((rows + 8, XBC), f32),
            pltpu.VMEM((rows + 16, XBC), f32),
            pltpu.VMEM((HEADS, rows, LANES), f32),
            pltpu.VMEM((PAIRS, rows, LANES), f32),
            pltpu.VMEM((PAIRS, rows, LANES), f32),
            pltpu.VMEM((LANES, rows), f32),
            pltpu.VMEM((rows, rows), f32),
            pltpu.VMEM((rows, LANES), f32),
            pltpu.VMEM((rows, LANES), f32),
            pltpu.VMEM((rows, LANES), f32),
            pltpu.VMEM((rows, LANES), f32),
            pltpu.VMEM((16, LANES), f32),
            pltpu.VMEM((rows, DI), f32),
            pltpu.VMEM((rows, LANES), f32),
            pltpu.VMEM((DI, NSTATE), bf16),
            pltpu.VMEM((DI, NSTATE), bf16),
            pltpu.VMEM((DI, NSTATE), f32),
            pltpu.VMEM((rows, XBC), f32),
            pltpu.VMEM((8, XBC), f32),
            pltpu.VMEM((8, XBC), f32),
            pltpu.SemaphoreType.DMA,
            pltpu.SemaphoreType.DMA,
            pltpu.SemaphoreType.DMA((CHAIN_STEPS,)),
            pltpu.SemaphoreType.DMA((CHAIN_STEPS,)),
        ),
        (pltpu.VMEM,) * 13,
        (pltpu.VMEM,) * 4,
        DI * NSTATE * 2,
    )
    grad_normed = dot_nt(grad_proj, w_in)
    grad_in, grad_out = weight_grads(normed, grad_proj, mixed, grad_branch)
    grad_prev, dpre_gain = norm_back(grad_normed, hidden, vec["pre_gain"])
    grad_vec = jnp.concatenate(
        [
            dconv[:CONV].reshape(-1),
            dconv[CONV],
            dsmall[0, :HEADS],
            dsmall[1, :HEADS],
            dsmall[2, :HEADS],
            dpre_gain,
            dgate[0],
        ]
    )
    return grad_hidden + grad_prev, grad_in, grad_out, grad_vec


def advance(weight, moment, average, grad, factor):
    scaled = grad * factor
    moment_new = 0.5 * moment + scaled
    weight_new = weight - step_rate * (scaled + 0.5 * moment_new)
    average_new = 0.5 * average + 0.5 * weight_new
    return (weight_new, moment_new, average_new, weight_new.astype(bf16))


def whole_step(
    token_ids,
    target_ids,
    seq_lengths,
    embedding,
    embedding_mom,
    embedding_avg,
    in_proj,
    in_proj_mom,
    in_proj_avg,
    out_proj,
    out_proj_mom,
    out_proj_avg,
    vector_params,
    vector_mom,
    vector_avg,
):
    groups = lax.axis_size("dp")
    shards = lax.axis_size("fsdp")
    group_index = lax.axis_index("dp")
    shard_index = lax.axis_index("fsdp")
    chunks = shards // MB
    seq_rows = token_ids.shape[2]
    rows = seq_rows // chunks
    vocab_rows, own_cols = embedding.shape
    tokens = MB * seq_rows
    total_count = jnp.sum(seq_lengths).astype(f32)
    in_low = in_proj.astype(bf16)
    out_low = out_proj.astype(bf16)

    lead = lax.all_gather(embedding[:VTILE].astype(bf16), "dp", axis=1, tiled=True)
    ids_all = group_call(share_kernel, 7, token_ids[:, 0, :], ((groups, MB, seq_rows), jnp.int32))
    ids_all = ids_all.reshape(groups, MB, chunks, rows).transpose(2, 1, 0, 3).reshape(-1)
    every = ids_all.shape[0]
    local_ids = ids_all - shard_index * vocab_rows
    inside = (local_ids >= 0) & (local_ids < vocab_rows)
    sorted_ids, sorted_tok = lax.sort(
        (jnp.where(inside, local_ids, vocab_rows), jnp.arange(every, dtype=jnp.int32)),
        num_keys=1,
    )
    held_here = sorted_ids < vocab_rows
    count = jnp.sum(held_here.astype(jnp.int32)).reshape(1)
    row_list = jnp.where(held_here, sorted_ids, 0)
    tok_list = jnp.where(held_here, sorted_tok, every)
    looked, embed_low, own_sums = local_call(
        lookup_kernel,
        (count, row_list, tok_list, embedding),
        (((every, own_cols), bf16), ((vocab_rows, own_cols), bf16), ((8, own_cols), f32)),
        scratch=(pltpu.VMEM((every + 8, own_cols), f32),),
        in_smem=(0, 1, 2),
    )
    mine = lax.psum_scatter(
        looked.reshape(shards * groups * rows, own_cols), "fsdp", scatter_dimension=0, tiled=True
    )
    hidden = group_call(
        to_rows_kernel,
        8,
        mine.reshape(groups, rows, own_cols),
        ((rows, D), f32),
        (pltpu.VMEM((groups, rows, own_cols), bf16),),
    )

    shards = []
    for l in range(LAYERS):
        shards += [in_low[l], out_low[l]]
    shards = after(shards, looked)
    gathered = gather_layers(shards)
    w_in, w_out = gathered[0::2], gathered[1::2]
    embed_low = after(embed_low, gathered)
    table = lax.all_gather(embed_low[VTILE:], "dp", axis=1, tiled=True)

    vecs = [layer_vectors(vector_params, l) for l in range(LAYERS)]
    final_gain = vector_params[LAYERS * PER :]
    records = []
    for l in range(LAYERS):
        hidden, record = layer_forward(hidden, w_in[l], w_out[l], vecs[l])
        records.append(record)

    final_low = (hidden * norm_scale(hidden) * final_gain).astype(bf16)

    def in_order(per_seq):
        return per_seq.reshape(MB, chunks, rows).transpose(1, 0, 2).reshape(1, tokens)

    labels = in_order(target_ids[:, 0, :])
    lengths = lax.dynamic_index_in_dim(seq_lengths, group_index, 1, keepdims=True)
    valid = in_order((jnp.arange(seq_rows)[None, :] < lengths).astype(f32))
    local_labels = labels - shard_index * vocab_rows
    weight = valid / total_count
    kept, group_hidden, lse, fac, target = head_stats(lead, table, final_low, local_labels, weight)
    own_mask = jnp.arange(tokens) // rows == shard_index
    per_row = jnp.where(own_mask, lse[0] + z_weight * lse[0] * lse[0], 0.0)
    loss_sum = jnp.sum((per_row - 0.9 * target[0]) * valid[0])
    own_valid = lax.dynamic_slice_in_dim(valid[0], shard_index * rows, rows)
    hidden_sum = jnp.sum(final_low.astype(f32) * own_valid[:, None], axis=0)
    column_sum = jnp.zeros((groups, own_cols), f32)
    column_sum = jnp.where(
        jnp.arange(groups)[:, None] == group_index, jnp.sum(own_sums, axis=0), column_sum
    ).reshape(D)

    rows_grad = head_rows(lead, table, kept, fac, weight, local_labels)
    own_grad = lax.psum_scatter(
        rows_grad, "fsdp", scatter_dimension=0, tiled=True
    ).astype(f32)
    table_grad = head_table(group_hidden, kept, fac, weight, local_labels, vocab_rows)
    table_part = lax.psum_scatter(table_grad, "dp", scatter_dimension=1, tiled=True)

    grad_hidden, dfinal = norm_back(after(own_grad, table_grad), hidden, final_gain)
    in_parts = [None] * LAYERS
    out_parts = [None] * LAYERS
    vec_parts = [None] * LAYERS
    for l in reversed(range(LAYERS)):
        grad_hidden, grad_in, grad_out, vec_parts[l] = layer_backward(
            grad_hidden, w_in[l], w_out[l], vecs[l], records[l]
        )
        if l == 0:
            sent = group_call(
                to_columns_kernel,
                9,
                grad_hidden,
                ((groups, rows, own_cols), bf16),
                (pltpu.VMEM((groups, rows, own_cols), bf16),),
            )
            spread = lax.all_gather(sent, "fsdp", axis=0).reshape(every, own_cols)
        in_parts[l], out_parts[l] = grad_in, grad_out
    whole = []
    for l in range(LAYERS):
        whole += [in_parts[l], out_parts[l]]
    summed_parts = reduce_layers(whole)
    spread = after(spread, summed_parts)
    table_total, table_squares = local_call(
        spread_kernel,
        (count, row_list, tok_list, spread, table_part),
        (((vocab_rows, own_cols), f32), ((8, own_cols), f32)),
        scratch=(pltpu.VMEM((every + 8, own_cols), f32),),
        in_smem=(0, 1, 2),
    )
    grad_in_all = jnp.stack(summed_parts[0::2])
    grad_out_all = jnp.stack(summed_parts[1::2])
    owner_squares = (
        jnp.sum(grad_in_all * grad_in_all)
        + jnp.sum(grad_out_all * grad_out_all)
        + jnp.sum(table_squares)
    )
    small = vector_params.shape[0]
    used = small + 2 * D + 2
    padded = pl.cdiv(used, 16 * LANES) * 16 * LANES
    packed = jnp.concatenate(
        vec_parts
        + [
            dfinal,
            hidden_sum,
            column_sum,
            owner_squares.reshape(1),
            loss_sum.reshape(1),
            jnp.zeros((padded - used,), f32),
        ]
    )
    packed = total_of(packed.reshape(-1, LANES)).reshape(-1)
    vector_total = packed[:small]
    hidden_total = packed[small : small + D]
    column_total = packed[small + D : small + 2 * D]
    squares_total = packed[used - 2]
    mean_part = jnp.sum(hidden_total * column_total) * (0.1 / VOCAB)
    loss_total = packed[used - 1] - mean_part
    grad_norm = jnp.sqrt(squares_total + jnp.sum(vector_total * vector_total))
    factor = jnp.minimum(1.0, clip_limit / grad_norm)
    loss_value = loss_total / total_count
    return (
        loss_value,
        grad_norm,
        *advance(embedding, embedding_mom, embedding_avg, table_total, factor),
        *advance(in_proj, in_proj_mom, in_proj_avg, grad_in_all, factor),
        *advance(out_proj, out_proj_mom, out_proj_avg, grad_out_all, factor),
        *advance(vector_params, vector_mom, vector_avg, vector_total, factor),
    )


def solution(mesh):
    table_spec = P("fsdp", "dp")
    weight_spec = P(None, ("dp", "fsdp"), None)
    return jax.shard_map(
        whole_step,
        mesh=mesh,
        in_specs=(
            P(None, "dp", None),
            P(None, "dp", None),
            P(),
            *(table_spec,) * 3,
            *(weight_spec,) * 6,
            *(P(),) * 3,
        ),
        out_specs=(
            P(),
            P(),
            *(table_spec,) * 4,
            *(weight_spec,) * 8,
            *(P(),) * 4,
        ),
        check_vma=False,
    )
```

```python
import functools

import jax
import jax.numpy as jnp
from jax import lax
from jax.experimental import pallas as pl
from jax.experimental.pallas import tpu as pltpu
from jax.sharding import PartitionSpec as P


D = 1024
HEADS = 32
HDIM = 64
NSTATE = 128
CONV = 4
VOCAB = 50288
LAYERS = 2
MB = 2
DI = 2048
XBC = 2304
ZW = 4384
PER = 14688
LANES = 128
PAIRS = DI // LANES

epsilon = 1e-05
z_weight = 0.001
clip_limit = 0.2
step_rate = 1000.0
highest = lax.Precision.HIGHEST
bf16 = jnp.bfloat16
f32 = jnp.float32
VMEM_LIMIT = 62 * 1024 * 1024
OFF = -1e30


def dot_nn(a, b, precision=None):
    return lax.dot_general(
        a, b, (((1,), (0,)), ((), ())), precision=precision, preferred_element_type=f32
    )


def dot_nt(a, b, precision=None):
    return lax.dot_general(
        a, b, (((1,), (1,)), ((), ())), precision=precision, preferred_element_type=f32
    )


def dot_tn(a, b, precision=None):
    return lax.dot_general(
        a, b, (((0,), (0,)), ((), ())), precision=precision, preferred_element_type=f32
    )


def silu(v):
    return v * lax.logistic(v)


def silu_grad(v):
    s = lax.logistic(v)
    return s * (1.0 + v * (1.0 - s))


def local_call(kernel, ins, outs, scratch=(), in_smem=(), flops=0):
    total = sum(a.size * a.dtype.itemsize for a in ins)
    return pl.pallas_call(
        kernel,
        out_shape=[jax.ShapeDtypeStruct(shape, kind) for shape, kind in outs],
        in_specs=[
            pl.BlockSpec(memory_space=pltpu.SMEM if i in in_smem else pltpu.VMEM)
            for i in range(len(ins))
        ],
        out_specs=[pl.BlockSpec(memory_space=pltpu.VMEM) for _ in outs],
        scratch_shapes=list(scratch),
        compiler_params=pltpu.CompilerParams(vmem_limit_bytes=VMEM_LIMIT),
        cost_estimate=pl.CostEstimate(
            flops=flops or total, transcendentals=0, bytes_accessed=2 * total
        ),
    )(*ins)


def lookup_kernel(count_ref, row_ref, tok_ref, table_ref, out_ref, low_ref, sum_ref, held):
    tokens = out_ref.shape[0]
    step = 512

    def clear(i, _):
        held[pl.ds(pl.multiple_of(i * step, step), step), :] = jnp.zeros(
            (step, held.shape[1]), f32
        )
        return 0

    lax.fori_loop(0, tokens // step, clear, 0)

    def move(i, _):
        for k in range(8):
            row = row_ref[i * 8 + k]
            tok = tok_ref[i * 8 + k]
            held[pl.ds(tok, 1), :] = table_ref[pl.ds(row, 1), :]
        return 0

    lax.fori_loop(0, (count_ref[0] + 7) // 8, move, 0)

    def put(i, _):
        rows = pl.ds(pl.multiple_of(i * step, step), step)
        out_ref[rows, :] = held[rows, :].astype(bf16)
        return 0

    lax.fori_loop(0, tokens // step, put, 0)
    rows_all = table_ref.shape[0]
    part = VTILE // 5
    whole = rows_all // part

    def low_rows(i):
        return table_ref[pl.ds(pl.multiple_of(i * part, part), part), :].astype(bf16)

    def add(low, total):
        return total + jnp.sum(low.astype(f32).reshape(part // 8, 8, -1), axis=0)

    def cast(i, total):
        low = low_rows(i)
        low_ref[pl.ds(pl.multiple_of(i * part - VTILE, part), part), :] = low
        return add(low, total)

    total = lax.fori_loop(
        0, VTILE // part, lambda i, t: add(low_rows(i), t), jnp.zeros(sum_ref.shape, f32)
    )
    sum_ref[...] = lax.fori_loop(VTILE // part, whole, cast, total)
    if rows_all > whole * part:
        low = table_ref[whole * part :, :].astype(bf16)
        low_ref[whole * part - VTILE :, :] = low
        sum_ref[0:1, :] += jnp.sum(low.astype(f32), axis=0, keepdims=True)


def spread_kernel(count_ref, row_ref, tok_ref, grad_ref, base_ref, out_ref, square_ref, held):
    tokens = grad_ref.shape[0]
    step = 512
    rows_all = out_ref.shape[0]

    def take(i, _):
        rows = pl.ds(pl.multiple_of(i * step, step), step)
        held[rows, :] = grad_ref[rows, :].astype(f32)
        return 0

    lax.fori_loop(0, tokens // step, take, 0)
    held[pl.ds(tokens, 8), :] = jnp.zeros((8, held.shape[1]), f32)

    whole = rows_all // step

    def start(i, _):
        rows = pl.ds(pl.multiple_of(i * step, step), step)
        out_ref[rows, :] = base_ref[rows, :].astype(f32)
        return 0

    lax.fori_loop(0, whole, start, 0)
    if rows_all > whole * step:
        out_ref[whole * step :, :] = base_ref[whole * step :, :].astype(f32)

    def move(i, _):
        for k in range(8):
            row = row_ref[i * 8 + k]
            tok = tok_ref[i * 8 + k]
            out_ref[pl.ds(row, 1), :] = out_ref[pl.ds(row, 1), :] + held[pl.ds(tok, 1), :]
        return 0

    lax.fori_loop(0, (count_ref[0] + 7) // 8, move, 0)

    def square(i, total):
        part = out_ref[pl.ds(pl.multiple_of(i * step, step), step), :]
        return total + jnp.sum((part * part).reshape(step // 8, 8, -1), axis=0)

    total = lax.fori_loop(0, whole, square, jnp.zeros(square_ref.shape, f32))
    square_ref[...] = total
    if rows_all > whole * step:
        part = out_ref[whole * step :, :]
        square_ref[0:1, :] += jnp.sum(part * part, axis=0, keepdims=True)


MESH = pl.DeviceIdType.MESH


def remote(src, dst, send, recv, dp, fsdp):
    return pltpu.make_async_remote_copy(
        src_ref=src,
        dst_ref=dst,
        send_sem=send,
        recv_sem=recv,
        device_id=(dp, fsdp),
        device_id_type=MESH,
    )


def comm_call(kernel, number, ins, outs, scratch, in_spaces, out_spaces, sent):
    return pl.pallas_call(
        kernel,
        out_shape=[jax.ShapeDtypeStruct(shape, kind) for shape, kind in outs],
        in_specs=[pl.BlockSpec(memory_space=space) for space in in_spaces],
        out_specs=[pl.BlockSpec(memory_space=space) for space in out_spaces],
        scratch_shapes=list(scratch),
        compiler_params=pltpu.CompilerParams(
            collective_id=number, has_side_effects=True, vmem_limit_bytes=VMEM_LIMIT
        ),
        cost_estimate=pl.CostEstimate(flops=sent, transcendentals=0, bytes_accessed=2 * sent),
    )(*ins)


def greet_groups():
    dp = lax.axis_index("dp")
    me = lax.axis_index("fsdp")
    groups = lax.axis_size("dp")
    barrier = pltpu.get_barrier_semaphore()
    others = [lax.rem(dp + other, groups) for other in range(1, groups)]
    for other in others:
        pl.semaphore_signal(barrier, inc=1, device_id=(other, me), device_id_type=MESH)
    pl.semaphore_wait(barrier, groups - 1)
    return dp, me, others


def share_kernel(in_ref, out_ref, send, recv):
    dp, me, others = greet_groups()
    for other in others:
        remote(in_ref, out_ref.at[dp], send.at[other], recv.at[dp], other, me).start()
    out_ref[dp] = in_ref[...]
    for other in others:
        copy = remote(in_ref, out_ref.at[other], send.at[other], recv.at[other], other, me)
        copy.wait_recv()
        copy.wait_send()


def to_rows_kernel(in_ref, out_ref, landed, send, recv):
    dp, me, others = greet_groups()
    for other in others:
        remote(in_ref.at[other], landed.at[dp], send.at[other], recv.at[dp], other, me).start()
    landed[dp] = in_ref[dp]
    for other in others:
        remote(in_ref.at[other], landed.at[other], send.at[other], recv.at[other], other, me).wait_recv()
    cols = in_ref.shape[2]
    for g in range(in_ref.shape[0]):
        out_ref[:, g * cols : (g + 1) * cols] = landed[g].astype(f32)
    for other in others:
        remote(in_ref.at[other], landed.at[other], send.at[other], recv.at[other], other, me).wait_send()


def to_columns_kernel(in_ref, out_ref, parts, send, recv):
    dp, me, others = greet_groups()
    cols = out_ref.shape[2]
    for g in range(out_ref.shape[0]):
        parts[g] = in_ref[:, g * cols : (g + 1) * cols].astype(bf16)
    for other in others:
        remote(parts.at[other], out_ref.at[dp], send.at[other], recv.at[dp], other, me).start()
    out_ref[dp] = parts[dp]
    for other in others:
        copy = remote(parts.at[other], out_ref.at[other], send.at[other], recv.at[other], other, me)
        copy.wait_recv()
        copy.wait_send()


def group_call(kernel, number, array, out, scratch=()):
    groups = lax.axis_size("dp")
    return comm_call(
        kernel,
        number,
        (array,),
        (out,),
        tuple(scratch)
        + (pltpu.SemaphoreType.DMA((groups,)), pltpu.SemaphoreType.DMA((groups,))),
        (pltpu.VMEM,),
        (pltpu.VMEM,),
        array.size * 2,
    )[0]


CHAIN_STEPS = 8
PART = DI // CHAIN_STEPS


def chunk_place(direction):
    place = lax.axis_index("fsdp") // MB
    count = lax.axis_size("fsdp") // MB
    first = place == (0 if direction > 0 else count - 1)
    final = place == (count - 1 if direction > 0 else 0)
    return first, final


def chain_barrier(direction, first, final):
    dp = lax.axis_index("dp")
    me = lax.axis_index("fsdp")
    barrier = pltpu.get_barrier_semaphore()

    @pl.when(jnp.logical_not(first))
    def _():
        pl.semaphore_signal(
            barrier, inc=1, device_id=(dp, me - MB * direction), device_id_type=MESH
        )

    @pl.when(jnp.logical_not(final))
    def _():
        pl.semaphore_wait(barrier, 1)


def to_next(src, dst, send, recv, direction):
    dp = lax.axis_index("dp")
    return remote(src, dst, send, recv, dp, lax.axis_index("fsdp") + MB * direction)


def chain_step(g, direction, first, final, got, give, local, col, rows, send, recv):
    def copy():
        at = pl.ds(pl.multiple_of(g * PART, PART), PART)
        return to_next(give.at[at], got.at[at], send.at[g], recv.at[g], direction)

    @pl.when(jnp.logical_not(first))
    def _():
        copy().wait_recv()

    @pl.when(jnp.logical_not(final))
    def _():
        for i in range(PART // HDIM):
            h = pl.ds(pl.multiple_of(g * PART + i * HDIM, HDIM), HDIM)
            decay = jnp.exp(col[g * (PART // HDIM) + i, rows - 1 : rows, :])
            give[h, :] = (decay * got[h, :].astype(f32) + local[h, :]).astype(bf16)
        copy().start()


def chain_end(direction, final, got, give, send, recv):
    @pl.when(jnp.logical_not(final))
    def _():
        for g in range(CHAIN_STEPS):
            at = pl.ds(g * PART, PART)
            to_next(give.at[at], got.at[at], send.at[g], recv.at[g], direction).wait_send()


def bits_of(size):
    return [1 << b for b in range(size.bit_length() - 1)]


TCHUNK = 512


def stepped(weight, moment, average, grad, factor):
    scaled = grad * factor
    moment_new = 0.5 * moment + scaled
    weight_new = weight - step_rate * (scaled + 0.5 * moment_new)
    return weight_new, moment_new, 0.5 * average + 0.5 * weight_new


def total_kernel(small, squares_at, packed_ref, total_ref, norm_ref, work, got, send, recv):
    dp = lax.axis_index("dp")
    me = lax.axis_index("fsdp")
    half = packed_ref.shape[0] // 2
    core = me % MB
    partners = [("f", b) for b in bits_of(lax.axis_size("fsdp")) if b > 1]
    partners += [("d", b) for b in bits_of(lax.axis_size("dp"))]

    def across(kind, bit):
        ids, other = (me, lambda v: (dp, v)) if kind == "f" else (dp, lambda v: (v, me))
        return other(jnp.where((ids // bit) % 2 == 1, ids - bit, ids + bit))

    mate = across("f", 1)
    barrier = pltpu.get_barrier_semaphore()
    for target in [mate] + [across(*p) for p in partners]:
        pl.semaphore_signal(barrier, inc=1, device_id=target, device_id_type=MESH)
    pl.semaphore_wait(barrier, 1 + len(partners))

    mine = pl.ds(pl.multiple_of(core * half, 8), half)
    theirs = pl.ds(pl.multiple_of((1 - core) * half, 8), half)
    copy = remote(packed_ref.at[theirs], got.at[0], send.at[0], recv.at[0], *mate)
    copy.start()
    copy.wait()
    work[0] = packed_ref[mine, :] + got[0]
    for i, p in enumerate(partners):
        copy = remote(work.at[i], got.at[i + 1], send.at[i + 1], recv.at[i + 1], *across(*p))
        copy.start()
        copy.wait()
        work[i + 1] = work[i] + got[i + 1]
    n = len(partners)
    copy = remote(work.at[n], got.at[n + 1], send.at[n + 1], recv.at[n + 1], *mate)
    copy.start()
    copy.wait()
    total_ref[mine, :] = work[n]
    total_ref[theirs, :] = got[n + 1]

    total = total_ref[...]
    index = lax.broadcasted_iota(jnp.int32, total.shape, 0) * LANES
    index = index + lax.broadcasted_iota(jnp.int32, total.shape, 1)
    parts = jnp.where(index < small, total * total, jnp.where(index == squares_at, total, 0.0))
    square = jnp.sum(jnp.sum(parts, axis=0, keepdims=True), axis=1, keepdims=True)
    norm = jnp.sqrt(square)
    factor = jnp.minimum(1.0, clip_limit / norm)
    norm_ref[0:1, :] = jnp.broadcast_to(norm, (1, LANES))
    norm_ref[1:2, :] = jnp.broadcast_to(factor, (1, LANES))
    norm_ref[2:8, :] = jnp.zeros((6, LANES), f32)


def total_of(packed, small, squares_at):
    steps = len(bits_of(lax.axis_size("fsdp"))) - 1 + len(bits_of(lax.axis_size("dp")))
    rows = packed.shape[0]
    return comm_call(
        functools.partial(total_kernel, small, squares_at),
        3,
        (packed,),
        ((packed.shape, f32), ((8, LANES), f32)),
        (
            pltpu.VMEM((steps + 1, rows // 2, LANES), f32),
            pltpu.VMEM((steps + 2, rows // 2, LANES), f32),
            pltpu.SemaphoreType.DMA((steps + 2,)),
            pltpu.SemaphoreType.DMA((steps + 2,)),
        ),
        (pltpu.VMEM,),
        (pltpu.VMEM, pltpu.VMEM),
        packed.size * 4 * 3,
    )


def update_table_kernel(norm_ref, w_ref, m_ref, a_ref, g_ref, *outs):
    new = stepped(w_ref[...], m_ref[...], a_ref[...], g_ref[...], norm_ref[1:2, 0:1])
    for out, value in zip(outs, new + (new[0].astype(bf16),)):
        out[...] = value


def update_table(norms, weight, moment, average, grad):
    rows, cols = weight.shape
    block = pl.BlockSpec((TCHUNK, cols), lambda i: (i, 0))
    return pl.pallas_call(
        update_table_kernel,
        name="update_table",
        grid=(pl.cdiv(rows, TCHUNK),),
        in_specs=[pl.BlockSpec((8, LANES), lambda i: (0, 0))] + [block] * 4,
        out_specs=[block] * 4,
        out_shape=[jax.ShapeDtypeStruct((rows, cols), kind) for kind in (f32, f32, f32, bf16)],
        compiler_params=pltpu.CompilerParams(vmem_limit_bytes=VMEM_LIMIT),
        cost_estimate=pl.CostEstimate(
            flops=8 * weight.size, transcendentals=0, bytes_accessed=30 * weight.size
        ),
    )(norms, weight, moment, average, grad)


def update_projections_kernel(norm_ref, *refs):
    factor = norm_ref[1:2, 0:1]
    sources = (refs[0:3], refs[3:6])
    grads = refs[6 : 6 + 2 * LAYERS]
    outs = refs[6 + 2 * LAYERS :]
    for group in (0, 1):
        for l in range(LAYERS):
            grad = grads[2 * l + group]
            step = min(grad.shape[0], 16)

            def some(r, _, l=l, group=group, grad=grad, step=step):
                rows = pl.ds(pl.multiple_of(r * step, step), step)
                new = stepped(*(ref[l, rows, :] for ref in sources[group]), grad[rows, :], factor)
                for i in range(3):
                    outs[4 * group + i][l, rows, :] = new[i]
                outs[4 * group + 3][l, rows, :] = new[0].astype(bf16)
                return 0

            lax.fori_loop(0, grad.shape[0] // step, some, 0)


def update_projections(norms, projections, grads):
    outs = []
    for i in (0, 3):
        outs += [(projections[i].shape, f32)] * 3 + [(projections[i].shape, bf16)]
    return local_call(update_projections_kernel, (norms, *projections, *grads), tuple(outs))


def snake(place, size):
    return jnp.where(place < size // 2, place, size // 2 + size - 1 - place)


def wrap(value, size):
    return lax.rem(value + size, size)


def gather_kernel(*refs):
    arrays = 2 * LAYERS
    own = refs[:arrays]
    full = refs[arrays : 2 * arrays]
    local_sem, z_send, z_recv, ring_send, ring_recv, mate_send, mate_recv = refs[2 * arrays :]
    dp = lax.axis_index("dp")
    me = lax.axis_index("fsdp")
    size = lax.axis_size("dp")
    count = lax.axis_size("fsdp") // MB
    core = me % MB
    k = me // MB
    ring = snake(dp, size)
    reach = size // 2
    right = snake(wrap(ring + 1, size), size)
    left = snake(wrap(ring - 1, size), size)
    mate = k * MB + 1 - core
    up, down = me + MB, me - MB
    has_up, has_down = k < count - 1, k > 0
    barrier = pltpu.get_barrier_semaphore()
    for target in ((right, me), (left, me), (dp, mate)):
        pl.semaphore_signal(barrier, inc=1, device_id=target, device_id_type=MESH)

    @pl.when(has_up)
    def _():
        pl.semaphore_signal(barrier, inc=1, device_id=(dp, up), device_id_type=MESH)

    @pl.when(has_down)
    def _():
        pl.semaphore_signal(barrier, inc=1, device_id=(dp, down), device_id_type=MESH)

    pl.semaphore_wait(barrier, 3 + jnp.where(has_up, 1, 0) + jnp.where(has_down, 1, 0))

    def spot(a, d, z, c):
        return full[a].at[d, z, c]

    def chain(a, src, z, side):
        return remote(
            src, spot(a, dp, z, core), z_send.at[a, z], z_recv.at[a, z], dp, up if side == 0 else down
        )

    def chain_own(a, side):
        return remote(
            own[a],
            spot(a, dp, k, core),
            z_send.at[a, count + side],
            z_recv.at[a, k],
            dp,
            up if side == 0 else down,
        )

    def round_ring(a, src, d, z, side):
        return remote(
            src,
            spot(a, d, z, core),
            ring_send.at[a, side],
            ring_recv.at[a, d, z],
            right if side == 0 else left,
            me,
        )

    def to_mate(a, src, d, z):
        return remote(src, spot(a, d, z, core), mate_send.at[a], mate_recv.at[a], dp, mate)

    def carried(a, side):
        return (a < arrays // 2) == (side == 0)

    for a in range(arrays):

        @pl.when(has_up)
        def _(a=a):
            chain_own(a, 0).start()

        @pl.when(has_down)
        def _(a=a):
            chain_own(a, 1).start()

    for a in range(arrays):
        for side in (0, 1):
            round_ring(a, own[a], dp, k, side).start()
    for a in range(arrays):
        to_mate(a, own[a], dp, k).start()
        pltpu.make_async_copy(own[a], spot(a, dp, k, core), local_sem.at[a]).start()

    def ring_step(z, s):
        for side in (0, 1):
            origin = snake(wrap(ring - s if side == 0 else ring + s, size), size)
            for a in range(arrays):
                if s == reach and not carried(a, side):
                    continue
                piece = spot(a, origin, z, core)
                round_ring(a, piece, origin, z, side).wait_recv()
                if s + 1 < reach or (s + 1 == reach and carried(a, side)):
                    round_ring(a, piece, origin, z, side).start()
                to_mate(a, piece, origin, z).start()

    def arrive(z, side):
        for a in range(arrays):
            piece = spot(a, dp, z, core)
            chain(a, piece, z, side).wait_recv()

            @pl.when(has_up if side == 0 else has_down)
            def _(a=a, piece=piece):
                chain(a, piece, z, side).start()

            for way in (0, 1):
                round_ring(a, piece, dp, z, way).start()
            to_mate(a, piece, dp, z).start()

    def both_ways(far, act):
        if far == 0:
            act(k, 0)
            return

        @pl.when(k >= far)
        def _():
            act(k - far, 0)

        @pl.when(k + far < count)
        def _():
            act(k + far, 1)

    for turn in range(1, count + reach):
        if turn < count:
            both_ways(turn, arrive)
        for s in range(1, reach + 1):
            if 0 <= turn - s < count:
                both_ways(turn - s, lambda z, side, s=s: ring_step(z, s))

    for a in range(arrays):
        pltpu.make_async_copy(own[a], spot(a, dp, k, core), local_sem.at[a]).wait()
        for side in (0, 1):
            sent = full[a].at[pl.ds(0, reach if carried(a, side) else reach - 1), :, core]
            remote(sent, sent, ring_send.at[a, side], ring_recv.at[a, 0, 0], dp, mate).wait_send()
        whole = full[a].at[:, :, core]
        remote(whole, whole, mate_send.at[a], mate_recv.at[a], dp, mate).wait_send()
        whole = full[a].at[:, :, 1 - core]
        remote(whole, whole, mate_send.at[a], mate_recv.at[a], dp, mate).wait_recv()

        @pl.when(has_up)
        def _(a=a):
            chain_own(a, 0).wait_send()

        @pl.when(has_down)
        def _(a=a):
            chain_own(a, 1).wait_send()

        for far in range(1, count):

            @pl.when(jnp.logical_and(k >= far, has_up))
            def _(a=a, far=far):
                chain(a, spot(a, dp, k - far, core), k - far, 0).wait_send()

            @pl.when(jnp.logical_and(k + far < count, has_down))
            def _(a=a, far=far):
                chain(a, spot(a, dp, k + far, core), k + far, 1).wait_send()


def gather_layers(shards):
    size, count = lax.axis_size("dp"), lax.axis_size("fsdp") // MB
    arrays = len(shards)
    outs = comm_call(
        gather_kernel,
        4,
        shards,
        tuple(((size, count, MB) + s.shape, bf16) for s in shards),
        (
            pltpu.SemaphoreType.DMA((arrays,)),
            pltpu.SemaphoreType.DMA((arrays, count + 2)),
            pltpu.SemaphoreType.DMA((arrays, count)),
            pltpu.SemaphoreType.DMA((arrays, 2)),
            pltpu.SemaphoreType.DMA((arrays, size, count)),
            pltpu.SemaphoreType.DMA((arrays,)),
            pltpu.SemaphoreType.DMA((arrays,)),
        ),
        (pltpu.VMEM,) * arrays,
        (pl.ANY,) * arrays,
        sum(s.size * 2 for s in shards) * 24,
    )
    return [o.reshape(size * count * MB * s.shape[0], s.shape[1]) for o, s in zip(outs, shards)]


def add_rows(dst, first, *others):
    rows = dst.shape[0]
    step = min(rows, 16)

    def one(i, _):
        at = pl.ds(pl.multiple_of(i * step, step), step)
        total = first[at, :].astype(f32)
        for other in others:
            total = total + other[at, :].astype(f32)
        dst[at, :] = total.astype(dst.dtype)
        return 0

    lax.fori_loop(0, rows // step, one, 0)


def reduce_kernel(*refs):
    arrays = 2 * LAYERS
    grads = refs[:arrays]
    outs = refs[arrays : 2 * arrays]
    held, given, come, chained = (
        refs[(2 + i) * arrays : (3 + i) * arrays] for i in range(4)
    )
    load_sem, mate_send, mate_recv, ring_send, ring_recv, z_send, z_recv = refs[6 * arrays :]
    dp = lax.axis_index("dp")
    me = lax.axis_index("fsdp")
    size = lax.axis_size("dp")
    count = lax.axis_size("fsdp") // MB
    core = me % MB
    k = me // MB
    ring = snake(dp, size)
    reach = size // 2
    right = snake(wrap(ring + 1, size), size)
    left = snake(wrap(ring - 1, size), size)
    mate = k * MB + 1 - core
    up, down = me + MB, me - MB
    has_up, has_down = k < count - 1, k > 0

    def load(a):
        return pltpu.make_async_copy(grads[a].at[:, :, core], held[a], load_sem.at[a])

    for a in range(arrays):
        load(a).start()
    barrier = pltpu.get_barrier_semaphore()
    for target in ((right, me), (left, me), (dp, mate)):
        pl.semaphore_signal(barrier, inc=1, device_id=target, device_id_type=MESH)

    @pl.when(has_up)
    def _():
        pl.semaphore_signal(barrier, inc=1, device_id=(dp, up), device_id_type=MESH)

    @pl.when(has_down)
    def _():
        pl.semaphore_signal(barrier, inc=1, device_id=(dp, down), device_id_type=MESH)

    pl.semaphore_wait(barrier, 3 + jnp.where(has_up, 1, 0) + jnp.where(has_down, 1, 0))

    def away(j, side):
        return snake(wrap(ring + j if side == 0 else ring - j, size), size)

    def to_mate(a, d):
        return remote(
            grads[a].at[d, :, 1 - core], given[a].at[d], mate_send.at[a], mate_recv.at[a, d], dp, mate
        )

    def carried(a, side):
        return (a < arrays // 2) == (side == 0)

    def targets(j):
        if j == 0:
            return [dp]
        if j == reach:
            return [away(j, 0)]
        return [away(j, 0), away(j, 1)]

    for j in range(reach, -1, -1):
        for d in targets(j):
            for a in range(arrays):
                to_mate(a, d).start()

    for a in range(arrays):
        load(a).wait()

    def add_mate(d):
        for a in range(arrays):
            to_mate(a, d).wait_recv()

            def one(z, _, a=a):
                add_rows(held[a].at[d, z], held[a].at[d, z], given[a].at[d, z])
                return 0

            lax.fori_loop(0, count, one, 0)

    def first_step(a, side):
        d = away(reach, 0)
        return remote(
            held[a].at[d], come[a].at[side, 0], ring_send.at[a, side], ring_recv.at[a, side, 0, 0],
            right if side == 0 else left, me,
        )

    def next_step(a, side, s, z):
        d = away(reach - s, side)
        return remote(
            held[a].at[d, z], come[a].at[side, s, z], ring_send.at[a, side],
            ring_recv.at[a, side, s, z], right if side == 0 else left, me,
        )

    far_most = jnp.maximum(k, count - 1 - k)
    near_most = jnp.minimum(k, count - 1 - k)
    uneven = far_most - near_most
    long_side = jnp.where(count - 1 - k > k, 1, -1)

    def chunk_at(i):
        j = jnp.maximum(i - uneven, 0)
        paired = k + (1 - 2 * (j % 2)) * (near_most - j // 2)
        return jnp.where(i < uneven, k + long_side * (far_most - i), paired)

    add_mate(away(reach, 0))
    for a in range(arrays):
        first_step(a, 0 if carried(a, 0) else 1).start()
    for s in range(1, reach):
        for side in (0, 1):
            add_mate(away(reach - s, side))
        if s == 1:
            for a in range(arrays):
                first_step(a, 0 if carried(a, 0) else 1).wait_recv()

        def pass_on(i, _, s=s):
            z = chunk_at(i)
            for side in (0, 1):
                d = away(reach - s, side)
                for a in range(arrays):
                    if s > 1:
                        next_step(a, side, s - 1, z).wait_recv()
                    if s > 1 or carried(a, side):
                        add_rows(held[a].at[d, z], held[a].at[d, z], come[a].at[side, s - 1, z])
                    next_step(a, side, s, z).start()
            return 0

        lax.fori_loop(0, count, pass_on, 0)
    add_mate(dp)

    def along(a, side, z):
        return remote(
            held[a].at[dp, z], chained[a].at[side, z], z_send.at[a, z], z_recv.at[a, side, z],
            dp, up if side == 0 else down,
        )

    def finish(i, _):
        z = chunk_at(i)
        for a in range(arrays):
            for side in (0, 1):
                next_step(a, side, reach - 1, z).wait_recv()
            add_rows(
                held[a].at[dp, z],
                held[a].at[dp, z],
                come[a].at[0, reach - 1, z],
                come[a].at[1, reach - 1, z],
            )
            for side in (0, 1):
                beyond = z > k if side == 0 else z < k
                fed = has_down if side == 0 else has_up

                @pl.when(jnp.logical_and(fed, jnp.logical_or(beyond, z == k)))
                def _(a=a, side=side):
                    along(a, side, z).wait_recv()
                    add_rows(held[a].at[dp, z], held[a].at[dp, z], chained[a].at[side, z])

                @pl.when(beyond)
                def _(a=a, side=side):
                    along(a, side, z).start()

        return 0

    lax.fori_loop(0, count, finish, 0)
    for a in range(arrays):
        add_rows(outs[a], held[a].at[dp, k])
        for side in (0, 1):
            sent = held[a].at[pl.ds(0, reach if carried(a, side) else reach - 1)]
            remote(
                sent, sent, ring_send.at[a, side], ring_recv.at[a, side, 0, 0], dp, mate
            ).wait_send()
        remote(
            given[a], given[a], mate_send.at[a], mate_recv.at[a, 0], dp, mate
        ).wait_send()

    def sent_along(z, _):
        for a in range(arrays):

            @pl.when(z != k)
            def _(a=a):
                along(a, 0, z).wait_send()

        return 0

    lax.fori_loop(0, count, sent_along, 0)


def reduce_layers(grads):
    size, count = lax.axis_size("dp"), lax.axis_size("fsdp") // MB
    arrays = len(grads)
    reach = size // 2
    shards = [(g.shape[0] // (size * count * MB), g.shape[1]) for g in grads]
    blocks = [g.reshape((size, count, MB) + s) for g, s in zip(grads, shards)]
    return comm_call(
        reduce_kernel,
        5,
        blocks,
        tuple((s, f32) for s in shards),
        tuple(pltpu.VMEM((size, count) + s, bf16) for s in shards) * 2
        + tuple(pltpu.VMEM((2, reach, count) + s, bf16) for s in shards)
        + tuple(pltpu.VMEM((2, count) + s, bf16) for s in shards)
        + (
            pltpu.SemaphoreType.DMA((arrays,)),
            pltpu.SemaphoreType.DMA((arrays,)),
            pltpu.SemaphoreType.DMA((arrays, size)),
            pltpu.SemaphoreType.DMA((arrays, 2)),
            pltpu.SemaphoreType.DMA((arrays, 2, reach, count)),
            pltpu.SemaphoreType.DMA((arrays, count)),
            pltpu.SemaphoreType.DMA((arrays, 2, count)),
        ),
        (pl.ANY,) * arrays,
        (pltpu.VMEM,) * arrays,
        sum(g.size * 2 for g in grads),
    )


def pair_lanes(p):
    return pl.ds(pl.multiple_of(p * LANES, LANES), LANES)


def first_half(rows):
    return lax.broadcasted_iota(jnp.int32, (rows, LANES), 1) < HDIM


def spread_columns(values, column, per_pair, rows):
    half = first_half(rows)
    for p in range(PAIRS):
        left = jnp.broadcast_to(values[:, 2 * p : 2 * p + 1], (rows, LANES))
        right = jnp.broadcast_to(values[:, 2 * p + 1 : 2 * p + 2], (rows, LANES))
        if column is not None:
            column[2 * p] = left
            column[2 * p + 1] = right
        if per_pair is not None:
            per_pair[p] = jnp.where(half, left, right)


def take_vectors(layer_ref, conv_ref, head_ref, gate_ref, cw_ref, dtb_ref, al_ref, sk_ref, gg_ref):
    layer = layer_ref[0]
    cw_ref[0 : CONV + 1, :] = conv_ref[layer]
    heads = head_ref[layer]
    dtb_ref[...] = heads[0:1, :]
    al_ref[...] = heads[1:2, :]
    half = first_half(1)
    for p in range(PAIRS):
        left = jnp.broadcast_to(heads[2:3, 2 * p : 2 * p + 1], (1, LANES))
        right = jnp.broadcast_to(heads[2:3, 2 * p + 1 : 2 * p + 2], (1, LANES))
        sk_ref[p : p + 1, :] = jnp.where(half, left, right)
    gg_ref[...] = gate_ref[layer]


VECTOR_SCRATCH = (
    pltpu.VMEM((8, XBC), f32),
    pltpu.VMEM((1, LANES), f32),
    pltpu.VMEM((1, LANES), f32),
    pltpu.VMEM((PAIRS, LANES), f32),
    pltpu.VMEM((1, DI), f32),
)


def scan_kernel(
    layer_ref, proj_ref, conv_ref, head_ref, gate_ref,
    pre_ref, y_ref, yn_ref, dt_ref, cum_ref, got, halo_ref,
    cw_ref, dtb_ref, al_ref, sk_ref, gg_ref, pad, col, tcol, lcol, lrow, st, give, square, edge_send, edge_recv, send, recv,
):
    rows = proj_ref.shape[0]
    take_vectors(layer_ref, conv_ref, head_ref, gate_ref, cw_ref, dtb_ref, al_ref, sk_ref, gg_ref)
    first, final = chunk_place(1)
    chain_barrier(1, first, final)
    edge = to_next(
        proj_ref.at[pl.ds(rows - 8, 8), pl.ds(DI, XBC)], halo_ref, edge_send, edge_recv, 1
    )

    @pl.when(jnp.logical_not(final))
    def _():
        edge.start()

    @pl.when(first)
    def _():
        halo_ref[...] = jnp.zeros(halo_ref.shape, f32)
        got[...] = jnp.zeros(got.shape, bf16)

    pad[8:, :] = proj_ref[:, DI : DI + XBC]
    dt_ref[...] = jnp.zeros((rows, LANES), f32)
    dt_ref[:, 0:HEADS] = proj_ref[:, DI + XBC :]
    drive = dt_ref[...] + dtb_ref[...]
    dt = jnp.maximum(drive, 0.0) + jnp.log1p(jnp.exp(-jnp.abs(drive)))
    dt_ref[...] = dt
    rate = dt * (-jnp.exp(al_ref[...]))
    ri = lax.broadcasted_iota(jnp.int32, (rows, rows), 0)
    ci = lax.broadcasted_iota(jnp.int32, (rows, rows), 1)
    causal = ri >= ci
    cum = dot_nn(jnp.where(causal, 1.0, 0.0), rate, highest)
    cum_ref[...] = cum
    lrow[...] = cum.T
    spread_columns(cum, col, lcol, rows)
    spread_columns(dt, None, tcol, rows)

    @pl.when(jnp.logical_not(first))
    def _():
        edge.wait_recv()

    pad[0:8, :] = halo_ref[...]

    def conv(i, _):
        xs = pair_lanes(i)
        out = jnp.broadcast_to(cw_ref[CONV : CONV + 1, xs], (rows, LANES))
        for k in range(CONV):
            out = out + cw_ref[k : k + 1, xs] * pad[5 + k : 5 + k + rows, xs]
        pre_ref[:, xs] = out
        return 0

    lax.fori_loop(0, XBC // LANES, conv, 0)
    bm = silu(pre_ref[:, DI : DI + NSTATE]).astype(bf16)
    cm = silu(pre_ref[:, DI + NSTATE :]).astype(bf16)
    cb = dot_nt(cm, bm)
    half = first_half(rows)

    def states(p, _):
        xs = pair_lanes(p)
        lp = lcol[p]
        tail = jnp.exp(lp[rows - 1 : rows, :] - lp) * tcol[p]
        st[xs, :] = dot_tn((tail * silu(pre_ref[:, xs])).astype(bf16), bm)
        return 0

    lax.fori_loop(0, PAIRS, states, 0, unroll=2)
    square[...] = jnp.zeros(square.shape, f32)

    def pair(p):
        xs = pair_lanes(p)
        x = silu(pre_ref[:, xs])
        xtb = (tcol[p] * x).astype(bf16)
        parts = []
        for j in range(2):
            h = 2 * p + j
            c = col[h]
            d = jnp.concatenate([c] * (rows // LANES), axis=1) - lrow[pl.ds(h, 1), :]
            m = (jnp.exp(jnp.where(causal, d, OFF)) * cb).astype(bf16)
            parts.append(dot_nn(m, xtb))
        y = jnp.where(half, parts[0], parts[1]) + sk_ref[pl.ds(p, 1), :] * x
        y = y + jnp.exp(lcol[p]) * dot_nt(cm, got[xs, :])
        y_ref[:, xs] = y
        g = y * silu(proj_ref[:, xs])
        return g * g

    def step(g, _):
        chain_step(g, 1, first, final, got, give, st, col, rows, send, recv)
        total = square[...]
        for i in range(PART // LANES):
            total = total + pair(g * (PART // LANES) + i)
        square[...] = total
        return 0

    lax.fori_loop(0, CHAIN_STEPS, step, 0)
    scale = lax.rsqrt(jnp.sum(square[...], axis=1, keepdims=True) / DI + epsilon)

    def put(p, _):
        xs = pair_lanes(p)
        g = y_ref[:, xs] * silu(proj_ref[:, xs])
        yn_ref[:, xs] = (g * scale * gg_ref[0:1, xs]).astype(bf16)
        return 0

    lax.fori_loop(0, PAIRS, put, 0, unroll=2)

    @pl.when(jnp.logical_not(final))
    def _():
        edge.wait_send()

    chain_end(1, final, got, give, send, recv)


def back_kernel(
    layer_ref, dyn_ref, y_ref, proj_ref, halo_ref, pre_ref, dt_ref, cum_ref, sin_ref,
    conv_ref, head_ref, gate_ref,
    dp_ref, dcw_ref, dsm_ref, dgg_ref,
    cw_ref, dtb_ref, al_ref, sk_ref, gg_ref, pad, grad, col, tcol, lcol, lrow, dcb, dbm, dcm, dlog, dtx, ends, dy_ref, drive_ref,
    got, give, gst, dx_ref, edge_ref, from_ref, edge_send, edge_recv, send, recv,
):
    rows = y_ref.shape[0]
    take_vectors(layer_ref, conv_ref, head_ref, gate_ref, cw_ref, dtb_ref, al_ref, sk_ref, gg_ref)
    first, final = chunk_place(-1)
    chain_barrier(-1, first, final)

    @pl.when(first)
    def _():
        from_ref[...] = jnp.zeros(from_ref.shape, f32)
        got[...] = jnp.zeros(got.shape, bf16)

    cum = cum_ref[...]
    dt = dt_ref[...]
    lrow[...] = cum.T
    spread_columns(cum, col, lcol, rows)
    spread_columns(dt, None, tcol, rows)
    bm = silu(pre_ref[:, DI : DI + NSTATE]).astype(bf16)
    cm = silu(pre_ref[:, DI + NSTATE :]).astype(bf16)
    zero = jnp.zeros((rows, LANES), f32)

    def sums(p, carry):
        xs = pair_lanes(p)
        g = y_ref[:, xs] * silu(proj_ref[:, xs])
        return carry[0] + g * g, carry[1] + g * (dyn_ref[:, xs] * gg_ref[0:1, xs])

    square, cross = lax.fori_loop(0, PAIRS, sums, (zero, zero))
    scale = lax.rsqrt(jnp.sum(square, axis=1, keepdims=True) / DI + epsilon)
    mean = jnp.sum(cross, axis=1, keepdims=True) * scale / DI

    def ungate(p, _):
        xs = pair_lanes(p)
        z = proj_ref[:, xs]
        y = y_ref[:, xs]
        sg = lax.logistic(z)
        sz = z * sg
        ghat = y * sz * scale
        dyn = dyn_ref[:, xs]
        dgg_ref[0:1, xs] = jnp.sum(dyn * ghat, axis=0, keepdims=True)
        dg = scale * (dyn * gg_ref[0:1, xs] - ghat * mean)
        dy = dg * sz
        dy_ref[:, xs] = dy
        dp_ref[:, xs] = (dg * y * (sg * (1.0 + z * (1.0 - sg)))).astype(bf16)
        gst[xs, :] = dot_tn((jnp.exp(lcol[p]) * dy).astype(bf16), cm)
        return 0

    lax.fori_loop(0, PAIRS, ungate, 0, unroll=2)
    pad[0:8, :] = halo_ref[...]
    pad[8:, :] = proj_ref[:, DI : DI + XBC]
    grad[0:8, :] = jnp.zeros((8, XBC), f32)
    grad[rows + 8 :, :] = jnp.zeros((8, XBC), f32)
    cbt = dot_nt(bm, cm)
    ri = lax.broadcasted_iota(jnp.int32, (rows, rows), 0)
    ci = lax.broadcasted_iota(jnp.int32, (rows, rows), 1)
    causal = ri <= ci
    half = first_half(rows)
    dcb[...] = jnp.zeros((rows, rows), f32)
    dbm[...] = zero
    dcm[...] = zero
    dlog[...] = zero
    dtx[...] = zero
    ends[...] = jnp.zeros((16, LANES), f32)
    lane_row = lax.broadcasted_iota(jnp.int32, (LANES, LANES), 0)
    lane_col = lax.broadcasted_iota(jnp.int32, (LANES, LANES), 1)
    ones = jnp.ones((8, NSTATE), f32)

    def pair(p):
        xs = pair_lanes(p)
        pre = pre_ref[:, xs]
        sg = lax.logistic(pre)
        x = pre * sg
        tp = tcol[p]
        xt = tp * x
        dy = dy_ref[:, xs]
        dyb = dy.astype(bf16)
        parts = []
        for j in range(2):
            h = 2 * p + j
            c = col[h]
            d = lrow[pl.ds(h, 1), :] - jnp.concatenate([c] * (rows // LANES), axis=1)
            w = jnp.exp(jnp.where(causal, d, OFF))
            parts.append(dot_nn((w * cbt).astype(bf16), dyb))
            own = half if j == 0 else jnp.logical_not(half)
            q = dot_nt(jnp.where(own, xt, 0.0).astype(bf16), dyb)
            dcb[...] += w * q
        lp = lcol[p]
        last = lp[rows - 1 : rows, :]
        tail = jnp.exp(last - lp)
        gin = got[xs, :]
        sin = sin_ref[xs, :]
        dst = tail * dot_nt(bm, gin)
        dxt = jnp.where(half, parts[0], parts[1]) + dst
        dbm[...] += dot_nn((tail * xt).astype(bf16), gin)
        dcm[...] += dot_nn((jnp.exp(lp) * dy).astype(bf16), sin)
        sk = sk_ref[pl.ds(p, 1), :]
        pick = jnp.where(lane_col == 2 * p + jnp.where(lane_row >= HDIM, 1, 0), 1.0, 0.0)
        dlog[...] += dot_nn(dy * (y_ref[:, xs] - sk * x) - xt * dxt, pick, highest)
        dtx[...] += dot_nn(x * dxt, pick, highest)
        held = dot_nt(ones, gin.astype(f32) * sin.astype(f32), highest)
        end = jnp.sum(xt * dst, axis=0, keepdims=True) + jnp.exp(last) * held[0:1, :]
        skip = jnp.sum(dy * x, axis=0, keepdims=True)
        stacked = jnp.concatenate(
            [jnp.broadcast_to(end, (8, LANES)), jnp.broadcast_to(skip, (8, LANES))], axis=0
        )
        ends[...] += dot_nn(stacked, pick, highest)
        grad[pl.ds(8, rows), xs] = (tp * dxt + sk * dy) * (sg * (1.0 + pre * (1.0 - sg)))

    def step(g, _):
        chain_step(g, -1, first, final, got, give, gst, col, rows, send, recv)
        for i in range(PART // LANES):
            pair(g * (PART // LANES) + i)
        return 0

    lax.fori_loop(0, CHAIN_STEPS, step, 0)
    dcbb = dcb[...].astype(bf16)
    dc = dcm[...] + dot_tn(dcbb, bm)
    db = dbm[...] + dot_nn(dcbb, cm)
    grad[8 : 8 + rows, DI : DI + NSTATE] = db * silu_grad(pre_ref[:, DI : DI + NSTATE])
    grad[8 : 8 + rows, DI + NSTATE :] = dc * silu_grad(pre_ref[:, DI + NSTATE :])

    def edges(i, _):
        xs = pair_lanes(i)
        edge = jnp.zeros((8, LANES), f32)
        for k in range(CONV):
            edge = edge + cw_ref[k : k + 1, xs] * grad[3 - k : 11 - k, xs]
        edge_ref[:, xs] = edge
        return 0

    lax.fori_loop(0, XBC // LANES, edges, 0)
    edge = to_next(edge_ref, from_ref, edge_send, edge_recv, -1)

    @pl.when(jnp.logical_not(final))
    def _():
        edge.start()

    last_row = lax.broadcasted_iota(jnp.int32, (rows, LANES), 0) == rows - 1
    dl = dlog[...] + jnp.where(last_row, ends[0:1, :], 0.0)
    da = dot_nn(jnp.where(causal, 1.0, 0.0), dl, highest)
    decay = -jnp.exp(al_ref[...])
    ddt = dtx[...] + da * decay
    drive_ref[...] = jnp.zeros((rows, LANES), f32)
    drive_ref[:, 0:HEADS] = proj_ref[:, DI + XBC :]
    ddr = ddt * lax.logistic(drive_ref[...] + dtb_ref[...])
    dp_ref[:, DI + XBC :] = ddr[:, 0:HEADS].astype(bf16)
    dsm_ref[...] = jnp.zeros((8, LANES), f32)
    dsm_ref[0:1, :] = jnp.sum(ddr, axis=0, keepdims=True)
    dsm_ref[1:2, :] = jnp.sum(da * dt, axis=0, keepdims=True) * decay
    dsm_ref[2:3, :] = ends[8:9, :]

    def conv(i, _):
        xs = pair_lanes(i)
        own = grad[pl.ds(8, rows), xs]
        out = jnp.zeros((rows, LANES), f32)
        for k in range(CONV):
            out = out + cw_ref[k : k + 1, xs] * grad[11 - k : 11 - k + rows, xs]
            dcw_ref[k : k + 1, xs] = jnp.sum(
                own * pad[5 + k : 5 + k + rows, xs], axis=0, keepdims=True
            )
        dcw_ref[4:5, xs] = jnp.sum(own, axis=0, keepdims=True)
        dx_ref[:, xs] = out
        return 0

    lax.fori_loop(0, XBC // LANES, conv, 0)

    @pl.when(jnp.logical_not(first))
    def _():
        edge.wait_recv()

    dx_ref[rows - 8 :, :] += from_ref[...]
    dp_ref[:, DI : DI + XBC] = dx_ref[...].astype(bf16)

    @pl.when(jnp.logical_not(final))
    def _():
        edge.wait_send()

    chain_end(-1, final, got, give, send, recv)


VTILE = 1280
NTILE = 256


def head_specs(width, tokens):
    return dict(
        table=pl.BlockSpec((VTILE, width), lambda i: (i, 0)),
        hidden=pl.BlockSpec((tokens, width), lambda i: (0, 0)),
        kept=pl.BlockSpec((VTILE, tokens), lambda i: (i, 0)),
        row=pl.BlockSpec((1, tokens), lambda i: (0, 0)),
        tile_row=pl.BlockSpec((1, 1, tokens), lambda i: (i, 0, 0)),
    )


def head_call(kernel, grid, in_specs, out_specs, outs, scratch, ins, cells):
    return pl.pallas_call(
        kernel,
        grid=(grid,),
        in_specs=in_specs,
        out_specs=out_specs,
        out_shape=[jax.ShapeDtypeStruct(shape, kind) for shape, kind in outs],
        scratch_shapes=list(scratch),
        compiler_params=pltpu.CompilerParams(
            dimension_semantics=("arbitrary",), vmem_limit_bytes=VMEM_LIMIT
        ),
        cost_estimate=pl.CostEstimate(
            flops=2 * cells * D, transcendentals=cells, bytes_accessed=4 * cells
        ),
    )(*ins)


UNROLL = 8


def head_stats_kernel(
    lead_ref, table_ref, own_ref, lab_ref, w_ref,
    q_ref, all_ref, lse_ref, fac_ref, hit_ref,
    kept, tops, sums, hits, shown, own_sem, put_sem, z_send, z_recv, m_send, m_recv, s_send, s_recv,
):
    dp = lax.axis_index("dp")
    me = lax.axis_index("fsdp")
    shards = lax.axis_size("fsdp")
    count = shards // MB
    core = me % MB
    k = me // MB
    mate = k * MB + 1 - core
    vocab_rows = lead_ref.shape[0] + table_ref.shape[0]
    rows = own_ref.shape[0]
    tiles = tops.shape[0]
    barrier = pltpu.get_barrier_semaphore()
    for other in range(1, shards):
        pl.semaphore_signal(
            barrier, inc=1, device_id=(dp, lax.rem(me + other, shards)), device_id_type=MESH
        )
    pl.semaphore_wait(barrier, shards - 1)

    near = jnp.minimum(k, count - 1 - k)
    long_side = jnp.where(count - 1 - k > k, 1, -1)

    def chunk_at(i):
        paired = k + (2 * (i % 2) - 1) * ((i + 1) // 2)
        return jnp.where(i <= 2 * near, paired, k + long_side * (i - near))

    def along(z, side):
        at = all_ref.at[z * MB + core]
        return remote(
            at, at, z_send.at[side, z], z_recv.at[z], dp, me + MB if side == 0 else me - MB
        )

    def to_mate(z):
        at = all_ref.at[z * MB + core]
        return remote(at, at, m_send.at[z], m_recv.at[z], dp, mate)

    def from_mate(z):
        at = all_ref.at[z * MB + 1 - core]
        return remote(at, at, m_send.at[z], m_recv.at[z], dp, mate)

    keep = pltpu.make_async_copy(own_ref, all_ref.at[me], own_sem)
    keep.start()
    keep.wait()

    @pl.when(k < count - 1)
    def _():
        along(k, 0).start()

    @pl.when(k > 0)
    def _():
        along(k, 1).start()

    to_mate(k).start()
    whole = vocab_rows - vocab_rows % 16
    for slot in range(2):
        kept[slot, whole:, :] = jnp.zeros((kept.shape[1] - whole, rows), bf16)

    def put(step, b):
        return pltpu.make_async_copy(
            kept.at[step % 2],
            q_ref.at[:, pl.ds(pl.multiple_of(b * rows, rows), rows)],
            put_sem.at[step % 2],
        )

    def block(step, b):
        @pl.when(step >= 2)
        def _():
            put(step, b).wait()

        slot = step % 2
        ns = pl.ds(pl.multiple_of(b * rows, rows), rows)
        h = all_ref[b]
        label = lab_ref[0:1, ns]
        for t in range(tiles):
            first = t * VTILE
            size = min(VTILE, vocab_rows - first)
            part = lead_ref[...] if t == 0 else table_ref[first - VTILE : first - VTILE + size, :]
            logits = dot_nt(part, h)
            top = jnp.max(logits, axis=0, keepdims=True)
            p = jnp.exp(logits - top)
            kept[slot, first : first + size, :] = p.astype(bf16)
            tops[t, 0:1, ns] = top
            sums[t, 0:1, ns] = jnp.sum(p, axis=0, keepdims=True)
            rid = lax.broadcasted_iota(jnp.int32, (size, rows), 0)
            hits[t, 0:1, ns] = jnp.sum(
                jnp.where(rid == label - first, logits, 0.0), axis=0, keepdims=True
            )
        put(step, b).start()

    def chunk(i, _):
        z = chunk_at(i)

        @pl.when(jnp.logical_and(i > 0, k >= i))
        def _():
            along(k - i, 0).wait_recv()

            @pl.when(k < count - 1)
            def _():
                along(k - i, 0).start()

            to_mate(k - i).start()

        @pl.when(jnp.logical_and(i > 0, k + i < count))
        def _():
            along(k + i, 1).wait_recv()

            @pl.when(k > 0)
            def _():
                along(k + i, 1).start()

            to_mate(k + i).start()

        block(2 * i, z * MB + core)
        from_mate(z).wait_recv()
        block(2 * i + 1, z * MB + 1 - core)
        return 0

    lax.fori_loop(0, count, chunk, 0)
    top = tops[0, 0:1, :]
    for t in range(1, tiles):
        top = jnp.maximum(top, tops[t, 0:1, :])
    total = jnp.zeros_like(top)
    hit = jnp.zeros_like(top)
    for t in range(tiles):
        total = total + sums[t, 0:1, :] * jnp.exp(tops[t, 0:1, :] - top)
        hit = hit + hits[t, 0:1, :]
    hit_ref[...] = hit
    shown[me, 0:1, :] = top
    shown[me, 1:2, :] = total

    def tell(other):
        at = shown.at[me]
        return remote(
            at, at, s_send.at[other], s_recv.at[me], dp, lax.rem(me + other, shards)
        )

    def told(other):
        at = shown.at[lax.rem(me + other, shards)]
        return remote(
            at, at, s_send.at[other], s_recv.at[lax.rem(me + other, shards)], dp, mate
        )

    for other in range(1, shards):
        tell(other).start()
    for other in range(1, shards):
        told(other).wait_recv()
    top = shown[0, 0:1, :]
    for f in range(1, shards):
        top = jnp.maximum(top, shown[f, 0:1, :])
    total = jnp.zeros_like(top)
    for f in range(shards):
        total = total + shown[f, 1:2, :] * jnp.exp(shown[f, 0:1, :] - top)
    lse = top + jnp.log(total)
    lse_ref[...] = lse
    scale = w_ref[...] * (1.0 + 2.0 * z_weight * lse)
    for t in range(tiles):
        fac_ref[t, 0:1, :] = scale * jnp.exp(tops[t, 0:1, :] - lse)
    for other in range(1, shards):
        tell(other).wait_send()
    for z in range(count):

        @pl.when(jnp.logical_and(k >= z, k < count - 1))
        def _(z=z):
            along(z, 0).wait_send()

        @pl.when(jnp.logical_and(k <= z, k > 0))
        def _(z=z):
            along(z, 1).wait_send()

        to_mate(z).wait_send()
    put(0, 0).wait()
    put(1, 0).wait()


def head_stats(lead, table, own, labels, weight):
    vocab_rows, width = lead.shape[0] + table.shape[0], table.shape[1]
    rows = own.shape[0]
    shards = lax.axis_size("fsdp")
    count = shards // MB
    tokens = shards * rows
    tiles = pl.cdiv(vocab_rows, VTILE)
    kept, everyone, lse, fac, hit = comm_call(
        head_stats_kernel,
        6,
        (lead, table, own, labels, weight),
        (
            ((tiles * VTILE, tokens), bf16),
            ((shards, rows, width), bf16),
            ((1, tokens), f32),
            ((tiles, 1, tokens), f32),
            ((1, tokens), f32),
        ),
        (
            pltpu.VMEM((2, tiles * VTILE, rows), bf16),
            pltpu.VMEM((tiles, 1, tokens), f32),
            pltpu.VMEM((tiles, 1, tokens), f32),
            pltpu.VMEM((tiles, 1, tokens), f32),
            pltpu.VMEM((shards, 2, tokens), f32),
            pltpu.SemaphoreType.DMA,
            pltpu.SemaphoreType.DMA((2,)),
            pltpu.SemaphoreType.DMA((2, count)),
            pltpu.SemaphoreType.DMA((count,)),
            pltpu.SemaphoreType.DMA((count,)),
            pltpu.SemaphoreType.DMA((count,)),
            pltpu.SemaphoreType.DMA((shards,)),
            pltpu.SemaphoreType.DMA((shards,)),
        ),
        (pltpu.VMEM,) * 5,
        (pl.ANY, pltpu.VMEM, pltpu.VMEM, pltpu.VMEM, pltpu.VMEM),
        own.size * 2 * 7,
    )
    return kept, everyone.reshape(tokens, width), lse, fac, hit


def logit_grads(q, fac, weight, rid, label):
    other = weight * (0.1 / VOCAB)
    return (q.astype(f32) * fac - jnp.where(rid == label, other + 0.9 * weight, other)).astype(bf16)


def head_rows_kernel(vocab_rows, lead_ref, e_ref, q_ref, fac_ref, w_ref, lab_ref, out_ref, acc, et):
    step = pl.program_id(0)
    first = step * VTILE
    tokens = q_ref.shape[1]

    @pl.when(step == 0)
    def _():
        acc[...] = jnp.zeros(acc.shape, f32)

    eid = lax.broadcasted_iota(jnp.int32, (VTILE, e_ref.shape[1]), 0)
    part = jnp.where(step == 0, lead_ref[...].astype(f32), e_ref[...].astype(f32))
    et[...] = jnp.where(eid < vocab_rows - first, part, 0.0).T.astype(bf16)

    def chunk(j, _):
        ns = pl.ds(pl.multiple_of(j * NTILE, NTILE), NTILE)
        rid = lax.broadcasted_iota(jnp.int32, (VTILE, NTILE), 0)
        dl = logit_grads(
            q_ref[:, ns], fac_ref[0, 0:1, ns], w_ref[0:1, ns], rid, lab_ref[0:1, ns] - first
        )
        acc[:, ns] += dot_nn(et[...], dl)
        return 0

    lax.fori_loop(0, tokens // NTILE, chunk, 0, unroll=UNROLL)

    @pl.when(step == pl.num_programs(0) - 1)
    def _():
        def put(j, _):
            ns = pl.ds(pl.multiple_of(j * NTILE, NTILE), NTILE)
            out_ref[ns, :] = acc[:, ns].T.astype(bf16)
            return 0

        lax.fori_loop(0, tokens // NTILE, put, 0)


def head_rows(lead, table, kept, fac, weight, labels):
    vocab_rows, width = lead.shape[0] + table.shape[0], table.shape[1]
    tokens = kept.shape[1]
    sp = head_specs(width, tokens)
    return head_call(
        functools.partial(head_rows_kernel, vocab_rows),
        pl.cdiv(vocab_rows, VTILE),
        [
            pl.BlockSpec((VTILE, width), lambda i: (0, 0)),
            pl.BlockSpec((VTILE, width), lambda i: (jnp.maximum(i - 1, 0), 0)),
            sp["kept"],
            sp["tile_row"],
            sp["row"],
            sp["row"],
        ],
        [sp["hidden"]],
        [((tokens, width), bf16)],
        (pltpu.VMEM((width, tokens), f32), pltpu.VMEM((width, VTILE), bf16)),
        (lead, table, kept, fac, weight, labels),
        vocab_rows * tokens,
    )[0]


def head_table_kernel(h_ref, q_ref, fac_ref, w_ref, lab_ref, out_ref, dl_ref):
    first = pl.program_id(0) * VTILE
    tokens = q_ref.shape[1]

    def chunk(j, _):
        ns = pl.ds(pl.multiple_of(j * NTILE, NTILE), NTILE)
        rid = lax.broadcasted_iota(jnp.int32, (VTILE, NTILE), 0)
        dl_ref[:, ns] = logit_grads(
            q_ref[:, ns], fac_ref[0, 0:1, ns], w_ref[0:1, ns], rid, lab_ref[0:1, ns] - first
        )
        return 0

    lax.fori_loop(0, tokens // NTILE, chunk, 0, unroll=UNROLL)

    def cols(j, _):
        ds = pl.ds(pl.multiple_of(j * 256, 256), 256)
        out_ref[:, ds] = dot_nn(dl_ref[...], h_ref[:, ds]).astype(bf16)
        return 0

    lax.fori_loop(0, h_ref.shape[1] // 256, cols, 0, unroll=True)


def head_table(hidden, kept, fac, weight, labels, vocab_rows):
    tokens, width = hidden.shape
    sp = head_specs(width, tokens)
    return head_call(
        head_table_kernel,
        pl.cdiv(vocab_rows, VTILE),
        [sp["hidden"], sp["kept"], sp["tile_row"], sp["row"], sp["row"]],
        [sp["table"]],
        [((vocab_rows, width), bf16)],
        (pltpu.VMEM((VTILE, tokens), bf16),),
        (hidden, kept, fac, weight, labels),
        vocab_rows * tokens,
    )[0]


def weight_grads_kernel(u_ref, dp_ref, yn_ref, db_ref, in_ref, out_ref):
    wide_cols = dp_ref.shape[1]
    for c in range(0, wide_cols, 1024):
        cs = pl.ds(c, min(1024, wide_cols - c))
        in_ref[:, cs] = dot_tn(u_ref[...], dp_ref[:, cs]).astype(bf16)
    out_ref[...] = dot_tn(yn_ref[...], db_ref[...]).astype(bf16)


def weight_grads(normed, grad_proj, mixed, grad_branch):
    rows = normed.shape[0]
    steps = D // LANES
    part = DI // steps
    return head_call(
        weight_grads_kernel,
        steps,
        [
            pl.BlockSpec((rows, LANES), lambda i: (0, i)),
            pl.BlockSpec((rows, ZW), lambda i: (0, 0)),
            pl.BlockSpec((rows, part), lambda i: (0, i)),
            pl.BlockSpec((rows, D), lambda i: (0, 0)),
        ],
        [pl.BlockSpec((LANES, ZW), lambda i: (i, 0)), pl.BlockSpec((part, D), lambda i: (i, 0))],
        [((D, ZW), bf16), ((DI, D), bf16)],
        (),
        (normed, grad_proj, mixed, grad_branch),
        rows * (ZW + DI),
    )


def after(value, earlier):
    return lax.optimization_barrier((value, earlier))[0]


def norm_scale(values):
    return lax.rsqrt(jnp.mean(values * values, axis=-1, keepdims=True) + epsilon)


def norm_back(grad, values, gain):
    scale = norm_scale(values)
    unit = values * scale
    inner = grad * gain
    back = scale * (inner - unit * jnp.mean(inner * unit, axis=-1, keepdims=True))
    return back, jnp.sum(grad * unit, axis=0)


def all_vectors(vector_params):
    rows = vector_params[: LAYERS * PER].reshape(LAYERS, PER)
    at = (CONV + 1) * XBC
    heads = rows[:, at : at + 3 * HEADS].reshape(LAYERS, 3, HEADS)
    after_heads = at + 3 * HEADS
    return dict(
        conv=rows[:, :at].reshape(LAYERS, CONV + 1, XBC),
        heads=jnp.pad(heads, ((0, 0), (0, 5), (0, LANES - HEADS))),
        gate=rows[:, after_heads + D :].reshape(LAYERS, 1, DI),
        pre=rows[:, after_heads : after_heads + D],
    )


def layer_forward(hidden, w_in, w_out, vec, layer):
    rows = hidden.shape[0]
    normed = (hidden * norm_scale(hidden) * vec["pre"][layer]).astype(bf16)
    proj = jnp.dot(normed, w_in, preferred_element_type=f32)
    pre, y, mixed, dt, cum, entering, halo = comm_call(
        scan_kernel,
        1,
        (jnp.full((1,), layer, jnp.int32), proj, vec["conv"], vec["heads"], vec["gate"]),
        (
            ((rows, XBC), f32),
            ((rows, DI), f32),
            ((rows, DI), bf16),
            ((rows, LANES), f32),
            ((rows, LANES), f32),
            ((DI, NSTATE), bf16),
            ((8, XBC), f32),
        ),
        VECTOR_SCRATCH
        + (
            pltpu.VMEM((rows + 8, XBC), f32),
            pltpu.VMEM((HEADS, rows, LANES), f32),
            pltpu.VMEM((PAIRS, rows, LANES), f32),
            pltpu.VMEM((PAIRS, rows, LANES), f32),
            pltpu.VMEM((LANES, rows), f32),
            pltpu.VMEM((DI, NSTATE), f32),
            pltpu.VMEM((DI, NSTATE), bf16),
            pltpu.VMEM((rows, LANES), f32),
            pltpu.SemaphoreType.DMA,
            pltpu.SemaphoreType.DMA,
            pltpu.SemaphoreType.DMA((CHAIN_STEPS,)),
            pltpu.SemaphoreType.DMA((CHAIN_STEPS,)),
        ),
        (pltpu.SMEM,) + (pltpu.VMEM,) * 4,
        (pltpu.VMEM,) * 7,
        DI * NSTATE * 2,
    )
    branch = jnp.dot(mixed, w_out, preferred_element_type=f32)
    record = (hidden, normed, proj, halo, pre, dt, cum, entering, y, mixed)
    return hidden + branch, record


def layer_backward(grad_hidden, w_in, w_out, vec, layer, record):
    hidden, normed, proj, halo, pre, dt, cum, entering, y, mixed = record
    rows = hidden.shape[0]
    grad_branch = grad_hidden.astype(bf16)
    grad_mixed = dot_nt(grad_branch, w_out)
    grad_proj, dconv, dsmall, dgate = comm_call(
        back_kernel,
        2,
        (
            jnp.full((1,), layer, jnp.int32), grad_mixed, y, proj, halo, pre, dt, cum, entering,
            vec["conv"], vec["heads"], vec["gate"],
        ),
        (
            ((rows, ZW), bf16),
            ((8, XBC), f32),
            ((8, LANES), f32),
            ((1, DI), f32),
        ),
        VECTOR_SCRATCH
        + (
            pltpu.VMEM((rows + 8, XBC), f32),
            pltpu.VMEM((rows + 16, XBC), f32),
            pltpu.VMEM((HEADS, rows, LANES), f32),
            pltpu.VMEM((PAIRS, rows, LANES), f32),
            pltpu.VMEM((PAIRS, rows, LANES), f32),
            pltpu.VMEM((LANES, rows), f32),
            pltpu.VMEM((rows, rows), f32),
            pltpu.VMEM((rows, LANES), f32),
            pltpu.VMEM((rows, LANES), f32),
            pltpu.VMEM((rows, LANES), f32),
            pltpu.VMEM((rows, LANES), f32),
            pltpu.VMEM((16, LANES), f32),
            pltpu.VMEM((rows, DI), f32),
            pltpu.VMEM((rows, LANES), f32),
            pltpu.VMEM((DI, NSTATE), bf16),
            pltpu.VMEM((DI, NSTATE), bf16),
            pltpu.VMEM((DI, NSTATE), f32),
            pltpu.VMEM((rows, XBC), f32),
            pltpu.VMEM((8, XBC), f32),
            pltpu.VMEM((8, XBC), f32),
            pltpu.SemaphoreType.DMA,
            pltpu.SemaphoreType.DMA,
            pltpu.SemaphoreType.DMA((CHAIN_STEPS,)),
            pltpu.SemaphoreType.DMA((CHAIN_STEPS,)),
        ),
        (pltpu.SMEM,) + (pltpu.VMEM,) * 11,
        (pltpu.VMEM,) * 4,
        DI * NSTATE * 2,
    )
    grad_normed = dot_nt(grad_proj, w_in)
    grad_in, grad_out = weight_grads(normed, grad_proj, mixed, grad_branch)
    grad_prev, dpre_gain = norm_back(grad_normed, hidden, vec["pre"][layer])
    grad_vec = jnp.concatenate(
        [
            dconv[: CONV + 1].reshape(-1),
            dsmall[0, :HEADS],
            dsmall[1, :HEADS],
            dsmall[2, :HEADS],
            dpre_gain,
            dgate[0],
        ]
    )
    return grad_hidden + grad_prev, grad_in, grad_out, grad_vec


def whole_step(
    token_ids,
    target_ids,
    seq_lengths,
    embedding,
    embedding_mom,
    embedding_avg,
    in_proj,
    in_proj_mom,
    in_proj_avg,
    out_proj,
    out_proj_mom,
    out_proj_avg,
    vector_params,
    vector_mom,
    vector_avg,
):
    groups = lax.axis_size("dp")
    shards = lax.axis_size("fsdp")
    group_index = lax.axis_index("dp")
    shard_index = lax.axis_index("fsdp")
    chunks = shards // MB
    seq_rows = token_ids.shape[2]
    rows = seq_rows // chunks
    vocab_rows, own_cols = embedding.shape
    tokens = MB * seq_rows
    total_count = jnp.sum(seq_lengths).astype(f32)
    in_low = in_proj.astype(bf16)
    out_low = out_proj.astype(bf16)

    lead = lax.all_gather(embedding[:VTILE].astype(bf16), "dp", axis=1, tiled=True)
    ids_all = group_call(share_kernel, 7, token_ids[:, 0, :], ((groups, MB, seq_rows), jnp.int32))
    ids_all = ids_all.reshape(groups, MB, chunks, rows).transpose(2, 1, 0, 3).reshape(-1)
    every = ids_all.shape[0]
    local_ids = ids_all - shard_index * vocab_rows
    inside = (local_ids >= 0) & (local_ids < vocab_rows)
    sorted_ids, sorted_tok = lax.sort(
        (jnp.where(inside, local_ids, vocab_rows), jnp.arange(every, dtype=jnp.int32)),
        num_keys=1,
    )
    held_here = sorted_ids < vocab_rows
    count = jnp.sum(held_here.astype(jnp.int32)).reshape(1)
    row_list = jnp.where(held_here, sorted_ids, 0)
    tok_list = jnp.where(held_here, sorted_tok, every)
    looked, embed_low, own_sums = local_call(
        lookup_kernel,
        (count, row_list, tok_list, embedding),
        (((every, own_cols), bf16), ((vocab_rows - VTILE, own_cols), bf16), ((8, own_cols), f32)),
        scratch=(pltpu.VMEM((every + 8, own_cols), f32),),
        in_smem=(0, 1, 2),
    )
    mine = lax.psum_scatter(
        looked.reshape(shards * groups * rows, own_cols), "fsdp", scatter_dimension=0, tiled=True
    )
    hidden = group_call(
        to_rows_kernel,
        8,
        mine.reshape(groups, rows, own_cols),
        ((rows, D), f32),
        (pltpu.VMEM((groups, rows, own_cols), bf16),),
    )

    shards = []
    for l in range(LAYERS):
        shards += [in_low[l], out_low[l]]
    shards = after(shards, looked)
    gathered = gather_layers(shards)
    w_in, w_out = gathered[0::2], gathered[1::2]
    embed_low = after(embed_low, gathered)
    table = lax.all_gather(embed_low, "dp", axis=1, tiled=True)

    vecs = all_vectors(vector_params)
    final_gain = vector_params[LAYERS * PER :]
    records = []
    for l in range(LAYERS):
        hidden, record = layer_forward(hidden, w_in[l], w_out[l], vecs, l)
        records.append(record)

    final_low = (hidden * norm_scale(hidden) * final_gain).astype(bf16)

    def in_order(per_seq):
        return per_seq.reshape(MB, chunks, rows).transpose(1, 0, 2).reshape(1, tokens)

    labels = in_order(target_ids[:, 0, :])
    lengths = lax.dynamic_index_in_dim(seq_lengths, group_index, 1, keepdims=True)
    valid = in_order((jnp.arange(seq_rows)[None, :] < lengths).astype(f32))
    local_labels = labels - shard_index * vocab_rows
    weight = valid / total_count
    kept, group_hidden, lse, fac, target = head_stats(lead, table, final_low, local_labels, weight)
    own_mask = jnp.arange(tokens) // rows == shard_index
    per_row = jnp.where(own_mask, lse[0] + z_weight * lse[0] * lse[0], 0.0)
    loss_sum = jnp.sum((per_row - 0.9 * target[0]) * valid[0])
    own_valid = lax.dynamic_slice_in_dim(valid[0], shard_index * rows, rows)
    hidden_sum = jnp.sum(final_low.astype(f32) * own_valid[:, None], axis=0)
    column_sum = jnp.zeros((groups, own_cols), f32)
    column_sum = jnp.where(
        jnp.arange(groups)[:, None] == group_index, jnp.sum(own_sums, axis=0), column_sum
    ).reshape(D)

    rows_grad = head_rows(lead, table, kept, fac, weight, local_labels)
    own_grad = lax.psum_scatter(
        rows_grad, "fsdp", scatter_dimension=0, tiled=True
    ).astype(f32)
    table_grad = head_table(group_hidden, kept, fac, weight, local_labels, vocab_rows)
    table_part = lax.psum_scatter(table_grad, "dp", scatter_dimension=1, tiled=True)

    grad_hidden, dfinal = norm_back(after(own_grad, table_grad), hidden, final_gain)
    in_parts = [None] * LAYERS
    out_parts = [None] * LAYERS
    vec_parts = [None] * LAYERS
    for l in reversed(range(LAYERS)):
        grad_hidden, grad_in, grad_out, vec_parts[l] = layer_backward(
            grad_hidden, w_in[l], w_out[l], vecs, l, records[l]
        )
        if l == 0:
            sent = group_call(
                to_columns_kernel,
                9,
                grad_hidden,
                ((groups, rows, own_cols), bf16),
                (pltpu.VMEM((groups, rows, own_cols), bf16),),
            )
            spread = lax.all_gather(sent, "fsdp", axis=0).reshape(every, own_cols)
        in_parts[l], out_parts[l] = grad_in, grad_out
    whole = []
    for l in range(LAYERS):
        whole += [in_parts[l], out_parts[l]]
    summed_parts = reduce_layers(whole)
    spread = after(spread, summed_parts)
    table_total, table_squares = local_call(
        spread_kernel,
        (count, row_list, tok_list, spread, table_part),
        (((vocab_rows, own_cols), f32), ((8, own_cols), f32)),
        scratch=(pltpu.VMEM((every + 8, own_cols), f32),),
        in_smem=(0, 1, 2),
    )
    owner_squares = jnp.sum(table_squares)
    for part in summed_parts:
        owner_squares = owner_squares + jnp.sum(part * part)
    small = vector_params.shape[0]
    used = small + 2 * D + 2
    padded = pl.cdiv(used, 16 * LANES) * 16 * LANES
    packed = jnp.concatenate(
        vec_parts
        + [
            dfinal,
            hidden_sum,
            column_sum,
            owner_squares.reshape(1),
            loss_sum.reshape(1),
            jnp.zeros((padded - used,), f32),
        ]
    )
    packed, norms = total_of(packed.reshape(-1, LANES), small, used - 2)
    updated = list(update_table(norms, embedding, embedding_mom, embedding_avg, table_total))
    updated += update_projections(
        norms,
        (in_proj, in_proj_mom, in_proj_avg, out_proj, out_proj_mom, out_proj_avg),
        summed_parts,
    )
    packed = packed.reshape(-1)
    vector_total = packed[:small]
    hidden_total = packed[small : small + D]
    column_total = packed[small + D : small + 2 * D]
    mean_part = jnp.sum(hidden_total * column_total) * (0.1 / VOCAB)
    loss_value = (packed[used - 1] - mean_part) / total_count
    vector_new, vector_mom_new, vector_avg_new = stepped(
        vector_params, vector_mom, vector_avg, vector_total, norms[1, 0]
    )
    return (
        loss_value,
        norms[0, 0],
        *updated,
        vector_new,
        vector_mom_new,
        vector_avg_new,
        vector_new.astype(bf16),
    )


def solution(mesh):
    table_spec = P("fsdp", "dp")
    weight_spec = P(None, ("dp", "fsdp"), None)
    return jax.shard_map(
        whole_step,
        mesh=mesh,
        in_specs=(
            P(None, "dp", None),
            P(None, "dp", None),
            P(),
            *(table_spec,) * 3,
            *(weight_spec,) * 6,
            *(P(),) * 3,
        ),
        out_specs=(
            P(),
            P(),
            *(table_spec,) * 4,
            *(weight_spec,) * 8,
            *(P(),) * 4,
        ),
        check_vma=False,
    )
```

```python
import functools

import jax
import jax.numpy as jnp
from jax import lax
from jax.experimental import pallas as pl
from jax.experimental.pallas import tpu as pltpu
from jax.sharding import PartitionSpec as P


D = 1024
HEADS = 32
HDIM = 64
NSTATE = 128
CONV = 4
VOCAB = 50288
LAYERS = 2
MB = 2
DI = 2048
XBC = 2304
ZW = 4384
PER = 14688
LANES = 128
PAIRS = DI // LANES

epsilon = 1e-05
z_weight = 0.001
clip_limit = 0.2
step_rate = 1000.0
highest = lax.Precision.HIGHEST
bf16 = jnp.bfloat16
f32 = jnp.float32
VMEM_LIMIT = 62 * 1024 * 1024
OFF = -1e30


def dot_nn(a, b, precision=None):
    return lax.dot_general(
        a, b, (((1,), (0,)), ((), ())), precision=precision, preferred_element_type=f32
    )


def dot_nt(a, b, precision=None):
    return lax.dot_general(
        a, b, (((1,), (1,)), ((), ())), precision=precision, preferred_element_type=f32
    )


def dot_tn(a, b, precision=None):
    return lax.dot_general(
        a, b, (((0,), (0,)), ((), ())), precision=precision, preferred_element_type=f32
    )


def silu(v):
    return v * lax.logistic(v)


def silu_grad(v):
    s = lax.logistic(v)
    return s * (1.0 + v * (1.0 - s))


def local_call(kernel, ins, outs, scratch=(), in_smem=(), flops=0):
    total = sum(a.size * a.dtype.itemsize for a in ins)
    return pl.pallas_call(
        kernel,
        out_shape=[jax.ShapeDtypeStruct(shape, kind) for shape, kind in outs],
        in_specs=[
            pl.BlockSpec(memory_space=pltpu.SMEM if i in in_smem else pltpu.VMEM)
            for i in range(len(ins))
        ],
        out_specs=[pl.BlockSpec(memory_space=pltpu.VMEM) for _ in outs],
        scratch_shapes=list(scratch),
        compiler_params=pltpu.CompilerParams(vmem_limit_bytes=VMEM_LIMIT),
        cost_estimate=pl.CostEstimate(
            flops=flops or total, transcendentals=0, bytes_accessed=2 * total
        ),
    )(*ins)


def lookup_kernel(count_ref, row_ref, tok_ref, table_ref, out_ref, low_ref, sum_ref, held):
    tokens = out_ref.shape[0]
    step = 512

    def clear(i, _):
        held[pl.ds(pl.multiple_of(i * step, step), step), :] = jnp.zeros(
            (step, held.shape[1]), f32
        )
        return 0

    lax.fori_loop(0, tokens // step, clear, 0)

    def move(i, _):
        for k in range(8):
            row = row_ref[i * 8 + k]
            tok = tok_ref[i * 8 + k]
            held[pl.ds(tok, 1), :] = table_ref[pl.ds(row, 1), :]
        return 0

    lax.fori_loop(0, (count_ref[0] + 7) // 8, move, 0)

    def put(i, _):
        rows = pl.ds(pl.multiple_of(i * step, step), step)
        out_ref[rows, :] = held[rows, :].astype(bf16)
        return 0

    lax.fori_loop(0, tokens // step, put, 0)
    rows_all = table_ref.shape[0]
    part = VTILE // 5
    whole = rows_all // part

    def low_rows(i):
        return table_ref[pl.ds(pl.multiple_of(i * part, part), part), :].astype(bf16)

    def add(low, total):
        return total + jnp.sum(low.astype(f32).reshape(part // 8, 8, -1), axis=0)

    def cast(i, total):
        low = low_rows(i)
        low_ref[pl.ds(pl.multiple_of(i * part - VTILE, part), part), :] = low
        return add(low, total)

    total = lax.fori_loop(
        0, VTILE // part, lambda i, t: add(low_rows(i), t), jnp.zeros(sum_ref.shape, f32)
    )
    sum_ref[...] = lax.fori_loop(VTILE // part, whole, cast, total)
    if rows_all > whole * part:
        low = table_ref[whole * part :, :].astype(bf16)
        low_ref[whole * part - VTILE :, :] = low
        sum_ref[0:1, :] += jnp.sum(low.astype(f32), axis=0, keepdims=True)


def spread_kernel(count_ref, row_ref, tok_ref, grad_ref, base_ref, out_ref, square_ref, held):
    tokens = grad_ref.shape[0]
    step = 512
    rows_all = out_ref.shape[0]

    def take(i, _):
        rows = pl.ds(pl.multiple_of(i * step, step), step)
        held[rows, :] = grad_ref[rows, :].astype(f32)
        return 0

    lax.fori_loop(0, tokens // step, take, 0)
    held[pl.ds(tokens, 8), :] = jnp.zeros((8, held.shape[1]), f32)

    whole = rows_all // step

    def start(i, _):
        rows = pl.ds(pl.multiple_of(i * step, step), step)
        out_ref[rows, :] = base_ref[rows, :].astype(f32)
        return 0

    lax.fori_loop(0, whole, start, 0)
    if rows_all > whole * step:
        out_ref[whole * step :, :] = base_ref[whole * step :, :].astype(f32)

    def move(i, _):
        for k in range(8):
            row = row_ref[i * 8 + k]
            tok = tok_ref[i * 8 + k]
            out_ref[pl.ds(row, 1), :] = out_ref[pl.ds(row, 1), :] + held[pl.ds(tok, 1), :]
        return 0

    lax.fori_loop(0, (count_ref[0] + 7) // 8, move, 0)

    def square(i, total):
        part = out_ref[pl.ds(pl.multiple_of(i * step, step), step), :]
        return total + jnp.sum((part * part).reshape(step // 8, 8, -1), axis=0)

    total = lax.fori_loop(0, whole, square, jnp.zeros(square_ref.shape, f32))
    square_ref[...] = total
    if rows_all > whole * step:
        part = out_ref[whole * step :, :]
        square_ref[0:1, :] += jnp.sum(part * part, axis=0, keepdims=True)


MESH = pl.DeviceIdType.MESH


def remote(src, dst, send, recv, dp, fsdp):
    return pltpu.make_async_remote_copy(
        src_ref=src,
        dst_ref=dst,
        send_sem=send,
        recv_sem=recv,
        device_id=(dp, fsdp),
        device_id_type=MESH,
    )


def comm_call(kernel, number, ins, outs, scratch, in_spaces, out_spaces, sent):
    return pl.pallas_call(
        kernel,
        out_shape=[jax.ShapeDtypeStruct(shape, kind) for shape, kind in outs],
        in_specs=[pl.BlockSpec(memory_space=space) for space in in_spaces],
        out_specs=[pl.BlockSpec(memory_space=space) for space in out_spaces],
        scratch_shapes=list(scratch),
        compiler_params=pltpu.CompilerParams(
            collective_id=number, has_side_effects=True, vmem_limit_bytes=VMEM_LIMIT
        ),
        cost_estimate=pl.CostEstimate(flops=sent, transcendentals=0, bytes_accessed=2 * sent),
    )(*ins)


def greet_groups():
    dp = lax.axis_index("dp")
    me = lax.axis_index("fsdp")
    groups = lax.axis_size("dp")
    barrier = pltpu.get_barrier_semaphore()
    others = [lax.rem(dp + other, groups) for other in range(1, groups)]
    for other in others:
        pl.semaphore_signal(barrier, inc=1, device_id=(other, me), device_id_type=MESH)
    pl.semaphore_wait(barrier, groups - 1)
    return dp, me, others


def share_kernel(in_ref, out_ref, send, recv):
    dp, me, others = greet_groups()
    for other in others:
        remote(in_ref, out_ref.at[dp], send.at[other], recv.at[dp], other, me).start()
    out_ref[dp] = in_ref[...]
    for other in others:
        copy = remote(in_ref, out_ref.at[other], send.at[other], recv.at[other], other, me)
        copy.wait_recv()
        copy.wait_send()


def to_rows_kernel(in_ref, out_ref, landed, send, recv):
    dp, me, others = greet_groups()
    for other in others:
        remote(in_ref.at[other], landed.at[dp], send.at[other], recv.at[dp], other, me).start()
    landed[dp] = in_ref[dp]
    for other in others:
        remote(in_ref.at[other], landed.at[other], send.at[other], recv.at[other], other, me).wait_recv()
    cols = in_ref.shape[2]
    for g in range(in_ref.shape[0]):
        out_ref[:, g * cols : (g + 1) * cols] = landed[g].astype(f32)
    for other in others:
        remote(in_ref.at[other], landed.at[other], send.at[other], recv.at[other], other, me).wait_send()


def to_columns_kernel(in_ref, out_ref, parts, send, recv):
    dp, me, others = greet_groups()
    cols = out_ref.shape[2]
    for g in range(out_ref.shape[0]):
        parts[g] = in_ref[:, g * cols : (g + 1) * cols].astype(bf16)
    for other in others:
        remote(parts.at[other], out_ref.at[dp], send.at[other], recv.at[dp], other, me).start()
    out_ref[dp] = parts[dp]
    for other in others:
        copy = remote(parts.at[other], out_ref.at[other], send.at[other], recv.at[other], other, me)
        copy.wait_recv()
        copy.wait_send()


def group_call(kernel, number, array, out, scratch=()):
    groups = lax.axis_size("dp")
    return comm_call(
        kernel,
        number,
        (array,),
        (out,),
        tuple(scratch)
        + (pltpu.SemaphoreType.DMA((groups,)), pltpu.SemaphoreType.DMA((groups,))),
        (pltpu.VMEM,),
        (pltpu.VMEM,),
        array.size * 2,
    )[0]


CHAIN_STEPS = 8
PART = DI // CHAIN_STEPS


def chunk_place(direction):
    place = lax.axis_index("fsdp") // MB
    count = lax.axis_size("fsdp") // MB
    first = place == (0 if direction > 0 else count - 1)
    final = place == (count - 1 if direction > 0 else 0)
    return first, final


def chain_barrier(direction, first, final):
    dp = lax.axis_index("dp")
    me = lax.axis_index("fsdp")
    barrier = pltpu.get_barrier_semaphore()

    @pl.when(jnp.logical_not(first))
    def _():
        pl.semaphore_signal(
            barrier, inc=1, device_id=(dp, me - MB * direction), device_id_type=MESH
        )

    @pl.when(jnp.logical_not(final))
    def _():
        pl.semaphore_wait(barrier, 1)


def to_next(src, dst, send, recv, direction):
    dp = lax.axis_index("dp")
    return remote(src, dst, send, recv, dp, lax.axis_index("fsdp") + MB * direction)


def chain_step(g, direction, first, final, got, give, local, col, rows, send, recv):
    def copy():
        at = pl.ds(pl.multiple_of(g * PART, PART), PART)
        return to_next(give.at[at], got.at[at], send.at[g], recv.at[g], direction)

    @pl.when(jnp.logical_not(first))
    def _():
        copy().wait_recv()

    @pl.when(jnp.logical_not(final))
    def _():
        for i in range(PART // HDIM):
            h = pl.ds(pl.multiple_of(g * PART + i * HDIM, HDIM), HDIM)
            decay = jnp.exp(col[g * (PART // HDIM) + i, rows - 1 : rows, :])
            give[h, :] = (decay * got[h, :].astype(f32) + local[h, :]).astype(bf16)
        copy().start()


def chain_end(direction, final, got, give, send, recv):
    @pl.when(jnp.logical_not(final))
    def _():
        for g in range(CHAIN_STEPS):
            at = pl.ds(g * PART, PART)
            to_next(give.at[at], got.at[at], send.at[g], recv.at[g], direction).wait_send()


def bits_of(size):
    return [1 << b for b in range(size.bit_length() - 1)]


def stepped(weight, moment, average, grad, factor):
    scaled = grad * factor
    moment_new = 0.5 * moment + scaled
    weight_new = weight - step_rate * (scaled + 0.5 * moment_new)
    return weight_new, moment_new, 0.5 * average + 0.5 * weight_new


def total_kernel(small, squares_at, packed_ref, total_ref, norm_ref, work, got, send, recv):
    dp = lax.axis_index("dp")
    me = lax.axis_index("fsdp")
    half = packed_ref.shape[0] // 2
    core = me % MB
    partners = [("f", b) for b in bits_of(lax.axis_size("fsdp")) if b > 1]
    partners += [("d", b) for b in bits_of(lax.axis_size("dp"))]

    def across(kind, bit):
        ids, other = (me, lambda v: (dp, v)) if kind == "f" else (dp, lambda v: (v, me))
        return other(jnp.where((ids // bit) % 2 == 1, ids - bit, ids + bit))

    mate = across("f", 1)
    barrier = pltpu.get_barrier_semaphore()
    for target in [mate] + [across(*p) for p in partners]:
        pl.semaphore_signal(barrier, inc=1, device_id=target, device_id_type=MESH)
    pl.semaphore_wait(barrier, 1 + len(partners))

    mine = pl.ds(pl.multiple_of(core * half, 8), half)
    theirs = pl.ds(pl.multiple_of((1 - core) * half, 8), half)
    copy = remote(packed_ref.at[theirs], got.at[0], send.at[0], recv.at[0], *mate)
    copy.start()
    copy.wait()
    work[0] = packed_ref[mine, :] + got[0]
    for i, p in enumerate(partners):
        copy = remote(work.at[i], got.at[i + 1], send.at[i + 1], recv.at[i + 1], *across(*p))
        copy.start()
        copy.wait()
        work[i + 1] = work[i] + got[i + 1]
    n = len(partners)
    copy = remote(work.at[n], got.at[n + 1], send.at[n + 1], recv.at[n + 1], *mate)
    copy.start()
    copy.wait()
    total_ref[mine, :] = work[n]
    total_ref[theirs, :] = got[n + 1]

    total = total_ref[...]
    index = lax.broadcasted_iota(jnp.int32, total.shape, 0) * LANES
    index = index + lax.broadcasted_iota(jnp.int32, total.shape, 1)
    parts = jnp.where(index < small, total * total, jnp.where(index == squares_at, total, 0.0))
    square = jnp.sum(jnp.sum(parts, axis=0, keepdims=True), axis=1, keepdims=True)
    norm = jnp.sqrt(square)
    factor = jnp.minimum(1.0, clip_limit / norm)
    norm_ref[0:1, :] = jnp.broadcast_to(norm, (1, LANES))
    norm_ref[1:2, :] = jnp.broadcast_to(factor, (1, LANES))
    norm_ref[2:8, :] = jnp.zeros((6, LANES), f32)


def total_of(packed, small, squares_at):
    steps = len(bits_of(lax.axis_size("fsdp"))) - 1 + len(bits_of(lax.axis_size("dp")))
    rows = packed.shape[0]
    return comm_call(
        functools.partial(total_kernel, small, squares_at),
        3,
        (packed,),
        ((packed.shape, f32), ((8, LANES), f32)),
        (
            pltpu.VMEM((steps + 1, rows // 2, LANES), f32),
            pltpu.VMEM((steps + 2, rows // 2, LANES), f32),
            pltpu.SemaphoreType.DMA((steps + 2,)),
            pltpu.SemaphoreType.DMA((steps + 2,)),
        ),
        (pltpu.VMEM,),
        (pltpu.VMEM, pltpu.VMEM),
        packed.size * 4 * 3,
    )


def update_projections_kernel(norm_ref, *refs):
    factor = norm_ref[1:2, 0:1]
    sources = (refs[0:3], refs[3:6])
    grads = refs[6 : 6 + 2 * LAYERS]
    outs = refs[6 + 2 * LAYERS :]
    for group in (0, 1):
        for l in range(LAYERS):
            grad = grads[2 * l + group]
            step = min(grad.shape[0], 16)

            def some(r, _, l=l, group=group, grad=grad, step=step):
                rows = pl.ds(pl.multiple_of(r * step, step), step)
                new = stepped(*(ref[l, rows, :] for ref in sources[group]), grad[rows, :], factor)
                for i in range(3):
                    outs[4 * group + i][l, rows, :] = new[i]
                outs[4 * group + 3][l, rows, :] = new[0].astype(bf16)
                return 0

            lax.fori_loop(0, grad.shape[0] // step, some, 0)


def update_projections(norms, projections, grads):
    outs = []
    for i in (0, 3):
        outs += [(projections[i].shape, f32)] * 3 + [(projections[i].shape, bf16)]
    return local_call(update_projections_kernel, (norms, *projections, *grads), tuple(outs))


def snake(place, size):
    return jnp.where(place < size // 2, place, size // 2 + size - 1 - place)


def wrap(value, size):
    return lax.rem(value + size, size)


def gather_kernel(*refs):
    arrays = 2 * LAYERS
    own = refs[:arrays]
    full = refs[arrays : 2 * arrays]
    local_sem, z_send, z_recv, ring_send, ring_recv, mate_send, mate_recv = refs[2 * arrays :]
    dp = lax.axis_index("dp")
    me = lax.axis_index("fsdp")
    size = lax.axis_size("dp")
    count = lax.axis_size("fsdp") // MB
    core = me % MB
    k = me // MB
    ring = snake(dp, size)
    reach = size // 2
    right = snake(wrap(ring + 1, size), size)
    left = snake(wrap(ring - 1, size), size)
    mate = k * MB + 1 - core
    up, down = me + MB, me - MB
    has_up, has_down = k < count - 1, k > 0
    barrier = pltpu.get_barrier_semaphore()
    for target in ((right, me), (left, me), (dp, mate)):
        pl.semaphore_signal(barrier, inc=1, device_id=target, device_id_type=MESH)

    @pl.when(has_up)
    def _():
        pl.semaphore_signal(barrier, inc=1, device_id=(dp, up), device_id_type=MESH)

    @pl.when(has_down)
    def _():
        pl.semaphore_signal(barrier, inc=1, device_id=(dp, down), device_id_type=MESH)

    pl.semaphore_wait(barrier, 3 + jnp.where(has_up, 1, 0) + jnp.where(has_down, 1, 0))

    def spot(a, d, z, c):
        return full[a].at[d, z, c]

    def chain(a, src, z, side):
        return remote(
            src, spot(a, dp, z, core), z_send.at[a, z], z_recv.at[a, z], dp, up if side == 0 else down
        )

    def chain_own(a, side):
        return remote(
            own[a],
            spot(a, dp, k, core),
            z_send.at[a, count + side],
            z_recv.at[a, k],
            dp,
            up if side == 0 else down,
        )

    def round_ring(a, src, d, z, side):
        return remote(
            src,
            spot(a, d, z, core),
            ring_send.at[a, side],
            ring_recv.at[a, d, z],
            right if side == 0 else left,
            me,
        )

    def to_mate(a, src, d, z):
        return remote(src, spot(a, d, z, core), mate_send.at[a], mate_recv.at[a], dp, mate)

    def carried(a, side):
        return (a < arrays // 2) == (side == 0)

    for a in range(arrays):

        @pl.when(has_up)
        def _(a=a):
            chain_own(a, 0).start()

        @pl.when(has_down)
        def _(a=a):
            chain_own(a, 1).start()

    for a in range(arrays):
        for side in (0, 1):
            round_ring(a, own[a], dp, k, side).start()
    for a in range(arrays):
        to_mate(a, own[a], dp, k).start()
        pltpu.make_async_copy(own[a], spot(a, dp, k, core), local_sem.at[a]).start()

    def ring_step(z, s):
        for side in (0, 1):
            origin = snake(wrap(ring - s if side == 0 else ring + s, size), size)
            for a in range(arrays):
                if s == reach and not carried(a, side):
                    continue
                piece = spot(a, origin, z, core)
                round_ring(a, piece, origin, z, side).wait_recv()
                if s + 1 < reach or (s + 1 == reach and carried(a, side)):
                    round_ring(a, piece, origin, z, side).start()
                to_mate(a, piece, origin, z).start()

    def arrive(z, side):
        for a in range(arrays):
            piece = spot(a, dp, z, core)
            chain(a, piece, z, side).wait_recv()

            @pl.when(has_up if side == 0 else has_down)
            def _(a=a, piece=piece):
                chain(a, piece, z, side).start()

            for way in (0, 1):
                round_ring(a, piece, dp, z, way).start()
            to_mate(a, piece, dp, z).start()

    def both_ways(far, act):
        if far == 0:
            act(k, 0)
            return

        @pl.when(k >= far)
        def _():
            act(k - far, 0)

        @pl.when(k + far < count)
        def _():
            act(k + far, 1)

    for turn in range(1, count + reach):
        if turn < count:
            both_ways(turn, arrive)
        for s in range(1, reach + 1):
            if 0 <= turn - s < count:
                both_ways(turn - s, lambda z, side, s=s: ring_step(z, s))

    for a in range(arrays):
        pltpu.make_async_copy(own[a], spot(a, dp, k, core), local_sem.at[a]).wait()
        for side in (0, 1):
            sent = full[a].at[pl.ds(0, reach if carried(a, side) else reach - 1), :, core]
            remote(sent, sent, ring_send.at[a, side], ring_recv.at[a, 0, 0], dp, mate).wait_send()
        whole = full[a].at[:, :, core]
        remote(whole, whole, mate_send.at[a], mate_recv.at[a], dp, mate).wait_send()
        whole = full[a].at[:, :, 1 - core]
        remote(whole, whole, mate_send.at[a], mate_recv.at[a], dp, mate).wait_recv()

        @pl.when(has_up)
        def _(a=a):
            chain_own(a, 0).wait_send()

        @pl.when(has_down)
        def _(a=a):
            chain_own(a, 1).wait_send()

        for far in range(1, count):

            @pl.when(jnp.logical_and(k >= far, has_up))
            def _(a=a, far=far):
                chain(a, spot(a, dp, k - far, core), k - far, 0).wait_send()

            @pl.when(jnp.logical_and(k + far < count, has_down))
            def _(a=a, far=far):
                chain(a, spot(a, dp, k + far, core), k + far, 1).wait_send()


def gather_layers(shards):
    size, count = lax.axis_size("dp"), lax.axis_size("fsdp") // MB
    arrays = len(shards)
    outs = comm_call(
        gather_kernel,
        4,
        shards,
        tuple(((size, count, MB) + s.shape, bf16) for s in shards),
        (
            pltpu.SemaphoreType.DMA((arrays,)),
            pltpu.SemaphoreType.DMA((arrays, count + 2)),
            pltpu.SemaphoreType.DMA((arrays, count)),
            pltpu.SemaphoreType.DMA((arrays, 2)),
            pltpu.SemaphoreType.DMA((arrays, size, count)),
            pltpu.SemaphoreType.DMA((arrays,)),
            pltpu.SemaphoreType.DMA((arrays,)),
        ),
        (pltpu.VMEM,) * arrays,
        (pl.ANY,) * arrays,
        sum(s.size * 2 for s in shards) * 24,
    )
    return [o.reshape(size * count * MB * s.shape[0], s.shape[1]) for o, s in zip(outs, shards)]


def add_rows(dst, first, *others):
    rows = dst.shape[0]
    step = min(rows, 16)

    def one(i, _):
        at = pl.ds(pl.multiple_of(i * step, step), step)
        total = first[at, :].astype(f32)
        for other in others:
            total = total + other[at, :].astype(f32)
        dst[at, :] = total.astype(dst.dtype)
        return 0

    lax.fori_loop(0, rows // step, one, 0)


def reduce_kernel(*refs):
    arrays = 2 * LAYERS
    grads = refs[:arrays]
    outs = refs[arrays : 2 * arrays]
    held, given, come, chained = (
        refs[(2 + i) * arrays : (3 + i) * arrays] for i in range(4)
    )
    load_sem, mate_send, mate_recv, ring_send, ring_recv, z_send, z_recv = refs[6 * arrays :]
    dp = lax.axis_index("dp")
    me = lax.axis_index("fsdp")
    size = lax.axis_size("dp")
    count = lax.axis_size("fsdp") // MB
    core = me % MB
    k = me // MB
    ring = snake(dp, size)
    reach = size // 2
    right = snake(wrap(ring + 1, size), size)
    left = snake(wrap(ring - 1, size), size)
    mate = k * MB + 1 - core
    up, down = me + MB, me - MB
    has_up, has_down = k < count - 1, k > 0

    def load(a, d):
        return pltpu.make_async_copy(grads[a].at[d, :, core], held[a].at[d], load_sem.at[a, d])

    for j in range(reach, -1, -1):
        for d in {reach: [(0, j)], 0: [(0, 0)]}.get(j, [(0, j), (1, j)]):
            side, step = d
            d = snake(wrap(ring + step if side == 0 else ring - step, size), size)
            for a in range(arrays):
                load(a, d).start()
    barrier = pltpu.get_barrier_semaphore()
    for target in ((right, me), (left, me), (dp, mate)):
        pl.semaphore_signal(barrier, inc=1, device_id=target, device_id_type=MESH)

    @pl.when(has_up)
    def _():
        pl.semaphore_signal(barrier, inc=1, device_id=(dp, up), device_id_type=MESH)

    @pl.when(has_down)
    def _():
        pl.semaphore_signal(barrier, inc=1, device_id=(dp, down), device_id_type=MESH)

    pl.semaphore_wait(barrier, 3 + jnp.where(has_up, 1, 0) + jnp.where(has_down, 1, 0))

    def away(j, side):
        return snake(wrap(ring + j if side == 0 else ring - j, size), size)

    def to_mate(a, d):
        return remote(
            grads[a].at[d, :, 1 - core], given[a].at[d], mate_send.at[a], mate_recv.at[a, d], dp, mate
        )

    def carried(a, side):
        return (a < arrays // 2) == (side == 0)

    def targets(j):
        if j == 0:
            return [dp]
        if j == reach:
            return [away(j, 0)]
        return [away(j, 0), away(j, 1)]

    def send_mate(j):
        for d in targets(j):
            for a in range(arrays):
                to_mate(a, d).start()

    def add_mate(d):
        for a in range(arrays):
            load(a, d).wait()
            to_mate(a, d).wait_recv()

            def one(z, _, a=a):
                add_rows(held[a].at[d, z], held[a].at[d, z], given[a].at[d, z])
                return 0

            lax.fori_loop(0, count, one, 0)

    def first_step(a, side):
        d = away(reach, 0)
        return remote(
            held[a].at[d], come[a].at[side, 0], ring_send.at[a, side], ring_recv.at[a, side, 0, 0],
            right if side == 0 else left, me,
        )

    def next_step(a, side, s, z):
        d = away(reach - s, side)
        return remote(
            held[a].at[d, z], come[a].at[side, s, z], ring_send.at[a, side],
            ring_recv.at[a, side, s, z], right if side == 0 else left, me,
        )

    far_most = jnp.maximum(k, count - 1 - k)
    near_most = jnp.minimum(k, count - 1 - k)
    uneven = far_most - near_most
    long_side = jnp.where(count - 1 - k > k, 1, -1)

    def chunk_at(i):
        j = jnp.maximum(i - uneven, 0)
        paired = k + (1 - 2 * (j % 2)) * (near_most - j // 2)
        return jnp.where(i < uneven, k + long_side * (far_most - i), paired)

    send_mate(reach)
    add_mate(away(reach, 0))
    for a in range(arrays):
        first_step(a, 0 if carried(a, 0) else 1).start()
    for j in range(reach - 1, -1, -1):
        send_mate(j)
    for s in range(1, reach):
        for side in (0, 1):
            add_mate(away(reach - s, side))
        if s == 1:
            for a in range(arrays):
                first_step(a, 0 if carried(a, 0) else 1).wait_recv()

        def pass_on(i, _, s=s):
            z = chunk_at(i)
            for side in (0, 1):
                d = away(reach - s, side)
                for a in range(arrays):
                    if s > 1:
                        next_step(a, side, s - 1, z).wait_recv()
                    if s > 1 or carried(a, side):
                        add_rows(held[a].at[d, z], held[a].at[d, z], come[a].at[side, s - 1, z])
                    next_step(a, side, s, z).start()
            return 0

        lax.fori_loop(0, count, pass_on, 0)
    add_mate(dp)

    def along(a, side, z):
        return remote(
            held[a].at[dp, z], chained[a].at[side, z], z_send.at[a, z], z_recv.at[a, side, z],
            dp, up if side == 0 else down,
        )

    def finish(i, _):
        z = chunk_at(i)
        for a in range(arrays):
            for side in (0, 1):
                next_step(a, side, reach - 1, z).wait_recv()
            add_rows(
                held[a].at[dp, z],
                held[a].at[dp, z],
                come[a].at[0, reach - 1, z],
                come[a].at[1, reach - 1, z],
            )
            for side in (0, 1):
                beyond = z > k if side == 0 else z < k
                fed = has_down if side == 0 else has_up

                @pl.when(jnp.logical_and(fed, jnp.logical_or(beyond, z == k)))
                def _(a=a, side=side):
                    along(a, side, z).wait_recv()
                    add_rows(held[a].at[dp, z], held[a].at[dp, z], chained[a].at[side, z])

                @pl.when(beyond)
                def _(a=a, side=side):
                    along(a, side, z).start()

        return 0

    lax.fori_loop(0, count, finish, 0)
    for a in range(arrays):
        add_rows(outs[a], held[a].at[dp, k])
        for side in (0, 1):
            sent = held[a].at[pl.ds(0, reach if carried(a, side) else reach - 1)]
            remote(
                sent, sent, ring_send.at[a, side], ring_recv.at[a, side, 0, 0], dp, mate
            ).wait_send()
        remote(
            given[a], given[a], mate_send.at[a], mate_recv.at[a, 0], dp, mate
        ).wait_send()

    def sent_along(z, _):
        for a in range(arrays):

            @pl.when(z != k)
            def _(a=a):
                along(a, 0, z).wait_send()

        return 0

    lax.fori_loop(0, count, sent_along, 0)


def reduce_layers(grads):
    size, count = lax.axis_size("dp"), lax.axis_size("fsdp") // MB
    arrays = len(grads)
    reach = size // 2
    shards = [(g.shape[0] // (size * count * MB), g.shape[1]) for g in grads]
    blocks = [g.reshape((size, count, MB) + s) for g, s in zip(grads, shards)]
    return comm_call(
        reduce_kernel,
        5,
        blocks,
        tuple((s, f32) for s in shards),
        tuple(pltpu.VMEM((size, count) + s, bf16) for s in shards) * 2
        + tuple(pltpu.VMEM((2, reach, count) + s, bf16) for s in shards)
        + tuple(pltpu.VMEM((2, count) + s, bf16) for s in shards)
        + (
            pltpu.SemaphoreType.DMA((arrays, size)),
            pltpu.SemaphoreType.DMA((arrays,)),
            pltpu.SemaphoreType.DMA((arrays, size)),
            pltpu.SemaphoreType.DMA((arrays, 2)),
            pltpu.SemaphoreType.DMA((arrays, 2, reach, count)),
            pltpu.SemaphoreType.DMA((arrays, count)),
            pltpu.SemaphoreType.DMA((arrays, 2, count)),
        ),
        (pl.ANY,) * arrays,
        (pltpu.VMEM,) * arrays,
        sum(g.size * 2 for g in grads),
    )


def pair_lanes(p):
    return pl.ds(pl.multiple_of(p * LANES, LANES), LANES)


def first_half(rows):
    return lax.broadcasted_iota(jnp.int32, (rows, LANES), 1) < HDIM


def spread_columns(values, column, per_pair, rows):
    half = first_half(rows)
    for p in range(PAIRS):
        left = jnp.broadcast_to(values[:, 2 * p : 2 * p + 1], (rows, LANES))
        right = jnp.broadcast_to(values[:, 2 * p + 1 : 2 * p + 2], (rows, LANES))
        if column is not None:
            column[2 * p] = left
            column[2 * p + 1] = right
        if per_pair is not None:
            per_pair[p] = jnp.where(half, left, right)


def take_vectors(layer_ref, conv_ref, head_ref, gate_ref, cw_ref, dtb_ref, al_ref, sk_ref, gg_ref):
    layer = layer_ref[0]
    cw_ref[0 : CONV + 1, :] = conv_ref[layer]
    heads = head_ref[layer]
    dtb_ref[...] = heads[0:1, :]
    al_ref[...] = heads[1:2, :]
    half = first_half(1)
    for p in range(PAIRS):
        left = jnp.broadcast_to(heads[2:3, 2 * p : 2 * p + 1], (1, LANES))
        right = jnp.broadcast_to(heads[2:3, 2 * p + 1 : 2 * p + 2], (1, LANES))
        sk_ref[p : p + 1, :] = jnp.where(half, left, right)
    gg_ref[...] = gate_ref[layer]


VECTOR_SCRATCH = (
    pltpu.VMEM((8, XBC), f32),
    pltpu.VMEM((1, LANES), f32),
    pltpu.VMEM((1, LANES), f32),
    pltpu.VMEM((PAIRS, LANES), f32),
    pltpu.VMEM((1, DI), f32),
)


def scan_kernel(
    layer_ref, proj_ref, conv_ref, head_ref, gate_ref,
    pre_ref, y_ref, yn_ref, dt_ref, cum_ref, got, halo_ref,
    cw_ref, dtb_ref, al_ref, sk_ref, gg_ref, pad, col, tcol, lcol, lrow, st, give, square, edge_send, edge_recv, send, recv,
):
    rows = proj_ref.shape[0]
    take_vectors(layer_ref, conv_ref, head_ref, gate_ref, cw_ref, dtb_ref, al_ref, sk_ref, gg_ref)
    first, final = chunk_place(1)
    chain_barrier(1, first, final)
    edge = to_next(
        proj_ref.at[pl.ds(rows - 8, 8), pl.ds(DI, XBC)], halo_ref, edge_send, edge_recv, 1
    )

    @pl.when(jnp.logical_not(final))
    def _():
        edge.start()

    @pl.when(first)
    def _():
        halo_ref[...] = jnp.zeros(halo_ref.shape, f32)
        got[...] = jnp.zeros(got.shape, bf16)

    pad[8:, :] = proj_ref[:, DI : DI + XBC]
    dt_ref[...] = jnp.zeros((rows, LANES), f32)
    dt_ref[:, 0:HEADS] = proj_ref[:, DI + XBC :]
    drive = dt_ref[...] + dtb_ref[...]
    dt = jnp.maximum(drive, 0.0) + jnp.log1p(jnp.exp(-jnp.abs(drive)))
    dt_ref[...] = dt
    rate = dt * (-jnp.exp(al_ref[...]))
    ri = lax.broadcasted_iota(jnp.int32, (rows, rows), 0)
    ci = lax.broadcasted_iota(jnp.int32, (rows, rows), 1)
    causal = ri >= ci
    cum = dot_nn(jnp.where(causal, 1.0, 0.0), rate, highest)
    cum_ref[...] = cum
    lrow[...] = cum.T
    spread_columns(cum, col, lcol, rows)
    spread_columns(dt, None, tcol, rows)

    @pl.when(jnp.logical_not(first))
    def _():
        edge.wait_recv()

    pad[0:8, :] = halo_ref[...]

    def conv(i, _):
        xs = pair_lanes(i)
        out = jnp.broadcast_to(cw_ref[CONV : CONV + 1, xs], (rows, LANES))
        for k in range(CONV):
            out = out + cw_ref[k : k + 1, xs] * pad[5 + k : 5 + k + rows, xs]
        pre_ref[:, xs] = out
        return 0

    lax.fori_loop(0, XBC // LANES, conv, 0)
    bm = silu(pre_ref[:, DI : DI + NSTATE]).astype(bf16)
    cm = silu(pre_ref[:, DI + NSTATE :]).astype(bf16)
    cb = dot_nt(cm, bm)
    half = first_half(rows)

    def states(p, _):
        xs = pair_lanes(p)
        lp = lcol[p]
        tail = jnp.exp(lp[rows - 1 : rows, :] - lp) * tcol[p]
        st[xs, :] = dot_tn((tail * silu(pre_ref[:, xs])).astype(bf16), bm)
        return 0

    lax.fori_loop(0, PAIRS, states, 0, unroll=2)
    square[...] = jnp.zeros(square.shape, f32)

    def pair(p):
        xs = pair_lanes(p)
        x = silu(pre_ref[:, xs])
        xtb = (tcol[p] * x).astype(bf16)
        parts = []
        for j in range(2):
            h = 2 * p + j
            c = col[h]
            d = jnp.concatenate([c] * (rows // LANES), axis=1) - lrow[pl.ds(h, 1), :]
            m = (jnp.exp(jnp.where(causal, d, OFF)) * cb).astype(bf16)
            parts.append(dot_nn(m, xtb))
        y = jnp.where(half, parts[0], parts[1]) + sk_ref[pl.ds(p, 1), :] * x
        y = y + jnp.exp(lcol[p]) * dot_nt(cm, got[xs, :])
        y_ref[:, xs] = y
        g = y * silu(proj_ref[:, xs])
        return g * g

    def step(g, _):
        chain_step(g, 1, first, final, got, give, st, col, rows, send, recv)
        total = square[...]
        for i in range(PART // LANES):
            total = total + pair(g * (PART // LANES) + i)
        square[...] = total
        return 0

    lax.fori_loop(0, CHAIN_STEPS, step, 0)
    scale = lax.rsqrt(jnp.sum(square[...], axis=1, keepdims=True) / DI + epsilon)

    def put(p, _):
        xs = pair_lanes(p)
        g = y_ref[:, xs] * silu(proj_ref[:, xs])
        yn_ref[:, xs] = (g * scale * gg_ref[0:1, xs]).astype(bf16)
        return 0

    lax.fori_loop(0, PAIRS, put, 0, unroll=2)

    @pl.when(jnp.logical_not(final))
    def _():
        edge.wait_send()

    chain_end(1, final, got, give, send, recv)


def back_kernel(
    layer_ref, dyn_ref, y_ref, proj_ref, halo_ref, pre_ref, dt_ref, cum_ref, sin_ref,
    conv_ref, head_ref, gate_ref,
    dp_ref, dcw_ref, dsm_ref, dgg_ref,
    cw_ref, dtb_ref, al_ref, sk_ref, gg_ref, pad, grad, col, tcol, lcol, lrow, dcb, dbm, dcm, dlog, dtx, ends, dy_ref, drive_ref,
    got, give, gst, dx_ref, edge_ref, from_ref, edge_send, edge_recv, send, recv,
):
    rows = y_ref.shape[0]
    take_vectors(layer_ref, conv_ref, head_ref, gate_ref, cw_ref, dtb_ref, al_ref, sk_ref, gg_ref)
    first, final = chunk_place(-1)
    chain_barrier(-1, first, final)

    @pl.when(first)
    def _():
        from_ref[...] = jnp.zeros(from_ref.shape, f32)
        got[...] = jnp.zeros(got.shape, bf16)

    cum = cum_ref[...]
    dt = dt_ref[...]
    lrow[...] = cum.T
    spread_columns(cum, col, lcol, rows)
    spread_columns(dt, None, tcol, rows)
    bm = silu(pre_ref[:, DI : DI + NSTATE]).astype(bf16)
    cm = silu(pre_ref[:, DI + NSTATE :]).astype(bf16)
    zero = jnp.zeros((rows, LANES), f32)

    def sums(p, carry):
        xs = pair_lanes(p)
        g = y_ref[:, xs] * silu(proj_ref[:, xs])
        return carry[0] + g * g, carry[1] + g * (dyn_ref[:, xs] * gg_ref[0:1, xs])

    square, cross = lax.fori_loop(0, PAIRS, sums, (zero, zero))
    scale = lax.rsqrt(jnp.sum(square, axis=1, keepdims=True) / DI + epsilon)
    mean = jnp.sum(cross, axis=1, keepdims=True) * scale / DI

    def ungate(p, _):
        xs = pair_lanes(p)
        z = proj_ref[:, xs]
        y = y_ref[:, xs]
        sg = lax.logistic(z)
        sz = z * sg
        ghat = y * sz * scale
        dyn = dyn_ref[:, xs]
        dgg_ref[0:1, xs] = jnp.sum(dyn * ghat, axis=0, keepdims=True)
        dg = scale * (dyn * gg_ref[0:1, xs] - ghat * mean)
        dy = dg * sz
        dy_ref[:, xs] = dy
        dp_ref[:, xs] = (dg * y * (sg * (1.0 + z * (1.0 - sg)))).astype(bf16)
        gst[xs, :] = dot_tn((jnp.exp(lcol[p]) * dy).astype(bf16), cm)
        return 0

    lax.fori_loop(0, PAIRS, ungate, 0, unroll=2)
    pad[0:8, :] = halo_ref[...]
    pad[8:, :] = proj_ref[:, DI : DI + XBC]
    grad[0:8, :] = jnp.zeros((8, XBC), f32)
    grad[rows + 8 :, :] = jnp.zeros((8, XBC), f32)
    cbt = dot_nt(bm, cm)
    ri = lax.broadcasted_iota(jnp.int32, (rows, rows), 0)
    ci = lax.broadcasted_iota(jnp.int32, (rows, rows), 1)
    causal = ri <= ci
    half = first_half(rows)
    dcb[...] = jnp.zeros((rows, rows), f32)
    dbm[...] = zero
    dcm[...] = zero
    dlog[...] = zero
    dtx[...] = zero
    ends[...] = jnp.zeros((16, LANES), f32)
    lane_row = lax.broadcasted_iota(jnp.int32, (LANES, LANES), 0)
    lane_col = lax.broadcasted_iota(jnp.int32, (LANES, LANES), 1)
    ones = jnp.ones((8, NSTATE), f32)

    def pair(p):
        xs = pair_lanes(p)
        pre = pre_ref[:, xs]
        sg = lax.logistic(pre)
        x = pre * sg
        tp = tcol[p]
        xt = tp * x
        dy = dy_ref[:, xs]
        dyb = dy.astype(bf16)
        parts = []
        for j in range(2):
            h = 2 * p + j
            c = col[h]
            d = lrow[pl.ds(h, 1), :] - jnp.concatenate([c] * (rows // LANES), axis=1)
            w = jnp.exp(jnp.where(causal, d, OFF))
            parts.append(dot_nn((w * cbt).astype(bf16), dyb))
            own = half if j == 0 else jnp.logical_not(half)
            q = dot_nt(jnp.where(own, xt, 0.0).astype(bf16), dyb)
            dcb[...] += w * q
        lp = lcol[p]
        last = lp[rows - 1 : rows, :]
        tail = jnp.exp(last - lp)
        gin = got[xs, :]
        sin = sin_ref[xs, :]
        dst = tail * dot_nt(bm, gin)
        dxt = jnp.where(half, parts[0], parts[1]) + dst
        dbm[...] += dot_nn((tail * xt).astype(bf16), gin)
        dcm[...] += dot_nn((jnp.exp(lp) * dy).astype(bf16), sin)
        sk = sk_ref[pl.ds(p, 1), :]
        pick = jnp.where(lane_col == 2 * p + jnp.where(lane_row >= HDIM, 1, 0), 1.0, 0.0)
        dlog[...] += dot_nn(dy * (y_ref[:, xs] - sk * x) - xt * dxt, pick, highest)
        dtx[...] += dot_nn(x * dxt, pick, highest)
        held = dot_nt(ones, gin.astype(f32) * sin.astype(f32), highest)
        end = jnp.sum(xt * dst, axis=0, keepdims=True) + jnp.exp(last) * held[0:1, :]
        skip = jnp.sum(dy * x, axis=0, keepdims=True)
        stacked = jnp.concatenate(
            [jnp.broadcast_to(end, (8, LANES)), jnp.broadcast_to(skip, (8, LANES))], axis=0
        )
        ends[...] += dot_nn(stacked, pick, highest)
        grad[pl.ds(8, rows), xs] = (tp * dxt + sk * dy) * (sg * (1.0 + pre * (1.0 - sg)))

    def step(g, _):
        chain_step(g, -1, first, final, got, give, gst, col, rows, send, recv)
        for i in range(PART // LANES):
            pair(g * (PART // LANES) + i)
        return 0

    lax.fori_loop(0, CHAIN_STEPS, step, 0)
    dcbb = dcb[...].astype(bf16)
    dc = dcm[...] + dot_tn(dcbb, bm)
    db = dbm[...] + dot_nn(dcbb, cm)
    grad[8 : 8 + rows, DI : DI + NSTATE] = db * silu_grad(pre_ref[:, DI : DI + NSTATE])
    grad[8 : 8 + rows, DI + NSTATE :] = dc * silu_grad(pre_ref[:, DI + NSTATE :])

    def edges(i, _):
        xs = pair_lanes(i)
        edge = jnp.zeros((8, LANES), f32)
        for k in range(CONV):
            edge = edge + cw_ref[k : k + 1, xs] * grad[3 - k : 11 - k, xs]
        edge_ref[:, xs] = edge
        return 0

    lax.fori_loop(0, XBC // LANES, edges, 0)
    edge = to_next(edge_ref, from_ref, edge_send, edge_recv, -1)

    @pl.when(jnp.logical_not(final))
    def _():
        edge.start()

    last_row = lax.broadcasted_iota(jnp.int32, (rows, LANES), 0) == rows - 1
    dl = dlog[...] + jnp.where(last_row, ends[0:1, :], 0.0)
    da = dot_nn(jnp.where(causal, 1.0, 0.0), dl, highest)
    decay = -jnp.exp(al_ref[...])
    ddt = dtx[...] + da * decay
    drive_ref[...] = jnp.zeros((rows, LANES), f32)
    drive_ref[:, 0:HEADS] = proj_ref[:, DI + XBC :]
    ddr = ddt * lax.logistic(drive_ref[...] + dtb_ref[...])
    dp_ref[:, DI + XBC :] = ddr[:, 0:HEADS].astype(bf16)
    dsm_ref[...] = jnp.zeros((8, LANES), f32)
    dsm_ref[0:1, :] = jnp.sum(ddr, axis=0, keepdims=True)
    dsm_ref[1:2, :] = jnp.sum(da * dt, axis=0, keepdims=True) * decay
    dsm_ref[2:3, :] = ends[8:9, :]

    def conv(i, _):
        xs = pair_lanes(i)
        own = grad[pl.ds(8, rows), xs]
        out = jnp.zeros((rows, LANES), f32)
        for k in range(CONV):
            out = out + cw_ref[k : k + 1, xs] * grad[11 - k : 11 - k + rows, xs]
            dcw_ref[k : k + 1, xs] = jnp.sum(
                own * pad[5 + k : 5 + k + rows, xs], axis=0, keepdims=True
            )
        dcw_ref[4:5, xs] = jnp.sum(own, axis=0, keepdims=True)
        dx_ref[:, xs] = out
        return 0

    lax.fori_loop(0, XBC // LANES, conv, 0)

    @pl.when(jnp.logical_not(first))
    def _():
        edge.wait_recv()

    dx_ref[rows - 8 :, :] += from_ref[...]
    dp_ref[:, DI : DI + XBC] = dx_ref[...].astype(bf16)

    @pl.when(jnp.logical_not(final))
    def _():
        edge.wait_send()

    chain_end(-1, final, got, give, send, recv)


VTILE = 1280
NTILE = 256


def head_specs(width, tokens):
    return dict(
        table=pl.BlockSpec((VTILE, width), lambda i: (i, 0)),
        hidden=pl.BlockSpec((tokens, width), lambda i: (0, 0)),
        kept=pl.BlockSpec((VTILE, tokens), lambda i: (i, 0)),
        row=pl.BlockSpec((1, tokens), lambda i: (0, 0)),
        tile_row=pl.BlockSpec((1, 1, tokens), lambda i: (i, 0, 0)),
    )


def head_call(kernel, grid, in_specs, out_specs, outs, scratch, ins, cells):
    return pl.pallas_call(
        kernel,
        grid=(grid,),
        in_specs=in_specs,
        out_specs=out_specs,
        out_shape=[jax.ShapeDtypeStruct(shape, kind) for shape, kind in outs],
        scratch_shapes=list(scratch),
        compiler_params=pltpu.CompilerParams(
            dimension_semantics=("arbitrary",), vmem_limit_bytes=VMEM_LIMIT
        ),
        cost_estimate=pl.CostEstimate(
            flops=2 * cells * D, transcendentals=cells, bytes_accessed=4 * cells
        ),
    )(*ins)


UNROLL = 8


def head_stats_kernel(
    lead_ref, table_ref, own_ref, lab_ref, w_ref,
    q_ref, all_ref, lse_ref, fac_ref, hit_ref,
    lead_v, table_v, kept, tops, sums, hits, shown, load_sem, own_sem, put_sem, z_send, z_recv, m_send, m_recv, s_send, s_recv,
):
    dp = lax.axis_index("dp")
    me = lax.axis_index("fsdp")
    shards = lax.axis_size("fsdp")
    count = shards // MB
    core = me % MB
    k = me // MB
    mate = k * MB + 1 - core
    vocab_rows = lead_ref.shape[0] + table_ref.shape[0]
    rows = own_ref.shape[0]
    tiles = tops.shape[0]

    def load(t):
        if t == 0:
            return pltpu.make_async_copy(lead_ref, lead_v, load_sem.at[0])
        first = (t - 1) * VTILE
        at = pl.ds(first, min(VTILE, table_ref.shape[0] - first))
        return pltpu.make_async_copy(table_ref.at[at], table_v.at[at], load_sem.at[t])

    for t in range(tiles):
        load(t).start()
    barrier = pltpu.get_barrier_semaphore()
    for other in range(1, shards):
        pl.semaphore_signal(
            barrier, inc=1, device_id=(dp, lax.rem(me + other, shards)), device_id_type=MESH
        )
    pl.semaphore_wait(barrier, shards - 1)

    near = jnp.minimum(k, count - 1 - k)
    long_side = jnp.where(count - 1 - k > k, 1, -1)

    def chunk_at(i):
        paired = k + (2 * (i % 2) - 1) * ((i + 1) // 2)
        return jnp.where(i <= 2 * near, paired, k + long_side * (i - near))

    def along(z, side):
        at = all_ref.at[z * MB + core]
        return remote(
            at, at, z_send.at[side, z], z_recv.at[z], dp, me + MB if side == 0 else me - MB
        )

    def to_mate(z):
        at = all_ref.at[z * MB + core]
        return remote(at, at, m_send.at[z], m_recv.at[z], dp, mate)

    def from_mate(z):
        at = all_ref.at[z * MB + 1 - core]
        return remote(at, at, m_send.at[z], m_recv.at[z], dp, mate)

    keep = pltpu.make_async_copy(own_ref, all_ref.at[me], own_sem)
    keep.start()
    keep.wait()

    @pl.when(k < count - 1)
    def _():
        along(k, 0).start()

    @pl.when(k > 0)
    def _():
        along(k, 1).start()

    to_mate(k).start()
    whole = vocab_rows - vocab_rows % 16
    for slot in range(2):
        kept[slot, whole:, :] = jnp.zeros((kept.shape[1] - whole, rows), bf16)

    def put(step, b):
        return pltpu.make_async_copy(
            kept.at[step % 2],
            q_ref.at[:, pl.ds(pl.multiple_of(b * rows, rows), rows)],
            put_sem.at[step % 2],
        )

    def block(step, b):
        @pl.when(step >= 2)
        def _():
            put(step, b).wait()

        slot = step % 2
        ns = pl.ds(pl.multiple_of(b * rows, rows), rows)
        h = all_ref[b]
        label = lab_ref[0:1, ns]
        for t in range(tiles):
            first = t * VTILE
            size = min(VTILE, vocab_rows - first)

            @pl.when(step == 0)
            def _(t=t):
                load(t).wait()

            part = lead_v[...] if t == 0 else table_v[first - VTILE : first - VTILE + size, :]
            logits = dot_nt(part, h)
            top = jnp.max(logits, axis=0, keepdims=True)
            p = jnp.exp(logits - top)
            kept[slot, first : first + size, :] = p.astype(bf16)
            tops[t, 0:1, ns] = top
            sums[t, 0:1, ns] = jnp.sum(p, axis=0, keepdims=True)
            rid = lax.broadcasted_iota(jnp.int32, (size, rows), 0)
            hits[t, 0:1, ns] = jnp.sum(
                jnp.where(rid == label - first, logits, 0.0), axis=0, keepdims=True
            )
        put(step, b).start()

    def chunk(i, _):
        z = chunk_at(i)

        @pl.when(jnp.logical_and(i > 0, k >= i))
        def _():
            along(k - i, 0).wait_recv()

            @pl.when(k < count - 1)
            def _():
                along(k - i, 0).start()

            to_mate(k - i).start()

        @pl.when(jnp.logical_and(i > 0, k + i < count))
        def _():
            along(k + i, 1).wait_recv()

            @pl.when(k > 0)
            def _():
                along(k + i, 1).start()

            to_mate(k + i).start()

        block(2 * i, z * MB + core)
        from_mate(z).wait_recv()
        block(2 * i + 1, z * MB + 1 - core)
        return 0

    lax.fori_loop(0, count, chunk, 0)
    top = tops[0, 0:1, :]
    for t in range(1, tiles):
        top = jnp.maximum(top, tops[t, 0:1, :])
    total = jnp.zeros_like(top)
    hit = jnp.zeros_like(top)
    for t in range(tiles):
        total = total + sums[t, 0:1, :] * jnp.exp(tops[t, 0:1, :] - top)
        hit = hit + hits[t, 0:1, :]
    hit_ref[...] = hit
    shown[me, 0:1, :] = top
    shown[me, 1:2, :] = total

    def tell(other):
        at = shown.at[me]
        return remote(
            at, at, s_send.at[other], s_recv.at[me], dp, lax.rem(me + other, shards)
        )

    def told(other):
        at = shown.at[lax.rem(me + other, shards)]
        return remote(
            at, at, s_send.at[other], s_recv.at[lax.rem(me + other, shards)], dp, mate
        )

    for other in range(1, shards):
        tell(other).start()
    for other in range(1, shards):
        told(other).wait_recv()
    top = shown[0, 0:1, :]
    for f in range(1, shards):
        top = jnp.maximum(top, shown[f, 0:1, :])
    total = jnp.zeros_like(top)
    for f in range(shards):
        total = total + shown[f, 1:2, :] * jnp.exp(shown[f, 0:1, :] - top)
    lse = top + jnp.log(total)
    lse_ref[...] = lse
    scale = w_ref[...] * (1.0 + 2.0 * z_weight * lse)
    for t in range(tiles):
        fac_ref[t, 0:1, :] = scale * jnp.exp(tops[t, 0:1, :] - lse)
    for other in range(1, shards):
        tell(other).wait_send()
    for z in range(count):

        @pl.when(jnp.logical_and(k >= z, k < count - 1))
        def _(z=z):
            along(z, 0).wait_send()

        @pl.when(jnp.logical_and(k <= z, k > 0))
        def _(z=z):
            along(z, 1).wait_send()

        to_mate(z).wait_send()
    put(0, 0).wait()
    put(1, 0).wait()


def head_stats(lead, table, own, labels, weight):
    vocab_rows, width = lead.shape[0] + table.shape[0], table.shape[1]
    rows = own.shape[0]
    shards = lax.axis_size("fsdp")
    count = shards // MB
    tokens = shards * rows
    tiles = pl.cdiv(vocab_rows, VTILE)
    kept, everyone, lse, fac, hit = comm_call(
        head_stats_kernel,
        6,
        (lead, table, own, labels, weight),
        (
            ((tiles * VTILE, tokens), bf16),
            ((shards, rows, width), bf16),
            ((1, tokens), f32),
            ((tiles, 1, tokens), f32),
            ((1, tokens), f32),
        ),
        (
            pltpu.VMEM(lead.shape, bf16),
            pltpu.VMEM(table.shape, bf16),
            pltpu.VMEM((2, tiles * VTILE, rows), bf16),
            pltpu.VMEM((tiles, 1, tokens), f32),
            pltpu.VMEM((tiles, 1, tokens), f32),
            pltpu.VMEM((tiles, 1, tokens), f32),
            pltpu.VMEM((shards, 2, tokens), f32),
            pltpu.SemaphoreType.DMA((tiles,)),
            pltpu.SemaphoreType.DMA,
            pltpu.SemaphoreType.DMA((2,)),
            pltpu.SemaphoreType.DMA((2, count)),
            pltpu.SemaphoreType.DMA((count,)),
            pltpu.SemaphoreType.DMA((count,)),
            pltpu.SemaphoreType.DMA((count,)),
            pltpu.SemaphoreType.DMA((shards,)),
            pltpu.SemaphoreType.DMA((shards,)),
        ),
        (pl.ANY, pl.ANY) + (pltpu.VMEM,) * 3,
        (pl.ANY, pltpu.VMEM, pltpu.VMEM, pltpu.VMEM, pltpu.VMEM),
        own.size * 2 * 7,
    )
    return kept, everyone.reshape(tokens, width), lse, fac, hit


def logit_grads(q, fac, weight, rid, label):
    other = weight * (0.1 / VOCAB)
    return (q.astype(f32) * fac - jnp.where(rid == label, other + 0.9 * weight, other)).astype(bf16)


def head_rows_kernel(vocab_rows, lead_ref, e_ref, q_ref, fac_ref, w_ref, lab_ref, out_ref, acc, et):
    step = pl.program_id(0)
    first = step * VTILE
    tokens = q_ref.shape[1]

    @pl.when(step == 0)
    def _():
        acc[...] = jnp.zeros(acc.shape, f32)

    eid = lax.broadcasted_iota(jnp.int32, (VTILE, e_ref.shape[1]), 0)
    part = jnp.where(step == 0, lead_ref[...].astype(f32), e_ref[...].astype(f32))
    et[...] = jnp.where(eid < vocab_rows - first, part, 0.0).T.astype(bf16)

    def chunk(j, _):
        ns = pl.ds(pl.multiple_of(j * NTILE, NTILE), NTILE)
        rid = lax.broadcasted_iota(jnp.int32, (VTILE, NTILE), 0)
        dl = logit_grads(
            q_ref[:, ns], fac_ref[0, 0:1, ns], w_ref[0:1, ns], rid, lab_ref[0:1, ns] - first
        )
        acc[:, ns] += dot_nn(et[...], dl)
        return 0

    lax.fori_loop(0, tokens // NTILE, chunk, 0, unroll=UNROLL)

    @pl.when(step == pl.num_programs(0) - 1)
    def _():
        def put(j, _):
            ns = pl.ds(pl.multiple_of(j * NTILE, NTILE), NTILE)
            out_ref[ns, :] = acc[:, ns].T.astype(bf16)
            return 0

        lax.fori_loop(0, tokens // NTILE, put, 0)


ROW_PARTS = 2


def head_rows(lead, table, kept, fac, weight, labels, part):
    vocab_rows, width = lead.shape[0] + table.shape[0], table.shape[1] // ROW_PARTS
    tokens = kept.shape[1]
    sp = head_specs(width, tokens)
    return head_call(
        functools.partial(head_rows_kernel, vocab_rows),
        pl.cdiv(vocab_rows, VTILE),
        [
            pl.BlockSpec((VTILE, width), lambda i: (0, part)),
            pl.BlockSpec((VTILE, width), lambda i: (jnp.maximum(i - 1, 0), part)),
            sp["kept"],
            sp["tile_row"],
            sp["row"],
            sp["row"],
        ],
        [sp["hidden"]],
        [((tokens, width), bf16)],
        (pltpu.VMEM((width, tokens), f32), pltpu.VMEM((width, VTILE), bf16)),
        (lead, table, kept, fac, weight, labels),
        vocab_rows * tokens,
    )[0]


def head_table_kernel(h_ref, q_ref, fac_ref, w_ref, lab_ref, out_ref, dl_ref):
    first = pl.program_id(0) * VTILE
    tokens = q_ref.shape[1]

    def chunk(j, _):
        ns = pl.ds(pl.multiple_of(j * NTILE, NTILE), NTILE)
        rid = lax.broadcasted_iota(jnp.int32, (VTILE, NTILE), 0)
        dl_ref[:, ns] = logit_grads(
            q_ref[:, ns], fac_ref[0, 0:1, ns], w_ref[0:1, ns], rid, lab_ref[0:1, ns] - first
        )
        return 0

    lax.fori_loop(0, tokens // NTILE, chunk, 0, unroll=UNROLL)

    def cols(j, _):
        ds = pl.ds(pl.multiple_of(j * 256, 256), 256)
        out_ref[:, ds] = dot_nn(dl_ref[...], h_ref[:, ds]).astype(bf16)
        return 0

    lax.fori_loop(0, h_ref.shape[1] // 256, cols, 0, unroll=True)


def head_table(hidden, kept, fac, weight, labels, vocab_rows):
    tokens, width = hidden.shape
    sp = head_specs(width, tokens)
    return head_call(
        head_table_kernel,
        pl.cdiv(vocab_rows, VTILE),
        [sp["hidden"], sp["kept"], sp["tile_row"], sp["row"], sp["row"]],
        [sp["table"]],
        [((vocab_rows, width), bf16)],
        (pltpu.VMEM((VTILE, tokens), bf16),),
        (hidden, kept, fac, weight, labels),
        vocab_rows * tokens,
    )[0]


def weight_grads_kernel(u_ref, dp_ref, yn_ref, db_ref, in_ref, out_ref):
    wide_cols = dp_ref.shape[1]
    for c in range(0, wide_cols, 1024):
        cs = pl.ds(c, min(1024, wide_cols - c))
        in_ref[:, cs] = dot_tn(u_ref[...], dp_ref[:, cs]).astype(bf16)
    out_ref[...] = dot_tn(yn_ref[...], db_ref[...]).astype(bf16)


def weight_grads(normed, grad_proj, mixed, grad_branch):
    rows = normed.shape[0]
    steps = D // 256
    part = DI // steps
    return head_call(
        weight_grads_kernel,
        steps,
        [
            pl.BlockSpec((rows, 256), lambda i: (0, i)),
            pl.BlockSpec((rows, ZW), lambda i: (0, 0)),
            pl.BlockSpec((rows, part), lambda i: (0, i)),
            pl.BlockSpec((rows, D), lambda i: (0, 0)),
        ],
        [pl.BlockSpec((256, ZW), lambda i: (i, 0)), pl.BlockSpec((part, D), lambda i: (i, 0))],
        [((D, ZW), bf16), ((DI, D), bf16)],
        (),
        (normed, grad_proj, mixed, grad_branch),
        rows * (ZW + DI),
    )


def after(value, earlier):
    return lax.optimization_barrier((value, earlier))[0]


def norm_scale(values):
    return lax.rsqrt(jnp.mean(values * values, axis=-1, keepdims=True) + epsilon)


def norm_back(grad, values, gain):
    scale = norm_scale(values)
    unit = values * scale
    inner = grad * gain
    back = scale * (inner - unit * jnp.mean(inner * unit, axis=-1, keepdims=True))
    return back, jnp.sum(grad * unit, axis=0)


def all_vectors(vector_params):
    rows = vector_params[: LAYERS * PER].reshape(LAYERS, PER)
    at = (CONV + 1) * XBC
    heads = rows[:, at : at + 3 * HEADS].reshape(LAYERS, 3, HEADS)
    after_heads = at + 3 * HEADS
    return dict(
        conv=rows[:, :at].reshape(LAYERS, CONV + 1, XBC),
        heads=jnp.pad(heads, ((0, 0), (0, 5), (0, LANES - HEADS))),
        gate=rows[:, after_heads + D :].reshape(LAYERS, 1, DI),
        pre=rows[:, after_heads : after_heads + D],
    )


def layer_forward(hidden, w_in, w_out, vec, layer):
    rows = hidden.shape[0]
    normed = (hidden * norm_scale(hidden) * vec["pre"][layer]).astype(bf16)
    proj = jnp.dot(normed, w_in, preferred_element_type=f32)
    pre, y, mixed, dt, cum, entering, halo = comm_call(
        scan_kernel,
        1,
        (jnp.full((1,), layer, jnp.int32), proj, vec["conv"], vec["heads"], vec["gate"]),
        (
            ((rows, XBC), f32),
            ((rows, DI), f32),
            ((rows, DI), bf16),
            ((rows, LANES), f32),
            ((rows, LANES), f32),
            ((DI, NSTATE), bf16),
            ((8, XBC), f32),
        ),
        VECTOR_SCRATCH
        + (
            pltpu.VMEM((rows + 8, XBC), f32),
            pltpu.VMEM((HEADS, rows, LANES), f32),
            pltpu.VMEM((PAIRS, rows, LANES), f32),
            pltpu.VMEM((PAIRS, rows, LANES), f32),
            pltpu.VMEM((LANES, rows), f32),
            pltpu.VMEM((DI, NSTATE), f32),
            pltpu.VMEM((DI, NSTATE), bf16),
            pltpu.VMEM((rows, LANES), f32),
            pltpu.SemaphoreType.DMA,
            pltpu.SemaphoreType.DMA,
            pltpu.SemaphoreType.DMA((CHAIN_STEPS,)),
            pltpu.SemaphoreType.DMA((CHAIN_STEPS,)),
        ),
        (pltpu.SMEM,) + (pltpu.VMEM,) * 4,
        (pltpu.VMEM,) * 7,
        DI * NSTATE * 2,
    )
    branch = jnp.dot(mixed, w_out, preferred_element_type=f32)
    record = (hidden, normed, proj, halo, pre, dt, cum, entering, y, mixed)
    return hidden + branch, record


def layer_backward(grad_hidden, w_in, w_out, vec, layer, record):
    hidden, normed, proj, halo, pre, dt, cum, entering, y, mixed = record
    rows = hidden.shape[0]
    grad_branch = grad_hidden.astype(bf16)
    grad_mixed = dot_nt(grad_branch, w_out)
    grad_proj, dconv, dsmall, dgate = comm_call(
        back_kernel,
        2,
        (
            jnp.full((1,), layer, jnp.int32), grad_mixed, y, proj, halo, pre, dt, cum, entering,
            vec["conv"], vec["heads"], vec["gate"],
        ),
        (
            ((rows, ZW), bf16),
            ((8, XBC), f32),
            ((8, LANES), f32),
            ((1, DI), f32),
        ),
        VECTOR_SCRATCH
        + (
            pltpu.VMEM((rows + 8, XBC), f32),
            pltpu.VMEM((rows + 16, XBC), f32),
            pltpu.VMEM((HEADS, rows, LANES), f32),
            pltpu.VMEM((PAIRS, rows, LANES), f32),
            pltpu.VMEM((PAIRS, rows, LANES), f32),
            pltpu.VMEM((LANES, rows), f32),
            pltpu.VMEM((rows, rows), f32),
            pltpu.VMEM((rows, LANES), f32),
            pltpu.VMEM((rows, LANES), f32),
            pltpu.VMEM((rows, LANES), f32),
            pltpu.VMEM((rows, LANES), f32),
            pltpu.VMEM((16, LANES), f32),
            pltpu.VMEM((rows, DI), f32),
            pltpu.VMEM((rows, LANES), f32),
            pltpu.VMEM((DI, NSTATE), bf16),
            pltpu.VMEM((DI, NSTATE), bf16),
            pltpu.VMEM((DI, NSTATE), f32),
            pltpu.VMEM((rows, XBC), f32),
            pltpu.VMEM((8, XBC), f32),
            pltpu.VMEM((8, XBC), f32),
            pltpu.SemaphoreType.DMA,
            pltpu.SemaphoreType.DMA,
            pltpu.SemaphoreType.DMA((CHAIN_STEPS,)),
            pltpu.SemaphoreType.DMA((CHAIN_STEPS,)),
        ),
        (pltpu.SMEM,) + (pltpu.VMEM,) * 11,
        (pltpu.VMEM,) * 4,
        DI * NSTATE * 2,
    )
    grad_normed = dot_nt(grad_proj, w_in)
    grad_in, grad_out = weight_grads(normed, grad_proj, mixed, grad_branch)
    grad_prev, dpre_gain = norm_back(grad_normed, hidden, vec["pre"][layer])
    grad_vec = jnp.concatenate(
        [
            dconv[: CONV + 1].reshape(-1),
            dsmall[0, :HEADS],
            dsmall[1, :HEADS],
            dsmall[2, :HEADS],
            dpre_gain,
            dgate[0],
        ]
    )
    return grad_hidden + grad_prev, grad_in, grad_out, grad_vec


def whole_step(
    token_ids,
    target_ids,
    seq_lengths,
    embedding,
    embedding_mom,
    embedding_avg,
    in_proj,
    in_proj_mom,
    in_proj_avg,
    out_proj,
    out_proj_mom,
    out_proj_avg,
    vector_params,
    vector_mom,
    vector_avg,
):
    groups = lax.axis_size("dp")
    shards = lax.axis_size("fsdp")
    group_index = lax.axis_index("dp")
    shard_index = lax.axis_index("fsdp")
    chunks = shards // MB
    seq_rows = token_ids.shape[2]
    rows = seq_rows // chunks
    vocab_rows, own_cols = embedding.shape
    tokens = MB * seq_rows
    total_count = jnp.sum(seq_lengths).astype(f32)
    in_low = in_proj.astype(bf16)
    out_low = out_proj.astype(bf16)

    lead = lax.all_gather(embedding[:VTILE].astype(bf16), "dp", axis=1, tiled=True)
    ids_all = group_call(share_kernel, 7, token_ids[:, 0, :], ((groups, MB, seq_rows), jnp.int32))
    ids_all = ids_all.reshape(groups, MB, chunks, rows).transpose(2, 1, 0, 3).reshape(-1)
    every = ids_all.shape[0]
    local_ids = ids_all - shard_index * vocab_rows
    inside = (local_ids >= 0) & (local_ids < vocab_rows)
    sorted_ids, sorted_tok = lax.sort(
        (jnp.where(inside, local_ids, vocab_rows), jnp.arange(every, dtype=jnp.int32)),
        num_keys=1,
    )
    held_here = sorted_ids < vocab_rows
    count = jnp.sum(held_here.astype(jnp.int32)).reshape(1)
    row_list = jnp.where(held_here, sorted_ids, 0)
    tok_list = jnp.where(held_here, sorted_tok, every)
    looked, embed_low, own_sums = local_call(
        lookup_kernel,
        (count, row_list, tok_list, embedding),
        (((every, own_cols), bf16), ((vocab_rows - VTILE, own_cols), bf16), ((8, own_cols), f32)),
        scratch=(pltpu.VMEM((every + 8, own_cols), f32),),
        in_smem=(0, 1, 2),
    )
    mine = lax.psum_scatter(
        looked.reshape(shards * groups * rows, own_cols), "fsdp", scatter_dimension=0, tiled=True
    )
    hidden = group_call(
        to_rows_kernel,
        8,
        mine.reshape(groups, rows, own_cols),
        ((rows, D), f32),
        (pltpu.VMEM((groups, rows, own_cols), bf16),),
    )

    shards = []
    for l in range(LAYERS):
        shards += [in_low[l], out_low[l]]
    shards = after(shards, looked)
    gathered = gather_layers(shards)
    w_in, w_out = gathered[0::2], gathered[1::2]
    embed_low = after(embed_low, gathered)
    table = lax.all_gather(embed_low, "dp", axis=1, tiled=True)

    vecs = all_vectors(vector_params)
    final_gain = vector_params[LAYERS * PER :]
    records = []
    for l in range(LAYERS):
        hidden, record = layer_forward(hidden, w_in[l], w_out[l], vecs, l)
        records.append(record)

    final_low = (hidden * norm_scale(hidden) * final_gain).astype(bf16)

    def in_order(per_seq):
        return per_seq.reshape(MB, chunks, rows).transpose(1, 0, 2).reshape(1, tokens)

    labels = in_order(target_ids[:, 0, :])
    lengths = lax.dynamic_index_in_dim(seq_lengths, group_index, 1, keepdims=True)
    valid = in_order((jnp.arange(seq_rows)[None, :] < lengths).astype(f32))
    local_labels = labels - shard_index * vocab_rows
    weight = valid / total_count
    kept, group_hidden, lse, fac, target = head_stats(lead, table, final_low, local_labels, weight)
    own_mask = jnp.arange(tokens) // rows == shard_index
    per_row = jnp.where(own_mask, lse[0] + z_weight * lse[0] * lse[0], 0.0)
    loss_sum = jnp.sum((per_row - 0.9 * target[0]) * valid[0])
    own_valid = lax.dynamic_slice_in_dim(valid[0], shard_index * rows, rows)
    hidden_sum = jnp.sum(final_low.astype(f32) * own_valid[:, None], axis=0)
    column_sum = jnp.zeros((groups, own_cols), f32)
    column_sum = jnp.where(
        jnp.arange(groups)[:, None] == group_index, jnp.sum(own_sums, axis=0), column_sum
    ).reshape(D)

    own_grad = []
    ready = kept
    for part in range(ROW_PARTS):
        part_grad = head_rows(lead, table, ready, fac, weight, local_labels, part)
        ready = after(kept, part_grad)
        own_grad.append(
            lax.psum_scatter(part_grad, "fsdp", scatter_dimension=0, tiled=True)
        )
    own_grad = jnp.concatenate(own_grad, axis=1).astype(f32)
    table_grad = head_table(group_hidden, ready, fac, weight, local_labels, vocab_rows)
    table_part = lax.psum_scatter(table_grad, "dp", scatter_dimension=1, tiled=True)

    grad_hidden, dfinal = norm_back(after(own_grad, table_grad), hidden, final_gain)
    in_parts = [None] * LAYERS
    out_parts = [None] * LAYERS
    vec_parts = [None] * LAYERS
    for l in reversed(range(LAYERS)):
        grad_hidden, grad_in, grad_out, vec_parts[l] = layer_backward(
            grad_hidden, w_in[l], w_out[l], vecs, l, records[l]
        )
        in_parts[l], out_parts[l] = grad_in, grad_out
    whole = []
    for l in range(LAYERS):
        whole += [in_parts[l], out_parts[l]]
    sent = group_call(
        to_columns_kernel,
        9,
        after(grad_hidden, whole),
        ((groups, rows, own_cols), bf16),
        (pltpu.VMEM((groups, rows, own_cols), bf16),),
    )
    whole = after(whole, sent)
    spread = lax.all_gather(sent, "fsdp", axis=0).reshape(every, own_cols)
    summed_parts = reduce_layers(whole)
    spread = after(spread, summed_parts)
    table_total, table_squares = local_call(
        spread_kernel,
        (count, row_list, tok_list, spread, table_part),
        (((vocab_rows, own_cols), f32), ((8, own_cols), f32)),
        scratch=(pltpu.VMEM((every + 8, own_cols), f32),),
        in_smem=(0, 1, 2),
    )
    owner_squares = jnp.sum(table_squares)
    for part in summed_parts:
        owner_squares = owner_squares + jnp.sum(part * part)
    small = vector_params.shape[0]
    used = small + 2 * D + 2
    padded = pl.cdiv(used, 16 * LANES) * 16 * LANES
    packed = jnp.concatenate(
        vec_parts
        + [
            dfinal,
            hidden_sum,
            column_sum,
            owner_squares.reshape(1),
            loss_sum.reshape(1),
            jnp.zeros((padded - used,), f32),
        ]
    )
    packed, norms = total_of(packed.reshape(-1, LANES), small, used - 2)
    factor = norms[1, 0]
    table_new, table_mom, table_avg = stepped(
        embedding, embedding_mom, embedding_avg, table_total, factor
    )
    updated = [table_new, table_mom, table_avg, table_new.astype(bf16)]
    updated += update_projections(
        norms,
        (in_proj, in_proj_mom, in_proj_avg, out_proj, out_proj_mom, out_proj_avg),
        summed_parts,
    )
    packed = packed.reshape(-1)
    vector_total = packed[:small]
    hidden_total = packed[small : small + D]
    column_total = packed[small + D : small + 2 * D]
    mean_part = jnp.sum(hidden_total * column_total) * (0.1 / VOCAB)
    loss_value = (packed[used - 1] - mean_part) / total_count
    vector_new, vector_mom_new, vector_avg_new = stepped(
        vector_params, vector_mom, vector_avg, vector_total, factor
    )
    return (
        loss_value,
        norms[0, 0],
        *updated,
        vector_new,
        vector_mom_new,
        vector_avg_new,
        vector_new.astype(bf16),
    )


def solution(mesh):
    table_spec = P("fsdp", "dp")
    weight_spec = P(None, ("dp", "fsdp"), None)
    return jax.shard_map(
        whole_step,
        mesh=mesh,
        in_specs=(
            P(None, "dp", None),
            P(None, "dp", None),
            P(),
            *(table_spec,) * 3,
            *(weight_spec,) * 6,
            *(P(),) * 3,
        ),
        out_specs=(
            P(),
            P(),
            *(table_spec,) * 4,
            *(weight_spec,) * 8,
            *(P(),) * 4,
        ),
        check_vma=False,
    )
```

```python
import functools

import jax
import jax.numpy as jnp
from jax import lax
from jax.experimental import pallas as pl
from jax.experimental.pallas import tpu as pltpu
from jax.sharding import PartitionSpec as P


D = 1024
HEADS = 32
HDIM = 64
NSTATE = 128
CONV = 4
VOCAB = 50288
LAYERS = 2
MB = 2
DI = 2048
XBC = 2304
ZW = 4384
PER = 14688
LANES = 128
PAIRS = DI // LANES

epsilon = 1e-05
z_weight = 0.001
clip_limit = 0.2
step_rate = 1000.0
highest = lax.Precision.HIGHEST
bf16 = jnp.bfloat16
f32 = jnp.float32
VMEM_LIMIT = 62 * 1024 * 1024
OFF = -1e30


def dot_nn(a, b, precision=None):
    return lax.dot_general(
        a, b, (((1,), (0,)), ((), ())), precision=precision, preferred_element_type=f32
    )


def dot_nt(a, b, precision=None):
    return lax.dot_general(
        a, b, (((1,), (1,)), ((), ())), precision=precision, preferred_element_type=f32
    )


def dot_tn(a, b, precision=None):
    return lax.dot_general(
        a, b, (((0,), (0,)), ((), ())), precision=precision, preferred_element_type=f32
    )


def silu(v):
    return v * lax.logistic(v)


def silu_grad(v):
    s = lax.logistic(v)
    return s * (1.0 + v * (1.0 - s))


def local_call(kernel, ins, outs, scratch=(), in_smem=(), flops=0):
    total = sum(a.size * a.dtype.itemsize for a in ins)
    return pl.pallas_call(
        kernel,
        out_shape=[jax.ShapeDtypeStruct(shape, kind) for shape, kind in outs],
        in_specs=[
            pl.BlockSpec(memory_space=pltpu.SMEM if i in in_smem else pltpu.VMEM)
            for i in range(len(ins))
        ],
        out_specs=[pl.BlockSpec(memory_space=pltpu.VMEM) for _ in outs],
        scratch_shapes=list(scratch),
        compiler_params=pltpu.CompilerParams(vmem_limit_bytes=VMEM_LIMIT),
        cost_estimate=pl.CostEstimate(
            flops=flops or total, transcendentals=0, bytes_accessed=2 * total
        ),
    )(*ins)


def lookup_kernel(count_ref, row_ref, tok_ref, table_ref, out_ref, low_ref, sum_ref, held):
    tokens = out_ref.shape[0]
    step = 512

    def clear(i, _):
        held[pl.ds(pl.multiple_of(i * step, step), step), :] = jnp.zeros(
            (step, held.shape[1]), f32
        )
        return 0

    lax.fori_loop(0, tokens // step, clear, 0)

    def move(i, _):
        for k in range(8):
            row = row_ref[i * 8 + k]
            tok = tok_ref[i * 8 + k]
            held[pl.ds(tok, 1), :] = table_ref[pl.ds(row, 1), :]
        return 0

    lax.fori_loop(0, (count_ref[0] + 7) // 8, move, 0)

    def put(i, _):
        rows = pl.ds(pl.multiple_of(i * step, step), step)
        out_ref[rows, :] = held[rows, :].astype(bf16)
        return 0

    lax.fori_loop(0, tokens // step, put, 0)
    rows_all = table_ref.shape[0]
    part = VTILE // 5
    whole = rows_all // part

    def low_rows(i):
        return table_ref[pl.ds(pl.multiple_of(i * part, part), part), :].astype(bf16)

    def add(low, total):
        return total + jnp.sum(low.astype(f32).reshape(part // 8, 8, -1), axis=0)

    def cast(i, total):
        low = low_rows(i)
        low_ref[pl.ds(pl.multiple_of(i * part - VTILE, part), part), :] = low
        return add(low, total)

    total = lax.fori_loop(
        0, VTILE // part, lambda i, t: add(low_rows(i), t), jnp.zeros(sum_ref.shape, f32)
    )
    sum_ref[...] = lax.fori_loop(VTILE // part, whole, cast, total)
    if rows_all > whole * part:
        low = table_ref[whole * part :, :].astype(bf16)
        low_ref[whole * part - VTILE :, :] = low
        sum_ref[0:1, :] += jnp.sum(low.astype(f32), axis=0, keepdims=True)


def spread_kernel(count_ref, row_ref, tok_ref, grad_ref, base_ref, out_ref, square_ref, held):
    tokens = grad_ref.shape[0]
    step = 512
    rows_all = out_ref.shape[0]

    def take(i, _):
        rows = pl.ds(pl.multiple_of(i * step, step), step)
        held[rows, :] = grad_ref[rows, :].astype(f32)
        return 0

    lax.fori_loop(0, tokens // step, take, 0)
    held[pl.ds(tokens, 8), :] = jnp.zeros((8, held.shape[1]), f32)

    whole = rows_all // step

    def start(i, _):
        rows = pl.ds(pl.multiple_of(i * step, step), step)
        out_ref[rows, :] = base_ref[rows, :].astype(f32)
        return 0

    lax.fori_loop(0, whole, start, 0)
    if rows_all > whole * step:
        out_ref[whole * step :, :] = base_ref[whole * step :, :].astype(f32)

    def move(i, _):
        for k in range(8):
            row = row_ref[i * 8 + k]
            tok = tok_ref[i * 8 + k]
            out_ref[pl.ds(row, 1), :] = out_ref[pl.ds(row, 1), :] + held[pl.ds(tok, 1), :]
        return 0

    lax.fori_loop(0, (count_ref[0] + 7) // 8, move, 0)

    def square(i, total):
        part = out_ref[pl.ds(pl.multiple_of(i * step, step), step), :]
        return total + jnp.sum((part * part).reshape(step // 8, 8, -1), axis=0)

    total = lax.fori_loop(0, whole, square, jnp.zeros(square_ref.shape, f32))
    square_ref[...] = total
    if rows_all > whole * step:
        part = out_ref[whole * step :, :]
        square_ref[0:1, :] += jnp.sum(part * part, axis=0, keepdims=True)


MESH = pl.DeviceIdType.MESH


def remote(src, dst, send, recv, dp, fsdp):
    return pltpu.make_async_remote_copy(
        src_ref=src,
        dst_ref=dst,
        send_sem=send,
        recv_sem=recv,
        device_id=(dp, fsdp),
        device_id_type=MESH,
    )


def comm_call(kernel, number, ins, outs, scratch, in_spaces, out_spaces, sent):
    return pl.pallas_call(
        kernel,
        out_shape=[jax.ShapeDtypeStruct(shape, kind) for shape, kind in outs],
        in_specs=[pl.BlockSpec(memory_space=space) for space in in_spaces],
        out_specs=[pl.BlockSpec(memory_space=space) for space in out_spaces],
        scratch_shapes=list(scratch),
        compiler_params=pltpu.CompilerParams(
            collective_id=number, has_side_effects=True, vmem_limit_bytes=VMEM_LIMIT
        ),
        cost_estimate=pl.CostEstimate(flops=sent, transcendentals=0, bytes_accessed=2 * sent),
    )(*ins)


def greet_groups():
    dp = lax.axis_index("dp")
    me = lax.axis_index("fsdp")
    groups = lax.axis_size("dp")
    barrier = pltpu.get_barrier_semaphore()
    others = [lax.rem(dp + other, groups) for other in range(1, groups)]
    for other in others:
        pl.semaphore_signal(barrier, inc=1, device_id=(other, me), device_id_type=MESH)
    pl.semaphore_wait(barrier, groups - 1)
    return dp, me, others


def share_kernel(in_ref, out_ref, send, recv):
    dp, me, others = greet_groups()
    for other in others:
        remote(in_ref, out_ref.at[dp], send.at[other], recv.at[dp], other, me).start()
    out_ref[dp] = in_ref[...]
    for other in others:
        copy = remote(in_ref, out_ref.at[other], send.at[other], recv.at[other], other, me)
        copy.wait_recv()
        copy.wait_send()


def to_rows_kernel(in_ref, out_ref, landed, send, recv):
    dp, me, others = greet_groups()
    for other in others:
        remote(in_ref.at[other], landed.at[dp], send.at[other], recv.at[dp], other, me).start()
    landed[dp] = in_ref[dp]
    for other in others:
        remote(in_ref.at[other], landed.at[other], send.at[other], recv.at[other], other, me).wait_recv()
    cols = in_ref.shape[2]
    for g in range(in_ref.shape[0]):
        out_ref[:, g * cols : (g + 1) * cols] = landed[g].astype(f32)
    for other in others:
        remote(in_ref.at[other], landed.at[other], send.at[other], recv.at[other], other, me).wait_send()


def to_columns_kernel(in_ref, out_ref, parts, send, recv):
    dp, me, others = greet_groups()
    cols = out_ref.shape[2]
    for g in range(out_ref.shape[0]):
        parts[g] = in_ref[:, g * cols : (g + 1) * cols].astype(bf16)
    for other in others:
        remote(parts.at[other], out_ref.at[dp], send.at[other], recv.at[dp], other, me).start()
    out_ref[dp] = parts[dp]
    for other in others:
        copy = remote(parts.at[other], out_ref.at[other], send.at[other], recv.at[other], other, me)
        copy.wait_recv()
        copy.wait_send()


def group_call(kernel, number, array, out, scratch=()):
    groups = lax.axis_size("dp")
    return comm_call(
        kernel,
        number,
        (array,),
        (out,),
        tuple(scratch)
        + (pltpu.SemaphoreType.DMA((groups,)), pltpu.SemaphoreType.DMA((groups,))),
        (pltpu.VMEM,),
        (pltpu.VMEM,),
        array.size * 2,
    )[0]


CHAIN_STEPS = 8
PART = DI // CHAIN_STEPS


def chunk_place(direction):
    place = lax.axis_index("fsdp") // MB
    count = lax.axis_size("fsdp") // MB
    first = place == (0 if direction > 0 else count - 1)
    final = place == (count - 1 if direction > 0 else 0)
    return first, final


def chain_barrier(direction, first, final):
    dp = lax.axis_index("dp")
    me = lax.axis_index("fsdp")
    barrier = pltpu.get_barrier_semaphore()

    @pl.when(jnp.logical_not(first))
    def _():
        pl.semaphore_signal(
            barrier, inc=1, device_id=(dp, me - MB * direction), device_id_type=MESH
        )

    @pl.when(jnp.logical_not(final))
    def _():
        pl.semaphore_wait(barrier, 1)


def to_next(src, dst, send, recv, direction):
    dp = lax.axis_index("dp")
    return remote(src, dst, send, recv, dp, lax.axis_index("fsdp") + MB * direction)


def chain_step(g, direction, first, final, got, give, local, col, rows, send, recv):
    def copy():
        at = pl.ds(pl.multiple_of(g * PART, PART), PART)
        return to_next(give.at[at], got.at[at], send.at[g], recv.at[g], direction)

    @pl.when(jnp.logical_not(first))
    def _():
        copy().wait_recv()

    @pl.when(jnp.logical_not(final))
    def _():
        for i in range(PART // HDIM):
            h = pl.ds(pl.multiple_of(g * PART + i * HDIM, HDIM), HDIM)
            decay = jnp.exp(col[g * (PART // HDIM) + i, rows - 1 : rows, :])
            give[h, :] = (decay * got[h, :].astype(f32) + local[h, :]).astype(bf16)
        copy().start()


def chain_end(direction, final, got, give, send, recv):
    @pl.when(jnp.logical_not(final))
    def _():
        for g in range(CHAIN_STEPS):
            at = pl.ds(g * PART, PART)
            to_next(give.at[at], got.at[at], send.at[g], recv.at[g], direction).wait_send()


def bits_of(size):
    return [1 << b for b in range(size.bit_length() - 1)]


def stepped(weight, moment, average, grad, factor):
    scaled = grad * factor
    moment_new = 0.5 * moment + scaled
    weight_new = weight - step_rate * (scaled + 0.5 * moment_new)
    return weight_new, moment_new, 0.5 * average + 0.5 * weight_new


def total_kernel(small, squares_at, packed_ref, total_ref, norm_ref, work, got, send, recv):
    dp = lax.axis_index("dp")
    me = lax.axis_index("fsdp")
    half = packed_ref.shape[0] // 2
    core = me % MB
    partners = [("f", b) for b in bits_of(lax.axis_size("fsdp")) if b > 1]
    partners += [("d", b) for b in bits_of(lax.axis_size("dp"))]

    def across(kind, bit):
        ids, other = (me, lambda v: (dp, v)) if kind == "f" else (dp, lambda v: (v, me))
        return other(jnp.where((ids // bit) % 2 == 1, ids - bit, ids + bit))

    mate = across("f", 1)
    barrier = pltpu.get_barrier_semaphore()
    for target in [mate] + [across(*p) for p in partners]:
        pl.semaphore_signal(barrier, inc=1, device_id=target, device_id_type=MESH)
    pl.semaphore_wait(barrier, 1 + len(partners))

    mine = pl.ds(pl.multiple_of(core * half, 8), half)
    theirs = pl.ds(pl.multiple_of((1 - core) * half, 8), half)
    copy = remote(packed_ref.at[theirs], got.at[0], send.at[0], recv.at[0], *mate)
    copy.start()
    copy.wait()
    work[0] = packed_ref[mine, :] + got[0]
    for i, p in enumerate(partners):
        copy = remote(work.at[i], got.at[i + 1], send.at[i + 1], recv.at[i + 1], *across(*p))
        copy.start()
        copy.wait()
        work[i + 1] = work[i] + got[i + 1]
    n = len(partners)
    copy = remote(work.at[n], got.at[n + 1], send.at[n + 1], recv.at[n + 1], *mate)
    copy.start()
    copy.wait()
    total_ref[mine, :] = work[n]
    total_ref[theirs, :] = got[n + 1]

    total = total_ref[...]
    index = lax.broadcasted_iota(jnp.int32, total.shape, 0) * LANES
    index = index + lax.broadcasted_iota(jnp.int32, total.shape, 1)
    parts = jnp.where(index < small, total * total, jnp.where(index == squares_at, total, 0.0))
    square = jnp.sum(jnp.sum(parts, axis=0, keepdims=True), axis=1, keepdims=True)
    norm = jnp.sqrt(square)
    factor = jnp.minimum(1.0, clip_limit / norm)
    norm_ref[0:1, :] = jnp.broadcast_to(norm, (1, LANES))
    norm_ref[1:2, :] = jnp.broadcast_to(factor, (1, LANES))
    norm_ref[2:8, :] = jnp.zeros((6, LANES), f32)


def total_of(packed, small, squares_at):
    steps = len(bits_of(lax.axis_size("fsdp"))) - 1 + len(bits_of(lax.axis_size("dp")))
    rows = packed.shape[0]
    return comm_call(
        functools.partial(total_kernel, small, squares_at),
        3,
        (packed,),
        ((packed.shape, f32), ((8, LANES), f32)),
        (
            pltpu.VMEM((steps + 1, rows // 2, LANES), f32),
            pltpu.VMEM((steps + 2, rows // 2, LANES), f32),
            pltpu.SemaphoreType.DMA((steps + 2,)),
            pltpu.SemaphoreType.DMA((steps + 2,)),
        ),
        (pltpu.VMEM,),
        (pltpu.VMEM, pltpu.VMEM),
        packed.size * 4 * 3,
    )


def snake(place, size):
    return jnp.where(place < size // 2, place, size // 2 + size - 1 - place)


def wrap(value, size):
    return lax.rem(value + size, size)


def gather_kernel(*refs):
    arrays = 2 * LAYERS
    own = refs[:arrays]
    full = refs[arrays : 2 * arrays]
    local_sem, z_send, z_recv, ring_send, ring_recv, mate_send, mate_recv = refs[2 * arrays :]
    dp = lax.axis_index("dp")
    me = lax.axis_index("fsdp")
    size = lax.axis_size("dp")
    count = lax.axis_size("fsdp") // MB
    core = me % MB
    k = me // MB
    ring = snake(dp, size)
    reach = size // 2
    right = snake(wrap(ring + 1, size), size)
    left = snake(wrap(ring - 1, size), size)
    mate = k * MB + 1 - core
    up, down = me + MB, me - MB
    has_up, has_down = k < count - 1, k > 0
    barrier = pltpu.get_barrier_semaphore()
    for target in ((right, me), (left, me), (dp, mate)):
        pl.semaphore_signal(barrier, inc=1, device_id=target, device_id_type=MESH)

    @pl.when(has_up)
    def _():
        pl.semaphore_signal(barrier, inc=1, device_id=(dp, up), device_id_type=MESH)

    @pl.when(has_down)
    def _():
        pl.semaphore_signal(barrier, inc=1, device_id=(dp, down), device_id_type=MESH)

    pl.semaphore_wait(barrier, 3 + jnp.where(has_up, 1, 0) + jnp.where(has_down, 1, 0))

    def spot(a, d, z, c):
        return full[a].at[d, z, c]

    def chain(a, src, z, side):
        return remote(
            src, spot(a, dp, z, core), z_send.at[a, z], z_recv.at[a, z], dp, up if side == 0 else down
        )

    def chain_own(a, side):
        return remote(
            own[a],
            spot(a, dp, k, core),
            z_send.at[a, count + side],
            z_recv.at[a, k],
            dp,
            up if side == 0 else down,
        )

    def round_ring(a, src, d, z, side):
        return remote(
            src,
            spot(a, d, z, core),
            ring_send.at[a, side],
            ring_recv.at[a, d, z],
            right if side == 0 else left,
            me,
        )

    def to_mate(a, src, d, z):
        return remote(src, spot(a, d, z, core), mate_send.at[a], mate_recv.at[a], dp, mate)

    def carried(a, side):
        return (a < arrays // 2) == (side == 0)

    for a in range(arrays):

        @pl.when(has_up)
        def _(a=a):
            chain_own(a, 0).start()

        @pl.when(has_down)
        def _(a=a):
            chain_own(a, 1).start()

    for a in range(arrays):
        for side in (0, 1):
            round_ring(a, own[a], dp, k, side).start()
    for a in range(arrays):
        to_mate(a, own[a], dp, k).start()
        pltpu.make_async_copy(own[a], spot(a, dp, k, core), local_sem.at[a]).start()

    def ring_step(z, s):
        for side in (0, 1):
            origin = snake(wrap(ring - s if side == 0 else ring + s, size), size)
            for a in range(arrays):
                if s == reach and not carried(a, side):
                    continue
                piece = spot(a, origin, z, core)
                round_ring(a, piece, origin, z, side).wait_recv()
                if s + 1 < reach or (s + 1 == reach and carried(a, side)):
                    round_ring(a, piece, origin, z, side).start()
                to_mate(a, piece, origin, z).start()

    def arrive(z, side):
        for a in range(arrays):
            piece = spot(a, dp, z, core)
            chain(a, piece, z, side).wait_recv()

            @pl.when(has_up if side == 0 else has_down)
            def _(a=a, piece=piece):
                chain(a, piece, z, side).start()

            for way in (0, 1):
                round_ring(a, piece, dp, z, way).start()
            to_mate(a, piece, dp, z).start()

    def both_ways(far, act):
        if far == 0:
            act(k, 0)
            return

        @pl.when(k >= far)
        def _():
            act(k - far, 0)

        @pl.when(k + far < count)
        def _():
            act(k + far, 1)

    for turn in range(1, count + reach):
        if turn < count:
            both_ways(turn, arrive)
        for s in range(1, reach + 1):
            if 0 <= turn - s < count:
                both_ways(turn - s, lambda z, side, s=s: ring_step(z, s))

    for a in range(arrays):
        pltpu.make_async_copy(own[a], spot(a, dp, k, core), local_sem.at[a]).wait()
        for side in (0, 1):
            sent = full[a].at[pl.ds(0, reach if carried(a, side) else reach - 1), :, core]
            remote(sent, sent, ring_send.at[a, side], ring_recv.at[a, 0, 0], dp, mate).wait_send()
        whole = full[a].at[:, :, core]
        remote(whole, whole, mate_send.at[a], mate_recv.at[a], dp, mate).wait_send()
        whole = full[a].at[:, :, 1 - core]
        remote(whole, whole, mate_send.at[a], mate_recv.at[a], dp, mate).wait_recv()

        @pl.when(has_up)
        def _(a=a):
            chain_own(a, 0).wait_send()

        @pl.when(has_down)
        def _(a=a):
            chain_own(a, 1).wait_send()

        for far in range(1, count):

            @pl.when(jnp.logical_and(k >= far, has_up))
            def _(a=a, far=far):
                chain(a, spot(a, dp, k - far, core), k - far, 0).wait_send()

            @pl.when(jnp.logical_and(k + far < count, has_down))
            def _(a=a, far=far):
                chain(a, spot(a, dp, k + far, core), k + far, 1).wait_send()


def gather_layers(shards):
    size, count = lax.axis_size("dp"), lax.axis_size("fsdp") // MB
    arrays = len(shards)
    outs = comm_call(
        gather_kernel,
        4,
        shards,
        tuple(((size, count, MB) + s.shape, bf16) for s in shards),
        (
            pltpu.SemaphoreType.DMA((arrays,)),
            pltpu.SemaphoreType.DMA((arrays, count + 2)),
            pltpu.SemaphoreType.DMA((arrays, count)),
            pltpu.SemaphoreType.DMA((arrays, 2)),
            pltpu.SemaphoreType.DMA((arrays, size, count)),
            pltpu.SemaphoreType.DMA((arrays,)),
            pltpu.SemaphoreType.DMA((arrays,)),
        ),
        (pltpu.VMEM,) * arrays,
        (pl.ANY,) * arrays,
        sum(s.size * 2 for s in shards) * 24,
    )
    return [o.reshape(size * count * MB * s.shape[0], s.shape[1]) for o, s in zip(outs, shards)]


def add_rows(dst, first, *others):
    rows = dst.shape[0]
    step = min(rows, 16)

    def one(i, _):
        at = pl.ds(pl.multiple_of(i * step, step), step)
        total = first[at, :].astype(f32)
        for other in others:
            total = total + other[at, :].astype(f32)
        dst[at, :] = total.astype(dst.dtype)
        return 0

    lax.fori_loop(0, rows // step, one, 0)


def reduce_kernel(*refs):
    arrays = 2 * LAYERS
    grads = refs[:arrays]
    outs = refs[arrays : 2 * arrays]
    held, given, come, chained = (
        refs[(2 + i) * arrays : (3 + i) * arrays] for i in range(4)
    )
    load_sem, mate_send, mate_recv, ring_send, ring_recv, z_send, z_recv = refs[6 * arrays :]
    dp = lax.axis_index("dp")
    me = lax.axis_index("fsdp")
    size = lax.axis_size("dp")
    count = lax.axis_size("fsdp") // MB
    core = me % MB
    k = me // MB
    ring = snake(dp, size)
    reach = size // 2
    right = snake(wrap(ring + 1, size), size)
    left = snake(wrap(ring - 1, size), size)
    mate = k * MB + 1 - core
    up, down = me + MB, me - MB
    has_up, has_down = k < count - 1, k > 0

    def load(a):
        return pltpu.make_async_copy(grads[a].at[:, :, core], held[a], load_sem.at[a])

    for a in range(arrays):
        load(a).start()
    barrier = pltpu.get_barrier_semaphore()
    for target in ((right, me), (left, me), (dp, mate)):
        pl.semaphore_signal(barrier, inc=1, device_id=target, device_id_type=MESH)

    @pl.when(has_up)
    def _():
        pl.semaphore_signal(barrier, inc=1, device_id=(dp, up), device_id_type=MESH)

    @pl.when(has_down)
    def _():
        pl.semaphore_signal(barrier, inc=1, device_id=(dp, down), device_id_type=MESH)

    pl.semaphore_wait(barrier, 3 + jnp.where(has_up, 1, 0) + jnp.where(has_down, 1, 0))

    def away(j, side):
        return snake(wrap(ring + j if side == 0 else ring - j, size), size)

    def to_mate(a, d):
        return remote(
            grads[a].at[d, :, 1 - core], given[a].at[d], mate_send.at[a], mate_recv.at[a, d], dp, mate
        )

    def carried(a, side):
        return (a < arrays // 2) == (side == 0)

    def targets(j):
        if j == 0:
            return [dp]
        if j == reach:
            return [away(j, 0)]
        return [away(j, 0), away(j, 1)]

    for j in range(reach, -1, -1):
        for d in targets(j):
            for a in range(arrays):
                to_mate(a, d).start()

    for a in range(arrays):
        load(a).wait()

    def add_mate(d):
        for a in range(arrays):
            to_mate(a, d).wait_recv()

            def one(z, _, a=a):
                add_rows(held[a].at[d, z], held[a].at[d, z], given[a].at[d, z])
                return 0

            lax.fori_loop(0, count, one, 0)

    def first_step(a, side):
        d = away(reach, 0)
        return remote(
            held[a].at[d], come[a].at[side, 0], ring_send.at[a, side], ring_recv.at[a, side, 0, 0],
            right if side == 0 else left, me,
        )

    def next_step(a, side, s, z):
        d = away(reach - s, side)
        return remote(
            held[a].at[d, z], come[a].at[side, s, z], ring_send.at[a, side],
            ring_recv.at[a, side, s, z], right if side == 0 else left, me,
        )

    far_most = jnp.maximum(k, count - 1 - k)
    near_most = jnp.minimum(k, count - 1 - k)
    uneven = far_most - near_most
    long_side = jnp.where(count - 1 - k > k, 1, -1)

    def chunk_at(i):
        j = jnp.maximum(i - uneven, 0)
        paired = k + (1 - 2 * (j % 2)) * (near_most - j // 2)
        return jnp.where(i < uneven, k + long_side * (far_most - i), paired)

    add_mate(away(reach, 0))
    for a in range(arrays):
        first_step(a, 0 if carried(a, 0) else 1).start()
    for s in range(1, reach):
        for side in (0, 1):
            add_mate(away(reach - s, side))
        if s == 1:
            for a in range(arrays):
                first_step(a, 0 if carried(a, 0) else 1).wait_recv()

        def pass_on(i, _, s=s):
            z = chunk_at(i)
            for side in (0, 1):
                d = away(reach - s, side)
                for a in range(arrays):
                    if s > 1:
                        next_step(a, side, s - 1, z).wait_recv()
                    if s > 1 or carried(a, side):
                        add_rows(held[a].at[d, z], held[a].at[d, z], come[a].at[side, s - 1, z])
                    next_step(a, side, s, z).start()
            return 0

        lax.fori_loop(0, count, pass_on, 0)
    add_mate(dp)

    def along(a, side, z):
        return remote(
            held[a].at[dp, z], chained[a].at[side, z], z_send.at[a, z], z_recv.at[a, side, z],
            dp, up if side == 0 else down,
        )

    def finish(i, _):
        z = chunk_at(i)
        for a in range(arrays):
            for side in (0, 1):
                next_step(a, side, reach - 1, z).wait_recv()
            add_rows(
                held[a].at[dp, z],
                held[a].at[dp, z],
                come[a].at[0, reach - 1, z],
                come[a].at[1, reach - 1, z],
            )
            for side in (0, 1):
                beyond = z > k if side == 0 else z < k
                fed = has_down if side == 0 else has_up

                @pl.when(jnp.logical_and(fed, jnp.logical_or(beyond, z == k)))
                def _(a=a, side=side):
                    along(a, side, z).wait_recv()
                    add_rows(held[a].at[dp, z], held[a].at[dp, z], chained[a].at[side, z])

                @pl.when(beyond)
                def _(a=a, side=side):
                    along(a, side, z).start()

        return 0

    lax.fori_loop(0, count, finish, 0)
    for a in range(arrays):
        add_rows(outs[a], held[a].at[dp, k])
        for side in (0, 1):
            sent = held[a].at[pl.ds(0, reach if carried(a, side) else reach - 1)]
            remote(
                sent, sent, ring_send.at[a, side], ring_recv.at[a, side, 0, 0], dp, mate
            ).wait_send()
        remote(
            given[a], given[a], mate_send.at[a], mate_recv.at[a, 0], dp, mate
        ).wait_send()

    def sent_along(z, _):
        for a in range(arrays):

            @pl.when(z != k)
            def _(a=a):
                along(a, 0, z).wait_send()

        return 0

    lax.fori_loop(0, count, sent_along, 0)


def reduce_layers(grads):
    size, count = lax.axis_size("dp"), lax.axis_size("fsdp") // MB
    arrays = len(grads)
    reach = size // 2
    shards = [(g.shape[0] // (size * count * MB), g.shape[1]) for g in grads]
    blocks = [g.reshape((size, count, MB) + s) for g, s in zip(grads, shards)]
    return comm_call(
        reduce_kernel,
        5,
        blocks,
        tuple((s, f32) for s in shards),
        tuple(pltpu.VMEM((size, count) + s, bf16) for s in shards) * 2
        + tuple(pltpu.VMEM((2, reach, count) + s, bf16) for s in shards)
        + tuple(pltpu.VMEM((2, count) + s, bf16) for s in shards)
        + (
            pltpu.SemaphoreType.DMA((arrays,)),
            pltpu.SemaphoreType.DMA((arrays,)),
            pltpu.SemaphoreType.DMA((arrays, size)),
            pltpu.SemaphoreType.DMA((arrays, 2)),
            pltpu.SemaphoreType.DMA((arrays, 2, reach, count)),
            pltpu.SemaphoreType.DMA((arrays, count)),
            pltpu.SemaphoreType.DMA((arrays, 2, count)),
        ),
        (pl.ANY,) * arrays,
        (pltpu.VMEM,) * arrays,
        sum(g.size * 2 for g in grads),
    )


def pair_lanes(p):
    return pl.ds(pl.multiple_of(p * LANES, LANES), LANES)


def first_half(rows):
    return lax.broadcasted_iota(jnp.int32, (rows, LANES), 1) < HDIM


def spread_columns(values, column, per_pair, rows):
    half = first_half(rows)
    for p in range(PAIRS):
        left = jnp.broadcast_to(values[:, 2 * p : 2 * p + 1], (rows, LANES))
        right = jnp.broadcast_to(values[:, 2 * p + 1 : 2 * p + 2], (rows, LANES))
        if column is not None:
            column[2 * p] = left
            column[2 * p + 1] = right
        if per_pair is not None:
            per_pair[p] = jnp.where(half, left, right)


def take_vectors(layer_ref, conv_ref, head_ref, gate_ref, cw_ref, dtb_ref, al_ref, sk_ref, gg_ref):
    layer = layer_ref[0]
    cw_ref[0 : CONV + 1, :] = conv_ref[layer]
    heads = head_ref[layer]
    dtb_ref[...] = heads[0:1, :]
    al_ref[...] = heads[1:2, :]
    half = first_half(1)
    for p in range(PAIRS):
        left = jnp.broadcast_to(heads[2:3, 2 * p : 2 * p + 1], (1, LANES))
        right = jnp.broadcast_to(heads[2:3, 2 * p + 1 : 2 * p + 2], (1, LANES))
        sk_ref[p : p + 1, :] = jnp.where(half, left, right)
    gg_ref[...] = gate_ref[layer]


VECTOR_SCRATCH = (
    pltpu.VMEM((8, XBC), f32),
    pltpu.VMEM((1, LANES), f32),
    pltpu.VMEM((1, LANES), f32),
    pltpu.VMEM((PAIRS, LANES), f32),
    pltpu.VMEM((1, DI), f32),
)


def scan_kernel(
    layer_ref, proj_ref, conv_ref, head_ref, gate_ref,
    pre_ref, y_ref, yn_ref, dt_ref, cum_ref, got, halo_ref,
    cw_ref, dtb_ref, al_ref, sk_ref, gg_ref, pad, col, tcol, lcol, lrow, st, give, square, edge_send, edge_recv, send, recv,
):
    rows = proj_ref.shape[0]
    take_vectors(layer_ref, conv_ref, head_ref, gate_ref, cw_ref, dtb_ref, al_ref, sk_ref, gg_ref)
    first, final = chunk_place(1)
    chain_barrier(1, first, final)
    edge = to_next(
        proj_ref.at[pl.ds(rows - 8, 8), pl.ds(DI, XBC)], halo_ref, edge_send, edge_recv, 1
    )

    @pl.when(jnp.logical_not(final))
    def _():
        edge.start()

    @pl.when(first)
    def _():
        halo_ref[...] = jnp.zeros(halo_ref.shape, f32)
        got[...] = jnp.zeros(got.shape, bf16)

    pad[8:, :] = proj_ref[:, DI : DI + XBC]
    dt_ref[...] = jnp.zeros((rows, LANES), f32)
    dt_ref[:, 0:HEADS] = proj_ref[:, DI + XBC :]
    drive = dt_ref[...] + dtb_ref[...]
    dt = jnp.maximum(drive, 0.0) + jnp.log1p(jnp.exp(-jnp.abs(drive)))
    dt_ref[...] = dt
    rate = dt * (-jnp.exp(al_ref[...]))
    ri = lax.broadcasted_iota(jnp.int32, (rows, rows), 0)
    ci = lax.broadcasted_iota(jnp.int32, (rows, rows), 1)
    causal = ri >= ci
    cum = dot_nn(jnp.where(causal, 1.0, 0.0), rate, highest)
    cum_ref[...] = cum
    lrow[...] = cum.T
    spread_columns(cum, col, lcol, rows)
    spread_columns(dt, None, tcol, rows)

    @pl.when(jnp.logical_not(first))
    def _():
        edge.wait_recv()

    pad[0:8, :] = halo_ref[...]

    def conv(i, _):
        xs = pair_lanes(i)
        out = jnp.broadcast_to(cw_ref[CONV : CONV + 1, xs], (rows, LANES))
        for k in range(CONV):
            out = out + cw_ref[k : k + 1, xs] * pad[5 + k : 5 + k + rows, xs]
        pre_ref[:, xs] = out
        return 0

    lax.fori_loop(0, XBC // LANES, conv, 0, unroll=3)
    bm = silu(pre_ref[:, DI : DI + NSTATE]).astype(bf16)
    cm = silu(pre_ref[:, DI + NSTATE :]).astype(bf16)
    cb = dot_nt(cm, bm)
    half = first_half(rows)

    def states(p, _):
        xs = pair_lanes(p)
        lp = lcol[p]
        tail = jnp.exp(lp[rows - 1 : rows, :] - lp) * tcol[p]
        st[xs, :] = dot_tn((tail * silu(pre_ref[:, xs])).astype(bf16), bm)
        return 0

    lax.fori_loop(0, PAIRS, states, 0, unroll=4)
    square[...] = jnp.zeros(square.shape, f32)

    def pair(p):
        xs = pair_lanes(p)
        x = silu(pre_ref[:, xs])
        xtb = (tcol[p] * x).astype(bf16)
        parts = []
        for j in range(2):
            h = 2 * p + j
            c = col[h]
            d = jnp.concatenate([c] * (rows // LANES), axis=1) - lrow[pl.ds(h, 1), :]
            m = (jnp.exp(jnp.where(causal, d, OFF)) * cb).astype(bf16)
            parts.append(dot_nn(m, xtb))
        y = jnp.where(half, parts[0], parts[1]) + sk_ref[pl.ds(p, 1), :] * x
        y = y + jnp.exp(lcol[p]) * dot_nt(cm, got[xs, :])
        y_ref[:, xs] = y
        g = y * silu(proj_ref[:, xs])
        return g * g

    def step(g, _):
        chain_step(g, 1, first, final, got, give, st, col, rows, send, recv)
        total = square[...]
        for i in range(PART // LANES):
            total = total + pair(g * (PART // LANES) + i)
        square[...] = total
        return 0

    lax.fori_loop(0, CHAIN_STEPS, step, 0)
    scale = lax.rsqrt(jnp.sum(square[...], axis=1, keepdims=True) / DI + epsilon)

    def put(p, _):
        xs = pair_lanes(p)
        g = y_ref[:, xs] * silu(proj_ref[:, xs])
        yn_ref[:, xs] = (g * scale * gg_ref[0:1, xs]).astype(bf16)
        return 0

    lax.fori_loop(0, PAIRS, put, 0, unroll=4)

    @pl.when(jnp.logical_not(final))
    def _():
        edge.wait_send()

    chain_end(1, final, got, give, send, recv)


def back_kernel(
    layer_ref, dyn_ref, y_ref, proj_ref, halo_ref, pre_ref, dt_ref, cum_ref, sin_ref,
    conv_ref, head_ref, gate_ref,
    dp_ref, dcw_ref, dsm_ref, dgg_ref,
    cw_ref, dtb_ref, al_ref, sk_ref, gg_ref, pad, grad, col, tcol, lcol, lrow, dcb, dbm, dcm, dlog, dtx, ends, dy_ref, drive_ref,
    got, give, gst, dx_ref, edge_ref, from_ref, edge_send, edge_recv, send, recv,
):
    rows = y_ref.shape[0]
    take_vectors(layer_ref, conv_ref, head_ref, gate_ref, cw_ref, dtb_ref, al_ref, sk_ref, gg_ref)
    first, final = chunk_place(-1)
    chain_barrier(-1, first, final)

    @pl.when(first)
    def _():
        from_ref[...] = jnp.zeros(from_ref.shape, f32)
        got[...] = jnp.zeros(got.shape, bf16)

    cum = cum_ref[...]
    dt = dt_ref[...]
    lrow[...] = cum.T
    spread_columns(cum, col, lcol, rows)
    spread_columns(dt, None, tcol, rows)
    bm = silu(pre_ref[:, DI : DI + NSTATE]).astype(bf16)
    cm = silu(pre_ref[:, DI + NSTATE :]).astype(bf16)
    zero = jnp.zeros((rows, LANES), f32)

    def sums(p, carry):
        xs = pair_lanes(p)
        g = y_ref[:, xs] * silu(proj_ref[:, xs])
        return carry[0] + g * g, carry[1] + g * (dyn_ref[:, xs] * gg_ref[0:1, xs])

    square, cross = lax.fori_loop(0, PAIRS, sums, (zero, zero), unroll=4)
    scale = lax.rsqrt(jnp.sum(square, axis=1, keepdims=True) / DI + epsilon)
    mean = jnp.sum(cross, axis=1, keepdims=True) * scale / DI

    def ungate(p, _):
        xs = pair_lanes(p)
        z = proj_ref[:, xs]
        y = y_ref[:, xs]
        sg = lax.logistic(z)
        sz = z * sg
        ghat = y * sz * scale
        dyn = dyn_ref[:, xs]
        dgg_ref[0:1, xs] = jnp.sum(dyn * ghat, axis=0, keepdims=True)
        dg = scale * (dyn * gg_ref[0:1, xs] - ghat * mean)
        dy = dg * sz
        dy_ref[:, xs] = dy
        dp_ref[:, xs] = (dg * y * (sg * (1.0 + z * (1.0 - sg)))).astype(bf16)
        gst[xs, :] = dot_tn((jnp.exp(lcol[p]) * dy).astype(bf16), cm)
        return 0

    lax.fori_loop(0, PAIRS, ungate, 0, unroll=4)
    pad[0:8, :] = halo_ref[...]
    pad[8:, :] = proj_ref[:, DI : DI + XBC]
    grad[0:8, :] = jnp.zeros((8, XBC), f32)
    grad[rows + 8 :, :] = jnp.zeros((8, XBC), f32)
    cbt = dot_nt(bm, cm)
    ri = lax.broadcasted_iota(jnp.int32, (rows, rows), 0)
    ci = lax.broadcasted_iota(jnp.int32, (rows, rows), 1)
    causal = ri <= ci
    half = first_half(rows)
    dcb[...] = jnp.zeros((rows, rows), f32)
    dbm[...] = zero
    dcm[...] = zero
    dlog[...] = zero
    dtx[...] = zero
    ends[...] = jnp.zeros((16, LANES), f32)
    lane_row = lax.broadcasted_iota(jnp.int32, (LANES, LANES), 0)
    lane_col = lax.broadcasted_iota(jnp.int32, (LANES, LANES), 1)
    ones = jnp.ones((8, NSTATE), f32)

    def pair(p):
        xs = pair_lanes(p)
        pre = pre_ref[:, xs]
        sg = lax.logistic(pre)
        x = pre * sg
        tp = tcol[p]
        xt = tp * x
        dy = dy_ref[:, xs]
        dyb = dy.astype(bf16)
        parts = []
        for j in range(2):
            h = 2 * p + j
            c = col[h]
            d = lrow[pl.ds(h, 1), :] - jnp.concatenate([c] * (rows // LANES), axis=1)
            w = jnp.exp(jnp.where(causal, d, OFF))
            parts.append(dot_nn((w * cbt).astype(bf16), dyb))
            own = half if j == 0 else jnp.logical_not(half)
            q = dot_nt(jnp.where(own, xt, 0.0).astype(bf16), dyb)
            dcb[...] += w * q
        lp = lcol[p]
        last = lp[rows - 1 : rows, :]
        tail = jnp.exp(last - lp)
        gin = got[xs, :]
        sin = sin_ref[xs, :]
        dst = tail * dot_nt(bm, gin)
        dxt = jnp.where(half, parts[0], parts[1]) + dst
        dbm[...] += dot_nn((tail * xt).astype(bf16), gin)
        dcm[...] += dot_nn((jnp.exp(lp) * dy).astype(bf16), sin)
        sk = sk_ref[pl.ds(p, 1), :]
        pick = jnp.where(lane_col == 2 * p + jnp.where(lane_row >= HDIM, 1, 0), 1.0, 0.0)
        dlog[...] += dot_nn(dy * (y_ref[:, xs] - sk * x) - xt * dxt, pick, highest)
        dtx[...] += dot_nn(x * dxt, pick, highest)
        held = dot_nt(ones, gin.astype(f32) * sin.astype(f32), highest)
        end = jnp.sum(xt * dst, axis=0, keepdims=True) + jnp.exp(last) * held[0:1, :]
        skip = jnp.sum(dy * x, axis=0, keepdims=True)
        stacked = jnp.concatenate(
            [jnp.broadcast_to(end, (8, LANES)), jnp.broadcast_to(skip, (8, LANES))], axis=0
        )
        ends[...] += dot_nn(stacked, pick, highest)
        grad[pl.ds(8, rows), xs] = (tp * dxt + sk * dy) * (sg * (1.0 + pre * (1.0 - sg)))

    def step(g, _):
        chain_step(g, -1, first, final, got, give, gst, col, rows, send, recv)
        for i in range(PART // LANES):
            pair(g * (PART // LANES) + i)
        return 0

    lax.fori_loop(0, CHAIN_STEPS, step, 0)
    dcbb = dcb[...].astype(bf16)
    dc = dcm[...] + dot_tn(dcbb, bm)
    db = dbm[...] + dot_nn(dcbb, cm)
    grad[8 : 8 + rows, DI : DI + NSTATE] = db * silu_grad(pre_ref[:, DI : DI + NSTATE])
    grad[8 : 8 + rows, DI + NSTATE :] = dc * silu_grad(pre_ref[:, DI + NSTATE :])

    def edges(i, _):
        xs = pair_lanes(i)
        edge = jnp.zeros((8, LANES), f32)
        for k in range(CONV):
            edge = edge + cw_ref[k : k + 1, xs] * grad[3 - k : 11 - k, xs]
        edge_ref[:, xs] = edge
        return 0

    lax.fori_loop(0, XBC // LANES, edges, 0, unroll=9)
    edge = to_next(edge_ref, from_ref, edge_send, edge_recv, -1)

    @pl.when(jnp.logical_not(final))
    def _():
        edge.start()

    last_row = lax.broadcasted_iota(jnp.int32, (rows, LANES), 0) == rows - 1
    dl = dlog[...] + jnp.where(last_row, ends[0:1, :], 0.0)
    da = dot_nn(jnp.where(causal, 1.0, 0.0), dl, highest)
    decay = -jnp.exp(al_ref[...])
    ddt = dtx[...] + da * decay
    drive_ref[...] = jnp.zeros((rows, LANES), f32)
    drive_ref[:, 0:HEADS] = proj_ref[:, DI + XBC :]
    ddr = ddt * lax.logistic(drive_ref[...] + dtb_ref[...])
    dp_ref[:, DI + XBC :] = ddr[:, 0:HEADS].astype(bf16)
    dsm_ref[...] = jnp.zeros((8, LANES), f32)
    dsm_ref[0:1, :] = jnp.sum(ddr, axis=0, keepdims=True)
    dsm_ref[1:2, :] = jnp.sum(da * dt, axis=0, keepdims=True) * decay
    dsm_ref[2:3, :] = ends[8:9, :]

    def conv(i, _):
        xs = pair_lanes(i)
        own = grad[pl.ds(8, rows), xs]
        out = jnp.zeros((rows, LANES), f32)
        for k in range(CONV):
            out = out + cw_ref[k : k + 1, xs] * grad[11 - k : 11 - k + rows, xs]
            dcw_ref[k : k + 1, xs] = jnp.sum(
                own * pad[5 + k : 5 + k + rows, xs], axis=0, keepdims=True
            )
        dcw_ref[4:5, xs] = jnp.sum(own, axis=0, keepdims=True)
        dx_ref[:, xs] = out
        return 0

    lax.fori_loop(0, XBC // LANES, conv, 0, unroll=3)

    @pl.when(jnp.logical_not(first))
    def _():
        edge.wait_recv()

    dx_ref[rows - 8 :, :] += from_ref[...]
    dp_ref[:, DI : DI + XBC] = dx_ref[...].astype(bf16)

    @pl.when(jnp.logical_not(final))
    def _():
        edge.wait_send()

    chain_end(-1, final, got, give, send, recv)


VTILE = 1280
NTILE = 256


def head_specs(width, tokens):
    return dict(
        table=pl.BlockSpec((VTILE, width), lambda i: (i, 0)),
        hidden=pl.BlockSpec((tokens, width), lambda i: (0, 0)),
        kept=pl.BlockSpec((VTILE, tokens), lambda i: (i, 0)),
        row=pl.BlockSpec((1, tokens), lambda i: (0, 0)),
        tile_row=pl.BlockSpec((1, 1, tokens), lambda i: (i, 0, 0)),
    )


def head_call(kernel, grid, in_specs, out_specs, outs, scratch, ins, cells):
    return pl.pallas_call(
        kernel,
        grid=(grid,),
        in_specs=in_specs,
        out_specs=out_specs,
        out_shape=[jax.ShapeDtypeStruct(shape, kind) for shape, kind in outs],
        scratch_shapes=list(scratch),
        compiler_params=pltpu.CompilerParams(
            dimension_semantics=("arbitrary",), vmem_limit_bytes=VMEM_LIMIT
        ),
        cost_estimate=pl.CostEstimate(
            flops=2 * cells * D, transcendentals=cells, bytes_accessed=4 * cells
        ),
    )(*ins)


UNROLL = 8


def head_stats_kernel(
    lead_ref, table_ref, own_ref, lab_ref, w_ref,
    q_ref, all_ref, lse_ref, fac_ref, hit_ref,
    kept, tops, sums, hits, shown, own_sem, put_sem, z_send, z_recv, m_send, m_recv, s_send, s_recv,
):
    dp = lax.axis_index("dp")
    me = lax.axis_index("fsdp")
    shards = lax.axis_size("fsdp")
    count = shards // MB
    core = me % MB
    k = me // MB
    mate = k * MB + 1 - core
    vocab_rows = lead_ref.shape[0] + table_ref.shape[0]
    rows = own_ref.shape[0]
    tiles = tops.shape[0]
    barrier = pltpu.get_barrier_semaphore()
    for other in range(1, shards):
        pl.semaphore_signal(
            barrier, inc=1, device_id=(dp, lax.rem(me + other, shards)), device_id_type=MESH
        )
    pl.semaphore_wait(barrier, shards - 1)

    near = jnp.minimum(k, count - 1 - k)
    long_side = jnp.where(count - 1 - k > k, 1, -1)

    def chunk_at(i):
        paired = k + (2 * (i % 2) - 1) * ((i + 1) // 2)
        return jnp.where(i <= 2 * near, paired, k + long_side * (i - near))

    def along(z, side):
        at = all_ref.at[z * MB + core]
        return remote(
            at, at, z_send.at[side, z], z_recv.at[z], dp, me + MB if side == 0 else me - MB
        )

    def to_mate(z):
        at = all_ref.at[z * MB + core]
        return remote(at, at, m_send.at[z], m_recv.at[z], dp, mate)

    def from_mate(z):
        at = all_ref.at[z * MB + 1 - core]
        return remote(at, at, m_send.at[z], m_recv.at[z], dp, mate)

    keep = pltpu.make_async_copy(own_ref, all_ref.at[me], own_sem)
    keep.start()
    keep.wait()

    @pl.when(k < count - 1)
    def _():
        along(k, 0).start()

    @pl.when(k > 0)
    def _():
        along(k, 1).start()

    to_mate(k).start()
    whole = vocab_rows - vocab_rows % 16
    for slot in range(2):
        kept[slot, whole:, :] = jnp.zeros((kept.shape[1] - whole, rows), bf16)

    def put(step, b):
        return pltpu.make_async_copy(
            kept.at[step % 2],
            q_ref.at[:, pl.ds(pl.multiple_of(b * rows, rows), rows)],
            put_sem.at[step % 2],
        )

    def block(step, b):
        @pl.when(step >= 2)
        def _():
            put(step, b).wait()

        slot = step % 2
        ns = pl.ds(pl.multiple_of(b * rows, rows), rows)
        h = all_ref[b]
        label = lab_ref[0:1, ns]
        for t in range(tiles):
            first = t * VTILE
            size = min(VTILE, vocab_rows - first)
            part = lead_ref[...] if t == 0 else table_ref[first - VTILE : first - VTILE + size, :]
            logits = dot_nt(part, h)
            top = jnp.max(logits, axis=0, keepdims=True)
            p = jnp.exp(logits - top)
            kept[slot, first : first + size, :] = p.astype(bf16)
            tops[t, 0:1, ns] = top
            sums[t, 0:1, ns] = jnp.sum(p, axis=0, keepdims=True)
            rid = lax.broadcasted_iota(jnp.int32, (size, rows), 0)
            hits[t, 0:1, ns] = jnp.sum(
                jnp.where(rid == label - first, logits, 0.0), axis=0, keepdims=True
            )
        put(step, b).start()

    def chunk(i, _):
        z = chunk_at(i)

        @pl.when(jnp.logical_and(i > 0, k >= i))
        def _():
            along(k - i, 0).wait_recv()

            @pl.when(k < count - 1)
            def _():
                along(k - i, 0).start()

            to_mate(k - i).start()

        @pl.when(jnp.logical_and(i > 0, k + i < count))
        def _():
            along(k + i, 1).wait_recv()

            @pl.when(k > 0)
            def _():
                along(k + i, 1).start()

            to_mate(k + i).start()

        block(2 * i, z * MB + core)
        from_mate(z).wait_recv()
        block(2 * i + 1, z * MB + 1 - core)
        return 0

    lax.fori_loop(0, count, chunk, 0)
    top = tops[0, 0:1, :]
    for t in range(1, tiles):
        top = jnp.maximum(top, tops[t, 0:1, :])
    total = jnp.zeros_like(top)
    hit = jnp.zeros_like(top)
    for t in range(tiles):
        total = total + sums[t, 0:1, :] * jnp.exp(tops[t, 0:1, :] - top)
        hit = hit + hits[t, 0:1, :]
    hit_ref[...] = hit
    shown[me, 0:1, :] = top
    shown[me, 1:2, :] = total

    def tell(other):
        at = shown.at[me]
        return remote(
            at, at, s_send.at[other], s_recv.at[me], dp, lax.rem(me + other, shards)
        )

    def told(other):
        at = shown.at[lax.rem(me + other, shards)]
        return remote(
            at, at, s_send.at[other], s_recv.at[lax.rem(me + other, shards)], dp, mate
        )

    for other in range(1, shards):
        tell(other).start()
    for other in range(1, shards):
        told(other).wait_recv()
    top = shown[0, 0:1, :]
    for f in range(1, shards):
        top = jnp.maximum(top, shown[f, 0:1, :])
    total = jnp.zeros_like(top)
    for f in range(shards):
        total = total + shown[f, 1:2, :] * jnp.exp(shown[f, 0:1, :] - top)
    lse = top + jnp.log(total)
    lse_ref[...] = lse
    scale = w_ref[...] * (1.0 + 2.0 * z_weight * lse)
    for t in range(tiles):
        fac_ref[t, 0:1, :] = scale * jnp.exp(tops[t, 0:1, :] - lse)
    for other in range(1, shards):
        tell(other).wait_send()
    for z in range(count):

        @pl.when(jnp.logical_and(k >= z, k < count - 1))
        def _(z=z):
            along(z, 0).wait_send()

        @pl.when(jnp.logical_and(k <= z, k > 0))
        def _(z=z):
            along(z, 1).wait_send()

        to_mate(z).wait_send()
    put(0, 0).wait()
    put(1, 0).wait()


def head_stats(lead, table, own, labels, weight):
    vocab_rows, width = lead.shape[0] + table.shape[0], table.shape[1]
    rows = own.shape[0]
    shards = lax.axis_size("fsdp")
    count = shards // MB
    tokens = shards * rows
    tiles = pl.cdiv(vocab_rows, VTILE)
    kept, everyone, lse, fac, hit = comm_call(
        head_stats_kernel,
        6,
        (lead, table, own, labels, weight),
        (
            ((tiles * VTILE, tokens), bf16),
            ((shards, rows, width), bf16),
            ((1, tokens), f32),
            ((tiles, 1, tokens), f32),
            ((1, tokens), f32),
        ),
        (
            pltpu.VMEM((2, tiles * VTILE, rows), bf16),
            pltpu.VMEM((tiles, 1, tokens), f32),
            pltpu.VMEM((tiles, 1, tokens), f32),
            pltpu.VMEM((tiles, 1, tokens), f32),
            pltpu.VMEM((shards, 2, tokens), f32),
            pltpu.SemaphoreType.DMA,
            pltpu.SemaphoreType.DMA((2,)),
            pltpu.SemaphoreType.DMA((2, count)),
            pltpu.SemaphoreType.DMA((count,)),
            pltpu.SemaphoreType.DMA((count,)),
            pltpu.SemaphoreType.DMA((count,)),
            pltpu.SemaphoreType.DMA((shards,)),
            pltpu.SemaphoreType.DMA((shards,)),
        ),
        (pltpu.VMEM,) * 5,
        (pl.ANY, pltpu.VMEM, pltpu.VMEM, pltpu.VMEM, pltpu.VMEM),
        own.size * 2 * 7,
    )
    return kept, everyone.reshape(tokens, width), lse, fac, hit


def logit_grads(q, fac, weight, rid, label):
    other = weight * (0.1 / VOCAB)
    return (q.astype(f32) * fac - jnp.where(rid == label, other + 0.9 * weight, other)).astype(bf16)


def head_rows_kernel(vocab_rows, lead_ref, e_ref, q_ref, fac_ref, w_ref, lab_ref, out_ref, acc, et):
    step = pl.program_id(0)
    first = step * VTILE
    tokens = q_ref.shape[1]

    @pl.when(step == 0)
    def _():
        acc[...] = jnp.zeros(acc.shape, f32)

    eid = lax.broadcasted_iota(jnp.int32, (VTILE, e_ref.shape[1]), 0)
    part = jnp.where(step == 0, lead_ref[...].astype(f32), e_ref[...].astype(f32))
    et[...] = jnp.where(eid < vocab_rows - first, part, 0.0).T.astype(bf16)

    def chunk(j, _):
        ns = pl.ds(pl.multiple_of(j * NTILE, NTILE), NTILE)
        rid = lax.broadcasted_iota(jnp.int32, (VTILE, NTILE), 0)
        dl = logit_grads(
            q_ref[:, ns], fac_ref[0, 0:1, ns], w_ref[0:1, ns], rid, lab_ref[0:1, ns] - first
        )
        acc[:, ns] += dot_nn(et[...], dl)
        return 0

    lax.fori_loop(0, tokens // NTILE, chunk, 0, unroll=UNROLL)

    @pl.when(step == pl.num_programs(0) - 1)
    def _():
        def put(j, _):
            ns = pl.ds(pl.multiple_of(j * NTILE, NTILE), NTILE)
            out_ref[ns, :] = acc[:, ns].T.astype(bf16)
            return 0

        lax.fori_loop(0, tokens // NTILE, put, 0)


def head_rows(lead, table, kept, fac, weight, labels):
    vocab_rows, width = lead.shape[0] + table.shape[0], table.shape[1]
    tokens = kept.shape[1]
    sp = head_specs(width, tokens)
    return head_call(
        functools.partial(head_rows_kernel, vocab_rows),
        pl.cdiv(vocab_rows, VTILE),
        [
            pl.BlockSpec((VTILE, width), lambda i: (0, 0)),
            pl.BlockSpec((VTILE, width), lambda i: (jnp.maximum(i - 1, 0), 0)),
            sp["kept"],
            sp["tile_row"],
            sp["row"],
            sp["row"],
        ],
        [sp["hidden"]],
        [((tokens, width), bf16)],
        (pltpu.VMEM((width, tokens), f32), pltpu.VMEM((width, VTILE), bf16)),
        (lead, table, kept, fac, weight, labels),
        vocab_rows * tokens,
    )[0]


def head_table_kernel(h_ref, q_ref, fac_ref, w_ref, lab_ref, out_ref, dl_ref):
    first = pl.program_id(0) * VTILE
    tokens = q_ref.shape[1]

    def chunk(j, _):
        ns = pl.ds(pl.multiple_of(j * NTILE, NTILE), NTILE)
        rid = lax.broadcasted_iota(jnp.int32, (VTILE, NTILE), 0)
        dl_ref[:, ns] = logit_grads(
            q_ref[:, ns], fac_ref[0, 0:1, ns], w_ref[0:1, ns], rid, lab_ref[0:1, ns] - first
        )
        return 0

    lax.fori_loop(0, tokens // NTILE, chunk, 0, unroll=UNROLL)

    def cols(j, _):
        ds = pl.ds(pl.multiple_of(j * 256, 256), 256)
        out_ref[:, ds] = dot_nn(dl_ref[...], h_ref[:, ds]).astype(bf16)
        return 0

    lax.fori_loop(0, h_ref.shape[1] // 256, cols, 0, unroll=True)


def head_table(hidden, kept, fac, weight, labels, vocab_rows):
    tokens, width = hidden.shape
    sp = head_specs(width, tokens)
    return head_call(
        head_table_kernel,
        pl.cdiv(vocab_rows, VTILE),
        [sp["hidden"], sp["kept"], sp["tile_row"], sp["row"], sp["row"]],
        [sp["table"]],
        [((vocab_rows, width), bf16)],
        (pltpu.VMEM((VTILE, tokens), bf16),),
        (hidden, kept, fac, weight, labels),
        vocab_rows * tokens,
    )[0]


def weight_grads_kernel(u_ref, dp_ref, yn_ref, db_ref, in_ref, out_ref):
    wide_cols = dp_ref.shape[1]
    for c in range(0, wide_cols, 1024):
        cs = pl.ds(c, min(1024, wide_cols - c))
        in_ref[:, cs] = dot_tn(u_ref[...], dp_ref[:, cs]).astype(bf16)
    out_ref[...] = dot_tn(yn_ref[...], db_ref[...]).astype(bf16)


def weight_grads(normed, grad_proj, mixed, grad_branch):
    rows = normed.shape[0]
    steps = D // 256
    part = DI // steps
    return head_call(
        weight_grads_kernel,
        steps,
        [
            pl.BlockSpec((rows, 256), lambda i: (0, i)),
            pl.BlockSpec((rows, ZW), lambda i: (0, 0)),
            pl.BlockSpec((rows, part), lambda i: (0, i)),
            pl.BlockSpec((rows, D), lambda i: (0, 0)),
        ],
        [pl.BlockSpec((256, ZW), lambda i: (i, 0)), pl.BlockSpec((part, D), lambda i: (i, 0))],
        [((D, ZW), bf16), ((DI, D), bf16)],
        (),
        (normed, grad_proj, mixed, grad_branch),
        rows * (ZW + DI),
    )


def after(value, earlier):
    return lax.optimization_barrier((value, earlier))[0]


def norm_scale(values):
    return lax.rsqrt(jnp.mean(values * values, axis=-1, keepdims=True) + epsilon)


def norm_back(grad, values, gain):
    scale = norm_scale(values)
    unit = values * scale
    inner = grad * gain
    back = scale * (inner - unit * jnp.mean(inner * unit, axis=-1, keepdims=True))
    return back, jnp.sum(grad * unit, axis=0)


def all_vectors(vector_params):
    rows = vector_params[: LAYERS * PER].reshape(LAYERS, PER)
    at = (CONV + 1) * XBC
    heads = rows[:, at : at + 3 * HEADS].reshape(LAYERS, 3, HEADS)
    after_heads = at + 3 * HEADS
    return dict(
        conv=rows[:, :at].reshape(LAYERS, CONV + 1, XBC),
        heads=jnp.pad(heads, ((0, 0), (0, 5), (0, LANES - HEADS))),
        gate=rows[:, after_heads + D :].reshape(LAYERS, 1, DI),
        pre=rows[:, after_heads : after_heads + D],
    )


def layer_forward(hidden, w_in, w_out, vec, layer):
    rows = hidden.shape[0]
    normed = (hidden * norm_scale(hidden) * vec["pre"][layer]).astype(bf16)
    proj = jnp.dot(normed, w_in, preferred_element_type=f32)
    pre, y, mixed, dt, cum, entering, halo = comm_call(
        scan_kernel,
        1,
        (jnp.full((1,), layer, jnp.int32), proj, vec["conv"], vec["heads"], vec["gate"]),
        (
            ((rows, XBC), f32),
            ((rows, DI), f32),
            ((rows, DI), bf16),
            ((rows, LANES), f32),
            ((rows, LANES), f32),
            ((DI, NSTATE), bf16),
            ((8, XBC), f32),
        ),
        VECTOR_SCRATCH
        + (
            pltpu.VMEM((rows + 8, XBC), f32),
            pltpu.VMEM((HEADS, rows, LANES), f32),
            pltpu.VMEM((PAIRS, rows, LANES), f32),
            pltpu.VMEM((PAIRS, rows, LANES), f32),
            pltpu.VMEM((LANES, rows), f32),
            pltpu.VMEM((DI, NSTATE), f32),
            pltpu.VMEM((DI, NSTATE), bf16),
            pltpu.VMEM((rows, LANES), f32),
            pltpu.SemaphoreType.DMA,
            pltpu.SemaphoreType.DMA,
            pltpu.SemaphoreType.DMA((CHAIN_STEPS,)),
            pltpu.SemaphoreType.DMA((CHAIN_STEPS,)),
        ),
        (pltpu.SMEM,) + (pltpu.VMEM,) * 4,
        (pltpu.VMEM,) * 7,
        DI * NSTATE * 2,
    )
    branch = jnp.dot(mixed, w_out, preferred_element_type=f32)
    record = (hidden, normed, proj, halo, pre, dt, cum, entering, y, mixed)
    return hidden + branch, record


def layer_backward(grad_hidden, w_in, w_out, vec, layer, record):
    hidden, normed, proj, halo, pre, dt, cum, entering, y, mixed = record
    rows = hidden.shape[0]
    grad_branch = grad_hidden.astype(bf16)
    grad_mixed = dot_nt(grad_branch, w_out)
    grad_proj, dconv, dsmall, dgate = comm_call(
        back_kernel,
        2,
        (
            jnp.full((1,), layer, jnp.int32), grad_mixed, y, proj, halo, pre, dt, cum, entering,
            vec["conv"], vec["heads"], vec["gate"],
        ),
        (
            ((rows, ZW), bf16),
            ((8, XBC), f32),
            ((8, LANES), f32),
            ((1, DI), f32),
        ),
        VECTOR_SCRATCH
        + (
            pltpu.VMEM((rows + 8, XBC), f32),
            pltpu.VMEM((rows + 16, XBC), f32),
            pltpu.VMEM((HEADS, rows, LANES), f32),
            pltpu.VMEM((PAIRS, rows, LANES), f32),
            pltpu.VMEM((PAIRS, rows, LANES), f32),
            pltpu.VMEM((LANES, rows), f32),
            pltpu.VMEM((rows, rows), f32),
            pltpu.VMEM((rows, LANES), f32),
            pltpu.VMEM((rows, LANES), f32),
            pltpu.VMEM((rows, LANES), f32),
            pltpu.VMEM((rows, LANES), f32),
            pltpu.VMEM((16, LANES), f32),
            pltpu.VMEM((rows, DI), f32),
            pltpu.VMEM((rows, LANES), f32),
            pltpu.VMEM((DI, NSTATE), bf16),
            pltpu.VMEM((DI, NSTATE), bf16),
            pltpu.VMEM((DI, NSTATE), f32),
            pltpu.VMEM((rows, XBC), f32),
            pltpu.VMEM((8, XBC), f32),
            pltpu.VMEM((8, XBC), f32),
            pltpu.SemaphoreType.DMA,
            pltpu.SemaphoreType.DMA,
            pltpu.SemaphoreType.DMA((CHAIN_STEPS,)),
            pltpu.SemaphoreType.DMA((CHAIN_STEPS,)),
        ),
        (pltpu.SMEM,) + (pltpu.VMEM,) * 11,
        (pltpu.VMEM,) * 4,
        DI * NSTATE * 2,
    )
    grad_normed = dot_nt(grad_proj, w_in)
    grad_in, grad_out = weight_grads(normed, grad_proj, mixed, grad_branch)
    grad_prev, dpre_gain = norm_back(grad_normed, hidden, vec["pre"][layer])
    grad_vec = jnp.concatenate(
        [
            dconv[: CONV + 1].reshape(-1),
            dsmall[0, :HEADS],
            dsmall[1, :HEADS],
            dsmall[2, :HEADS],
            dpre_gain,
            dgate[0],
        ]
    )
    return grad_hidden + grad_prev, grad_in, grad_out, grad_vec


def whole_step(
    token_ids,
    target_ids,
    seq_lengths,
    embedding,
    embedding_mom,
    embedding_avg,
    in_proj,
    in_proj_mom,
    in_proj_avg,
    out_proj,
    out_proj_mom,
    out_proj_avg,
    vector_params,
    vector_mom,
    vector_avg,
):
    groups = lax.axis_size("dp")
    shards = lax.axis_size("fsdp")
    group_index = lax.axis_index("dp")
    shard_index = lax.axis_index("fsdp")
    chunks = shards // MB
    seq_rows = token_ids.shape[2]
    rows = seq_rows // chunks
    vocab_rows, own_cols = embedding.shape
    tokens = MB * seq_rows
    total_count = jnp.sum(seq_lengths).astype(f32)
    in_low = in_proj.astype(bf16)
    out_low = out_proj.astype(bf16)

    lead = lax.all_gather(embedding[:VTILE].astype(bf16), "dp", axis=1, tiled=True)
    ids_all = group_call(share_kernel, 7, token_ids[:, 0, :], ((groups, MB, seq_rows), jnp.int32))
    ids_all = ids_all.reshape(groups, MB, chunks, rows).transpose(2, 1, 0, 3).reshape(-1)
    every = ids_all.shape[0]
    local_ids = ids_all - shard_index * vocab_rows
    inside = (local_ids >= 0) & (local_ids < vocab_rows)
    sorted_ids, sorted_tok = lax.sort(
        (jnp.where(inside, local_ids, vocab_rows), jnp.arange(every, dtype=jnp.int32)),
        num_keys=1,
    )
    held_here = sorted_ids < vocab_rows
    count = jnp.sum(held_here.astype(jnp.int32)).reshape(1)
    row_list = jnp.where(held_here, sorted_ids, 0)
    tok_list = jnp.where(held_here, sorted_tok, every)
    looked, embed_low, own_sums = local_call(
        lookup_kernel,
        (count, row_list, tok_list, embedding),
        (((every, own_cols), bf16), ((vocab_rows - VTILE, own_cols), bf16), ((8, own_cols), f32)),
        scratch=(pltpu.VMEM((every + 8, own_cols), f32),),
        in_smem=(0, 1, 2),
    )
    mine = lax.psum_scatter(
        looked.reshape(shards * groups * rows, own_cols), "fsdp", scatter_dimension=0, tiled=True
    )
    hidden = group_call(
        to_rows_kernel,
        8,
        mine.reshape(groups, rows, own_cols),
        ((rows, D), f32),
        (pltpu.VMEM((groups, rows, own_cols), bf16),),
    )

    shards = []
    for l in range(LAYERS):
        shards += [in_low[l], out_low[l]]
    shards = after(shards, looked)
    gathered = gather_layers(shards)
    w_in, w_out = gathered[0::2], gathered[1::2]
    embed_low = after(embed_low, gathered)
    table = lax.all_gather(embed_low, "dp", axis=1, tiled=True)

    vecs = all_vectors(vector_params)
    final_gain = vector_params[LAYERS * PER :]
    records = []
    for l in range(LAYERS):
        hidden, record = layer_forward(hidden, w_in[l], w_out[l], vecs, l)
        records.append(record)

    final_low = (hidden * norm_scale(hidden) * final_gain).astype(bf16)

    def in_order(per_seq):
        return per_seq.reshape(MB, chunks, rows).transpose(1, 0, 2).reshape(1, tokens)

    labels = in_order(target_ids[:, 0, :])
    lengths = lax.dynamic_index_in_dim(seq_lengths, group_index, 1, keepdims=True)
    valid = in_order((jnp.arange(seq_rows)[None, :] < lengths).astype(f32))
    local_labels = labels - shard_index * vocab_rows
    weight = valid / total_count
    kept, group_hidden, lse, fac, target = head_stats(lead, table, final_low, local_labels, weight)
    own_mask = jnp.arange(tokens) // rows == shard_index
    per_row = jnp.where(own_mask, lse[0] + z_weight * lse[0] * lse[0], 0.0)
    loss_sum = jnp.sum((per_row - 0.9 * target[0]) * valid[0])
    own_valid = lax.dynamic_slice_in_dim(valid[0], shard_index * rows, rows)
    hidden_sum = jnp.sum(final_low.astype(f32) * own_valid[:, None], axis=0)
    column_sum = jnp.zeros((groups, own_cols), f32)
    column_sum = jnp.where(
        jnp.arange(groups)[:, None] == group_index, jnp.sum(own_sums, axis=0), column_sum
    ).reshape(D)

    rows_grad = head_rows(lead, table, kept, fac, weight, local_labels)
    own_grad = lax.psum_scatter(
        rows_grad, "fsdp", scatter_dimension=0, tiled=True
    ).astype(f32)
    table_grad = head_table(group_hidden, kept, fac, weight, local_labels, vocab_rows)
    table_part = lax.psum_scatter(table_grad, "dp", scatter_dimension=1, tiled=True)

    grad_hidden, dfinal = norm_back(after(own_grad, table_grad), hidden, final_gain)
    in_parts = [None] * LAYERS
    out_parts = [None] * LAYERS
    vec_parts = [None] * LAYERS
    for l in reversed(range(LAYERS)):
        grad_hidden, grad_in, grad_out, vec_parts[l] = layer_backward(
            grad_hidden, w_in[l], w_out[l], vecs, l, records[l]
        )
        in_parts[l], out_parts[l] = grad_in, grad_out
    whole = []
    for l in range(LAYERS):
        whole += [in_parts[l], out_parts[l]]
    sent = group_call(
        to_columns_kernel,
        9,
        after(grad_hidden, whole),
        ((groups, rows, own_cols), bf16),
        (pltpu.VMEM((groups, rows, own_cols), bf16),),
    )
    whole = after(whole, sent)
    spread = lax.all_gather(sent, "fsdp", axis=0).reshape(every, own_cols)
    summed_parts = reduce_layers(whole)
    spread = after(spread, summed_parts)
    table_total, table_squares = local_call(
        spread_kernel,
        (count, row_list, tok_list, spread, table_part),
        (((vocab_rows, own_cols), f32), ((8, own_cols), f32)),
        scratch=(pltpu.VMEM((every + 8, own_cols), f32),),
        in_smem=(0, 1, 2),
    )
    owner_squares = jnp.sum(table_squares)
    for part in summed_parts:
        owner_squares = owner_squares + jnp.sum(part * part)
    small = vector_params.shape[0]
    used = small + 2 * D + 2
    padded = pl.cdiv(used, 16 * LANES) * 16 * LANES
    packed = jnp.concatenate(
        vec_parts
        + [
            dfinal,
            hidden_sum,
            column_sum,
            owner_squares.reshape(1),
            loss_sum.reshape(1),
            jnp.zeros((padded - used,), f32),
        ]
    )
    packed, norms = total_of(packed.reshape(-1, LANES), small, used - 2)
    factor = norms[1, 0]
    updated = []
    for master, moment, average, grad in (
        (embedding, embedding_mom, embedding_avg, table_total),
        (in_proj, in_proj_mom, in_proj_avg, jnp.stack(summed_parts[0::2])),
        (out_proj, out_proj_mom, out_proj_avg, jnp.stack(summed_parts[1::2])),
    ):
        new = stepped(master, moment, average, grad, factor)
        updated += [*new, new[0].astype(bf16)]
    packed = packed.reshape(-1)
    vector_total = packed[:small]
    hidden_total = packed[small : small + D]
    column_total = packed[small + D : small + 2 * D]
    mean_part = jnp.sum(hidden_total * column_total) * (0.1 / VOCAB)
    loss_value = (packed[used - 1] - mean_part) / total_count
    vector_new, vector_mom_new, vector_avg_new = stepped(
        vector_params, vector_mom, vector_avg, vector_total, factor
    )
    return (
        loss_value,
        norms[0, 0],
        *updated,
        vector_new,
        vector_mom_new,
        vector_avg_new,
        vector_new.astype(bf16),
    )


def solution(mesh):
    table_spec = P("fsdp", "dp")
    weight_spec = P(None, ("dp", "fsdp"), None)
    return jax.shard_map(
        whole_step,
        mesh=mesh,
        in_specs=(
            P(None, "dp", None),
            P(None, "dp", None),
            P(),
            *(table_spec,) * 3,
            *(weight_spec,) * 6,
            *(P(),) * 3,
        ),
        out_specs=(
            P(),
            P(),
            *(table_spec,) * 4,
            *(weight_spec,) * 8,
            *(P(),) * 4,
        ),
        check_vma=False,
    )
```

```python
import functools

import jax
import jax.numpy as jnp
from jax import lax
from jax.experimental import pallas as pl
from jax.experimental.pallas import tpu as pltpu
from jax.sharding import PartitionSpec as P


D = 1024
HEADS = 32
HDIM = 64
NSTATE = 128
CONV = 4
VOCAB = 50288
LAYERS = 2
MB = 2
DI = 2048
XBC = 2304
ZW = 4384
PER = 14688
LANES = 128
PAIRS = DI // LANES

epsilon = 1e-05
z_weight = 0.001
clip_limit = 0.2
step_rate = 1000.0
highest = lax.Precision.HIGHEST
bf16 = jnp.bfloat16
f32 = jnp.float32
VMEM_LIMIT = 62 * 1024 * 1024
OFF = -1e30


def dot_nn(a, b, precision=None):
    return lax.dot_general(
        a, b, (((1,), (0,)), ((), ())), precision=precision, preferred_element_type=f32
    )


def dot_nt(a, b, precision=None):
    return lax.dot_general(
        a, b, (((1,), (1,)), ((), ())), precision=precision, preferred_element_type=f32
    )


def dot_tn(a, b, precision=None):
    return lax.dot_general(
        a, b, (((0,), (0,)), ((), ())), precision=precision, preferred_element_type=f32
    )


def silu(v):
    return v * lax.logistic(v)


def silu_grad(v):
    s = lax.logistic(v)
    return s * (1.0 + v * (1.0 - s))


def local_call(kernel, ins, outs, scratch=(), in_smem=(), flops=0):
    total = sum(a.size * a.dtype.itemsize for a in ins)
    return pl.pallas_call(
        kernel,
        out_shape=[jax.ShapeDtypeStruct(shape, kind) for shape, kind in outs],
        in_specs=[
            pl.BlockSpec(memory_space=pltpu.SMEM if i in in_smem else pltpu.VMEM)
            for i in range(len(ins))
        ],
        out_specs=[pl.BlockSpec(memory_space=pltpu.VMEM) for _ in outs],
        scratch_shapes=list(scratch),
        compiler_params=pltpu.CompilerParams(vmem_limit_bytes=VMEM_LIMIT),
        cost_estimate=pl.CostEstimate(
            flops=flops or total, transcendentals=0, bytes_accessed=2 * total
        ),
    )(*ins)


def lookup_kernel(count_ref, row_ref, tok_ref, table_ref, out_ref, low_ref, sum_ref, held):
    tokens = out_ref.shape[0]
    step = 512

    def clear(i, _):
        held[pl.ds(pl.multiple_of(i * step, step), step), :] = jnp.zeros(
            (step, held.shape[1]), f32
        )
        return 0

    lax.fori_loop(0, tokens // step, clear, 0)

    def move(i, _):
        for k in range(8):
            row = row_ref[i * 8 + k]
            tok = tok_ref[i * 8 + k]
            held[pl.ds(tok, 1), :] = table_ref[pl.ds(row, 1), :]
        return 0

    lax.fori_loop(0, (count_ref[0] + 7) // 8, move, 0)

    def put(i, _):
        rows = pl.ds(pl.multiple_of(i * step, step), step)
        out_ref[rows, :] = held[rows, :].astype(bf16)
        return 0

    lax.fori_loop(0, tokens // step, put, 0)
    rows_all = table_ref.shape[0]
    part = VTILE // 5
    whole = rows_all // part

    def low_rows(i):
        return table_ref[pl.ds(pl.multiple_of(i * part, part), part), :].astype(bf16)

    def add(low, total):
        return total + jnp.sum(low.astype(f32).reshape(part // 8, 8, -1), axis=0)

    def cast(i, total):
        low = low_rows(i)
        low_ref[pl.ds(pl.multiple_of(i * part - VTILE, part), part), :] = low
        return add(low, total)

    total = lax.fori_loop(
        0, VTILE // part, lambda i, t: add(low_rows(i), t), jnp.zeros(sum_ref.shape, f32)
    )
    sum_ref[...] = lax.fori_loop(VTILE // part, whole, cast, total)
    if rows_all > whole * part:
        low = table_ref[whole * part :, :].astype(bf16)
        low_ref[whole * part - VTILE :, :] = low
        sum_ref[0:1, :] += jnp.sum(low.astype(f32), axis=0, keepdims=True)


def spread_kernel(count_ref, row_ref, tok_ref, grad_ref, base_ref, out_ref, square_ref, held):
    tokens = grad_ref.shape[0]
    step = 512
    rows_all = out_ref.shape[0]

    def take(i, _):
        rows = pl.ds(pl.multiple_of(i * step, step), step)
        held[rows, :] = grad_ref[rows, :].astype(f32)
        return 0

    lax.fori_loop(0, tokens // step, take, 0)
    held[pl.ds(tokens, 8), :] = jnp.zeros((8, held.shape[1]), f32)

    whole = rows_all // step

    def start(i, _):
        rows = pl.ds(pl.multiple_of(i * step, step), step)
        out_ref[rows, :] = base_ref[rows, :].astype(f32)
        return 0

    lax.fori_loop(0, whole, start, 0)
    if rows_all > whole * step:
        out_ref[whole * step :, :] = base_ref[whole * step :, :].astype(f32)

    def move(i, _):
        for k in range(8):
            row = row_ref[i * 8 + k]
            tok = tok_ref[i * 8 + k]
            out_ref[pl.ds(row, 1), :] = out_ref[pl.ds(row, 1), :] + held[pl.ds(tok, 1), :]
        return 0

    lax.fori_loop(0, (count_ref[0] + 7) // 8, move, 0)

    def square(i, total):
        part = out_ref[pl.ds(pl.multiple_of(i * step, step), step), :]
        return total + jnp.sum((part * part).reshape(step // 8, 8, -1), axis=0)

    total = lax.fori_loop(0, whole, square, jnp.zeros(square_ref.shape, f32))
    square_ref[...] = total
    if rows_all > whole * step:
        part = out_ref[whole * step :, :]
        square_ref[0:1, :] += jnp.sum(part * part, axis=0, keepdims=True)


MESH = pl.DeviceIdType.MESH


def remote(src, dst, send, recv, dp, fsdp):
    return pltpu.make_async_remote_copy(
        src_ref=src,
        dst_ref=dst,
        send_sem=send,
        recv_sem=recv,
        device_id=(dp, fsdp),
        device_id_type=MESH,
    )


def comm_call(kernel, number, ins, outs, scratch, in_spaces, out_spaces, sent):
    return pl.pallas_call(
        kernel,
        out_shape=[jax.ShapeDtypeStruct(shape, kind) for shape, kind in outs],
        in_specs=[pl.BlockSpec(memory_space=space) for space in in_spaces],
        out_specs=[pl.BlockSpec(memory_space=space) for space in out_spaces],
        scratch_shapes=list(scratch),
        compiler_params=pltpu.CompilerParams(
            collective_id=number, has_side_effects=True, vmem_limit_bytes=VMEM_LIMIT
        ),
        cost_estimate=pl.CostEstimate(flops=sent, transcendentals=0, bytes_accessed=2 * sent),
    )(*ins)


def greet_groups():
    dp = lax.axis_index("dp")
    me = lax.axis_index("fsdp")
    groups = lax.axis_size("dp")
    barrier = pltpu.get_barrier_semaphore()
    others = [lax.rem(dp + other, groups) for other in range(1, groups)]
    for other in others:
        pl.semaphore_signal(barrier, inc=1, device_id=(other, me), device_id_type=MESH)
    pl.semaphore_wait(barrier, groups - 1)
    return dp, me, others


def share_kernel(in_ref, out_ref, send, recv):
    dp, me, others = greet_groups()
    for other in others:
        remote(in_ref, out_ref.at[dp], send.at[other], recv.at[dp], other, me).start()
    out_ref[dp] = in_ref[...]
    for other in others:
        copy = remote(in_ref, out_ref.at[other], send.at[other], recv.at[other], other, me)
        copy.wait_recv()
        copy.wait_send()


def to_rows_kernel(in_ref, out_ref, landed, send, recv):
    dp, me, others = greet_groups()
    for other in others:
        remote(in_ref.at[other], landed.at[dp], send.at[other], recv.at[dp], other, me).start()
    landed[dp] = in_ref[dp]
    for other in others:
        remote(in_ref.at[other], landed.at[other], send.at[other], recv.at[other], other, me).wait_recv()
    cols = in_ref.shape[2]
    for g in range(in_ref.shape[0]):
        out_ref[:, g * cols : (g + 1) * cols] = landed[g].astype(f32)
    for other in others:
        remote(in_ref.at[other], landed.at[other], send.at[other], recv.at[other], other, me).wait_send()


def to_columns_kernel(in_ref, out_ref, parts, send, recv):
    dp, me, others = greet_groups()
    cols = out_ref.shape[2]
    for g in range(out_ref.shape[0]):
        parts[g] = in_ref[:, g * cols : (g + 1) * cols].astype(bf16)
    for other in others:
        remote(parts.at[other], out_ref.at[dp], send.at[other], recv.at[dp], other, me).start()
    out_ref[dp] = parts[dp]
    for other in others:
        copy = remote(parts.at[other], out_ref.at[other], send.at[other], recv.at[other], other, me)
        copy.wait_recv()
        copy.wait_send()


def group_call(kernel, number, array, out, scratch=()):
    groups = lax.axis_size("dp")
    return comm_call(
        kernel,
        number,
        (array,),
        (out,),
        tuple(scratch)
        + (pltpu.SemaphoreType.DMA((groups,)), pltpu.SemaphoreType.DMA((groups,))),
        (pltpu.VMEM,),
        (pltpu.VMEM,),
        array.size * 2,
    )[0]


CHAIN_STEPS = 8
PART = DI // CHAIN_STEPS


def chunk_place(direction):
    place = lax.axis_index("fsdp") // MB
    count = lax.axis_size("fsdp") // MB
    first = place == (0 if direction > 0 else count - 1)
    final = place == (count - 1 if direction > 0 else 0)
    return first, final


def chain_barrier(direction, first, final):
    dp = lax.axis_index("dp")
    me = lax.axis_index("fsdp")
    barrier = pltpu.get_barrier_semaphore()

    @pl.when(jnp.logical_not(first))
    def _():
        pl.semaphore_signal(
            barrier, inc=1, device_id=(dp, me - MB * direction), device_id_type=MESH
        )

    @pl.when(jnp.logical_not(final))
    def _():
        pl.semaphore_wait(barrier, 1)


def to_next(src, dst, send, recv, direction):
    dp = lax.axis_index("dp")
    return remote(src, dst, send, recv, dp, lax.axis_index("fsdp") + MB * direction)


def chain_step(g, direction, first, final, got, give, local, col, rows, send, recv):
    def copy():
        at = pl.ds(pl.multiple_of(g * PART, PART), PART)
        return to_next(give.at[at], got.at[at], send.at[g], recv.at[g], direction)

    @pl.when(jnp.logical_not(first))
    def _():
        copy().wait_recv()

    @pl.when(jnp.logical_not(final))
    def _():
        for i in range(PART // HDIM):
            h = pl.ds(pl.multiple_of(g * PART + i * HDIM, HDIM), HDIM)
            decay = jnp.exp(col[g * (PART // HDIM) + i, rows - 1 : rows, :])
            give[h, :] = (decay * got[h, :].astype(f32) + local[h, :]).astype(bf16)
        copy().start()


def chain_end(direction, final, got, give, send, recv):
    @pl.when(jnp.logical_not(final))
    def _():
        for g in range(CHAIN_STEPS):
            at = pl.ds(g * PART, PART)
            to_next(give.at[at], got.at[at], send.at[g], recv.at[g], direction).wait_send()


def bits_of(size):
    return [1 << b for b in range(size.bit_length() - 1)]


def stepped(weight, moment, average, grad, factor):
    scaled = grad * factor
    moment_new = 0.5 * moment + scaled
    weight_new = weight - step_rate * (scaled + 0.5 * moment_new)
    return weight_new, moment_new, 0.5 * average + 0.5 * weight_new


def across(kind, bit):
    dp = lax.axis_index("dp")
    me = lax.axis_index("fsdp")
    ids, other = (me, lambda v: (dp, v)) if kind == "f" else (dp, lambda v: (v, me))
    return other(jnp.where((ids // bit) % 2 == 1, ids - bit, ids + bit))


def total_partners():
    partners = [("f", b) for b in bits_of(lax.axis_size("fsdp")) if b > 1]
    return partners + [("d", b) for b in bits_of(lax.axis_size("dp"))]


def total_steps(in_ref, out_ref, work, got, send, recv):
    half = in_ref.shape[0] // 2
    core = lax.axis_index("fsdp") % MB
    mate = across("f", 1)
    mine = pl.ds(pl.multiple_of(core * half, 8), half)
    theirs = pl.ds(pl.multiple_of((1 - core) * half, 8), half)
    partners = total_partners()
    n = len(partners)
    copies = [remote(in_ref.at[theirs], got.at[0], send.at[0], recv.at[0], *mate)]
    for i, p in enumerate(partners):
        copies.append(remote(work.at[i], got.at[i + 1], send.at[i + 1], recv.at[i + 1], *across(*p)))
    copies.append(remote(work.at[n], got.at[n + 1], send.at[n + 1], recv.at[n + 1], *mate))
    copies[0].start()
    for i in range(n + 1):
        yield
        copies[i].wait()
        work[i] = (in_ref[mine, :] if i == 0 else work[i - 1]) + got[i]
        copies[i + 1].start()
    yield
    copies[n + 1].wait()
    out_ref[mine, :] = work[n]
    out_ref[theirs, :] = got[n + 1]


def norm_kernel(small, square_ref, total_ref, norm_ref, inner, outer, send, recv, send2, recv2):
    dp = lax.axis_index("dp")
    me = lax.axis_index("fsdp")
    shards = lax.axis_size("fsdp")
    groups = lax.axis_size("dp")
    near = [lax.rem(me + other, shards) for other in range(1, shards)]
    far = [lax.rem(dp + other, groups) for other in range(1, groups)]
    barrier = pltpu.get_barrier_semaphore()
    for other in near:
        pl.semaphore_signal(barrier, inc=1, device_id=(dp, other), device_id_type=MESH)
    for other in far:
        pl.semaphore_signal(barrier, inc=1, device_id=(other, me), device_id_type=MESH)
    pl.semaphore_wait(barrier, shards + groups - 2)
    for other in near:
        remote(square_ref, inner.at[me], send.at[other], recv.at[me], dp, other).start()
    inner[me] = square_ref[...]
    for other in near:
        copy = remote(square_ref, inner.at[other], send.at[other], recv.at[other], dp, other)
        copy.wait_recv()
        copy.wait_send()
    total = inner[0]
    for f in range(1, shards):
        total = total + inner[f]
    outer[dp] = total
    for other in far:
        remote(outer.at[dp], outer.at[dp], send2.at[other], recv2.at[dp], other, me).start()
    for other in far:
        copy = remote(outer.at[other], outer.at[other], send2.at[other], recv2.at[other], other, me)
        copy.wait_recv()
        copy.wait_send()
    total = outer[0]
    for d in range(1, groups):
        total = total + outer[d]
    vector = total_ref[...]
    index = lax.broadcasted_iota(jnp.int32, vector.shape, 0) * LANES
    index = index + lax.broadcasted_iota(jnp.int32, vector.shape, 1)
    parts = jnp.sum(jnp.where(index < small, vector * vector, 0.0), axis=0, keepdims=True)
    square = jnp.sum(parts, axis=1, keepdims=True)
    square = square + jnp.sum(jnp.sum(total, axis=0, keepdims=True), axis=1, keepdims=True)
    norm = jnp.sqrt(square)
    factor = jnp.minimum(1.0, clip_limit / norm)
    norm_ref[0:1, :] = jnp.broadcast_to(norm, (1, LANES))
    norm_ref[1:2, :] = jnp.broadcast_to(factor, (1, LANES))
    norm_ref[2:8, :] = jnp.zeros((6, LANES), f32)


def norm_of(squares, vector_total, small):
    shards, groups = lax.axis_size("fsdp"), lax.axis_size("dp")
    return comm_call(
        functools.partial(norm_kernel, small),
        3,
        (squares, vector_total),
        (((8, LANES), f32),),
        (
            pltpu.VMEM((shards, 8, LANES), f32),
            pltpu.VMEM((groups, 8, LANES), f32),
            pltpu.SemaphoreType.DMA((shards,)),
            pltpu.SemaphoreType.DMA((shards,)),
            pltpu.SemaphoreType.DMA((groups,)),
            pltpu.SemaphoreType.DMA((groups,)),
        ),
        (pltpu.VMEM, pltpu.VMEM),
        (pltpu.VMEM,),
        squares.size * 4 * 10,
    )[0]


def snake(place, size):
    return jnp.where(place < size // 2, place, size // 2 + size - 1 - place)


def wrap(value, size):
    return lax.rem(value + size, size)


def gather_kernel(*refs):
    arrays = 2 * LAYERS
    own = refs[:arrays]
    full = refs[arrays : 2 * arrays]
    local_sem, z_send, z_recv, ring_send, ring_recv, mate_send, mate_recv = refs[2 * arrays :]
    dp = lax.axis_index("dp")
    me = lax.axis_index("fsdp")
    size = lax.axis_size("dp")
    count = lax.axis_size("fsdp") // MB
    core = me % MB
    k = me // MB
    ring = snake(dp, size)
    reach = size // 2
    right = snake(wrap(ring + 1, size), size)
    left = snake(wrap(ring - 1, size), size)
    mate = k * MB + 1 - core
    up, down = me + MB, me - MB
    has_up, has_down = k < count - 1, k > 0
    barrier = pltpu.get_barrier_semaphore()
    for target in ((right, me), (left, me), (dp, mate)):
        pl.semaphore_signal(barrier, inc=1, device_id=target, device_id_type=MESH)

    @pl.when(has_up)
    def _():
        pl.semaphore_signal(barrier, inc=1, device_id=(dp, up), device_id_type=MESH)

    @pl.when(has_down)
    def _():
        pl.semaphore_signal(barrier, inc=1, device_id=(dp, down), device_id_type=MESH)

    pl.semaphore_wait(barrier, 3 + jnp.where(has_up, 1, 0) + jnp.where(has_down, 1, 0))

    def spot(a, d, z, c):
        return full[a].at[d, z, c]

    def chain(a, src, z, side):
        return remote(
            src, spot(a, dp, z, core), z_send.at[a, z], z_recv.at[a, z], dp, up if side == 0 else down
        )

    def chain_own(a, side):
        return remote(
            own[a],
            spot(a, dp, k, core),
            z_send.at[a, count + side],
            z_recv.at[a, k],
            dp,
            up if side == 0 else down,
        )

    def round_ring(a, src, d, z, side):
        return remote(
            src,
            spot(a, d, z, core),
            ring_send.at[a, side],
            ring_recv.at[a, d, z],
            right if side == 0 else left,
            me,
        )

    def to_mate(a, src, d, z):
        return remote(src, spot(a, d, z, core), mate_send.at[a], mate_recv.at[a], dp, mate)

    def carried(a, side):
        return (a < arrays // 2) == (side == 0)

    for a in range(arrays):

        @pl.when(has_up)
        def _(a=a):
            chain_own(a, 0).start()

        @pl.when(has_down)
        def _(a=a):
            chain_own(a, 1).start()

    for a in range(arrays):
        for side in (0, 1):
            round_ring(a, own[a], dp, k, side).start()
    for a in range(arrays):
        to_mate(a, own[a], dp, k).start()
        pltpu.make_async_copy(own[a], spot(a, dp, k, core), local_sem.at[a]).start()

    def ring_step(z, s):
        for side in (0, 1):
            origin = snake(wrap(ring - s if side == 0 else ring + s, size), size)
            for a in range(arrays):
                if s == reach and not carried(a, side):
                    continue
                piece = spot(a, origin, z, core)
                round_ring(a, piece, origin, z, side).wait_recv()
                if s + 1 < reach or (s + 1 == reach and carried(a, side)):
                    round_ring(a, piece, origin, z, side).start()
                to_mate(a, piece, origin, z).start()

    def arrive(z, side):
        for a in range(arrays):
            piece = spot(a, dp, z, core)
            chain(a, piece, z, side).wait_recv()

            @pl.when(has_up if side == 0 else has_down)
            def _(a=a, piece=piece):
                chain(a, piece, z, side).start()

            for way in (0, 1):
                round_ring(a, piece, dp, z, way).start()
            to_mate(a, piece, dp, z).start()

    def both_ways(far, act):
        if far == 0:
            act(k, 0)
            return

        @pl.when(k >= far)
        def _():
            act(k - far, 0)

        @pl.when(k + far < count)
        def _():
            act(k + far, 1)

    for turn in range(1, count + reach):
        if turn < count:
            both_ways(turn, arrive)
        for s in range(1, reach + 1):
            if 0 <= turn - s < count:
                both_ways(turn - s, lambda z, side, s=s: ring_step(z, s))

    for a in range(arrays):
        pltpu.make_async_copy(own[a], spot(a, dp, k, core), local_sem.at[a]).wait()
        for side in (0, 1):
            sent = full[a].at[pl.ds(0, reach if carried(a, side) else reach - 1), :, core]
            remote(sent, sent, ring_send.at[a, side], ring_recv.at[a, 0, 0], dp, mate).wait_send()
        whole = full[a].at[:, :, core]
        remote(whole, whole, mate_send.at[a], mate_recv.at[a], dp, mate).wait_send()
        whole = full[a].at[:, :, 1 - core]
        remote(whole, whole, mate_send.at[a], mate_recv.at[a], dp, mate).wait_recv()

        @pl.when(has_up)
        def _(a=a):
            chain_own(a, 0).wait_send()

        @pl.when(has_down)
        def _(a=a):
            chain_own(a, 1).wait_send()

        for far in range(1, count):

            @pl.when(jnp.logical_and(k >= far, has_up))
            def _(a=a, far=far):
                chain(a, spot(a, dp, k - far, core), k - far, 0).wait_send()

            @pl.when(jnp.logical_and(k + far < count, has_down))
            def _(a=a, far=far):
                chain(a, spot(a, dp, k + far, core), k + far, 1).wait_send()


def gather_layers(shards):
    size, count = lax.axis_size("dp"), lax.axis_size("fsdp") // MB
    arrays = len(shards)
    outs = comm_call(
        gather_kernel,
        4,
        shards,
        tuple(((size, count, MB) + s.shape, bf16) for s in shards),
        (
            pltpu.SemaphoreType.DMA((arrays,)),
            pltpu.SemaphoreType.DMA((arrays, count + 2)),
            pltpu.SemaphoreType.DMA((arrays, count)),
            pltpu.SemaphoreType.DMA((arrays, 2)),
            pltpu.SemaphoreType.DMA((arrays, size, count)),
            pltpu.SemaphoreType.DMA((arrays,)),
            pltpu.SemaphoreType.DMA((arrays,)),
        ),
        (pltpu.VMEM,) * arrays,
        (pl.ANY,) * arrays,
        sum(s.size * 2 for s in shards) * 24,
    )
    return [o.reshape(size * count * MB * s.shape[0], s.shape[1]) for o, s in zip(outs, shards)]


def add_rows(dst, first, *others):
    rows = dst.shape[0]
    step = min(rows, 16)

    def one(i, _):
        at = pl.ds(pl.multiple_of(i * step, step), step)
        total = first[at, :].astype(f32)
        for other in others:
            total = total + other[at, :].astype(f32)
        dst[at, :] = total.astype(dst.dtype)
        return 0

    lax.fori_loop(0, rows // step, one, 0)


def reduce_kernel(*refs):
    arrays = 2 * LAYERS
    small_ref, *refs = refs
    grads = refs[:arrays]
    total_ref, *refs = refs[arrays:]
    refs = list(grads) + refs
    outs = refs[arrays : 2 * arrays]
    held, given, come, chained = (
        refs[(2 + i) * arrays : (3 + i) * arrays] for i in range(4)
    )
    load_sem, mate_send, mate_recv, ring_send, ring_recv, z_send, z_recv, *rest = refs[6 * arrays :]
    dp = lax.axis_index("dp")
    me = lax.axis_index("fsdp")
    size = lax.axis_size("dp")
    count = lax.axis_size("fsdp") // MB
    core = me % MB
    k = me // MB
    ring = snake(dp, size)
    reach = size // 2
    right = snake(wrap(ring + 1, size), size)
    left = snake(wrap(ring - 1, size), size)
    mate = k * MB + 1 - core
    up, down = me + MB, me - MB
    has_up, has_down = k < count - 1, k > 0

    def load(a):
        return pltpu.make_async_copy(grads[a].at[:, :, core], held[a], load_sem.at[a])

    for a in range(arrays):
        load(a).start()
    barrier = pltpu.get_barrier_semaphore()
    partners = [across(*p) for p in total_partners()]
    for target in [(right, me), (left, me), (dp, mate)] + partners:
        pl.semaphore_signal(barrier, inc=1, device_id=target, device_id_type=MESH)

    @pl.when(has_up)
    def _():
        pl.semaphore_signal(barrier, inc=1, device_id=(dp, up), device_id_type=MESH)

    @pl.when(has_down)
    def _():
        pl.semaphore_signal(barrier, inc=1, device_id=(dp, down), device_id_type=MESH)

    peers = 3 + len(partners)
    pl.semaphore_wait(barrier, peers + jnp.where(has_up, 1, 0) + jnp.where(has_down, 1, 0))
    small = total_steps(small_ref, total_ref, *rest)
    next(small)

    def away(j, side):
        return snake(wrap(ring + j if side == 0 else ring - j, size), size)

    def to_mate(a, d):
        return remote(
            grads[a].at[d, :, 1 - core], given[a].at[d], mate_send.at[a], mate_recv.at[a, d], dp, mate
        )

    def carried(a, side):
        return (a < arrays // 2) == (side == 0)

    def targets(j):
        if j == 0:
            return [dp]
        if j == reach:
            return [away(j, 0)]
        return [away(j, 0), away(j, 1)]

    for j in range(reach, -1, -1):
        for d in targets(j):
            for a in range(arrays):
                to_mate(a, d).start()

    for a in range(arrays):
        load(a).wait()

    def add_mate(d):
        for a in range(arrays):
            to_mate(a, d).wait_recv()

            def one(z, _, a=a):
                add_rows(held[a].at[d, z], held[a].at[d, z], given[a].at[d, z])
                return 0

            lax.fori_loop(0, count, one, 0)

    def first_step(a, side):
        d = away(reach, 0)
        return remote(
            held[a].at[d], come[a].at[side, 0], ring_send.at[a, side], ring_recv.at[a, side, 0, 0],
            right if side == 0 else left, me,
        )

    def next_step(a, side, s, z):
        d = away(reach - s, side)
        return remote(
            held[a].at[d, z], come[a].at[side, s, z], ring_send.at[a, side],
            ring_recv.at[a, side, s, z], right if side == 0 else left, me,
        )

    far_most = jnp.maximum(k, count - 1 - k)
    near_most = jnp.minimum(k, count - 1 - k)
    uneven = far_most - near_most
    long_side = jnp.where(count - 1 - k > k, 1, -1)

    def chunk_at(i):
        j = jnp.maximum(i - uneven, 0)
        paired = k + (1 - 2 * (j % 2)) * (near_most - j // 2)
        return jnp.where(i < uneven, k + long_side * (far_most - i), paired)

    add_mate(away(reach, 0))
    next(small, None)
    for a in range(arrays):
        first_step(a, 0 if carried(a, 0) else 1).start()
    for s in range(1, reach):
        for side in (0, 1):
            add_mate(away(reach - s, side))
            next(small, None)
        if s == 1:
            for a in range(arrays):
                first_step(a, 0 if carried(a, 0) else 1).wait_recv()
            next(small, None)

        def pass_on(i, _, s=s):
            z = chunk_at(i)
            for side in (0, 1):
                d = away(reach - s, side)
                for a in range(arrays):
                    if s > 1:
                        next_step(a, side, s - 1, z).wait_recv()
                    if s > 1 or carried(a, side):
                        add_rows(held[a].at[d, z], held[a].at[d, z], come[a].at[side, s - 1, z])
                    next_step(a, side, s, z).start()
            return 0

        lax.fori_loop(0, count, pass_on, 0)
        next(small, None)
    add_mate(dp)
    for _ in small:
        pass

    def along(a, side, z):
        return remote(
            held[a].at[dp, z], chained[a].at[side, z], z_send.at[a, z], z_recv.at[a, side, z],
            dp, up if side == 0 else down,
        )

    def finish(i, _):
        z = chunk_at(i)
        for a in range(arrays):
            for side in (0, 1):
                next_step(a, side, reach - 1, z).wait_recv()
            add_rows(
                held[a].at[dp, z],
                held[a].at[dp, z],
                come[a].at[0, reach - 1, z],
                come[a].at[1, reach - 1, z],
            )
            for side in (0, 1):
                beyond = z > k if side == 0 else z < k
                fed = has_down if side == 0 else has_up

                @pl.when(jnp.logical_and(fed, jnp.logical_or(beyond, z == k)))
                def _(a=a, side=side):
                    along(a, side, z).wait_recv()
                    add_rows(held[a].at[dp, z], held[a].at[dp, z], chained[a].at[side, z])

                @pl.when(beyond)
                def _(a=a, side=side):
                    along(a, side, z).start()

        return 0

    lax.fori_loop(0, count, finish, 0)
    for a in range(arrays):
        add_rows(outs[a], held[a].at[dp, k])
        for side in (0, 1):
            sent = held[a].at[pl.ds(0, reach if carried(a, side) else reach - 1)]
            remote(
                sent, sent, ring_send.at[a, side], ring_recv.at[a, side, 0, 0], dp, mate
            ).wait_send()
        remote(
            given[a], given[a], mate_send.at[a], mate_recv.at[a, 0], dp, mate
        ).wait_send()

    def sent_along(z, _):
        for a in range(arrays):

            @pl.when(z != k)
            def _(a=a):
                along(a, 0, z).wait_send()

        return 0

    lax.fori_loop(0, count, sent_along, 0)


def reduce_layers(small, grads):
    size, count = lax.axis_size("dp"), lax.axis_size("fsdp") // MB
    arrays = len(grads)
    reach = size // 2
    shards = [(g.shape[0] // (size * count * MB), g.shape[1]) for g in grads]
    blocks = [g.reshape((size, count, MB) + s) for g, s in zip(grads, shards)]
    steps = len(total_partners())
    half = small.shape[0] // 2
    return comm_call(
        reduce_kernel,
        5,
        (small, *blocks),
        ((small.shape, f32),) + tuple((s, f32) for s in shards),
        tuple(pltpu.VMEM((size, count) + s, bf16) for s in shards) * 2
        + tuple(pltpu.VMEM((2, reach, count) + s, bf16) for s in shards)
        + tuple(pltpu.VMEM((2, count) + s, bf16) for s in shards)
        + (
            pltpu.SemaphoreType.DMA((arrays,)),
            pltpu.SemaphoreType.DMA((arrays,)),
            pltpu.SemaphoreType.DMA((arrays, size)),
            pltpu.SemaphoreType.DMA((arrays, 2)),
            pltpu.SemaphoreType.DMA((arrays, 2, reach, count)),
            pltpu.SemaphoreType.DMA((arrays, count)),
            pltpu.SemaphoreType.DMA((arrays, 2, count)),
            pltpu.VMEM((steps + 1, half, LANES), f32),
            pltpu.VMEM((steps + 2, half, LANES), f32),
            pltpu.SemaphoreType.DMA((steps + 2,)),
            pltpu.SemaphoreType.DMA((steps + 2,)),
        ),
        (pltpu.VMEM,) + (pl.ANY,) * arrays,
        (pltpu.VMEM,) * (1 + arrays),
        sum(g.size * 2 for g in grads),
    )


def pair_lanes(p):
    return pl.ds(pl.multiple_of(p * LANES, LANES), LANES)


def first_half(rows):
    return lax.broadcasted_iota(jnp.int32, (rows, LANES), 1) < HDIM


def spread_columns(values, column, per_pair, rows):
    half = first_half(rows)
    for p in range(PAIRS):
        left = jnp.broadcast_to(values[:, 2 * p : 2 * p + 1], (rows, LANES))
        right = jnp.broadcast_to(values[:, 2 * p + 1 : 2 * p + 2], (rows, LANES))
        if column is not None:
            column[2 * p] = left
            column[2 * p + 1] = right
        if per_pair is not None:
            per_pair[p] = jnp.where(half, left, right)


def take_vectors(layer_ref, conv_ref, head_ref, gate_ref, cw_ref, dtb_ref, al_ref, sk_ref, gg_ref):
    layer = layer_ref[0]
    cw_ref[0 : CONV + 1, :] = conv_ref[layer]
    heads = head_ref[layer]
    dtb_ref[...] = heads[0:1, :]
    al_ref[...] = heads[1:2, :]
    half = first_half(1)
    for p in range(PAIRS):
        left = jnp.broadcast_to(heads[2:3, 2 * p : 2 * p + 1], (1, LANES))
        right = jnp.broadcast_to(heads[2:3, 2 * p + 1 : 2 * p + 2], (1, LANES))
        sk_ref[p : p + 1, :] = jnp.where(half, left, right)
    gg_ref[...] = gate_ref[layer]


VECTOR_SCRATCH = (
    pltpu.VMEM((8, XBC), f32),
    pltpu.VMEM((1, LANES), f32),
    pltpu.VMEM((1, LANES), f32),
    pltpu.VMEM((PAIRS, LANES), f32),
    pltpu.VMEM((1, DI), f32),
)


def scan_kernel(
    layer_ref, proj_ref, conv_ref, head_ref, gate_ref,
    pre_ref, y_ref, yn_ref, dt_ref, cum_ref, got, halo_ref,
    cw_ref, dtb_ref, al_ref, sk_ref, gg_ref, pad, col, tcol, lcol, lrow, st, give, square, edge_send, edge_recv, send, recv,
):
    rows = proj_ref.shape[0]
    take_vectors(layer_ref, conv_ref, head_ref, gate_ref, cw_ref, dtb_ref, al_ref, sk_ref, gg_ref)
    first, final = chunk_place(1)
    chain_barrier(1, first, final)
    edge = to_next(
        proj_ref.at[pl.ds(rows - 8, 8), pl.ds(DI, XBC)], halo_ref, edge_send, edge_recv, 1
    )

    @pl.when(jnp.logical_not(final))
    def _():
        edge.start()

    @pl.when(first)
    def _():
        halo_ref[...] = jnp.zeros(halo_ref.shape, f32)
        got[...] = jnp.zeros(got.shape, bf16)

    pad[8:, :] = proj_ref[:, DI : DI + XBC]
    dt_ref[...] = jnp.zeros((rows, LANES), f32)
    dt_ref[:, 0:HEADS] = proj_ref[:, DI + XBC :]
    drive = dt_ref[...] + dtb_ref[...]
    dt = jnp.maximum(drive, 0.0) + jnp.log1p(jnp.exp(-jnp.abs(drive)))
    dt_ref[...] = dt
    rate = dt * (-jnp.exp(al_ref[...]))
    ri = lax.broadcasted_iota(jnp.int32, (rows, rows), 0)
    ci = lax.broadcasted_iota(jnp.int32, (rows, rows), 1)
    causal = ri >= ci
    cum = dot_nn(jnp.where(causal, 1.0, 0.0), rate, highest)
    cum_ref[...] = cum
    lrow[...] = cum.T
    spread_columns(cum, col, lcol, rows)
    spread_columns(dt, None, tcol, rows)

    @pl.when(jnp.logical_not(first))
    def _():
        edge.wait_recv()

    pad[0:8, :] = halo_ref[...]

    def conv(i, _):
        xs = pair_lanes(i)
        out = jnp.broadcast_to(cw_ref[CONV : CONV + 1, xs], (rows, LANES))
        for k in range(CONV):
            out = out + cw_ref[k : k + 1, xs] * pad[5 + k : 5 + k + rows, xs]
        pre_ref[:, xs] = out
        return 0

    lax.fori_loop(0, XBC // LANES, conv, 0, unroll=3)
    bm = silu(pre_ref[:, DI : DI + NSTATE]).astype(bf16)
    cm = silu(pre_ref[:, DI + NSTATE :]).astype(bf16)
    cb = dot_nt(cm, bm)
    half = first_half(rows)

    def states(p, _):
        xs = pair_lanes(p)
        lp = lcol[p]
        tail = jnp.exp(lp[rows - 1 : rows, :] - lp) * tcol[p]
        st[xs, :] = dot_tn((tail * silu(pre_ref[:, xs])).astype(bf16), bm)
        return 0

    lax.fori_loop(0, PAIRS, states, 0, unroll=4)
    square[...] = jnp.zeros(square.shape, f32)

    def pair(p):
        xs = pair_lanes(p)
        x = silu(pre_ref[:, xs])
        xtb = (tcol[p] * x).astype(bf16)
        parts = []
        for j in range(2):
            h = 2 * p + j
            c = col[h]
            d = jnp.concatenate([c] * (rows // LANES), axis=1) - lrow[pl.ds(h, 1), :]
            m = (jnp.exp(jnp.where(causal, d, OFF)) * cb).astype(bf16)
            parts.append(dot_nn(m, xtb))
        y = jnp.where(half, parts[0], parts[1]) + sk_ref[pl.ds(p, 1), :] * x
        y = y + jnp.exp(lcol[p]) * dot_nt(cm, got[xs, :])
        y_ref[:, xs] = y
        g = y * silu(proj_ref[:, xs])
        return g * g

    def step(g, _):
        chain_step(g, 1, first, final, got, give, st, col, rows, send, recv)
        total = square[...]
        for i in range(PART // LANES):
            total = total + pair(g * (PART // LANES) + i)
        square[...] = total
        return 0

    lax.fori_loop(0, CHAIN_STEPS, step, 0)
    scale = lax.rsqrt(jnp.sum(square[...], axis=1, keepdims=True) / DI + epsilon)

    def put(p, _):
        xs = pair_lanes(p)
        g = y_ref[:, xs] * silu(proj_ref[:, xs])
        yn_ref[:, xs] = (g * scale * gg_ref[0:1, xs]).astype(bf16)
        return 0

    lax.fori_loop(0, PAIRS, put, 0, unroll=4)

    @pl.when(jnp.logical_not(final))
    def _():
        edge.wait_send()

    chain_end(1, final, got, give, send, recv)


def back_kernel(
    layer_ref, dyn_ref, y_ref, proj_ref, halo_ref, pre_ref, dt_ref, cum_ref, sin_ref,
    conv_ref, head_ref, gate_ref,
    dp_ref, dcw_ref, dsm_ref, dgg_ref,
    cw_ref, dtb_ref, al_ref, sk_ref, gg_ref, pad, grad, col, tcol, lcol, lrow, dcb, dbm, dcm, dlog, dtx, ends, dy_ref, drive_ref,
    got, give, gst, dx_ref, edge_ref, from_ref, edge_send, edge_recv, send, recv,
):
    rows = y_ref.shape[0]
    take_vectors(layer_ref, conv_ref, head_ref, gate_ref, cw_ref, dtb_ref, al_ref, sk_ref, gg_ref)
    first, final = chunk_place(-1)
    chain_barrier(-1, first, final)

    @pl.when(first)
    def _():
        from_ref[...] = jnp.zeros(from_ref.shape, f32)
        got[...] = jnp.zeros(got.shape, bf16)

    cum = cum_ref[...]
    dt = dt_ref[...]
    lrow[...] = cum.T
    spread_columns(cum, col, lcol, rows)
    spread_columns(dt, None, tcol, rows)
    bm = silu(pre_ref[:, DI : DI + NSTATE]).astype(bf16)
    cm = silu(pre_ref[:, DI + NSTATE :]).astype(bf16)
    zero = jnp.zeros((rows, LANES), f32)

    def sums(p, carry):
        xs = pair_lanes(p)
        g = y_ref[:, xs] * silu(proj_ref[:, xs])
        return carry[0] + g * g, carry[1] + g * (dyn_ref[:, xs] * gg_ref[0:1, xs])

    square, cross = lax.fori_loop(0, PAIRS, sums, (zero, zero), unroll=4)
    scale = lax.rsqrt(jnp.sum(square, axis=1, keepdims=True) / DI + epsilon)
    mean = jnp.sum(cross, axis=1, keepdims=True) * scale / DI

    def ungate(p, _):
        xs = pair_lanes(p)
        z = proj_ref[:, xs]
        y = y_ref[:, xs]
        sg = lax.logistic(z)
        sz = z * sg
        ghat = y * sz * scale
        dyn = dyn_ref[:, xs]
        dgg_ref[0:1, xs] = jnp.sum(dyn * ghat, axis=0, keepdims=True)
        dg = scale * (dyn * gg_ref[0:1, xs] - ghat * mean)
        dy = dg * sz
        dy_ref[:, xs] = dy
        dp_ref[:, xs] = (dg * y * (sg * (1.0 + z * (1.0 - sg)))).astype(bf16)
        gst[xs, :] = dot_tn((jnp.exp(lcol[p]) * dy).astype(bf16), cm)
        return 0

    lax.fori_loop(0, PAIRS, ungate, 0, unroll=4)
    pad[0:8, :] = halo_ref[...]
    pad[8:, :] = proj_ref[:, DI : DI + XBC]
    grad[0:8, :] = jnp.zeros((8, XBC), f32)
    grad[rows + 8 :, :] = jnp.zeros((8, XBC), f32)
    cbt = dot_nt(bm, cm)
    ri = lax.broadcasted_iota(jnp.int32, (rows, rows), 0)
    ci = lax.broadcasted_iota(jnp.int32, (rows, rows), 1)
    causal = ri <= ci
    half = first_half(rows)
    dcb[...] = jnp.zeros((rows, rows), f32)
    dbm[...] = zero
    dcm[...] = zero
    dlog[...] = zero
    dtx[...] = zero
    ends[...] = jnp.zeros((16, LANES), f32)
    lane_row = lax.broadcasted_iota(jnp.int32, (LANES, LANES), 0)
    lane_col = lax.broadcasted_iota(jnp.int32, (LANES, LANES), 1)
    ones = jnp.ones((8, NSTATE), f32)

    def pair(p):
        xs = pair_lanes(p)
        pre = pre_ref[:, xs]
        sg = lax.logistic(pre)
        x = pre * sg
        tp = tcol[p]
        xt = tp * x
        dy = dy_ref[:, xs]
        dyb = dy.astype(bf16)
        parts = []
        for j in range(2):
            h = 2 * p + j
            c = col[h]
            d = lrow[pl.ds(h, 1), :] - jnp.concatenate([c] * (rows // LANES), axis=1)
            w = jnp.exp(jnp.where(causal, d, OFF))
            parts.append(dot_nn((w * cbt).astype(bf16), dyb))
            own = half if j == 0 else jnp.logical_not(half)
            q = dot_nt(jnp.where(own, xt, 0.0).astype(bf16), dyb)
            dcb[...] += w * q
        lp = lcol[p]
        last = lp[rows - 1 : rows, :]
        tail = jnp.exp(last - lp)
        gin = got[xs, :]
        sin = sin_ref[xs, :]
        dst = tail * dot_nt(bm, gin)
        dxt = jnp.where(half, parts[0], parts[1]) + dst
        dbm[...] += dot_nn((tail * xt).astype(bf16), gin)
        dcm[...] += dot_nn((jnp.exp(lp) * dy).astype(bf16), sin)
        sk = sk_ref[pl.ds(p, 1), :]
        pick = jnp.where(lane_col == 2 * p + jnp.where(lane_row >= HDIM, 1, 0), 1.0, 0.0)
        dlog[...] += dot_nn(dy * (y_ref[:, xs] - sk * x) - xt * dxt, pick, highest)
        dtx[...] += dot_nn(x * dxt, pick, highest)
        held = dot_nt(ones, gin.astype(f32) * sin.astype(f32), highest)
        end = jnp.sum(xt * dst, axis=0, keepdims=True) + jnp.exp(last) * held[0:1, :]
        skip = jnp.sum(dy * x, axis=0, keepdims=True)
        stacked = jnp.concatenate(
            [jnp.broadcast_to(end, (8, LANES)), jnp.broadcast_to(skip, (8, LANES))], axis=0
        )
        ends[...] += dot_nn(stacked, pick, highest)
        grad[pl.ds(8, rows), xs] = (tp * dxt + sk * dy) * (sg * (1.0 + pre * (1.0 - sg)))

    def step(g, _):
        chain_step(g, -1, first, final, got, give, gst, col, rows, send, recv)
        for i in range(PART // LANES):
            pair(g * (PART // LANES) + i)
        return 0

    lax.fori_loop(0, CHAIN_STEPS, step, 0)
    dcbb = dcb[...].astype(bf16)
    dc = dcm[...] + dot_tn(dcbb, bm)
    db = dbm[...] + dot_nn(dcbb, cm)
    grad[8 : 8 + rows, DI : DI + NSTATE] = db * silu_grad(pre_ref[:, DI : DI + NSTATE])
    grad[8 : 8 + rows, DI + NSTATE :] = dc * silu_grad(pre_ref[:, DI + NSTATE :])

    def edges(i, _):
        xs = pair_lanes(i)
        edge = jnp.zeros((8, LANES), f32)
        for k in range(CONV):
            edge = edge + cw_ref[k : k + 1, xs] * grad[3 - k : 11 - k, xs]
        edge_ref[:, xs] = edge
        return 0

    lax.fori_loop(0, XBC // LANES, edges, 0, unroll=9)
    edge = to_next(edge_ref, from_ref, edge_send, edge_recv, -1)

    @pl.when(jnp.logical_not(final))
    def _():
        edge.start()

    last_row = lax.broadcasted_iota(jnp.int32, (rows, LANES), 0) == rows - 1
    dl = dlog[...] + jnp.where(last_row, ends[0:1, :], 0.0)
    da = dot_nn(jnp.where(causal, 1.0, 0.0), dl, highest)
    decay = -jnp.exp(al_ref[...])
    ddt = dtx[...] + da * decay
    drive_ref[...] = jnp.zeros((rows, LANES), f32)
    drive_ref[:, 0:HEADS] = proj_ref[:, DI + XBC :]
    ddr = ddt * lax.logistic(drive_ref[...] + dtb_ref[...])
    dp_ref[:, DI + XBC :] = ddr[:, 0:HEADS].astype(bf16)
    dsm_ref[...] = jnp.zeros((8, LANES), f32)
    dsm_ref[0:1, :] = jnp.sum(ddr, axis=0, keepdims=True)
    dsm_ref[1:2, :] = jnp.sum(da * dt, axis=0, keepdims=True) * decay
    dsm_ref[2:3, :] = ends[8:9, :]

    def conv(i, _):
        xs = pair_lanes(i)
        own = grad[pl.ds(8, rows), xs]
        out = jnp.zeros((rows, LANES), f32)
        for k in range(CONV):
            out = out + cw_ref[k : k + 1, xs] * grad[11 - k : 11 - k + rows, xs]
            dcw_ref[k : k + 1, xs] = jnp.sum(
                own * pad[5 + k : 5 + k + rows, xs], axis=0, keepdims=True
            )
        dcw_ref[4:5, xs] = jnp.sum(own, axis=0, keepdims=True)
        dx_ref[:, xs] = out
        return 0

    lax.fori_loop(0, XBC // LANES, conv, 0, unroll=3)

    @pl.when(jnp.logical_not(first))
    def _():
        edge.wait_recv()

    dx_ref[rows - 8 :, :] += from_ref[...]
    dp_ref[:, DI : DI + XBC] = dx_ref[...].astype(bf16)

    @pl.when(jnp.logical_not(final))
    def _():
        edge.wait_send()

    chain_end(-1, final, got, give, send, recv)


VTILE = 1280
NTILE = 256


def head_specs(width, tokens):
    return dict(
        table=pl.BlockSpec((VTILE, width), lambda i: (i, 0)),
        hidden=pl.BlockSpec((tokens, width), lambda i: (0, 0)),
        kept=pl.BlockSpec((VTILE, tokens), lambda i: (i, 0)),
        row=pl.BlockSpec((1, tokens), lambda i: (0, 0)),
        tile_row=pl.BlockSpec((1, 1, tokens), lambda i: (i, 0, 0)),
    )


def head_call(kernel, grid, in_specs, out_specs, outs, scratch, ins, cells):
    return pl.pallas_call(
        kernel,
        grid=(grid,),
        in_specs=in_specs,
        out_specs=out_specs,
        out_shape=[jax.ShapeDtypeStruct(shape, kind) for shape, kind in outs],
        scratch_shapes=list(scratch),
        compiler_params=pltpu.CompilerParams(
            dimension_semantics=("arbitrary",), vmem_limit_bytes=VMEM_LIMIT
        ),
        cost_estimate=pl.CostEstimate(
            flops=2 * cells * D, transcendentals=cells, bytes_accessed=4 * cells
        ),
    )(*ins)


UNROLL = 8


def head_stats_kernel(
    lead_ref, table_ref, own_ref, lab_ref, w_ref,
    q_ref, all_ref, lse_ref, fac_ref, hit_ref,
    kept, tops, sums, hits, shown, own_sem, put_sem, z_send, z_recv, m_send, m_recv, s_send, s_recv,
):
    dp = lax.axis_index("dp")
    me = lax.axis_index("fsdp")
    shards = lax.axis_size("fsdp")
    count = shards // MB
    core = me % MB
    k = me // MB
    mate = k * MB + 1 - core
    vocab_rows = lead_ref.shape[0] + table_ref.shape[0]
    rows = own_ref.shape[0]
    tiles = tops.shape[0]
    barrier = pltpu.get_barrier_semaphore()
    for other in range(1, shards):
        pl.semaphore_signal(
            barrier, inc=1, device_id=(dp, lax.rem(me + other, shards)), device_id_type=MESH
        )
    pl.semaphore_wait(barrier, shards - 1)

    near = jnp.minimum(k, count - 1 - k)
    long_side = jnp.where(count - 1 - k > k, 1, -1)

    def chunk_at(i):
        paired = k + (2 * (i % 2) - 1) * ((i + 1) // 2)
        return jnp.where(i <= 2 * near, paired, k + long_side * (i - near))

    def along(z, side):
        at = all_ref.at[z * MB + core]
        return remote(
            at, at, z_send.at[side, z], z_recv.at[z], dp, me + MB if side == 0 else me - MB
        )

    def to_mate(z):
        at = all_ref.at[z * MB + core]
        return remote(at, at, m_send.at[z], m_recv.at[z], dp, mate)

    def from_mate(z):
        at = all_ref.at[z * MB + 1 - core]
        return remote(at, at, m_send.at[z], m_recv.at[z], dp, mate)

    keep = pltpu.make_async_copy(own_ref, all_ref.at[me], own_sem)
    keep.start()
    keep.wait()

    @pl.when(k < count - 1)
    def _():
        along(k, 0).start()

    @pl.when(k > 0)
    def _():
        along(k, 1).start()

    to_mate(k).start()
    whole = vocab_rows - vocab_rows % 16
    for slot in range(2):
        kept[slot, whole:, :] = jnp.zeros((kept.shape[1] - whole, rows), bf16)

    def put(step, b):
        return pltpu.make_async_copy(
            kept.at[step % 2],
            q_ref.at[:, pl.ds(pl.multiple_of(b * rows, rows), rows)],
            put_sem.at[step % 2],
        )

    def block(step, b):
        @pl.when(step >= 2)
        def _():
            put(step, b).wait()

        slot = step % 2
        ns = pl.ds(pl.multiple_of(b * rows, rows), rows)
        h = all_ref[b]
        label = lab_ref[0:1, ns]
        for t in range(tiles):
            first = t * VTILE
            size = min(VTILE, vocab_rows - first)
            part = lead_ref[...] if t == 0 else table_ref[first - VTILE : first - VTILE + size, :]
            logits = dot_nt(part, h)
            top = jnp.max(logits, axis=0, keepdims=True)
            p = jnp.exp(logits - top)
            kept[slot, first : first + size, :] = p.astype(bf16)
            tops[t, 0:1, ns] = top
            sums[t, 0:1, ns] = jnp.sum(p, axis=0, keepdims=True)
            rid = lax.broadcasted_iota(jnp.int32, (size, rows), 0)
            hits[t, 0:1, ns] = jnp.sum(
                jnp.where(rid == label - first, logits, 0.0), axis=0, keepdims=True
            )
        put(step, b).start()

    def chunk(i, _):
        z = chunk_at(i)

        @pl.when(jnp.logical_and(i > 0, k >= i))
        def _():
            along(k - i, 0).wait_recv()

            @pl.when(k < count - 1)
            def _():
                along(k - i, 0).start()

            to_mate(k - i).start()

        @pl.when(jnp.logical_and(i > 0, k + i < count))
        def _():
            along(k + i, 1).wait_recv()

            @pl.when(k > 0)
            def _():
                along(k + i, 1).start()

            to_mate(k + i).start()

        block(2 * i, z * MB + core)
        from_mate(z).wait_recv()
        block(2 * i + 1, z * MB + 1 - core)
        return 0

    lax.fori_loop(0, count, chunk, 0)
    top = tops[0, 0:1, :]
    for t in range(1, tiles):
        top = jnp.maximum(top, tops[t, 0:1, :])
    total = jnp.zeros_like(top)
    hit = jnp.zeros_like(top)
    for t in range(tiles):
        total = total + sums[t, 0:1, :] * jnp.exp(tops[t, 0:1, :] - top)
        hit = hit + hits[t, 0:1, :]
    hit_ref[...] = hit
    shown[me, 0:1, :] = top
    shown[me, 1:2, :] = total

    def tell(other):
        at = shown.at[me]
        return remote(
            at, at, s_send.at[other], s_recv.at[me], dp, lax.rem(me + other, shards)
        )

    def told(other):
        at = shown.at[lax.rem(me + other, shards)]
        return remote(
            at, at, s_send.at[other], s_recv.at[lax.rem(me + other, shards)], dp, mate
        )

    for other in range(1, shards):
        tell(other).start()
    for other in range(1, shards):
        told(other).wait_recv()
    top = shown[0, 0:1, :]
    for f in range(1, shards):
        top = jnp.maximum(top, shown[f, 0:1, :])
    total = jnp.zeros_like(top)
    for f in range(shards):
        total = total + shown[f, 1:2, :] * jnp.exp(shown[f, 0:1, :] - top)
    lse = top + jnp.log(total)
    lse_ref[...] = lse
    scale = w_ref[...] * (1.0 + 2.0 * z_weight * lse)
    for t in range(tiles):
        fac_ref[t, 0:1, :] = scale * jnp.exp(tops[t, 0:1, :] - lse)
    for other in range(1, shards):
        tell(other).wait_send()
    for z in range(count):

        @pl.when(jnp.logical_and(k >= z, k < count - 1))
        def _(z=z):
            along(z, 0).wait_send()

        @pl.when(jnp.logical_and(k <= z, k > 0))
        def _(z=z):
            along(z, 1).wait_send()

        to_mate(z).wait_send()
    put(0, 0).wait()
    put(1, 0).wait()


def head_stats(lead, table, own, labels, weight):
    vocab_rows, width = lead.shape[0] + table.shape[0], table.shape[1]
    rows = own.shape[0]
    shards = lax.axis_size("fsdp")
    count = shards // MB
    tokens = shards * rows
    tiles = pl.cdiv(vocab_rows, VTILE)
    kept, everyone, lse, fac, hit = comm_call(
        head_stats_kernel,
        6,
        (lead, table, own, labels, weight),
        (
            ((tiles * VTILE, tokens), bf16),
            ((shards, rows, width), bf16),
            ((1, tokens), f32),
            ((tiles, 1, tokens), f32),
            ((1, tokens), f32),
        ),
        (
            pltpu.VMEM((2, tiles * VTILE, rows), bf16),
            pltpu.VMEM((tiles, 1, tokens), f32),
            pltpu.VMEM((tiles, 1, tokens), f32),
            pltpu.VMEM((tiles, 1, tokens), f32),
            pltpu.VMEM((shards, 2, tokens), f32),
            pltpu.SemaphoreType.DMA,
            pltpu.SemaphoreType.DMA((2,)),
            pltpu.SemaphoreType.DMA((2, count)),
            pltpu.SemaphoreType.DMA((count,)),
            pltpu.SemaphoreType.DMA((count,)),
            pltpu.SemaphoreType.DMA((count,)),
            pltpu.SemaphoreType.DMA((shards,)),
            pltpu.SemaphoreType.DMA((shards,)),
        ),
        (pltpu.VMEM,) * 5,
        (pl.ANY, pltpu.VMEM, pltpu.VMEM, pltpu.VMEM, pltpu.VMEM),
        own.size * 2 * 7,
    )
    return kept, everyone.reshape(tokens, width), lse, fac, hit


def logit_grads(q, fac, weight, rid, label):
    other = weight * (0.1 / VOCAB)
    return (q.astype(f32) * fac - jnp.where(rid == label, other + 0.9 * weight, other)).astype(bf16)


def head_rows_kernel(vocab_rows, lead_ref, e_ref, q_ref, fac_ref, w_ref, lab_ref, out_ref, acc, et):
    step = pl.program_id(0)
    first = step * VTILE
    tokens = q_ref.shape[1]

    @pl.when(step == 0)
    def _():
        acc[...] = jnp.zeros(acc.shape, f32)

    eid = lax.broadcasted_iota(jnp.int32, (VTILE, e_ref.shape[1]), 0)
    part = jnp.where(step == 0, lead_ref[...], e_ref[...]).astype(f32)
    et[...] = jnp.where(eid < vocab_rows - first, part, 0.0).T.astype(bf16)

    def chunk(j, _):
        ns = pl.ds(pl.multiple_of(j * NTILE, NTILE), NTILE)
        rid = lax.broadcasted_iota(jnp.int32, (VTILE, NTILE), 0)
        dl = logit_grads(
            q_ref[:, ns], fac_ref[0, 0:1, ns], w_ref[0:1, ns], rid, lab_ref[0:1, ns] - first
        )
        acc[:, ns] += dot_nn(et[...], dl)
        return 0

    lax.fori_loop(0, tokens // NTILE, chunk, 0, unroll=UNROLL)

    @pl.when(step == pl.num_programs(0) - 1)
    def _():
        def put(j, _):
            ns = pl.ds(pl.multiple_of(j * NTILE, NTILE), NTILE)
            out_ref[ns, :] = acc[:, ns].T.astype(bf16)
            return 0

        lax.fori_loop(0, tokens // NTILE, put, 0)


def head_rows(lead, table, kept, fac, weight, labels):
    vocab_rows, width = lead.shape[0] + table.shape[0], table.shape[1]
    tokens = kept.shape[1]
    sp = head_specs(width, tokens)
    return head_call(
        functools.partial(head_rows_kernel, vocab_rows),
        pl.cdiv(vocab_rows, VTILE),
        [
            pl.BlockSpec((VTILE, width), lambda i: (0, 0)),
            pl.BlockSpec((VTILE, width), lambda i: (jnp.maximum(i - 1, 0), 0)),
            sp["kept"],
            sp["tile_row"],
            sp["row"],
            sp["row"],
        ],
        [sp["hidden"]],
        [((tokens, width), bf16)],
        (pltpu.VMEM((width, tokens), f32), pltpu.VMEM((width, VTILE), bf16)),
        (lead, table, kept, fac, weight, labels),
        vocab_rows * tokens,
    )[0]


def head_table_kernel(h_ref, q_ref, fac_ref, w_ref, lab_ref, out_ref, dl_ref):
    first = pl.program_id(0) * VTILE
    tokens = q_ref.shape[1]

    def chunk(j, _):
        ns = pl.ds(pl.multiple_of(j * NTILE, NTILE), NTILE)
        rid = lax.broadcasted_iota(jnp.int32, (VTILE, NTILE), 0)
        dl_ref[:, ns] = logit_grads(
            q_ref[:, ns], fac_ref[0, 0:1, ns], w_ref[0:1, ns], rid, lab_ref[0:1, ns] - first
        )
        return 0

    lax.fori_loop(0, tokens // NTILE, chunk, 0, unroll=UNROLL)

    def cols(j, _):
        ds = pl.ds(pl.multiple_of(j * 256, 256), 256)
        out_ref[:, ds] = dot_nn(dl_ref[...], h_ref[:, ds]).astype(bf16)
        return 0

    lax.fori_loop(0, h_ref.shape[1] // 256, cols, 0, unroll=True)


def head_table(hidden, kept, fac, weight, labels, vocab_rows):
    tokens, width = hidden.shape
    sp = head_specs(width, tokens)
    return head_call(
        head_table_kernel,
        pl.cdiv(vocab_rows, VTILE),
        [sp["hidden"], sp["kept"], sp["tile_row"], sp["row"], sp["row"]],
        [sp["table"]],
        [((vocab_rows, width), bf16)],
        (pltpu.VMEM((VTILE, tokens), bf16),),
        (hidden, kept, fac, weight, labels),
        vocab_rows * tokens,
    )[0]


def weight_grads_kernel(u_ref, dp_ref, yn_ref, db_ref, in_ref, out_ref):
    wide_cols = dp_ref.shape[1]
    for c in range(0, wide_cols, 1024):
        cs = pl.ds(c, min(1024, wide_cols - c))
        in_ref[:, cs] = dot_tn(u_ref[...], dp_ref[:, cs]).astype(bf16)
    out_ref[...] = dot_tn(yn_ref[...], db_ref[...]).astype(bf16)


def weight_grads(normed, grad_proj, mixed, grad_branch):
    rows = normed.shape[0]
    steps = D // 256
    part = DI // steps
    return head_call(
        weight_grads_kernel,
        steps,
        [
            pl.BlockSpec((rows, 256), lambda i: (0, i)),
            pl.BlockSpec((rows, ZW), lambda i: (0, 0)),
            pl.BlockSpec((rows, part), lambda i: (0, i)),
            pl.BlockSpec((rows, D), lambda i: (0, 0)),
        ],
        [pl.BlockSpec((256, ZW), lambda i: (i, 0)), pl.BlockSpec((part, D), lambda i: (i, 0))],
        [((D, ZW), bf16), ((DI, D), bf16)],
        (),
        (normed, grad_proj, mixed, grad_branch),
        rows * (ZW + DI),
    )


def after(value, earlier):
    return lax.optimization_barrier((value, earlier))[0]


def norm_scale(values):
    return lax.rsqrt(jnp.mean(values * values, axis=-1, keepdims=True) + epsilon)


def norm_back(grad, values, gain):
    scale = norm_scale(values)
    unit = values * scale
    inner = grad * gain
    back = scale * (inner - unit * jnp.mean(inner * unit, axis=-1, keepdims=True))
    return back, jnp.sum(grad * unit, axis=0)


def all_vectors(vector_params):
    rows = vector_params[: LAYERS * PER].reshape(LAYERS, PER)
    at = (CONV + 1) * XBC
    heads = rows[:, at : at + 3 * HEADS].reshape(LAYERS, 3, HEADS)
    after_heads = at + 3 * HEADS
    return dict(
        conv=rows[:, :at].reshape(LAYERS, CONV + 1, XBC),
        heads=jnp.pad(heads, ((0, 0), (0, 5), (0, LANES - HEADS))),
        gate=rows[:, after_heads + D :].reshape(LAYERS, 1, DI),
        pre=rows[:, after_heads : after_heads + D],
    )


def layer_forward(hidden, w_in, w_out, vec, layer):
    rows = hidden.shape[0]
    normed = (hidden * norm_scale(hidden) * vec["pre"][layer]).astype(bf16)
    proj = jnp.dot(normed, w_in, preferred_element_type=f32)
    pre, y, mixed, dt, cum, entering, halo = comm_call(
        scan_kernel,
        1,
        (jnp.full((1,), layer, jnp.int32), proj, vec["conv"], vec["heads"], vec["gate"]),
        (
            ((rows, XBC), f32),
            ((rows, DI), f32),
            ((rows, DI), bf16),
            ((rows, LANES), f32),
            ((rows, LANES), f32),
            ((DI, NSTATE), bf16),
            ((8, XBC), f32),
        ),
        VECTOR_SCRATCH
        + (
            pltpu.VMEM((rows + 8, XBC), f32),
            pltpu.VMEM((HEADS, rows, LANES), f32),
            pltpu.VMEM((PAIRS, rows, LANES), f32),
            pltpu.VMEM((PAIRS, rows, LANES), f32),
            pltpu.VMEM((LANES, rows), f32),
            pltpu.VMEM((DI, NSTATE), f32),
            pltpu.VMEM((DI, NSTATE), bf16),
            pltpu.VMEM((rows, LANES), f32),
            pltpu.SemaphoreType.DMA,
            pltpu.SemaphoreType.DMA,
            pltpu.SemaphoreType.DMA((CHAIN_STEPS,)),
            pltpu.SemaphoreType.DMA((CHAIN_STEPS,)),
        ),
        (pltpu.SMEM,) + (pltpu.VMEM,) * 4,
        (pltpu.VMEM,) * 7,
        DI * NSTATE * 2,
    )
    branch = jnp.dot(mixed, w_out, preferred_element_type=f32)
    record = (hidden, normed, proj, halo, pre, dt, cum, entering, y, mixed)
    return hidden + branch, record


def layer_backward(grad_hidden, w_in, w_out, vec, layer, record):
    hidden, normed, proj, halo, pre, dt, cum, entering, y, mixed = record
    rows = hidden.shape[0]
    grad_branch = grad_hidden.astype(bf16)
    grad_mixed = dot_nt(grad_branch, w_out)
    grad_proj, dconv, dsmall, dgate = comm_call(
        back_kernel,
        2,
        (
            jnp.full((1,), layer, jnp.int32), grad_mixed, y, proj, halo, pre, dt, cum, entering,
            vec["conv"], vec["heads"], vec["gate"],
        ),
        (
            ((rows, ZW), bf16),
            ((8, XBC), f32),
            ((8, LANES), f32),
            ((1, DI), f32),
        ),
        VECTOR_SCRATCH
        + (
            pltpu.VMEM((rows + 8, XBC), f32),
            pltpu.VMEM((rows + 16, XBC), f32),
            pltpu.VMEM((HEADS, rows, LANES), f32),
            pltpu.VMEM((PAIRS, rows, LANES), f32),
            pltpu.VMEM((PAIRS, rows, LANES), f32),
            pltpu.VMEM((LANES, rows), f32),
            pltpu.VMEM((rows, rows), f32),
            pltpu.VMEM((rows, LANES), f32),
            pltpu.VMEM((rows, LANES), f32),
            pltpu.VMEM((rows, LANES), f32),
            pltpu.VMEM((rows, LANES), f32),
            pltpu.VMEM((16, LANES), f32),
            pltpu.VMEM((rows, DI), f32),
            pltpu.VMEM((rows, LANES), f32),
            pltpu.VMEM((DI, NSTATE), bf16),
            pltpu.VMEM((DI, NSTATE), bf16),
            pltpu.VMEM((DI, NSTATE), f32),
            pltpu.VMEM((rows, XBC), f32),
            pltpu.VMEM((8, XBC), f32),
            pltpu.VMEM((8, XBC), f32),
            pltpu.SemaphoreType.DMA,
            pltpu.SemaphoreType.DMA,
            pltpu.SemaphoreType.DMA((CHAIN_STEPS,)),
            pltpu.SemaphoreType.DMA((CHAIN_STEPS,)),
        ),
        (pltpu.SMEM,) + (pltpu.VMEM,) * 11,
        (pltpu.VMEM,) * 4,
        DI * NSTATE * 2,
    )
    grad_normed = dot_nt(grad_proj, w_in)
    grad_in, grad_out = weight_grads(normed, grad_proj, mixed, grad_branch)
    grad_prev, dpre_gain = norm_back(grad_normed, hidden, vec["pre"][layer])
    grad_vec = jnp.concatenate(
        [
            dconv[: CONV + 1].reshape(-1),
            dsmall[0, :HEADS],
            dsmall[1, :HEADS],
            dsmall[2, :HEADS],
            dpre_gain,
            dgate[0],
        ]
    )
    return grad_hidden + grad_prev, grad_in, grad_out, grad_vec


def whole_step(
    token_ids,
    target_ids,
    seq_lengths,
    embedding,
    embedding_mom,
    embedding_avg,
    in_proj,
    in_proj_mom,
    in_proj_avg,
    out_proj,
    out_proj_mom,
    out_proj_avg,
    vector_params,
    vector_mom,
    vector_avg,
):
    groups = lax.axis_size("dp")
    shards = lax.axis_size("fsdp")
    group_index = lax.axis_index("dp")
    shard_index = lax.axis_index("fsdp")
    chunks = shards // MB
    seq_rows = token_ids.shape[2]
    rows = seq_rows // chunks
    vocab_rows, own_cols = embedding.shape
    tokens = MB * seq_rows
    total_count = jnp.sum(seq_lengths).astype(f32)
    in_low = in_proj.astype(bf16)
    out_low = out_proj.astype(bf16)

    lead = lax.all_gather(embedding[:VTILE].astype(bf16), "dp", axis=1, tiled=True)
    ids_all = group_call(share_kernel, 7, token_ids[:, 0, :], ((groups, MB, seq_rows), jnp.int32))
    ids_all = ids_all.reshape(groups, MB, chunks, rows).transpose(2, 1, 0, 3).reshape(-1)
    every = ids_all.shape[0]
    local_ids = ids_all - shard_index * vocab_rows
    inside = (local_ids >= 0) & (local_ids < vocab_rows)
    sorted_ids, sorted_tok = lax.sort(
        (jnp.where(inside, local_ids, vocab_rows), jnp.arange(every, dtype=jnp.int32)),
        num_keys=1,
    )
    held_here = sorted_ids < vocab_rows
    count = jnp.sum(held_here.astype(jnp.int32)).reshape(1)
    row_list = jnp.where(held_here, sorted_ids, 0)
    tok_list = jnp.where(held_here, sorted_tok, every)
    looked, embed_low, own_sums = local_call(
        lookup_kernel,
        (count, row_list, tok_list, embedding),
        (((every, own_cols), bf16), ((vocab_rows - VTILE, own_cols), bf16), ((8, own_cols), f32)),
        scratch=(pltpu.VMEM((every + 8, own_cols), f32),),
        in_smem=(0, 1, 2),
    )
    mine = lax.psum_scatter(
        looked.reshape(shards * groups * rows, own_cols), "fsdp", scatter_dimension=0, tiled=True
    )
    hidden = group_call(
        to_rows_kernel,
        8,
        mine.reshape(groups, rows, own_cols),
        ((rows, D), f32),
        (pltpu.VMEM((groups, rows, own_cols), bf16),),
    )

    shards = []
    for l in range(LAYERS):
        shards += [in_low[l], out_low[l]]
    shards = after(shards, looked)
    gathered = gather_layers(shards)
    w_in, w_out = gathered[0::2], gathered[1::2]
    embed_low = after(embed_low, gathered)
    table = lax.all_gather(embed_low, "dp", axis=1, tiled=True)

    vecs = all_vectors(vector_params)
    final_gain = vector_params[LAYERS * PER :]
    records = []
    for l in range(LAYERS):
        hidden, record = layer_forward(hidden, w_in[l], w_out[l], vecs, l)
        records.append(record)

    final_low = (hidden * norm_scale(hidden) * final_gain).astype(bf16)

    def in_order(per_seq):
        return per_seq.reshape(MB, chunks, rows).transpose(1, 0, 2).reshape(1, tokens)

    labels = in_order(target_ids[:, 0, :])
    lengths = lax.dynamic_index_in_dim(seq_lengths, group_index, 1, keepdims=True)
    valid = in_order((jnp.arange(seq_rows)[None, :] < lengths).astype(f32))
    local_labels = labels - shard_index * vocab_rows
    weight = valid / total_count
    kept, group_hidden, lse, fac, target = head_stats(lead, table, final_low, local_labels, weight)
    own_mask = jnp.arange(tokens) // rows == shard_index
    per_row = jnp.where(own_mask, lse[0] + z_weight * lse[0] * lse[0], 0.0)
    loss_sum = jnp.sum((per_row - 0.9 * target[0]) * valid[0])
    own_valid = lax.dynamic_slice_in_dim(valid[0], shard_index * rows, rows)
    hidden_sum = jnp.sum(final_low.astype(f32) * own_valid[:, None], axis=0)
    column_sum = jnp.zeros((groups, own_cols), f32)
    column_sum = jnp.where(
        jnp.arange(groups)[:, None] == group_index, jnp.sum(own_sums, axis=0), column_sum
    ).reshape(D)

    rows_grad = head_rows(lead, table, kept, fac, weight, local_labels)
    own_grad = lax.psum_scatter(
        rows_grad, "fsdp", scatter_dimension=0, tiled=True
    ).astype(f32)
    table_grad = head_table(group_hidden, kept, fac, weight, local_labels, vocab_rows)
    table_part = lax.psum_scatter(table_grad, "dp", scatter_dimension=1, tiled=True)

    grad_hidden, dfinal = norm_back(after(own_grad, table_grad), hidden, final_gain)
    in_parts = [None] * LAYERS
    out_parts = [None] * LAYERS
    vec_parts = [None] * LAYERS
    for l in reversed(range(LAYERS)):
        grad_hidden, grad_in, grad_out, vec_parts[l] = layer_backward(
            grad_hidden, w_in[l], w_out[l], vecs, l, records[l]
        )
        in_parts[l], out_parts[l] = grad_in, grad_out
    whole = []
    for l in range(LAYERS):
        whole += [in_parts[l], out_parts[l]]
    sent = group_call(
        to_columns_kernel,
        9,
        after(grad_hidden, whole),
        ((groups, rows, own_cols), bf16),
        (pltpu.VMEM((groups, rows, own_cols), bf16),),
    )
    whole = after(whole, sent)
    spread = lax.all_gather(sent, "fsdp", axis=0).reshape(every, own_cols)
    small = vector_params.shape[0]
    used = small + 2 * D + 1
    padded = pl.cdiv(used, 16 * LANES) * 16 * LANES
    packed = jnp.concatenate(
        vec_parts
        + [dfinal, hidden_sum, column_sum, loss_sum.reshape(1), jnp.zeros((padded - used,), f32)]
    )
    packed, *summed_parts = reduce_layers(packed.reshape(-1, LANES), whole)
    spread = after(spread, summed_parts)
    table_total, table_squares = local_call(
        spread_kernel,
        (count, row_list, tok_list, spread, table_part),
        (((vocab_rows, own_cols), f32), ((8, own_cols), f32)),
        scratch=(pltpu.VMEM((every + 8, own_cols), f32),),
        in_smem=(0, 1, 2),
    )
    owner_squares = jnp.sum(table_squares)
    for part in summed_parts:
        owner_squares = owner_squares + jnp.sum(part * part)
    squares = jnp.pad(owner_squares.reshape(1, 1), ((0, 7), (0, LANES - 1)))
    norms = norm_of(squares, packed, small)
    factor = norms[1, 0]
    updated = []
    for master, moment, average, grad in (
        (embedding, embedding_mom, embedding_avg, table_total),
        (in_proj, in_proj_mom, in_proj_avg, jnp.stack(summed_parts[0::2])),
        (out_proj, out_proj_mom, out_proj_avg, jnp.stack(summed_parts[1::2])),
    ):
        new = stepped(master, moment, average, grad, factor)
        updated += [*new, new[0].astype(bf16)]
    packed = packed.reshape(-1)
    vector_total = packed[:small]
    hidden_total = packed[small : small + D]
    column_total = packed[small + D : small + 2 * D]
    mean_part = jnp.sum(hidden_total * column_total) * (0.1 / VOCAB)
    loss_value = (packed[used - 1] - mean_part) / total_count
    vector_new, vector_mom_new, vector_avg_new = stepped(
        vector_params, vector_mom, vector_avg, vector_total, factor
    )
    return (
        loss_value,
        norms[0, 0],
        *updated,
        vector_new,
        vector_mom_new,
        vector_avg_new,
        vector_new.astype(bf16),
    )


def solution(mesh):
    table_spec = P("fsdp", "dp")
    weight_spec = P(None, ("dp", "fsdp"), None)
    return jax.shard_map(
        whole_step,
        mesh=mesh,
        in_specs=(
            P(None, "dp", None),
            P(None, "dp", None),
            P(),
            *(table_spec,) * 3,
            *(weight_spec,) * 6,
            *(P(),) * 3,
        ),
        out_specs=(
            P(),
            P(),
            *(table_spec,) * 4,
            *(weight_spec,) * 8,
            *(P(),) * 4,
        ),
        check_vma=False,
    )
```

```python
import functools

import jax
import jax.numpy as jnp
from jax import lax
from jax.experimental import pallas as pl
from jax.experimental.pallas import tpu as pltpu
from jax.sharding import PartitionSpec as P


D = 1024
HEADS = 32
HDIM = 64
NSTATE = 128
CONV = 4
VOCAB = 50288
LAYERS = 2
MB = 2
DI = 2048
XBC = 2304
ZW = 4384
PER = 14688
LANES = 128
PAIRS = DI // LANES

epsilon = 1e-05
z_weight = 0.001
clip_limit = 0.2
step_rate = 1000.0
highest = lax.Precision.HIGHEST
bf16 = jnp.bfloat16
f32 = jnp.float32
VMEM_LIMIT = 62 * 1024 * 1024
OFF = -1e30


def dot_nn(a, b, precision=None):
    return lax.dot_general(
        a, b, (((1,), (0,)), ((), ())), precision=precision, preferred_element_type=f32
    )


def dot_nt(a, b, precision=None):
    return lax.dot_general(
        a, b, (((1,), (1,)), ((), ())), precision=precision, preferred_element_type=f32
    )


def dot_tn(a, b, precision=None):
    return lax.dot_general(
        a, b, (((0,), (0,)), ((), ())), precision=precision, preferred_element_type=f32
    )


def silu(v):
    return v * lax.logistic(v)


def silu_grad(v):
    s = lax.logistic(v)
    return s * (1.0 + v * (1.0 - s))


def local_call(kernel, ins, outs, scratch=(), in_smem=(), flops=0):
    total = sum(a.size * a.dtype.itemsize for a in ins)
    return pl.pallas_call(
        kernel,
        out_shape=[jax.ShapeDtypeStruct(shape, kind) for shape, kind in outs],
        in_specs=[
            pl.BlockSpec(memory_space=pltpu.SMEM if i in in_smem else pltpu.VMEM)
            for i in range(len(ins))
        ],
        out_specs=[pl.BlockSpec(memory_space=pltpu.VMEM) for _ in outs],
        scratch_shapes=list(scratch),
        compiler_params=pltpu.CompilerParams(vmem_limit_bytes=VMEM_LIMIT),
        cost_estimate=pl.CostEstimate(
            flops=flops or total, transcendentals=0, bytes_accessed=2 * total
        ),
    )(*ins)


def lookup_kernel(count_ref, row_ref, tok_ref, table_ref, out_ref, low_ref, sum_ref, held):
    tokens = out_ref.shape[0]
    step = 512

    def clear(i, _):
        held[pl.ds(pl.multiple_of(i * step, step), step), :] = jnp.zeros(
            (step, held.shape[1]), f32
        )
        return 0

    lax.fori_loop(0, tokens // step, clear, 0)

    def move(i, _):
        for k in range(8):
            row = row_ref[i * 8 + k]
            tok = tok_ref[i * 8 + k]
            held[pl.ds(tok, 1), :] = table_ref[pl.ds(row, 1), :]
        return 0

    lax.fori_loop(0, (count_ref[0] + 7) // 8, move, 0)

    def put(i, _):
        rows = pl.ds(pl.multiple_of(i * step, step), step)
        out_ref[rows, :] = held[rows, :].astype(bf16)
        return 0

    lax.fori_loop(0, tokens // step, put, 0)
    rows_all = table_ref.shape[0]
    part = VTILE // 5
    whole = rows_all // part

    def low_rows(i):
        return table_ref[pl.ds(pl.multiple_of(i * part, part), part), :].astype(bf16)

    def add(low, total):
        return total + jnp.sum(low.astype(f32).reshape(part // 8, 8, -1), axis=0)

    def cast(i, total):
        low = low_rows(i)
        low_ref[pl.ds(pl.multiple_of(i * part - VTILE, part), part), :] = low
        return add(low, total)

    total = lax.fori_loop(
        0, VTILE // part, lambda i, t: add(low_rows(i), t), jnp.zeros(sum_ref.shape, f32)
    )
    sum_ref[...] = lax.fori_loop(VTILE // part, whole, cast, total)
    if rows_all > whole * part:
        low = table_ref[whole * part :, :].astype(bf16)
        low_ref[whole * part - VTILE :, :] = low
        sum_ref[0:1, :] += jnp.sum(low.astype(f32), axis=0, keepdims=True)


def spread_kernel(count_ref, row_ref, tok_ref, grad_ref, base_ref, out_ref, square_ref, held):
    tokens = grad_ref.shape[0]
    step = 512
    rows_all = out_ref.shape[0]

    def take(i, _):
        rows = pl.ds(pl.multiple_of(i * step, step), step)
        held[rows, :] = grad_ref[rows, :].astype(f32)
        return 0

    lax.fori_loop(0, tokens // step, take, 0)
    held[pl.ds(tokens, 8), :] = jnp.zeros((8, held.shape[1]), f32)

    whole = rows_all // step

    def start(i, _):
        rows = pl.ds(pl.multiple_of(i * step, step), step)
        out_ref[rows, :] = base_ref[rows, :].astype(f32)
        return 0

    lax.fori_loop(0, whole, start, 0)
    if rows_all > whole * step:
        out_ref[whole * step :, :] = base_ref[whole * step :, :].astype(f32)

    def move(i, _):
        for k in range(8):
            row = row_ref[i * 8 + k]
            tok = tok_ref[i * 8 + k]
            out_ref[pl.ds(row, 1), :] = out_ref[pl.ds(row, 1), :] + held[pl.ds(tok, 1), :]
        return 0

    lax.fori_loop(0, (count_ref[0] + 7) // 8, move, 0)

    def square(i, total):
        part = out_ref[pl.ds(pl.multiple_of(i * step, step), step), :]
        return total + jnp.sum((part * part).reshape(step // 8, 8, -1), axis=0)

    total = lax.fori_loop(0, whole, square, jnp.zeros(square_ref.shape, f32))
    square_ref[...] = total
    if rows_all > whole * step:
        part = out_ref[whole * step :, :]
        square_ref[0:1, :] += jnp.sum(part * part, axis=0, keepdims=True)


MESH = pl.DeviceIdType.MESH


def remote(src, dst, send, recv, dp, fsdp):
    return pltpu.make_async_remote_copy(
        src_ref=src,
        dst_ref=dst,
        send_sem=send,
        recv_sem=recv,
        device_id=(dp, fsdp),
        device_id_type=MESH,
    )


def comm_call(kernel, number, ins, outs, scratch, in_spaces, out_spaces, sent):
    return pl.pallas_call(
        kernel,
        out_shape=[jax.ShapeDtypeStruct(shape, kind) for shape, kind in outs],
        in_specs=[pl.BlockSpec(memory_space=space) for space in in_spaces],
        out_specs=[pl.BlockSpec(memory_space=space) for space in out_spaces],
        scratch_shapes=list(scratch),
        compiler_params=pltpu.CompilerParams(
            collective_id=number, has_side_effects=True, vmem_limit_bytes=VMEM_LIMIT
        ),
        cost_estimate=pl.CostEstimate(flops=sent, transcendentals=0, bytes_accessed=2 * sent),
    )(*ins)


def greet_groups():
    dp = lax.axis_index("dp")
    me = lax.axis_index("fsdp")
    groups = lax.axis_size("dp")
    barrier = pltpu.get_barrier_semaphore()
    others = [lax.rem(dp + other, groups) for other in range(1, groups)]
    for other in others:
        pl.semaphore_signal(barrier, inc=1, device_id=(other, me), device_id_type=MESH)
    pl.semaphore_wait(barrier, groups - 1)
    return dp, me, others


def share_kernel(in_ref, out_ref, send, recv):
    dp, me, others = greet_groups()
    for other in others:
        remote(in_ref, out_ref.at[dp], send.at[other], recv.at[dp], other, me).start()
    out_ref[dp] = in_ref[...]
    for other in others:
        copy = remote(in_ref, out_ref.at[other], send.at[other], recv.at[other], other, me)
        copy.wait_recv()
        copy.wait_send()


def to_rows_kernel(in_ref, out_ref, landed, send, recv):
    dp, me, others = greet_groups()
    for other in others:
        remote(in_ref.at[other], landed.at[dp], send.at[other], recv.at[dp], other, me).start()
    landed[dp] = in_ref[dp]
    for other in others:
        remote(in_ref.at[other], landed.at[other], send.at[other], recv.at[other], other, me).wait_recv()
    cols = in_ref.shape[2]
    for g in range(in_ref.shape[0]):
        out_ref[:, g * cols : (g + 1) * cols] = landed[g].astype(f32)
    for other in others:
        remote(in_ref.at[other], landed.at[other], send.at[other], recv.at[other], other, me).wait_send()


def to_columns_kernel(in_ref, out_ref, parts, send, recv):
    dp, me, others = greet_groups()
    cols = out_ref.shape[2]
    for g in range(out_ref.shape[0]):
        parts[g] = in_ref[:, g * cols : (g + 1) * cols].astype(bf16)
    for other in others:
        remote(parts.at[other], out_ref.at[dp], send.at[other], recv.at[dp], other, me).start()
    out_ref[dp] = parts[dp]
    for other in others:
        copy = remote(parts.at[other], out_ref.at[other], send.at[other], recv.at[other], other, me)
        copy.wait_recv()
        copy.wait_send()


def group_call(kernel, number, array, out, scratch=()):
    groups = lax.axis_size("dp")
    return comm_call(
        kernel,
        number,
        (array,),
        (out,),
        tuple(scratch)
        + (pltpu.SemaphoreType.DMA((groups,)), pltpu.SemaphoreType.DMA((groups,))),
        (pltpu.VMEM,),
        (pltpu.VMEM,),
        array.size * 2,
    )[0]


CHAIN_STEPS = 8
PART = DI // CHAIN_STEPS


def chunk_place(direction):
    place = lax.axis_index("fsdp") // MB
    count = lax.axis_size("fsdp") // MB
    first = place == (0 if direction > 0 else count - 1)
    final = place == (count - 1 if direction > 0 else 0)
    return first, final


def chain_barrier(direction, first, final):
    dp = lax.axis_index("dp")
    me = lax.axis_index("fsdp")
    barrier = pltpu.get_barrier_semaphore()

    @pl.when(jnp.logical_not(first))
    def _():
        pl.semaphore_signal(
            barrier, inc=1, device_id=(dp, me - MB * direction), device_id_type=MESH
        )

    @pl.when(jnp.logical_not(final))
    def _():
        pl.semaphore_wait(barrier, 1)


def to_next(src, dst, send, recv, direction):
    dp = lax.axis_index("dp")
    return remote(src, dst, send, recv, dp, lax.axis_index("fsdp") + MB * direction)


def chain_step(g, direction, first, final, got, give, local, col, rows, send, recv):
    def copy():
        at = pl.ds(pl.multiple_of(g * PART, PART), PART)
        return to_next(give.at[at], got.at[at], send.at[g], recv.at[g], direction)

    @pl.when(jnp.logical_not(first))
    def _():
        copy().wait_recv()

    @pl.when(jnp.logical_not(final))
    def _():
        for i in range(PART // HDIM):
            h = pl.ds(pl.multiple_of(g * PART + i * HDIM, HDIM), HDIM)
            decay = jnp.exp(col[g * (PART // HDIM) + i, rows - 1 : rows, :])
            give[h, :] = (decay * got[h, :].astype(f32) + local[h, :]).astype(bf16)
        copy().start()


def chain_end(direction, final, got, give, send, recv):
    @pl.when(jnp.logical_not(final))
    def _():
        for g in range(CHAIN_STEPS):
            at = pl.ds(g * PART, PART)
            to_next(give.at[at], got.at[at], send.at[g], recv.at[g], direction).wait_send()


def bits_of(size):
    return [1 << b for b in range(size.bit_length() - 1)]


def stepped(weight, moment, average, grad, factor):
    scaled = grad * factor
    moment_new = 0.5 * moment + scaled
    weight_new = weight - step_rate * (scaled + 0.5 * moment_new)
    return weight_new, moment_new, 0.5 * average + 0.5 * weight_new


def total_kernel(small, squares_at, packed_ref, total_ref, norm_ref, work, got, send, recv):
    dp = lax.axis_index("dp")
    me = lax.axis_index("fsdp")
    half = packed_ref.shape[0] // 2
    core = me % MB
    partners = [("f", b) for b in bits_of(lax.axis_size("fsdp")) if b > 1]
    partners += [("d", b) for b in bits_of(lax.axis_size("dp"))]

    def across(kind, bit):
        ids, other = (me, lambda v: (dp, v)) if kind == "f" else (dp, lambda v: (v, me))
        return other(jnp.where((ids // bit) % 2 == 1, ids - bit, ids + bit))

    mate = across("f", 1)
    barrier = pltpu.get_barrier_semaphore()
    for target in [mate] + [across(*p) for p in partners]:
        pl.semaphore_signal(barrier, inc=1, device_id=target, device_id_type=MESH)
    pl.semaphore_wait(barrier, 1 + len(partners))

    mine = pl.ds(pl.multiple_of(core * half, 8), half)
    theirs = pl.ds(pl.multiple_of((1 - core) * half, 8), half)
    copy = remote(packed_ref.at[theirs], got.at[0], send.at[0], recv.at[0], *mate)
    copy.start()
    copy.wait()
    work[0] = packed_ref[mine, :] + got[0]
    for i, p in enumerate(partners):
        copy = remote(work.at[i], got.at[i + 1], send.at[i + 1], recv.at[i + 1], *across(*p))
        copy.start()
        copy.wait()
        work[i + 1] = work[i] + got[i + 1]
    n = len(partners)
    copy = remote(work.at[n], got.at[n + 1], send.at[n + 1], recv.at[n + 1], *mate)
    copy.start()
    copy.wait()
    total_ref[mine, :] = work[n]
    total_ref[theirs, :] = got[n + 1]

    total = total_ref[...]
    index = lax.broadcasted_iota(jnp.int32, total.shape, 0) * LANES
    index = index + lax.broadcasted_iota(jnp.int32, total.shape, 1)
    parts = jnp.where(index < small, total * total, jnp.where(index == squares_at, total, 0.0))
    square = jnp.sum(jnp.sum(parts, axis=0, keepdims=True), axis=1, keepdims=True)
    norm = jnp.sqrt(square)
    factor = jnp.minimum(1.0, clip_limit / norm)
    norm_ref[0:1, :] = jnp.broadcast_to(norm, (1, LANES))
    norm_ref[1:2, :] = jnp.broadcast_to(factor, (1, LANES))
    norm_ref[2:8, :] = jnp.zeros((6, LANES), f32)


def total_of(packed, small, squares_at):
    steps = len(bits_of(lax.axis_size("fsdp"))) - 1 + len(bits_of(lax.axis_size("dp")))
    rows = packed.shape[0]
    return comm_call(
        functools.partial(total_kernel, small, squares_at),
        3,
        (packed,),
        ((packed.shape, f32), ((8, LANES), f32)),
        (
            pltpu.VMEM((steps + 1, rows // 2, LANES), f32),
            pltpu.VMEM((steps + 2, rows // 2, LANES), f32),
            pltpu.SemaphoreType.DMA((steps + 2,)),
            pltpu.SemaphoreType.DMA((steps + 2,)),
        ),
        (pltpu.VMEM,),
        (pltpu.VMEM, pltpu.VMEM),
        packed.size * 4 * 3,
    )


def snake(place, size):
    return jnp.where(place < size // 2, place, size // 2 + size - 1 - place)


def wrap(value, size):
    return lax.rem(value + size, size)


def gather_kernel(*refs):
    arrays = 2 * LAYERS
    own = refs[:arrays]
    full = refs[arrays : 2 * arrays]
    local_sem, z_send, z_recv, ring_send, ring_recv, mate_send, mate_recv = refs[2 * arrays :]
    dp = lax.axis_index("dp")
    me = lax.axis_index("fsdp")
    size = lax.axis_size("dp")
    count = lax.axis_size("fsdp") // MB
    core = me % MB
    k = me // MB
    ring = snake(dp, size)
    reach = size // 2
    right = snake(wrap(ring + 1, size), size)
    left = snake(wrap(ring - 1, size), size)
    mate = k * MB + 1 - core
    up, down = me + MB, me - MB
    has_up, has_down = k < count - 1, k > 0
    barrier = pltpu.get_barrier_semaphore()
    for target in ((right, me), (left, me), (dp, mate)):
        pl.semaphore_signal(barrier, inc=1, device_id=target, device_id_type=MESH)

    @pl.when(has_up)
    def _():
        pl.semaphore_signal(barrier, inc=1, device_id=(dp, up), device_id_type=MESH)

    @pl.when(has_down)
    def _():
        pl.semaphore_signal(barrier, inc=1, device_id=(dp, down), device_id_type=MESH)

    pl.semaphore_wait(barrier, 3 + jnp.where(has_up, 1, 0) + jnp.where(has_down, 1, 0))

    def spot(a, d, z, c):
        return full[a].at[d, z, c]

    def chain(a, src, z, side):
        return remote(
            src, spot(a, dp, z, core), z_send.at[a, z], z_recv.at[a, z], dp, up if side == 0 else down
        )

    def chain_own(a, side):
        return remote(
            own[a],
            spot(a, dp, k, core),
            z_send.at[a, count + side],
            z_recv.at[a, k],
            dp,
            up if side == 0 else down,
        )

    def round_ring(a, src, d, z, side):
        return remote(
            src,
            spot(a, d, z, core),
            ring_send.at[a, side],
            ring_recv.at[a, d, z],
            right if side == 0 else left,
            me,
        )

    def to_mate(a, src, d, z):
        return remote(src, spot(a, d, z, core), mate_send.at[a], mate_recv.at[a], dp, mate)

    def carried(a, side):
        return (a < arrays // 2) == (side == 0)

    for a in range(arrays):

        @pl.when(has_up)
        def _(a=a):
            chain_own(a, 0).start()

        @pl.when(has_down)
        def _(a=a):
            chain_own(a, 1).start()

    for a in range(arrays):
        for side in (0, 1):
            round_ring(a, own[a], dp, k, side).start()
    for a in range(arrays):
        to_mate(a, own[a], dp, k).start()
        pltpu.make_async_copy(own[a], spot(a, dp, k, core), local_sem.at[a]).start()

    def ring_step(z, s):
        for side in (0, 1):
            origin = snake(wrap(ring - s if side == 0 else ring + s, size), size)
            for a in range(arrays):
                if s == reach and not carried(a, side):
                    continue
                piece = spot(a, origin, z, core)
                round_ring(a, piece, origin, z, side).wait_recv()
                if s + 1 < reach or (s + 1 == reach and carried(a, side)):
                    round_ring(a, piece, origin, z, side).start()
                to_mate(a, piece, origin, z).start()

    def arrive(z, side):
        for a in range(arrays):
            piece = spot(a, dp, z, core)
            chain(a, piece, z, side).wait_recv()

            @pl.when(has_up if side == 0 else has_down)
            def _(a=a, piece=piece):
                chain(a, piece, z, side).start()

            for way in (0, 1):
                round_ring(a, piece, dp, z, way).start()
            to_mate(a, piece, dp, z).start()

    def both_ways(far, act):
        if far == 0:
            act(k, 0)
            return

        @pl.when(k >= far)
        def _():
            act(k - far, 0)

        @pl.when(k + far < count)
        def _():
            act(k + far, 1)

    for turn in range(1, count + reach):
        if turn < count:
            both_ways(turn, arrive)
        for s in range(1, reach + 1):
            if 0 <= turn - s < count:
                both_ways(turn - s, lambda z, side, s=s: ring_step(z, s))

    for a in range(arrays):
        pltpu.make_async_copy(own[a], spot(a, dp, k, core), local_sem.at[a]).wait()
        for side in (0, 1):
            sent = full[a].at[pl.ds(0, reach if carried(a, side) else reach - 1), :, core]
            remote(sent, sent, ring_send.at[a, side], ring_recv.at[a, 0, 0], dp, mate).wait_send()
        whole = full[a].at[:, :, core]
        remote(whole, whole, mate_send.at[a], mate_recv.at[a], dp, mate).wait_send()
        whole = full[a].at[:, :, 1 - core]
        remote(whole, whole, mate_send.at[a], mate_recv.at[a], dp, mate).wait_recv()

        @pl.when(has_up)
        def _(a=a):
            chain_own(a, 0).wait_send()

        @pl.when(has_down)
        def _(a=a):
            chain_own(a, 1).wait_send()

        for far in range(1, count):

            @pl.when(jnp.logical_and(k >= far, has_up))
            def _(a=a, far=far):
                chain(a, spot(a, dp, k - far, core), k - far, 0).wait_send()

            @pl.when(jnp.logical_and(k + far < count, has_down))
            def _(a=a, far=far):
                chain(a, spot(a, dp, k + far, core), k + far, 1).wait_send()


def gather_layers(shards):
    size, count = lax.axis_size("dp"), lax.axis_size("fsdp") // MB
    arrays = len(shards)
    outs = comm_call(
        gather_kernel,
        4,
        shards,
        tuple(((size, count, MB) + s.shape, bf16) for s in shards),
        (
            pltpu.SemaphoreType.DMA((arrays,)),
            pltpu.SemaphoreType.DMA((arrays, count + 2)),
            pltpu.SemaphoreType.DMA((arrays, count)),
            pltpu.SemaphoreType.DMA((arrays, 2)),
            pltpu.SemaphoreType.DMA((arrays, size, count)),
            pltpu.SemaphoreType.DMA((arrays,)),
            pltpu.SemaphoreType.DMA((arrays,)),
        ),
        (pltpu.VMEM,) * arrays,
        (pl.ANY,) * arrays,
        sum(s.size * 2 for s in shards) * 24,
    )
    return [o.reshape(size * count * MB * s.shape[0], s.shape[1]) for o, s in zip(outs, shards)]


def add_rows(dst, first, *others):
    rows = dst.shape[0]
    step = min(rows, 16)

    def one(i, _):
        at = pl.ds(pl.multiple_of(i * step, step), step)
        total = first[at, :].astype(f32)
        for other in others:
            total = total + other[at, :].astype(f32)
        dst[at, :] = total.astype(dst.dtype)
        return 0

    lax.fori_loop(0, rows // step, one, 0)


def reduce_kernel(*refs):
    arrays = 2 * LAYERS
    grads = refs[:arrays]
    outs = refs[arrays : 2 * arrays]
    held, given, come, chained = (
        refs[(2 + i) * arrays : (3 + i) * arrays] for i in range(4)
    )
    load_sem, mate_send, mate_recv, ring_send, ring_recv, z_send, z_recv = refs[6 * arrays :]
    dp = lax.axis_index("dp")
    me = lax.axis_index("fsdp")
    size = lax.axis_size("dp")
    count = lax.axis_size("fsdp") // MB
    core = me % MB
    k = me // MB
    ring = snake(dp, size)
    reach = size // 2
    right = snake(wrap(ring + 1, size), size)
    left = snake(wrap(ring - 1, size), size)
    mate = k * MB + 1 - core
    up, down = me + MB, me - MB
    has_up, has_down = k < count - 1, k > 0

    def load(a):
        return pltpu.make_async_copy(grads[a].at[:, :, core], held[a], load_sem.at[a])

    for a in range(arrays):
        load(a).start()
    barrier = pltpu.get_barrier_semaphore()
    for target in ((right, me), (left, me), (dp, mate)):
        pl.semaphore_signal(barrier, inc=1, device_id=target, device_id_type=MESH)

    @pl.when(has_up)
    def _():
        pl.semaphore_signal(barrier, inc=1, device_id=(dp, up), device_id_type=MESH)

    @pl.when(has_down)
    def _():
        pl.semaphore_signal(barrier, inc=1, device_id=(dp, down), device_id_type=MESH)

    pl.semaphore_wait(barrier, 3 + jnp.where(has_up, 1, 0) + jnp.where(has_down, 1, 0))

    def away(j, side):
        return snake(wrap(ring + j if side == 0 else ring - j, size), size)

    def to_mate(a, d):
        return remote(
            grads[a].at[d, :, 1 - core], given[a].at[d], mate_send.at[a], mate_recv.at[a, d], dp, mate
        )

    def carried(a, side):
        return (a < arrays // 2) == (side == 0)

    def targets(j):
        if j == 0:
            return [dp]
        if j == reach:
            return [away(j, 0)]
        return [away(j, 0), away(j, 1)]

    for j in range(reach, -1, -1):
        for d in targets(j):
            for a in range(arrays):
                to_mate(a, d).start()

    for a in range(arrays):
        load(a).wait()

    def add_mate(d):
        for a in range(arrays):
            to_mate(a, d).wait_recv()

            def one(z, _, a=a):
                add_rows(held[a].at[d, z], held[a].at[d, z], given[a].at[d, z])
                return 0

            lax.fori_loop(0, count, one, 0)

    def first_step(a, side):
        d = away(reach, 0)
        return remote(
            held[a].at[d], come[a].at[side, 0], ring_send.at[a, side], ring_recv.at[a, side, 0, 0],
            right if side == 0 else left, me,
        )

    def next_step(a, side, s, z):
        d = away(reach - s, side)
        return remote(
            held[a].at[d, z], come[a].at[side, s, z], ring_send.at[a, side],
            ring_recv.at[a, side, s, z], right if side == 0 else left, me,
        )

    far_most = jnp.maximum(k, count - 1 - k)
    near_most = jnp.minimum(k, count - 1 - k)
    uneven = far_most - near_most
    long_side = jnp.where(count - 1 - k > k, 1, -1)

    def chunk_at(i):
        j = jnp.maximum(i - uneven, 0)
        paired = k + (1 - 2 * (j % 2)) * (near_most - j // 2)
        return jnp.where(i < uneven, k + long_side * (far_most - i), paired)

    add_mate(away(reach, 0))
    for a in range(arrays):
        first_step(a, 0 if carried(a, 0) else 1).start()
    for s in range(1, reach):
        for side in (0, 1):
            add_mate(away(reach - s, side))
        if s == 1:
            for a in range(arrays):
                first_step(a, 0 if carried(a, 0) else 1).wait_recv()

        def pass_on(i, _, s=s):
            z = chunk_at(i)
            for side in (0, 1):
                d = away(reach - s, side)
                for a in range(arrays):
                    if s > 1:
                        next_step(a, side, s - 1, z).wait_recv()
                    if s > 1 or carried(a, side):
                        add_rows(held[a].at[d, z], held[a].at[d, z], come[a].at[side, s - 1, z])
                    next_step(a, side, s, z).start()
            return 0

        lax.fori_loop(0, count, pass_on, 0)
    add_mate(dp)

    def along(a, side, z):
        return remote(
            held[a].at[dp, z], chained[a].at[side, z], z_send.at[a, z], z_recv.at[a, side, z],
            dp, up if side == 0 else down,
        )

    def finish(i, _):
        z = chunk_at(i)
        for a in range(arrays):
            for side in (0, 1):
                next_step(a, side, reach - 1, z).wait_recv()
            add_rows(
                held[a].at[dp, z],
                held[a].at[dp, z],
                come[a].at[0, reach - 1, z],
                come[a].at[1, reach - 1, z],
            )
            for side in (0, 1):
                beyond = z > k if side == 0 else z < k
                fed = has_down if side == 0 else has_up

                @pl.when(jnp.logical_and(fed, jnp.logical_or(beyond, z == k)))
                def _(a=a, side=side):
                    along(a, side, z).wait_recv()
                    add_rows(held[a].at[dp, z], held[a].at[dp, z], chained[a].at[side, z])

                @pl.when(beyond)
                def _(a=a, side=side):
                    along(a, side, z).start()

        return 0

    lax.fori_loop(0, count, finish, 0)
    for a in range(arrays):
        add_rows(outs[a], held[a].at[dp, k])
        for side in (0, 1):
            sent = held[a].at[pl.ds(0, reach if carried(a, side) else reach - 1)]
            remote(
                sent, sent, ring_send.at[a, side], ring_recv.at[a, side, 0, 0], dp, mate
            ).wait_send()
        remote(
            given[a], given[a], mate_send.at[a], mate_recv.at[a, 0], dp, mate
        ).wait_send()

    def sent_along(z, _):
        for a in range(arrays):

            @pl.when(z != k)
            def _(a=a):
                along(a, 0, z).wait_send()

        return 0

    lax.fori_loop(0, count, sent_along, 0)


def reduce_layers(grads):
    size, count = lax.axis_size("dp"), lax.axis_size("fsdp") // MB
    arrays = len(grads)
    reach = size // 2
    shards = [(g.shape[0] // (size * count * MB), g.shape[1]) for g in grads]
    blocks = [g.reshape((size, count, MB) + s) for g, s in zip(grads, shards)]
    return comm_call(
        reduce_kernel,
        5,
        blocks,
        tuple((s, f32) for s in shards),
        tuple(pltpu.VMEM((size, count) + s, bf16) for s in shards) * 2
        + tuple(pltpu.VMEM((2, reach, count) + s, bf16) for s in shards)
        + tuple(pltpu.VMEM((2, count) + s, bf16) for s in shards)
        + (
            pltpu.SemaphoreType.DMA((arrays,)),
            pltpu.SemaphoreType.DMA((arrays,)),
            pltpu.SemaphoreType.DMA((arrays, size)),
            pltpu.SemaphoreType.DMA((arrays, 2)),
            pltpu.SemaphoreType.DMA((arrays, 2, reach, count)),
            pltpu.SemaphoreType.DMA((arrays, count)),
            pltpu.SemaphoreType.DMA((arrays, 2, count)),
        ),
        (pl.ANY,) * arrays,
        (pltpu.VMEM,) * arrays,
        sum(g.size * 2 for g in grads),
    )


def pair_lanes(p):
    return pl.ds(pl.multiple_of(p * LANES, LANES), LANES)


def first_half(rows):
    return lax.broadcasted_iota(jnp.int32, (rows, LANES), 1) < HDIM


def spread_columns(values, column, per_pair, rows):
    half = first_half(rows)
    for p in range(PAIRS):
        left = jnp.broadcast_to(values[:, 2 * p : 2 * p + 1], (rows, LANES))
        right = jnp.broadcast_to(values[:, 2 * p + 1 : 2 * p + 2], (rows, LANES))
        if column is not None:
            column[2 * p] = left
            column[2 * p + 1] = right
        if per_pair is not None:
            per_pair[p] = jnp.where(half, left, right)


def take_vectors(layer_ref, conv_ref, head_ref, gate_ref, cw_ref, dtb_ref, al_ref, sk_ref, gg_ref):
    layer = layer_ref[0]
    cw_ref[0 : CONV + 1, :] = conv_ref[layer]
    heads = head_ref[layer]
    dtb_ref[...] = heads[0:1, :]
    al_ref[...] = heads[1:2, :]
    half = first_half(1)
    for p in range(PAIRS):
        left = jnp.broadcast_to(heads[2:3, 2 * p : 2 * p + 1], (1, LANES))
        right = jnp.broadcast_to(heads[2:3, 2 * p + 1 : 2 * p + 2], (1, LANES))
        sk_ref[p : p + 1, :] = jnp.where(half, left, right)
    gg_ref[...] = gate_ref[layer]


VECTOR_SCRATCH = (
    pltpu.VMEM((8, XBC), f32),
    pltpu.VMEM((1, LANES), f32),
    pltpu.VMEM((1, LANES), f32),
    pltpu.VMEM((PAIRS, LANES), f32),
    pltpu.VMEM((1, DI), f32),
)


def scan_kernel(
    layer_ref, proj_ref, conv_ref, head_ref, gate_ref,
    pre_ref, y_ref, yn_ref, dt_ref, cum_ref, got, halo_ref,
    cw_ref, dtb_ref, al_ref, sk_ref, gg_ref, pad, col, tcol, lcol, lrow, st, give, square, edge_send, edge_recv, send, recv,
):
    rows = proj_ref.shape[0]
    take_vectors(layer_ref, conv_ref, head_ref, gate_ref, cw_ref, dtb_ref, al_ref, sk_ref, gg_ref)
    first, final = chunk_place(1)
    chain_barrier(1, first, final)
    edge = to_next(
        proj_ref.at[pl.ds(rows - 8, 8), pl.ds(DI, XBC)], halo_ref, edge_send, edge_recv, 1
    )

    @pl.when(jnp.logical_not(final))
    def _():
        edge.start()

    @pl.when(first)
    def _():
        halo_ref[...] = jnp.zeros(halo_ref.shape, f32)
        got[...] = jnp.zeros(got.shape, bf16)

    pad[8:, :] = proj_ref[:, DI : DI + XBC]
    dt_ref[...] = jnp.zeros((rows, LANES), f32)
    dt_ref[:, 0:HEADS] = proj_ref[:, DI + XBC :]
    drive = dt_ref[...] + dtb_ref[...]
    dt = jnp.maximum(drive, 0.0) + jnp.log1p(jnp.exp(-jnp.abs(drive)))
    dt_ref[...] = dt
    rate = dt * (-jnp.exp(al_ref[...]))
    ri = lax.broadcasted_iota(jnp.int32, (rows, rows), 0)
    ci = lax.broadcasted_iota(jnp.int32, (rows, rows), 1)
    causal = ri >= ci
    cum = dot_nn(jnp.where(causal, 1.0, 0.0), rate, highest)
    cum_ref[...] = cum
    lrow[...] = cum.T
    spread_columns(cum, col, lcol, rows)
    spread_columns(dt, None, tcol, rows)

    @pl.when(jnp.logical_not(first))
    def _():
        edge.wait_recv()

    pad[0:8, :] = halo_ref[...]

    def conv(i, _):
        xs = pair_lanes(i)
        out = jnp.broadcast_to(cw_ref[CONV : CONV + 1, xs], (rows, LANES))
        for k in range(CONV):
            out = out + cw_ref[k : k + 1, xs] * pad[5 + k : 5 + k + rows, xs]
        pre_ref[:, xs] = out
        return 0

    lax.fori_loop(0, XBC // LANES, conv, 0, unroll=3)
    bm = silu(pre_ref[:, DI : DI + NSTATE]).astype(bf16)
    cm = silu(pre_ref[:, DI + NSTATE :]).astype(bf16)
    cb = dot_nt(cm, bm)
    half = first_half(rows)

    def states(p, _):
        xs = pair_lanes(p)
        lp = lcol[p]
        tail = jnp.exp(lp[rows - 1 : rows, :] - lp) * tcol[p]
        st[xs, :] = dot_tn((tail * silu(pre_ref[:, xs])).astype(bf16), bm)
        return 0

    lax.fori_loop(0, PAIRS, states, 0, unroll=4)
    square[...] = jnp.zeros(square.shape, f32)

    def pair(p):
        xs = pair_lanes(p)
        x = silu(pre_ref[:, xs])
        xtb = (tcol[p] * x).astype(bf16)
        parts = []
        for j in range(2):
            h = 2 * p + j
            c = col[h]
            d = jnp.concatenate([c] * (rows // LANES), axis=1) - lrow[pl.ds(h, 1), :]
            m = (jnp.exp(jnp.where(causal, d, OFF)) * cb).astype(bf16)
            parts.append(dot_nn(m, xtb))
        y = jnp.where(half, parts[0], parts[1]) + sk_ref[pl.ds(p, 1), :] * x
        y = y + jnp.exp(lcol[p]) * dot_nt(cm, got[xs, :])
        y_ref[:, xs] = y
        g = y * silu(proj_ref[:, xs])
        return g * g

    def step(g, _):
        chain_step(g, 1, first, final, got, give, st, col, rows, send, recv)
        total = square[...]
        for i in range(PART // LANES):
            total = total + pair(g * (PART // LANES) + i)
        square[...] = total
        return 0

    lax.fori_loop(0, CHAIN_STEPS, step, 0)
    scale = lax.rsqrt(jnp.sum(square[...], axis=1, keepdims=True) / DI + epsilon)

    def put(p, _):
        xs = pair_lanes(p)
        g = y_ref[:, xs] * silu(proj_ref[:, xs])
        yn_ref[:, xs] = (g * scale * gg_ref[0:1, xs]).astype(bf16)
        return 0

    lax.fori_loop(0, PAIRS, put, 0, unroll=4)

    @pl.when(jnp.logical_not(final))
    def _():
        edge.wait_send()

    chain_end(1, final, got, give, send, recv)


def back_kernel(
    layer_ref, dyn_ref, y_ref, proj_ref, halo_ref, pre_ref, dt_ref, cum_ref, sin_ref,
    conv_ref, head_ref, gate_ref,
    dp_ref, dcw_ref, dsm_ref, dgg_ref,
    cw_ref, dtb_ref, al_ref, sk_ref, gg_ref, pad, grad, col, tcol, lcol, lrow, dcb, dbm, dcm, dlog, dtx, ends, dy_ref, drive_ref,
    got, give, gst, dx_ref, edge_ref, from_ref, edge_send, edge_recv, send, recv,
):
    rows = y_ref.shape[0]
    take_vectors(layer_ref, conv_ref, head_ref, gate_ref, cw_ref, dtb_ref, al_ref, sk_ref, gg_ref)
    first, final = chunk_place(-1)
    chain_barrier(-1, first, final)

    @pl.when(first)
    def _():
        from_ref[...] = jnp.zeros(from_ref.shape, f32)
        got[...] = jnp.zeros(got.shape, bf16)

    cum = cum_ref[...]
    dt = dt_ref[...]
    lrow[...] = cum.T
    spread_columns(cum, col, lcol, rows)
    spread_columns(dt, None, tcol, rows)
    bm = silu(pre_ref[:, DI : DI + NSTATE]).astype(bf16)
    cm = silu(pre_ref[:, DI + NSTATE :]).astype(bf16)
    zero = jnp.zeros((rows, LANES), f32)

    def sums(p, carry):
        xs = pair_lanes(p)
        g = y_ref[:, xs] * silu(proj_ref[:, xs])
        return carry[0] + g * g, carry[1] + g * (dyn_ref[:, xs] * gg_ref[0:1, xs])

    square, cross = lax.fori_loop(0, PAIRS, sums, (zero, zero), unroll=4)
    scale = lax.rsqrt(jnp.sum(square, axis=1, keepdims=True) / DI + epsilon)
    mean = jnp.sum(cross, axis=1, keepdims=True) * scale / DI

    def ungate(p, _):
        xs = pair_lanes(p)
        z = proj_ref[:, xs]
        y = y_ref[:, xs]
        sg = lax.logistic(z)
        sz = z * sg
        ghat = y * sz * scale
        dyn = dyn_ref[:, xs]
        dgg_ref[0:1, xs] = jnp.sum(dyn * ghat, axis=0, keepdims=True)
        dg = scale * (dyn * gg_ref[0:1, xs] - ghat * mean)
        dy = dg * sz
        dy_ref[:, xs] = dy
        dp_ref[:, xs] = (dg * y * (sg * (1.0 + z * (1.0 - sg)))).astype(bf16)
        gst[xs, :] = dot_tn((jnp.exp(lcol[p]) * dy).astype(bf16), cm)
        return 0

    lax.fori_loop(0, PAIRS, ungate, 0, unroll=4)
    pad[0:8, :] = halo_ref[...]
    pad[8:, :] = proj_ref[:, DI : DI + XBC]
    grad[0:8, :] = jnp.zeros((8, XBC), f32)
    grad[rows + 8 :, :] = jnp.zeros((8, XBC), f32)
    cbt = dot_nt(bm, cm)
    ri = lax.broadcasted_iota(jnp.int32, (rows, rows), 0)
    ci = lax.broadcasted_iota(jnp.int32, (rows, rows), 1)
    causal = ri <= ci
    half = first_half(rows)
    dcb[...] = jnp.zeros((rows, rows), f32)
    dbm[...] = zero
    dcm[...] = zero
    dlog[...] = zero
    dtx[...] = zero
    ends[...] = jnp.zeros((16, LANES), f32)
    lane_row = lax.broadcasted_iota(jnp.int32, (LANES, LANES), 0)
    lane_col = lax.broadcasted_iota(jnp.int32, (LANES, LANES), 1)
    ones = jnp.ones((8, NSTATE), f32)

    def pair(p):
        xs = pair_lanes(p)
        pre = pre_ref[:, xs]
        sg = lax.logistic(pre)
        x = pre * sg
        tp = tcol[p]
        xt = tp * x
        dy = dy_ref[:, xs]
        dyb = dy.astype(bf16)
        parts = []
        pairs = []
        for j in range(2):
            h = 2 * p + j
            c = col[h]
            d = lrow[pl.ds(h, 1), :] - jnp.concatenate([c] * (rows // LANES), axis=1)
            w = jnp.exp(jnp.where(causal, d, OFF))
            parts.append(dot_nn((w * cbt).astype(bf16), dyb))
            own = half if j == 0 else jnp.logical_not(half)
            q = dot_nt(jnp.where(own, xt, 0.0).astype(bf16), dyb)
            pairs.append(w * q)
        dcb[...] += pairs[0] + pairs[1]
        lp = lcol[p]
        last = lp[rows - 1 : rows, :]
        tail = jnp.exp(last - lp)
        gin = got[xs, :]
        sin = sin_ref[xs, :]
        dst = tail * dot_nt(bm, gin)
        dxt = jnp.where(half, parts[0], parts[1]) + dst
        dbm[...] += dot_nn((tail * xt).astype(bf16), gin)
        dcm[...] += dot_nn((jnp.exp(lp) * dy).astype(bf16), sin)
        sk = sk_ref[pl.ds(p, 1), :]
        pick = jnp.where(lane_col == 2 * p + jnp.where(lane_row >= HDIM, 1, 0), 1.0, 0.0)
        dlog[...] += dot_nn(dy * (y_ref[:, xs] - sk * x) - xt * dxt, pick, highest)
        dtx[...] += dot_nn((x * dxt).astype(bf16), pick.astype(bf16))
        held = dot_nt(ones, gin.astype(f32) * sin.astype(f32), highest)
        end = jnp.sum(xt * dst, axis=0, keepdims=True) + jnp.exp(last) * held[0:1, :]
        skip = jnp.sum(dy * x, axis=0, keepdims=True)
        stacked = jnp.concatenate(
            [jnp.broadcast_to(end, (8, LANES)), jnp.broadcast_to(skip, (8, LANES))], axis=0
        )
        ends[...] += dot_nn(stacked, pick, highest)
        grad[pl.ds(8, rows), xs] = (tp * dxt + sk * dy) * (sg * (1.0 + pre * (1.0 - sg)))

    def step(g, _):
        chain_step(g, -1, first, final, got, give, gst, col, rows, send, recv)
        for i in range(PART // LANES):
            pair(g * (PART // LANES) + i)
        return 0

    lax.fori_loop(0, CHAIN_STEPS, step, 0)
    dcbb = dcb[...].astype(bf16)
    dc = dcm[...] + dot_tn(dcbb, bm)
    db = dbm[...] + dot_nn(dcbb, cm)
    grad[8 : 8 + rows, DI : DI + NSTATE] = db * silu_grad(pre_ref[:, DI : DI + NSTATE])
    grad[8 : 8 + rows, DI + NSTATE :] = dc * silu_grad(pre_ref[:, DI + NSTATE :])

    def edges(i, _):
        xs = pair_lanes(i)
        edge = jnp.zeros((8, LANES), f32)
        for k in range(CONV):
            edge = edge + cw_ref[k : k + 1, xs] * grad[3 - k : 11 - k, xs]
        edge_ref[:, xs] = edge
        return 0

    lax.fori_loop(0, XBC // LANES, edges, 0, unroll=9)
    edge = to_next(edge_ref, from_ref, edge_send, edge_recv, -1)

    @pl.when(jnp.logical_not(final))
    def _():
        edge.start()

    last_row = lax.broadcasted_iota(jnp.int32, (rows, LANES), 0) == rows - 1
    dl = dlog[...] + jnp.where(last_row, ends[0:1, :], 0.0)
    da = dot_nn(jnp.where(causal, 1.0, 0.0), dl, highest)
    decay = -jnp.exp(al_ref[...])
    ddt = dtx[...] + da * decay
    drive_ref[...] = jnp.zeros((rows, LANES), f32)
    drive_ref[:, 0:HEADS] = proj_ref[:, DI + XBC :]
    ddr = ddt * lax.logistic(drive_ref[...] + dtb_ref[...])
    dp_ref[:, DI + XBC :] = ddr[:, 0:HEADS].astype(bf16)
    dsm_ref[...] = jnp.zeros((8, LANES), f32)
    dsm_ref[0:1, :] = jnp.sum(ddr, axis=0, keepdims=True)
    dsm_ref[1:2, :] = jnp.sum(da * dt, axis=0, keepdims=True) * decay
    dsm_ref[2:3, :] = ends[8:9, :]

    def conv(i, _):
        xs = pair_lanes(i)
        own = grad[pl.ds(8, rows), xs]
        out = jnp.zeros((rows, LANES), f32)
        for k in range(CONV):
            out = out + cw_ref[k : k + 1, xs] * grad[11 - k : 11 - k + rows, xs]
            dcw_ref[k : k + 1, xs] = jnp.sum(
                own * pad[5 + k : 5 + k + rows, xs], axis=0, keepdims=True
            )
        dcw_ref[4:5, xs] = jnp.sum(own, axis=0, keepdims=True)
        dx_ref[:, xs] = out
        return 0

    lax.fori_loop(0, XBC // LANES, conv, 0, unroll=3)

    @pl.when(jnp.logical_not(first))
    def _():
        edge.wait_recv()

    dx_ref[rows - 8 :, :] += from_ref[...]
    dp_ref[:, DI : DI + XBC] = dx_ref[...].astype(bf16)

    @pl.when(jnp.logical_not(final))
    def _():
        edge.wait_send()

    chain_end(-1, final, got, give, send, recv)


VTILE = 1280
NTILE = 256


def head_specs(width, tokens):
    return dict(
        table=pl.BlockSpec((VTILE, width), lambda i: (i, 0)),
        hidden=pl.BlockSpec((tokens, width), lambda i: (0, 0)),
        kept=pl.BlockSpec((VTILE, tokens), lambda i: (i, 0)),
        row=pl.BlockSpec((1, tokens), lambda i: (0, 0)),
        tile_row=pl.BlockSpec((1, 1, tokens), lambda i: (i, 0, 0)),
    )


def head_call(kernel, grid, in_specs, out_specs, outs, scratch, ins, cells):
    return pl.pallas_call(
        kernel,
        grid=(grid,),
        in_specs=in_specs,
        out_specs=out_specs,
        out_shape=[jax.ShapeDtypeStruct(shape, kind) for shape, kind in outs],
        scratch_shapes=list(scratch),
        compiler_params=pltpu.CompilerParams(
            dimension_semantics=("arbitrary",), vmem_limit_bytes=VMEM_LIMIT
        ),
        cost_estimate=pl.CostEstimate(
            flops=2 * cells * D, transcendentals=cells, bytes_accessed=4 * cells
        ),
    )(*ins)


UNROLL = 8


def head_stats_kernel(
    lead_ref, table_ref, own_ref, lab_ref, w_ref,
    q_ref, all_ref, lse_ref, fac_ref, hit_ref,
    kept, tops, sums, hits, shown, own_sem, put_sem, z_send, z_recv, m_send, m_recv, s_send, s_recv,
):
    dp = lax.axis_index("dp")
    me = lax.axis_index("fsdp")
    shards = lax.axis_size("fsdp")
    count = shards // MB
    core = me % MB
    k = me // MB
    mate = k * MB + 1 - core
    vocab_rows = lead_ref.shape[0] + table_ref.shape[0]
    rows = own_ref.shape[0]
    tiles = tops.shape[0]
    barrier = pltpu.get_barrier_semaphore()
    for other in range(1, shards):
        pl.semaphore_signal(
            barrier, inc=1, device_id=(dp, lax.rem(me + other, shards)), device_id_type=MESH
        )
    pl.semaphore_wait(barrier, shards - 1)

    near = jnp.minimum(k, count - 1 - k)
    long_side = jnp.where(count - 1 - k > k, 1, -1)

    def chunk_at(i):
        paired = k + (2 * (i % 2) - 1) * ((i + 1) // 2)
        return jnp.where(i <= 2 * near, paired, k + long_side * (i - near))

    def along(z, side):
        at = all_ref.at[z * MB + core]
        return remote(
            at, at, z_send.at[side, z], z_recv.at[z], dp, me + MB if side == 0 else me - MB
        )

    def to_mate(z):
        at = all_ref.at[z * MB + core]
        return remote(at, at, m_send.at[z], m_recv.at[z], dp, mate)

    def from_mate(z):
        at = all_ref.at[z * MB + 1 - core]
        return remote(at, at, m_send.at[z], m_recv.at[z], dp, mate)

    keep = pltpu.make_async_copy(own_ref, all_ref.at[me], own_sem)
    keep.start()
    keep.wait()

    @pl.when(k < count - 1)
    def _():
        along(k, 0).start()

    @pl.when(k > 0)
    def _():
        along(k, 1).start()

    to_mate(k).start()
    whole = vocab_rows - vocab_rows % 16
    for slot in range(2):
        kept[slot, whole:, :] = jnp.zeros((kept.shape[1] - whole, rows), bf16)

    def put(step, b):
        return pltpu.make_async_copy(
            kept.at[step % 2],
            q_ref.at[:, pl.ds(pl.multiple_of(b * rows, rows), rows)],
            put_sem.at[step % 2],
        )

    def block(step, b):
        @pl.when(step >= 2)
        def _():
            put(step, b).wait()

        slot = step % 2
        ns = pl.ds(pl.multiple_of(b * rows, rows), rows)
        h = all_ref[b]
        label = lab_ref[0:1, ns]
        for t in range(tiles):
            first = t * VTILE
            size = min(VTILE, vocab_rows - first)
            part = lead_ref[...] if t == 0 else table_ref[first - VTILE : first - VTILE + size, :]
            logits = dot_nt(part, h)
            top = jnp.max(logits, axis=0, keepdims=True)
            p = jnp.exp(logits - top)
            kept[slot, first : first + size, :] = p.astype(bf16)
            tops[t, 0:1, ns] = top
            sums[t, 0:1, ns] = jnp.sum(p, axis=0, keepdims=True)
            rid = lax.broadcasted_iota(jnp.int32, (size, rows), 0)
            hits[t, 0:1, ns] = jnp.sum(
                jnp.where(rid == label - first, logits, 0.0), axis=0, keepdims=True
            )
        put(step, b).start()

    def chunk(i, _):
        z = chunk_at(i)

        @pl.when(jnp.logical_and(i > 0, k >= i))
        def _():
            along(k - i, 0).wait_recv()

            @pl.when(k < count - 1)
            def _():
                along(k - i, 0).start()

            to_mate(k - i).start()

        @pl.when(jnp.logical_and(i > 0, k + i < count))
        def _():
            along(k + i, 1).wait_recv()

            @pl.when(k > 0)
            def _():
                along(k + i, 1).start()

            to_mate(k + i).start()

        block(2 * i, z * MB + core)
        from_mate(z).wait_recv()
        block(2 * i + 1, z * MB + 1 - core)
        return 0

    lax.fori_loop(0, count, chunk, 0)
    top = tops[0, 0:1, :]
    for t in range(1, tiles):
        top = jnp.maximum(top, tops[t, 0:1, :])
    total = jnp.zeros_like(top)
    hit = jnp.zeros_like(top)
    for t in range(tiles):
        total = total + sums[t, 0:1, :] * jnp.exp(tops[t, 0:1, :] - top)
        hit = hit + hits[t, 0:1, :]
    hit_ref[...] = hit
    shown[me, 0:1, :] = top
    shown[me, 1:2, :] = total

    def tell(other):
        at = shown.at[me]
        return remote(
            at, at, s_send.at[other], s_recv.at[me], dp, lax.rem(me + other, shards)
        )

    def told(other):
        at = shown.at[lax.rem(me + other, shards)]
        return remote(
            at, at, s_send.at[other], s_recv.at[lax.rem(me + other, shards)], dp, mate
        )

    for other in range(1, shards):
        tell(other).start()
    for other in range(1, shards):
        told(other).wait_recv()
    top = shown[0, 0:1, :]
    for f in range(1, shards):
        top = jnp.maximum(top, shown[f, 0:1, :])
    total = jnp.zeros_like(top)
    for f in range(shards):
        total = total + shown[f, 1:2, :] * jnp.exp(shown[f, 0:1, :] - top)
    lse = top + jnp.log(total)
    lse_ref[...] = lse
    scale = w_ref[...] * (1.0 + 2.0 * z_weight * lse)
    for t in range(tiles):
        fac_ref[t, 0:1, :] = scale * jnp.exp(tops[t, 0:1, :] - lse)
    for other in range(1, shards):
        tell(other).wait_send()
    for z in range(count):

        @pl.when(jnp.logical_and(k >= z, k < count - 1))
        def _(z=z):
            along(z, 0).wait_send()

        @pl.when(jnp.logical_and(k <= z, k > 0))
        def _(z=z):
            along(z, 1).wait_send()

        to_mate(z).wait_send()
    put(0, 0).wait()
    put(1, 0).wait()


def head_stats(lead, table, own, labels, weight):
    vocab_rows, width = lead.shape[0] + table.shape[0], table.shape[1]
    rows = own.shape[0]
    shards = lax.axis_size("fsdp")
    count = shards // MB
    tokens = shards * rows
    tiles = pl.cdiv(vocab_rows, VTILE)
    kept, everyone, lse, fac, hit = comm_call(
        head_stats_kernel,
        6,
        (lead, table, own, labels, weight),
        (
            ((tiles * VTILE, tokens), bf16),
            ((shards, rows, width), bf16),
            ((1, tokens), f32),
            ((tiles, 1, tokens), f32),
            ((1, tokens), f32),
        ),
        (
            pltpu.VMEM((2, tiles * VTILE, rows), bf16),
            pltpu.VMEM((tiles, 1, tokens), f32),
            pltpu.VMEM((tiles, 1, tokens), f32),
            pltpu.VMEM((tiles, 1, tokens), f32),
            pltpu.VMEM((shards, 2, tokens), f32),
            pltpu.SemaphoreType.DMA,
            pltpu.SemaphoreType.DMA((2,)),
            pltpu.SemaphoreType.DMA((2, count)),
            pltpu.SemaphoreType.DMA((count,)),
            pltpu.SemaphoreType.DMA((count,)),
            pltpu.SemaphoreType.DMA((count,)),
            pltpu.SemaphoreType.DMA((shards,)),
            pltpu.SemaphoreType.DMA((shards,)),
        ),
        (pltpu.VMEM,) * 5,
        (pl.ANY, pltpu.VMEM, pltpu.VMEM, pltpu.VMEM, pltpu.VMEM),
        own.size * 2 * 7,
    )
    return kept, everyone.reshape(tokens, width), lse, fac, hit


def logit_grads(q, fac, weight, rid, label):
    other = weight * (0.1 / VOCAB)
    return (q.astype(f32) * fac - jnp.where(rid == label, other + 0.9 * weight, other)).astype(bf16)


def head_rows_kernel(vocab_rows, lead_ref, e_ref, q_ref, fac_ref, w_ref, lab_ref, out_ref, acc, et):
    step = pl.program_id(0)
    first = step * VTILE
    tokens = q_ref.shape[1]

    @pl.when(step == 0)
    def _():
        acc[...] = jnp.zeros(acc.shape, f32)

    eid = lax.broadcasted_iota(jnp.int32, (VTILE, e_ref.shape[1]), 0)
    part = jnp.where(step == 0, lead_ref[...], e_ref[...]).astype(f32)
    et[...] = jnp.where(eid < vocab_rows - first, part, 0.0).T.astype(bf16)

    def chunk(j, _):
        ns = pl.ds(pl.multiple_of(j * NTILE, NTILE), NTILE)
        rid = lax.broadcasted_iota(jnp.int32, (VTILE, NTILE), 0)
        dl = logit_grads(
            q_ref[:, ns], fac_ref[0, 0:1, ns], w_ref[0:1, ns], rid, lab_ref[0:1, ns] - first
        )
        acc[:, ns] += dot_nn(et[...], dl)
        return 0

    lax.fori_loop(0, tokens // NTILE, chunk, 0, unroll=UNROLL)

    @pl.when(step == pl.num_programs(0) - 1)
    def _():
        def put(j, _):
            ns = pl.ds(pl.multiple_of(j * NTILE, NTILE), NTILE)
            out_ref[ns, :] = acc[:, ns].T.astype(bf16)
            return 0

        lax.fori_loop(0, tokens // NTILE, put, 0)


def head_rows(lead, table, kept, fac, weight, labels):
    vocab_rows, width = lead.shape[0] + table.shape[0], table.shape[1]
    tokens = kept.shape[1]
    sp = head_specs(width, tokens)
    return head_call(
        functools.partial(head_rows_kernel, vocab_rows),
        pl.cdiv(vocab_rows, VTILE),
        [
            pl.BlockSpec((VTILE, width), lambda i: (0, 0)),
            pl.BlockSpec((VTILE, width), lambda i: (jnp.maximum(i - 1, 0), 0)),
            sp["kept"],
            sp["tile_row"],
            sp["row"],
            sp["row"],
        ],
        [sp["hidden"]],
        [((tokens, width), bf16)],
        (pltpu.VMEM((width, tokens), f32), pltpu.VMEM((width, VTILE), bf16)),
        (lead, table, kept, fac, weight, labels),
        vocab_rows * tokens,
    )[0]


def head_table_kernel(h_ref, q_ref, fac_ref, w_ref, lab_ref, out_ref, dl_ref):
    first = pl.program_id(0) * VTILE
    tokens = q_ref.shape[1]

    def chunk(j, _):
        ns = pl.ds(pl.multiple_of(j * NTILE, NTILE), NTILE)
        rid = lax.broadcasted_iota(jnp.int32, (VTILE, NTILE), 0)
        dl_ref[:, ns] = logit_grads(
            q_ref[:, ns], fac_ref[0, 0:1, ns], w_ref[0:1, ns], rid, lab_ref[0:1, ns] - first
        )
        return 0

    lax.fori_loop(0, tokens // NTILE, chunk, 0, unroll=UNROLL)

    def cols(j, _):
        ds = pl.ds(pl.multiple_of(j * 256, 256), 256)
        out_ref[:, ds] = dot_nn(dl_ref[...], h_ref[:, ds]).astype(bf16)
        return 0

    lax.fori_loop(0, h_ref.shape[1] // 256, cols, 0, unroll=True)


def head_table(hidden, kept, fac, weight, labels, vocab_rows):
    tokens, width = hidden.shape
    sp = head_specs(width, tokens)
    return head_call(
        head_table_kernel,
        pl.cdiv(vocab_rows, VTILE),
        [sp["hidden"], sp["kept"], sp["tile_row"], sp["row"], sp["row"]],
        [sp["table"]],
        [((vocab_rows, width), bf16)],
        (pltpu.VMEM((VTILE, tokens), bf16),),
        (hidden, kept, fac, weight, labels),
        vocab_rows * tokens,
    )[0]


def weight_grads_kernel(u_ref, dp_ref, yn_ref, db_ref, in_ref, out_ref):
    wide_cols = dp_ref.shape[1]
    for c in range(0, wide_cols, 1024):
        cs = pl.ds(c, min(1024, wide_cols - c))
        in_ref[:, cs] = dot_tn(u_ref[...], dp_ref[:, cs]).astype(bf16)
    out_ref[...] = dot_tn(yn_ref[...], db_ref[...]).astype(bf16)


def weight_grads(normed, grad_proj, mixed, grad_branch):
    rows = normed.shape[0]
    steps = D // 256
    part = DI // steps
    return head_call(
        weight_grads_kernel,
        steps,
        [
            pl.BlockSpec((rows, 256), lambda i: (0, i)),
            pl.BlockSpec((rows, ZW), lambda i: (0, 0)),
            pl.BlockSpec((rows, part), lambda i: (0, i)),
            pl.BlockSpec((rows, D), lambda i: (0, 0)),
        ],
        [pl.BlockSpec((256, ZW), lambda i: (i, 0)), pl.BlockSpec((part, D), lambda i: (i, 0))],
        [((D, ZW), bf16), ((DI, D), bf16)],
        (),
        (normed, grad_proj, mixed, grad_branch),
        rows * (ZW + DI),
    )


def after(value, earlier):
    return lax.optimization_barrier((value, earlier))[0]


def norm_scale(values):
    return lax.rsqrt(jnp.mean(values * values, axis=-1, keepdims=True) + epsilon)


def norm_back(grad, values, gain):
    scale = norm_scale(values)
    unit = values * scale
    inner = grad * gain
    back = scale * (inner - unit * jnp.mean(inner * unit, axis=-1, keepdims=True))
    return back, jnp.sum(grad * unit, axis=0)


def all_vectors(vector_params):
    rows = vector_params[: LAYERS * PER].reshape(LAYERS, PER)
    at = (CONV + 1) * XBC
    heads = rows[:, at : at + 3 * HEADS].reshape(LAYERS, 3, HEADS)
    after_heads = at + 3 * HEADS
    return dict(
        conv=rows[:, :at].reshape(LAYERS, CONV + 1, XBC),
        heads=jnp.pad(heads, ((0, 0), (0, 5), (0, LANES - HEADS))),
        gate=rows[:, after_heads + D :].reshape(LAYERS, 1, DI),
        pre=rows[:, after_heads : after_heads + D],
    )


def layer_forward(hidden, w_in, w_out, vec, layer):
    rows = hidden.shape[0]
    normed = (hidden * norm_scale(hidden) * vec["pre"][layer]).astype(bf16)
    proj = jnp.dot(normed, w_in, preferred_element_type=f32)
    pre, y, mixed, dt, cum, entering, halo = comm_call(
        scan_kernel,
        1,
        (jnp.full((1,), layer, jnp.int32), proj, vec["conv"], vec["heads"], vec["gate"]),
        (
            ((rows, XBC), f32),
            ((rows, DI), f32),
            ((rows, DI), bf16),
            ((rows, LANES), f32),
            ((rows, LANES), f32),
            ((DI, NSTATE), bf16),
            ((8, XBC), f32),
        ),
        VECTOR_SCRATCH
        + (
            pltpu.VMEM((rows + 8, XBC), f32),
            pltpu.VMEM((HEADS, rows, LANES), f32),
            pltpu.VMEM((PAIRS, rows, LANES), f32),
            pltpu.VMEM((PAIRS, rows, LANES), f32),
            pltpu.VMEM((LANES, rows), f32),
            pltpu.VMEM((DI, NSTATE), f32),
            pltpu.VMEM((DI, NSTATE), bf16),
            pltpu.VMEM((rows, LANES), f32),
            pltpu.SemaphoreType.DMA,
            pltpu.SemaphoreType.DMA,
            pltpu.SemaphoreType.DMA((CHAIN_STEPS,)),
            pltpu.SemaphoreType.DMA((CHAIN_STEPS,)),
        ),
        (pltpu.SMEM,) + (pltpu.VMEM,) * 4,
        (pltpu.VMEM,) * 7,
        DI * NSTATE * 2,
    )
    branch = jnp.dot(mixed, w_out, preferred_element_type=f32)
    record = (hidden, normed, proj, halo, pre, dt, cum, entering, y, mixed)
    return hidden + branch, record


def layer_backward(grad_hidden, w_in, w_out, vec, layer, record):
    hidden, normed, proj, halo, pre, dt, cum, entering, y, mixed = record
    rows = hidden.shape[0]
    grad_branch = grad_hidden.astype(bf16)
    grad_mixed = dot_nt(grad_branch, w_out)
    grad_proj, dconv, dsmall, dgate = comm_call(
        back_kernel,
        2,
        (
            jnp.full((1,), layer, jnp.int32), grad_mixed, y, proj, halo, pre, dt, cum, entering,
            vec["conv"], vec["heads"], vec["gate"],
        ),
        (
            ((rows, ZW), bf16),
            ((8, XBC), f32),
            ((8, LANES), f32),
            ((1, DI), f32),
        ),
        VECTOR_SCRATCH
        + (
            pltpu.VMEM((rows + 8, XBC), f32),
            pltpu.VMEM((rows + 16, XBC), f32),
            pltpu.VMEM((HEADS, rows, LANES), f32),
            pltpu.VMEM((PAIRS, rows, LANES), f32),
            pltpu.VMEM((PAIRS, rows, LANES), f32),
            pltpu.VMEM((LANES, rows), f32),
            pltpu.VMEM((rows, rows), f32),
            pltpu.VMEM((rows, LANES), f32),
            pltpu.VMEM((rows, LANES), f32),
            pltpu.VMEM((rows, LANES), f32),
            pltpu.VMEM((rows, LANES), f32),
            pltpu.VMEM((16, LANES), f32),
            pltpu.VMEM((rows, DI), f32),
            pltpu.VMEM((rows, LANES), f32),
            pltpu.VMEM((DI, NSTATE), bf16),
            pltpu.VMEM((DI, NSTATE), bf16),
            pltpu.VMEM((DI, NSTATE), f32),
            pltpu.VMEM((rows, XBC), f32),
            pltpu.VMEM((8, XBC), f32),
            pltpu.VMEM((8, XBC), f32),
            pltpu.SemaphoreType.DMA,
            pltpu.SemaphoreType.DMA,
            pltpu.SemaphoreType.DMA((CHAIN_STEPS,)),
            pltpu.SemaphoreType.DMA((CHAIN_STEPS,)),
        ),
        (pltpu.SMEM,) + (pltpu.VMEM,) * 11,
        (pltpu.VMEM,) * 4,
        DI * NSTATE * 2,
    )
    grad_normed = dot_nt(grad_proj, w_in)
    grad_in, grad_out = weight_grads(normed, grad_proj, mixed, grad_branch)
    grad_prev, dpre_gain = norm_back(grad_normed, hidden, vec["pre"][layer])
    grad_vec = jnp.concatenate(
        [
            dconv[: CONV + 1].reshape(-1),
            dsmall[0, :HEADS],
            dsmall[1, :HEADS],
            dsmall[2, :HEADS],
            dpre_gain,
            dgate[0],
        ]
    )
    return grad_hidden + grad_prev, grad_in, grad_out, grad_vec


def whole_step(
    token_ids,
    target_ids,
    seq_lengths,
    embedding,
    embedding_mom,
    embedding_avg,
    in_proj,
    in_proj_mom,
    in_proj_avg,
    out_proj,
    out_proj_mom,
    out_proj_avg,
    vector_params,
    vector_mom,
    vector_avg,
):
    groups = lax.axis_size("dp")
    shards = lax.axis_size("fsdp")
    group_index = lax.axis_index("dp")
    shard_index = lax.axis_index("fsdp")
    chunks = shards // MB
    seq_rows = token_ids.shape[2]
    rows = seq_rows // chunks
    vocab_rows, own_cols = embedding.shape
    tokens = MB * seq_rows
    total_count = jnp.sum(seq_lengths).astype(f32)
    in_low = in_proj.astype(bf16)
    out_low = out_proj.astype(bf16)

    lead = lax.all_gather(embedding[:VTILE].astype(bf16), "dp", axis=1, tiled=True)
    ids_all = group_call(share_kernel, 7, token_ids[:, 0, :], ((groups, MB, seq_rows), jnp.int32))
    ids_all = ids_all.reshape(groups, MB, chunks, rows).transpose(2, 1, 0, 3).reshape(-1)
    every = ids_all.shape[0]
    local_ids = ids_all - shard_index * vocab_rows
    inside = (local_ids >= 0) & (local_ids < vocab_rows)
    sorted_ids, sorted_tok = lax.sort(
        (jnp.where(inside, local_ids, vocab_rows), jnp.arange(every, dtype=jnp.int32)),
        num_keys=1,
    )
    held_here = sorted_ids < vocab_rows
    count = jnp.sum(held_here.astype(jnp.int32)).reshape(1)
    row_list = jnp.where(held_here, sorted_ids, 0)
    tok_list = jnp.where(held_here, sorted_tok, every)
    looked, embed_low, own_sums = local_call(
        lookup_kernel,
        (count, row_list, tok_list, embedding),
        (((every, own_cols), bf16), ((vocab_rows - VTILE, own_cols), bf16), ((8, own_cols), f32)),
        scratch=(pltpu.VMEM((every + 8, own_cols), f32),),
        in_smem=(0, 1, 2),
    )
    mine = lax.psum_scatter(
        looked.reshape(shards * groups * rows, own_cols), "fsdp", scatter_dimension=0, tiled=True
    )
    hidden = group_call(
        to_rows_kernel,
        8,
        mine.reshape(groups, rows, own_cols),
        ((rows, D), f32),
        (pltpu.VMEM((groups, rows, own_cols), bf16),),
    )

    shards = []
    for l in range(LAYERS):
        shards += [in_low[l], out_low[l]]
    shards = after(shards, looked)
    gathered = gather_layers(shards)
    w_in, w_out = gathered[0::2], gathered[1::2]
    embed_low = after(embed_low, gathered)
    table = lax.all_gather(embed_low, "dp", axis=1, tiled=True)

    vecs = all_vectors(vector_params)
    final_gain = vector_params[LAYERS * PER :]
    records = []
    for l in range(LAYERS):
        hidden, record = layer_forward(hidden, w_in[l], w_out[l], vecs, l)
        records.append(record)

    final_low = (hidden * norm_scale(hidden) * final_gain).astype(bf16)

    def in_order(per_seq):
        return per_seq.reshape(MB, chunks, rows).transpose(1, 0, 2).reshape(1, tokens)

    labels = in_order(target_ids[:, 0, :])
    lengths = lax.dynamic_index_in_dim(seq_lengths, group_index, 1, keepdims=True)
    valid = in_order((jnp.arange(seq_rows)[None, :] < lengths).astype(f32))
    local_labels = labels - shard_index * vocab_rows
    weight = valid / total_count
    kept, group_hidden, lse, fac, target = head_stats(lead, table, final_low, local_labels, weight)
    own_mask = jnp.arange(tokens) // rows == shard_index
    per_row = jnp.where(own_mask, lse[0] + z_weight * lse[0] * lse[0], 0.0)
    loss_sum = jnp.sum((per_row - 0.9 * target[0]) * valid[0])
    own_valid = lax.dynamic_slice_in_dim(valid[0], shard_index * rows, rows)
    hidden_sum = jnp.sum(final_low.astype(f32) * own_valid[:, None], axis=0)
    column_sum = jnp.zeros((groups, own_cols), f32)
    column_sum = jnp.where(
        jnp.arange(groups)[:, None] == group_index, jnp.sum(own_sums, axis=0), column_sum
    ).reshape(D)

    rows_grad = head_rows(lead, table, kept, fac, weight, local_labels)
    own_grad = lax.psum_scatter(
        rows_grad, "fsdp", scatter_dimension=0, tiled=True
    ).astype(f32)
    table_grad = head_table(group_hidden, kept, fac, weight, local_labels, vocab_rows)
    table_part = lax.psum_scatter(table_grad, "dp", scatter_dimension=1, tiled=True)

    grad_hidden, dfinal = norm_back(after(own_grad, table_grad), hidden, final_gain)
    in_parts = [None] * LAYERS
    out_parts = [None] * LAYERS
    vec_parts = [None] * LAYERS
    for l in reversed(range(LAYERS)):
        grad_hidden, grad_in, grad_out, vec_parts[l] = layer_backward(
            grad_hidden, w_in[l], w_out[l], vecs, l, records[l]
        )
        in_parts[l], out_parts[l] = grad_in, grad_out
    whole = []
    for l in range(LAYERS):
        whole += [in_parts[l], out_parts[l]]
    sent = group_call(
        to_columns_kernel,
        9,
        after(grad_hidden, whole),
        ((groups, rows, own_cols), bf16),
        (pltpu.VMEM((groups, rows, own_cols), bf16),),
    )
    whole = after(whole, sent)
    spread = lax.all_gather(sent, "fsdp", axis=0).reshape(every, own_cols)
    summed_parts = reduce_layers(whole)
    spread = after(spread, summed_parts)
    table_total, table_squares = local_call(
        spread_kernel,
        (count, row_list, tok_list, spread, table_part),
        (((vocab_rows, own_cols), f32), ((8, own_cols), f32)),
        scratch=(pltpu.VMEM((every + 8, own_cols), f32),),
        in_smem=(0, 1, 2),
    )
    owner_squares = jnp.sum(table_squares)
    for part in summed_parts:
        owner_squares = owner_squares + jnp.sum(part * part)
    small = vector_params.shape[0]
    used = small + 2 * D + 2
    padded = pl.cdiv(used, 16 * LANES) * 16 * LANES
    packed = jnp.concatenate(
        vec_parts
        + [
            dfinal,
            hidden_sum,
            column_sum,
            owner_squares.reshape(1),
            loss_sum.reshape(1),
            jnp.zeros((padded - used,), f32),
        ]
    )
    packed, norms = total_of(packed.reshape(-1, LANES), small, used - 2)
    factor = norms[1, 0]
    updated = []
    for master, moment, average, grad in (
        (embedding, embedding_mom, embedding_avg, table_total),
        (in_proj, in_proj_mom, in_proj_avg, jnp.stack(summed_parts[0::2])),
        (out_proj, out_proj_mom, out_proj_avg, jnp.stack(summed_parts[1::2])),
    ):
        new = stepped(master, moment, average, grad, factor)
        updated += [*new, new[0].astype(bf16)]
    packed = packed.reshape(-1)
    vector_total = packed[:small]
    hidden_total = packed[small : small + D]
    column_total = packed[small + D : small + 2 * D]
    mean_part = jnp.sum(hidden_total * column_total) * (0.1 / VOCAB)
    loss_value = (packed[used - 1] - mean_part) / total_count
    vector_new, vector_mom_new, vector_avg_new = stepped(
        vector_params, vector_mom, vector_avg, vector_total, factor
    )
    return (
        loss_value,
        norms[0, 0],
        *updated,
        vector_new,
        vector_mom_new,
        vector_avg_new,
        vector_new.astype(bf16),
    )


def solution(mesh):
    table_spec = P("fsdp", "dp")
    weight_spec = P(None, ("dp", "fsdp"), None)
    return jax.shard_map(
        whole_step,
        mesh=mesh,
        in_specs=(
            P(None, "dp", None),
            P(None, "dp", None),
            P(),
            *(table_spec,) * 3,
            *(weight_spec,) * 6,
            *(P(),) * 3,
        ),
        out_specs=(
            P(),
            P(),
            *(table_spec,) * 4,
            *(weight_spec,) * 8,
            *(P(),) * 4,
        ),
        check_vma=False,
    )
```
